32 devices in a mesh: fsdp: 2 (over x), ctx: 4 (over z), tp: 4 (over y, core).
Axes of the slice: x: 2, y: 2, z: 4, core: 2. Of those that a mesh axis runs over, the one named last changes fastest.
Arguments:
- tokens: bfloat16 [2, 1024, 2048], P('fsdp', 'ctx'), may hold values from -6 to 6
- log_decay: float32 [2, 1024, 8], P('fsdp', 'ctx', 'tp'), may hold values from -0.6 to 0, as said below
- w_query: bfloat16 [2048, 2048], P(('fsdp', 'ctx'), 'tp'), may hold values from -0.125 to 0.125
- w_key: bfloat16 [2048, 2048], P(('fsdp', 'ctx'), 'tp'), may hold values from -0.125 to 0.125
- w_value: bfloat16 [2048, 4096], P(('fsdp', 'ctx'), 'tp'), may hold values from -0.125 to 0.125
- w_gate: bfloat16 [2048, 4096], P(('fsdp', 'ctx'), 'tp'), may hold values from -0.125 to 0.125
- w_out: bfloat16 [2048, 4096], P(('fsdp', 'ctx'), 'tp'), may hold values from -0.125 to 0.125
- norm1_gain: bfloat16 [2048], P(('fsdp', 'ctx')), may hold values from 0.099609375 to 1.8984375
- norm1_bias: bfloat16 [2048], P(('fsdp', 'ctx')), may hold values from -3 to 3
- w_ffgate: bfloat16 [2048, 4096], P(('fsdp', 'ctx'), 'tp'), may hold values from -0.125 to 0.125
- w_ffup: bfloat16 [2048, 4096], P(('fsdp', 'ctx'), 'tp'), may hold values from -0.125 to 0.125
- w_down: bfloat16 [2048, 4096], P(('fsdp', 'ctx'), 'tp'), may hold values from -0.125 to 0.125
- norm2_gain: bfloat16 [2048], P(('fsdp', 'ctx')), may hold values from 0.099609375 to 1.8984375
- norm2_bias: bfloat16 [2048], P(('fsdp', 'ctx')), may hold values from -3 to 3
- grad_out: bfloat16 [2, 1024, 2048], P('fsdp', 'ctx'), may hold values from -6 to 6
Outputs:
- output: bfloat16 [2, 1024, 2048], P('fsdp', 'ctx')
- grad_tokens: bfloat16 [2, 1024, 2048], P('fsdp', 'ctx')
- grad_w_query: float32 [2048, 2048], P(('fsdp', 'ctx'), 'tp')
- grad_w_key: float32 [2048, 2048], P(('fsdp', 'ctx'), 'tp')
- grad_w_value: float32 [2048, 4096], P(('fsdp', 'ctx'), 'tp')
- grad_w_gate: float32 [2048, 4096], P(('fsdp', 'ctx'), 'tp')
- grad_w_out: float32 [2048, 4096], P(('fsdp', 'ctx'), 'tp')
- grad_norm1_gain: float32 [2048], P(('fsdp', 'ctx'))
- grad_norm1_bias: float32 [2048], P(('fsdp', 'ctx'))
- grad_w_ffgate: float32 [2048, 4096], P(('fsdp', 'ctx'), 'tp')
- grad_w_ffup: float32 [2048, 4096], P(('fsdp', 'ctx'), 'tp')
- grad_w_down: float32 [2048, 4096], P(('fsdp', 'ctx'), 'tp')
- grad_norm2_gain: float32 [2048], P(('fsdp', 'ctx'))
- grad_norm2_bias: float32 [2048], P(('fsdp', 'ctx'))
The draws below stay inside these ranges and needn't reach their ends.
Inputs may be any that keep to these rules, and one draw needn't show every extreme that they name: `log_decay`: log of the factor by which a head's state shrinks at a position.
All inputs are finite; a program needn't handle non-finite values.
Results may differ from the reference program's by a relative error of at most 0.018.
Values may be sent and summed in bfloat16 or wider, within the bound.
A program may use at most 192 MiB of HBM per device.

```python
import math
import jax
import jax.numpy as jnp
from jax import lax

D = 2048
HEADS = 8
KEY = 256
HEAD_V = 512
FF = 4096
LENGTH = 1024
SEQS = 2
BLOCK = 256
QK = 2048
VAL = 4096
N_CTX = 4


def draw_log_decay(key, part):
    streams = jax.random.split(key, 6)
    fast = jax.random.uniform(streams[0], (HEADS,)) < 0.5
    slow_rate = jnp.exp(jax.random.uniform(streams[1], (HEADS,), minval=jnp.log(0.1), maxval=jnp.log(0.35))) / LENGTH
    fast_rate = jnp.exp(jax.random.uniform(streams[2], (HEADS,), minval=jnp.log(1.0 / 50.0), maxval=jnp.log(1.0 / 30.0)))
    rate = jnp.where(fast, fast_rate, slow_rate)
    span = max(LENGTH // 32, 1)
    pieces = LENGTH // span + 1
    swing_table = jnp.exp(jax.random.uniform(streams[3], (SEQS, pieces, HEADS), minval=jnp.log(0.5), maxval=jnp.log(2.0)))
    where_piece = jnp.arange(LENGTH) // span
    swing = swing_table[:, where_piece, :]
    spots = jax.random.randint(streams[4], (SEQS, 3), 1, LENGTH)
    struck = jnp.any(jnp.arange(LENGTH)[None, :, None] == spots[:, None, :], axis=2)
    dropped = jax.random.uniform(streams[5], (SEQS, LENGTH, HEADS), minval=-0.45, maxval=-0.22)
    values = -rate[None, None, :] * swing + jnp.where(struck[:, :, None], dropped, 0.0)
    return values.astype(jnp.float32)


def raised(array, rng, source, target, shards_of, factor):
    owner, partner = [(jnp.arange(array.shape[position]) // (array.shape[position] // shards_of)).reshape([-1 if axis == position else 1 for axis in range(array.ndim)]) for position in (source, target)]
    chosen = jax.random.permutation(rng, shards_of)[partner]
    strong = (owner == chosen) | (owner == (partner + shards_of // 2) % shards_of)
    return jnp.where(strong, factor * array, array)


def block_scale(key, dims, cuts, low, largest):
    def one(dim, parts):
        draws = jax.random.uniform(jax.random.fold_in(jax.random.fold_in(key, 6), dim), (parts,), jnp.float32, low / len(cuts), largest / len(cuts))
        return jnp.repeat(jnp.exp(draws), dims[dim] // parts).reshape((-1,) + (1,) * (len(dims) - dim - 1))

    loudness = one(*cuts[0])
    for cut in cuts[1:]:
        loudness = loudness * one(*cut)
    return loudness


def gaussian(rng, shape, scale, limit, shards=(), dtype=jnp.bfloat16):
    level = block_scale(rng, shape, shards, -0.22, 0.18) if shards else 1.0
    entries = jax.random.normal(rng, shape, jnp.float32) * scale * level
    return jnp.minimum(jnp.maximum(entries, -limit), limit).astype(dtype)


def heavy_noise(stream_key, dims, scale, reach, cuts, heavy, dtype=jnp.bfloat16):
    array = scale * jax.random.normal(stream_key, dims, jnp.float32)
    if cuts:
        array = array * block_scale(stream_key, dims, cuts, -0.22, 0.18)
    return jnp.clip(raised(array, jax.random.fold_in(stream_key, 3), *heavy), -reach, reach).astype(dtype)


def setup_inputs(seed: int = 0) -> dict:
    seeds = jax.random.split(jax.random.key(seed), 16)
    tokens = gaussian(seeds[0], (SEQS, LENGTH, D), 1.0, 6.0, ((0, 2), (1, 4)))
    log_decay = draw_log_decay(jax.random.fold_in(seeds[15], 71), 0)
    w_query = gaussian(seeds[2], (D, QK), D ** -0.5, 0.125, ((0, 8), (1, 4)))
    w_key = gaussian(seeds[3], (D, QK), D ** -0.5, 0.125, ((0, 8), (1, 4)))
    w_value = gaussian(seeds[4], (D, VAL), D ** -0.5, 0.125, ((0, 8), (1, 4)))
    w_gate = gaussian(seeds[5], (D, VAL), D ** -0.5, 0.125, ((0, 8), (1, 4)))
    w_out = gaussian(seeds[6], (D, VAL), (VAL // 2) ** -0.5, 0.125, ((0, 8), (1, 4)))
    norm1_gain = jnp.clip(1.0 + 0.18 * jax.random.normal(seeds[7], (D,), jnp.float32), 0.099609375, 1.8984375).astype(jnp.bfloat16)
    norm1_bias = gaussian(seeds[8], (D,), 0.5, 3.0, ((0, 8),))
    w_ffgate = gaussian(seeds[9], (D, FF), D ** -0.5, 0.125, ((0, 8), (1, 4)))
    w_ffup = gaussian(seeds[10], (D, FF), D ** -0.5, 0.125, ((0, 8), (1, 4)))
    w_down = gaussian(seeds[11], (D, FF), (FF // 2) ** -0.5, 0.125, ((0, 8), (1, 4)))
    norm2_gain = jnp.clip(1.0 + 0.18 * jax.random.normal(seeds[12], (D,), jnp.float32), 0.099609375, 1.8984375).astype(jnp.bfloat16)
    norm2_bias = gaussian(seeds[13], (D,), 0.5, 3.0, ((0, 8),))
    grad_out = heavy_noise(seeds[14], (SEQS, LENGTH, D), 1.0, 6.0, ((0, 2), (1, 4)), (1, 2, 4, 2.0))
    return {"tokens": tokens, "log_decay": log_decay, "w_query": w_query, "w_key": w_key, "w_value": w_value, "w_gate": w_gate, "w_out": w_out, "norm1_gain": norm1_gain, "norm1_bias": norm1_bias, "w_ffgate": w_ffgate, "w_ffup": w_ffup, "w_down": w_down, "norm2_gain": norm2_gain, "norm2_bias": norm2_bias, "grad_out": grad_out}


EPSILON = 1e-05
PRECISE = lax.Precision.HIGHEST

@jax.custom_vjp
def low(v):
    return lax.optimization_barrier(v.astype(jnp.bfloat16)).astype(jnp.float32)

@jax.custom_vjp
def low_back(v):
    return v

def low_keep(v):
    return (low(v), None)

def low_pass(kept, grad):
    return (grad,)

def back_keep(v):
    return (v, None)

def back_low(kept, grad):
    return (low(grad),)
low.defvjp(low_keep, low_pass)
low_back.defvjp(back_keep, back_low)

def round_both(values):
    return low_back(low(values))

def layer_norm(values, scaling, offset):
    center = values - lax.optimization_barrier(jnp.mean(values, axis=-1, keepdims=True))
    spread = lax.optimization_barrier(jnp.mean(center * center, axis=-1, keepdims=True))
    return center * lax.rsqrt(spread + EPSILON) * scaling + offset

def gate_norm(gate_vals, mixed_vals):
    center = mixed_vals - lax.optimization_barrier(jnp.mean(mixed_vals, axis=-1, keepdims=True))
    spread = lax.optimization_barrier(jnp.mean(center * center, axis=-1, keepdims=True))
    normal = center * lax.rsqrt(spread + EPSILON)
    return jax.nn.silu(gate_vals) * normal.reshape(gate_vals.shape)

def gelu_gate(ff_gate, ff_up):
    return jax.nn.gelu(ff_gate, approximate=True) * ff_up

def matmul(operand, other):
    return jnp.dot(operand, other, precision=PRECISE)

def matmul_last(operand, other):
    return lax.dot_general(operand, other, (((1,), (1,)), ((), ())), precision=PRECISE)

def retain_block(carry_state, pieces):
    queries, key_rows, value_rows, log_rate = pieces
    cumulative = jnp.cumsum(log_rate, axis=0)
    block_total = cumulative[-1]
    by_head = cumulative.T
    positions = jnp.arange(BLOCK)
    causal = positions[:, None] >= positions[None, :]
    decay_table = jnp.where(causal[None], jnp.exp(jnp.minimum(by_head[:, :, None] - by_head[:, None, :], 0.0)), 0.0)
    scores = low_back(jnp.einsum('thd,shd->hts', queries, key_rows, precision=PRECISE))
    weights = low(scores * float(KEY) ** (-0.5) * decay_table)
    growth = jnp.exp(cumulative)[:, :, None]
    keeping = jnp.exp(block_total[None, :] - cumulative)[:, :, None]
    mixer_out = jnp.einsum('hts,she->the', weights, value_rows, precision=PRECISE)
    mixer_out = mixer_out + jnp.einsum('thd,hde->the', queries * growth, carry_state, precision=PRECISE)
    fresh_state = jnp.einsum('shd,she->hde', key_rows * keeping, value_rows, precision=PRECISE)
    next_state = jnp.exp(block_total)[:, None, None] * carry_state + fresh_state
    return (next_state, mixer_out)

def one_sequence(pieces):
    queries, key_rows, value_rows, log_rate = pieces
    blocks = (queries.reshape(N_CTX, BLOCK, HEADS, KEY), key_rows.reshape(N_CTX, BLOCK, HEADS, KEY), value_rows.reshape(N_CTX, BLOCK, HEADS, HEAD_V), log_rate.reshape(N_CTX, BLOCK, HEADS))
    initial_state = jnp.zeros((HEADS, KEY, HEAD_V), jnp.float32)
    final_state, mixer_out = lax.scan(jax.checkpoint(retain_block), initial_state, blocks)
    return mixer_out.reshape(LENGTH, HEADS, HEAD_V)

def forward(token_rows, log_rate, params):
    w_query, w_key, w_value, w_gate, w_out, norm1_gain, norm1_bias, w_ffgate, w_ffup, w_down, norm2_gain, norm2_bias = params
    per_round = token_rows.shape[0]
    row_count = per_round * LENGTH
    flat_rows = token_rows.reshape(row_count, D)
    normed = low(layer_norm(flat_rows, norm1_gain, norm1_bias))
    queries = round_both(matmul(normed, w_query)).reshape(per_round, LENGTH, HEADS, KEY)
    key_rows = round_both(matmul(normed, w_key)).reshape(per_round, LENGTH, HEADS, KEY)
    value_rows = round_both(matmul(normed, w_value)).reshape(per_round, LENGTH, HEADS, HEAD_V)
    gate_rows = round_both(matmul(normed, w_gate))
    mixer_out = low_back(lax.map(one_sequence, (queries, key_rows, value_rows, log_rate)))
    gated_out = low(gate_norm(gate_rows, mixer_out.reshape(row_count, HEADS, HEAD_V)))
    middle = flat_rows + low_back(matmul_last(gated_out, w_out))
    second_normed = low(layer_norm(middle, norm2_gain, norm2_bias))
    ff_gate = round_both(matmul(second_normed, w_ffgate))
    ff_up = round_both(matmul(second_normed, w_ffup))
    hidden = low(gelu_gate(ff_gate, ff_up))
    result = middle + low_back(matmul_last(hidden, w_down))
    return result.reshape(per_round, LENGTH, D)

def reference(tokens, log_decay, w_query, w_key, w_value, w_gate, w_out, norm1_gain, norm1_bias, w_ffgate, w_ffup, w_down, norm2_gain, norm2_bias, grad_out):
    params = tuple((weight_arg.astype(jnp.float32) for weight_arg in (w_query, w_key, w_value, w_gate, w_out, norm1_gain, norm1_bias, w_ffgate, w_ffup, w_down, norm2_gain, norm2_bias)))
    per_round = math.gcd(SEQS, max(1, 4096 // LENGTH))
    rounds = SEQS // per_round
    token_groups = tokens.astype(jnp.float32).reshape(rounds, per_round, LENGTH, D)
    decay_groups = log_decay.reshape(rounds, per_round, LENGTH, HEADS)
    grad_groups = grad_out.astype(jnp.float32).reshape(rounds, per_round, LENGTH, D)

    def one_round(running, pieces):
        token_part, decay_part, grad_part = pieces

        def run_layer(token_arg, param_arg):
            return forward(token_arg, decay_part, param_arg)
        result, pull_back = jax.vjp(run_layer, token_part, params)
        token_grad, param_grads = pull_back(grad_part)
        running = jax.tree.map(jnp.add, running, param_grads)
        return (running, (result.astype(jnp.bfloat16), token_grad.astype(jnp.bfloat16)))
    initial = tuple((jnp.zeros_like(weight_arg) for weight_arg in params))
    totals, (results, token_grads) = lax.scan(one_round, initial, (token_groups, decay_groups, grad_groups))
    return (results.reshape(SEQS, LENGTH, D), token_grads.reshape(SEQS, LENGTH, D), totals[0], totals[1], totals[2], totals[3], totals[4], totals[5], totals[6], totals[7], totals[8], totals[9], totals[10], totals[11])
```

```python
import functools

import jax
import jax.numpy as jnp
from jax import lax
from jax.experimental import pallas as pl
from jax.experimental.pallas import tpu as pltpu
from jax.sharding import PartitionSpec as P

KEY = 256
HEAD_V = 512
EPSILON = 1e-05
MESH = pl.DeviceIdType.MESH
ANY = pl.BlockSpec(memory_space=pl.ANY)
VMEM = pl.BlockSpec(memory_space=pltpu.VMEM)
BF = jnp.bfloat16
F32 = jnp.float32


def dot(a, b, dims):
    return lax.dot_general(a, b, (dims, ((), ())), preferred_element_type=F32)


def nn(a, b):
    return dot(a, b, ((1,), (0,)))


def nt(a, b):
    return dot(a, b, ((1,), (1,)))


def tn(a, b):
    return dot(a, b, ((0,), (0,)))


class Place:
    def __init__(self, F, C, T):
        self.F, self.C, self.T = F, C, T
        self.f = lax.axis_index("fsdp")
        self.z = lax.axis_index("ctx")
        self.t = lax.axis_index("tp")
        self.lo = lax.rem(self.t, 2)
        self.hi = self.t // 2
        self.near = self.t + 1 - 2 * self.lo
        self.far = lax.rem(self.t + 2, 4)

    def ahead(self, d):
        return lax.rem(self.z + d, self.C)

    def behind(self, d):
        return lax.rem(self.z + self.C - d, self.C)

    def fahead(self, d):
        return lax.rem(self.f + d, self.F)

    def fbehind(self, d):
        return lax.rem(self.f + self.F - d, self.F)

    def barrier(self, ctx=True, fsdp=False, tp=True):
        sem = pltpu.get_barrier_semaphore()
        peers = []
        if tp:
            peers += [{"tp": self.near}, {"tp": self.far}]
        if fsdp:
            peers += [{"fsdp": self.fahead(d)} for d in range(1, self.F)]
        if ctx:
            peers += [{"ctx": self.ahead(d)} for d in range(1, self.C)]
        for peer in peers:
            pl.semaphore_signal(sem, inc=1, device_id=peer, device_id_type=MESH)
        pl.semaphore_wait(sem, len(peers))


def remote(src, dst, ssem, rsem, peer):
    return pltpu.make_async_remote_copy(
        src_ref=src, dst_ref=dst, send_sem=ssem, recv_sem=rsem, device_id=peer, device_id_type=MESH
    )


def sem(*shape):
    return pltpu.SemaphoreType.DMA(shape)


def gather_sems(C):
    return [sem(C), sem(C), sem(C), sem(C), sem(C, 2), sem(C, 2)]


def gather_stage(pc, x, out, lsem, sems, owned=False):
    C = pc.C
    zs, zr, ys, yr, cs, cr = sems
    z, t = pc.z, pc.t
    started = []
    local = pltpu.make_async_copy(x, out.at[z, t], lsem)
    local.start()
    zc = [None] * C
    for d in range(1, C):
        zc[d] = remote(x, out.at[z, t], zs.at[d], zr.at[d], {"ctx": pc.ahead(d)})
        zc[d].start()
    yc = [None] * C
    cc = [[None, None] for _ in range(C)]
    for d in range(C):
        c = pc.behind(d)
        src = x if d == 0 else out.at[c, t]
        if d:
            zc[d].wait_recv()
        yc[d] = remote(src, out.at[c, t], ys.at[d], yr.at[d], {"tp": pc.far})
        yc[d].start()
        cc[d][0] = remote(src, out.at[c, t], cs.at[d, 0], cr.at[d, 0], {"tp": pc.near})
        cc[d][0].start()
    for d in range(C):
        c = pc.behind(d)
        yc[d].wait_recv()
        src = out.at[c, pc.far]
        cc[d][1] = remote(src, src, cs.at[d, 1], cr.at[d, 1], {"tp": pc.near})
        cc[d][1].start()
    local.wait()
    for d in range(C):
        if d:
            zc[d].wait_send()
        yc[d].wait_send()
        for j in range(2):
            cc[d][j].wait()


def share_sems():
    return [sem(3), sem(3)]


def share_stage(pc, x, out, lsem, sems):
    ss, rs = sems
    t = pc.t
    local = pltpu.make_async_copy(x, out.at[t], lsem)
    local.start()
    a = remote(x, out.at[t], ss.at[0], rs.at[0], {"tp": pc.far})
    a.start()
    b = remote(x, out.at[t], ss.at[1], rs.at[1], {"tp": pc.near})
    b.start()
    a.wait_recv()
    src = out.at[pc.far]
    c = remote(src, src, ss.at[2], rs.at[2], {"tp": pc.near})
    c.start()
    local.wait()
    a.wait_send()
    b.wait()
    c.wait()


def scatter_scratch(C, Q, W):
    return [
        pltpu.VMEM((C, 2, Q, W), BF),
        pltpu.VMEM((C, 2, Q, W), BF),
        pltpu.VMEM((C, Q, W), BF),
        pltpu.VMEM((C, Q, W), BF),
        pltpu.VMEM((C, Q, W), BF),
        pltpu.VMEM((C, Q, W), BF),
        sem(C, 2),
        sem(C, 2),
        sem(C, 2),
        sem(C),
        sem(C),
        sem(C),
        sem(C),
    ]


class Scatter:
    def __init__(self, pc, p, scratch):
        self.pc, self.p = pc, p
        (self.loc, self.buf1, self.snd2, self.buf2, self.snd3, self.buf3) = scratch[:6]
        self.ls, self.s1, self.r1, self.s2, self.r2, self.s3, self.r3 = scratch[6:]

    def start(self):
        pc, p = self.pc, self.p
        C = pc.C
        self.order = list(range(1, C)) + [0]
        self.lc, self.c1 = {}, {}
        for d in self.order:
            c = pc.ahead(d)
            for j in range(2):
                hi = 1 - pc.hi if j == 0 else pc.hi
                cp = remote(
                    p.at[c, hi * 2 + 1 - pc.lo],
                    self.buf1.at[d, j],
                    self.s1.at[d, j],
                    self.r1.at[d, j],
                    {"tp": pc.near},
                )
                cp.start()
                self.c1[d, j] = cp
                lc = pltpu.make_async_copy(
                    p.at[c, hi * 2 + pc.lo], self.loc.at[d, j], self.ls.at[d, j]
                )
                lc.start()
                self.lc[d, j] = lc

    def finish(self):
        pc = self.pc
        c2, c3 = {}, {}
        for d in self.order:
            self.lc[d, 0].wait()
            self.c1[d, 0].wait_recv()
            self.snd2[d] = (self.loc[d, 0].astype(F32) + self.buf1[d, 0].astype(F32)).astype(BF)
            c2[d] = remote(
                self.snd2.at[d], self.buf2.at[d], self.s2.at[d], self.r2.at[d], {"tp": pc.far}
            )
            c2[d].start()
        total = None
        for d in self.order:
            self.lc[d, 1].wait()
            self.c1[d, 1].wait_recv()
            c2[d].wait_recv()
            part = (
                self.loc[d, 1].astype(F32)
                + self.buf1[d, 1].astype(F32)
                + self.buf2[d].astype(F32)
            )
            if d:
                self.snd3[d] = part.astype(BF)
                c3[d] = remote(
                    self.snd3.at[d],
                    self.buf3.at[d],
                    self.s3.at[d],
                    self.r3.at[d],
                    {"ctx": pc.ahead(d)},
                )
                c3[d].start()
            else:
                total = part
        for d in range(1, pc.C):
            c3[d].wait_recv()
            total = total + self.buf3[d].astype(F32)
        for d in self.order:
            self.c1[d, 0].wait_send()
            self.c1[d, 1].wait_send()
            c2[d].wait_send()
            if d:
                c3[d].wait_send()
        return total


def first_kernel(
    dims, win, wrest, vec, ld, tok, go, owin, owrest, ovec, old, otok, ogo, ls, zs, zr, xs, xr, ys, yr, cs, cr
):
    pc = Place(*dims)
    F, C, T = dims
    f, z, t = pc.f, pc.z, pc.t
    pc.barrier(True, True, True)
    pieces = [win, wrest, vec, ld]
    outs = [owin, owrest, ovec, old]

    def piece(i, dst):
        return pieces[i].at[dst] if i < 2 else pieces[i]

    def slot(i, ff, c):
        return outs[i].at[ff, c] if i < 3 else outs[i].at[c]

    acts, oacts = [tok, go], [otok, ogo]
    zc, xc, yc, cc = {}, {}, {}, {}

    def send_piece(i):
        for d in range(1, C):
            dst = pc.ahead(d)
            zc[i, d] = remote(piece(i, dst), slot(i, f, z), zs.at[i, d], zr.at[i, d], {"ctx": dst})
            zc[i, d].start()

    def send_act(i):
        for d in range(1, C):
            k = 4 + i
            zc[k, d] = remote(
                acts[i].at[t], oacts[i].at[z, t], zs.at[k, d], zr.at[k, d], {"ctx": pc.ahead(d)}
            )
            zc[k, d].start()

    def across(i, d):
        c = pc.behind(d)
        src = piece(i, z) if d == 0 else slot(i, f, c)
        for e in range(1, F):
            xc[i, d, e] = remote(
                src, slot(i, f, c), xs.at[i, d, e], xr.at[i, d, e], {"fsdp": pc.fahead(e)}
            )
            xc[i, d, e].start()

    def spread(i, d):
        c = pc.behind(d)
        src = oacts[i].at[c, t]
        yc[i, d] = remote(src, src, ys.at[i, d], yr.at[i, d], {"tp": pc.far})
        yc[i, d].start()
        cc[i, d, 0] = remote(src, src, cs.at[i, d, 0], cr.at[i, d, 0], {"tp": pc.near})
        cc[i, d, 0].start()

    def spread_on(i, d):
        c = pc.behind(d)
        yc[i, d].wait_recv()
        src = oacts[i].at[c, pc.far]
        cc[i, d, 1] = remote(src, src, cs.at[i, d, 1], cr.at[i, d, 1], {"tp": pc.near})
        cc[i, d, 1].start()

    for i in (2, 3):
        send_piece(i)
    send_act(0)
    send_piece(0)
    for i in (2, 0):
        across(i, 0)
    send_piece(1)
    send_act(1)
    across(1, 0)
    local = []
    for i in range(4):
        local.append(pltpu.make_async_copy(piece(i, z), slot(i, f, z), ls.at[i]))
    for i in range(2):
        local.append(pltpu.make_async_copy(acts[i], oacts[i].at[z], ls.at[4 + i]))
    for cp in local:
        cp.start()
    for d in range(1, C):
        zc[2, d].wait_recv()
        across(2, d)
        zc[4, d].wait_recv()
        spread(0, d)
    for d in range(1, C):
        zc[0, d].wait_recv()
        across(0, d)
    for d in range(1, C):
        spread_on(0, d)
    for d in range(1, C):
        zc[1, d].wait_recv()
        across(1, d)
        zc[5, d].wait_recv()
        spread(1, d)
    for d in range(1, C):
        spread_on(1, d)
        zc[3, d].wait_recv()
    for cp in local:
        cp.wait()
    for cp in zc.values():
        cp.wait_send()
    for cp in xc.values():
        cp.wait()
    for cp in yc.values():
        cp.wait_send()
    for cp in cc.values():
        cp.wait()


def out_kernel(dims, p, tok, gain, bias, mid, sn, x, lsem, *scratch):
    pc = Place(*dims)
    pc.barrier()
    n = len(gather_sems(pc.C))
    rs = Scatter(pc, p, scratch[n:])
    rs.start()
    total = rs.finish() + tok[...].astype(F32)
    mid[...] = total
    center = total - jnp.mean(total, axis=-1, keepdims=True)
    spread = jnp.mean(center * center, axis=-1, keepdims=True)
    x[...] = (center * lax.rsqrt(spread + EPSILON) * gain[...] + bias[...]).astype(BF)
    gather_stage(pc, x, sn, lsem, scratch[:n])


def norm_pull(values, gain, grad):
    center = values - jnp.mean(values, axis=-1, keepdims=True)
    spread = jnp.mean(center * center, axis=-1, keepdims=True)
    inv = lax.rsqrt(spread + EPSILON)
    xhat = center * inv
    g = grad * gain
    back = inv * (
        g - jnp.mean(g, axis=-1, keepdims=True) - xhat * jnp.mean(g * xhat, axis=-1, keepdims=True)
    )
    return (
        back,
        jnp.sum(grad * xhat, axis=0, keepdims=True),
        jnp.sum(grad, axis=0, keepdims=True),
    )


def mlp_kernel(
    dims, pg, pd, mid, go, gain, gm, gb, out, dgain, dbias, x, y, lsem, *scratch
):
    pc = Place(*dims)
    pc.barrier()
    n = len(gather_sems(pc.C))
    m = (len(scratch) - n - 2) // 2
    gs, ss = scratch[:n], scratch[n : n + 2]
    rg = Scatter(pc, pg, scratch[n + 2 : n + 2 + m])
    rd = Scatter(pc, pd, scratch[n + 2 + m :])
    rg.start()
    rd.start()
    back, dg, db = norm_pull(mid[...], gain[...], rg.finish())
    dgain[...] = dg
    dbias[...] = db
    grad_middle = go[...].astype(F32) + back
    gm[...] = grad_middle
    x[...] = grad_middle.astype(BF)
    gather_stage(pc, x, gb, lsem.at[0], gs)
    y[...] = (mid[...] + rd.finish()).astype(BF)
    share_stage(pc, y, out, lsem.at[1], ss)


def last_kernel(dims, p, gm, tok, gain, gt, dgain, dbias, y, lsem, s0, s1, *scratch):
    pc = Place(*dims)
    pc.barrier()
    rs = Scatter(pc, p, scratch)
    rs.start()
    back, dg, db = norm_pull(tok[...].astype(F32), gain[...], rs.finish())
    dgain[...] = dg
    dbias[...] = db
    y[...] = (gm[...] + back).astype(BF)
    share_stage(pc, y, gt, lsem, (s0, s1))


def grads_kernel(
    dims, g, v, out, vout, own, xbuf, zsnd, va, vb, vc, vd, vx, vz, ls, osem, xs, xr, zs, zr, ts, tr, vxs, vxr, vzs, vzr
):
    pc = Place(*dims)
    F, C, T = dims
    f, z = pc.f, pc.z
    pc.barrier(True, True, True)
    order = list(range(1, C)) + [0]
    loc, xc, zc = {}, {}, {}
    t0 = remote(v, vb, ts.at[0], tr.at[0], {"tp": pc.near})
    t0.start()
    for d in order:
        c = pc.ahead(d)
        for e in range(1, F):
            xc[d, e] = remote(
                g.at[pc.fahead(e), c], xbuf.at[e - 1, d], xs.at[d, e], xr.at[d, e], {"fsdp": pc.fahead(e)}
            )
            xc[d, e].start()
        loc[d] = pltpu.make_async_copy(g.at[f, c], own.at[d], ls.at[d])
        loc[d].start()
    t0.wait_recv()
    va[...] = v[...] + vb[...]
    t1 = remote(va, vc, ts.at[1], tr.at[1], {"tp": pc.far})
    t1.start()
    t1.wait_recv()
    vd[...] = va[...] + vc[...]
    vxc = {}
    for e in range(1, F):
        vxc[e] = remote(
            vd.at[pc.fahead(e)], vx.at[e - 1], vxs.at[e], vxr.at[e], {"fsdp": pc.fahead(e)}
        )
        vxc[e].start()
    vs = vd[f]
    for e in range(1, F):
        vxc[e].wait_recv()
        vs = vs + vx[e - 1]
    vxs_ref = vz.at[0]
    vxs_ref[...] = vs
    vzc = {}
    for d in range(1, C):
        vzc[d] = remote(
            vz.at[0, pc.ahead(d)], vz.at[1, d], vzs.at[d], vzr.at[d], {"ctx": pc.ahead(d)}
        )
        vzc[d].start()
    keep = None
    for d in order:
        loc[d].wait()
        total = own[d].astype(F32)
        for e in range(1, F):
            xc[d, e].wait_recv()
            total = total + xbuf[e - 1, d].astype(F32)
        zsnd[d] = total.astype(BF)
        if d:
            zc[d] = remote(
                zsnd.at[d], out.at[z], zs.at[d], zr.at[d], {"ctx": pc.ahead(d)}
            )
            zc[d].start()
        else:
            keep = pltpu.make_async_copy(zsnd.at[0], out.at[z], osem)
            keep.start()
    acc = vz[0, z]
    for d in range(1, C):
        vzc[d].wait_recv()
        acc = acc + vz[1, d]
    vout[...] = acc
    keep.wait()
    for cp in zc.values():
        cp.wait()
    for cp in xc.values():
        cp.wait_send()
    for cp in [t0, t1] + list(vxc.values()) + list(vzc.values()):
        cp.wait_send()


def params(cid):
    return pltpu.CompilerParams(collective_id=cid, has_side_effects=True)


def silu_parts(g):
    s = jax.nn.sigmoid(g)
    return g * s, s * (1.0 + g * (1.0 - s))


def shards(
    dims,
    tokens,
    log_decay,
    w_query,
    w_key,
    w_value,
    w_gate,
    w_out,
    norm1_gain,
    norm1_bias,
    w_ffgate,
    w_ffup,
    w_down,
    norm2_gain,
    norm2_bias,
    grad_out,
):
    F, C, T = dims
    S, B, W = tokens.shape
    L = S * B
    Q = L // T
    N = C * L
    R = w_query.shape[0]
    heads = log_decay.shape[2]
    halves = C // heads
    HV = HEAD_V // halves
    U = w_ffgate.shape[1] // C
    z = lax.axis_index("ctx")
    t = lax.axis_index("tp")
    scale = float(KEY) ** (-0.5)

    def cols(w, i, n):
        return w[:, i * n : (i + 1) * n]

    win = jnp.stack(
        [
            jnp.concatenate(
                [
                    cols(w_query, c // halves, KEY),
                    cols(w_key, c // halves, KEY),
                    cols(w_value, c, HV),
                    cols(w_gate, c, HV),
                ],
                axis=1,
            )
            for c in range(C)
        ]
    )
    wrest = jnp.stack(
        [
            jnp.concatenate(
                [cols(w_out, c, HV), cols(w_ffgate, c, U), cols(w_ffup, c, U), cols(w_down, c, U)],
                axis=1,
            )
            for c in range(C)
        ]
    )
    NI, NR = win.shape[2], wrest.shape[2]
    vec = jnp.stack([norm1_gain, norm1_bias, norm2_gain, norm2_bias]).astype(F32)
    vec = jnp.pad(vec, ((0, 4), (0, 0)))
    ld = jnp.pad(jnp.transpose(log_decay, (2, 0, 1)).reshape(heads, L), ((0, 8 - heads), (0, 0)))
    tok = tokens.reshape(T, Q, W)
    go = grad_out.reshape(T, Q, W)
    sds = jax.ShapeDtypeStruct
    owin, owrest, ovec, old, otok, ogo = pl.pallas_call(
        functools.partial(first_kernel, dims),
        out_shape=(
            sds((F, C, R, NI), BF),
            sds((F, C, R, NR), BF),
            sds((F, C, 8, R), F32),
            sds((C, 8, L), F32),
            sds((C, T, Q, W), BF),
            sds((C, T, Q, W), BF),
        ),
        in_specs=[ANY] * 6,
        out_specs=[ANY] * 6,
        scratch_shapes=[
            sem(6),
            sem(6, C),
            sem(6, C),
            sem(3, C, F),
            sem(3, C, F),
            sem(2, C),
            sem(2, C),
            sem(2, C, 2),
            sem(2, C, 2),
        ],
        compiler_params=params(1),
        name="k_first",
    )(win, wrest, vec, ld, tok, go)

    vecs = jnp.transpose(ovec[:, :, :4], (2, 0, 1, 3)).reshape(4, 1, W)
    gain1, bias1, gain2, bias2 = vecs[0], vecs[1], vecs[2], vecs[3]
    w_in = owin.reshape(W, NI)
    w_rest = owrest.reshape(W, NR)
    w_o, w_fg, w_fu, w_d = w_rest[:, :HV], w_rest[:, HV : HV + U], w_rest[:, HV + U : HV + 2 * U], w_rest[:, HV + 2 * U :]
    xs = otok.reshape(N, W).astype(F32)
    center = xs - jnp.mean(xs, axis=-1, keepdims=True)
    spread = jnp.mean(center * center, axis=-1, keepdims=True)
    normed = (center * lax.rsqrt(spread + EPSILON) * gain1 + bias1).astype(BF)
    proj = nn(normed, w_in).astype(BF)
    q = proj[:, :KEY].reshape(C, S, B, KEY)
    k = proj[:, KEY : 2 * KEY].reshape(C, S, B, KEY)
    v = proj[:, 2 * KEY : 2 * KEY + HV].reshape(C, S, B, HV)
    g = proj[:, 2 * KEY + HV :].reshape(C, S, B, HV).astype(F32)

    rates = lax.dynamic_index_in_dim(old, z // halves, 1, False).reshape(C, S, B)
    cum = jnp.cumsum(rates, axis=-1)
    total = cum[..., -1]
    positions = jnp.arange(B)
    causal = positions[:, None] >= positions[None, :]
    table = jnp.where(
        causal, jnp.exp(jnp.minimum(cum[..., :, None] - cum[..., None, :], 0.0)), 0.0
    )
    growth = jnp.exp(cum)[..., None]
    keeping = jnp.exp(total[..., None] - cum)[..., None]
    through = jnp.exp(total)[..., None, None]

    def ein(spec, a, b):
        return jnp.einsum(spec, a, b, preferred_element_type=F32)

    weights = (ein("cstd,csud->cstu", q, k) * scale * table).astype(BF)
    q_grown = (q.astype(F32) * growth).astype(BF)
    k_kept = (k.astype(F32) * keeping).astype(BF)
    fresh = ein("csud,csue->csde", k_kept, v)
    state = jnp.zeros_like(fresh[0])
    states = []
    for c in range(C):
        states.append(state.astype(BF))
        state = through[c] * state + fresh[c]
    states = jnp.stack(states)
    mixer = ein("cstu,csue->cste", weights, v) + ein("cstd,csde->cste", q_grown, states)

    def pair(stats):
        got = [stats]
        for j in range(1, halves):
            perm = []
            for c in range(C):
                base = c - c % halves
                perm.append((c, base + (c % halves + j) % halves))
            got.append(lax.ppermute(stats, "ctx", perm))
        return got

    mean_here = jnp.mean(mixer, axis=-1)
    dev = mixer - mean_here[..., None]
    m2_here = jnp.sum(dev * dev, axis=-1)
    got = pair(jnp.stack([mean_here, m2_here]))
    mean = sum(x[0] for x in got) / halves
    m2 = sum(x[1] + HV * (x[0] - mean) ** 2 for x in got)
    inv = lax.rsqrt(m2 / HEAD_V + EPSILON)[..., None]
    normal = (mixer - mean[..., None]) * inv
    silu, dsilu = silu_parts(g)
    gated = (silu * normal).astype(BF).reshape(N, HV)

    part = nt(gated, w_o).astype(BF).reshape(C, T, Q, W)
    mytok = lax.dynamic_index_in_dim(tok, t, 0, False)
    mygo = lax.dynamic_index_in_dim(go, t, 0, False)
    mid, sn = pl.pallas_call(
        functools.partial(out_kernel, dims),
        out_shape=(sds((Q, W), F32), sds((C, T, Q, W), BF)),
        in_specs=[ANY, VMEM, VMEM, VMEM],
        out_specs=[VMEM, ANY],
        scratch_shapes=[pltpu.VMEM((Q, W), BF), pltpu.SemaphoreType.DMA]
        + gather_sems(C)
        + scatter_scratch(C, Q, W),
        compiler_params=params(2),
        name="k_out",
    )(part, mytok, gain2, bias2)

    second = sn.reshape(N, W)
    ff_gate = nn(second, w_fg).astype(BF)
    ff_up = nn(second, w_fu).astype(BF)
    hidden, gelu_pull = jax.vjp(
        lambda a, b: jax.nn.gelu(a, approximate=True) * b, ff_gate.astype(F32), ff_up.astype(F32)
    )
    hidden = hidden.astype(BF)
    down = nt(hidden, w_d).astype(BF).reshape(C, T, Q, W)
    gout = ogo.reshape(N, W)
    grad_hidden = nn(gout, w_d)
    gfg, gfu = gelu_pull(grad_hidden)
    gfg, gfu = gfg.astype(BF), gfu.astype(BF)
    gsecond = (nt(gfg, w_fg) + nt(gfu, w_fu)).astype(BF).reshape(C, T, Q, W)
    gm, gb, out, dgain2, dbias2 = pl.pallas_call(
        functools.partial(mlp_kernel, dims),
        out_shape=(
            sds((Q, W), F32),
            sds((C, T, Q, W), BF),
            sds((T, Q, W), BF),
            sds((1, W), F32),
            sds((1, W), F32),
        ),
        in_specs=[ANY, ANY, VMEM, VMEM, VMEM],
        out_specs=[VMEM, ANY, ANY, VMEM, VMEM],
        scratch_shapes=[pltpu.VMEM((Q, W), BF), pltpu.VMEM((Q, W), BF), sem(2)]
        + gather_sems(C)
        + share_sems()
        + scatter_scratch(C, Q, W)
        + scatter_scratch(C, Q, W),
        compiler_params=params(3),
        name="k_mlp",
    )(gsecond, down, mid, mygo, gain2)
    output = out.reshape(tokens.shape)

    branch = gb.reshape(N, W)
    ggated = nn(branch, w_o).reshape(C, S, B, HV)
    ggate = (ggated * normal * dsilu).astype(BF)
    gn = ggated * silu
    sums = pair(jnp.stack([jnp.sum(gn, axis=-1), jnp.sum(gn * normal, axis=-1)]))
    s1 = sum(x[0] for x in sums)[..., None] / HEAD_V
    s2 = sum(x[1] for x in sums)[..., None] / HEAD_V
    gmixer = (inv * (gn - s1 - normal * s2)).astype(BF)
    gscores = (ein("cste,csue->cstu", gmixer, v) * scale * table).astype(BF)
    pulled = ein("cstd,cste->csde", q_grown, gmixer)
    later = jnp.zeros_like(pulled[0])
    laters = [None] * C
    for c in reversed(range(C)):
        laters[c] = later.astype(BF)
        later = through[c] * later + pulled[c]
    laters = jnp.stack(laters)
    gq = ein("cstu,csud->cstd", gscores, k) + growth * ein("cste,csde->cstd", gmixer, states)
    gk = ein("cstu,cstd->csud", gscores, q) + keeping * ein("csue,csde->csud", v, laters)
    gv = ein("cstu,cste->csue", weights, gmixer) + ein("csud,csde->csue", k_kept, laters)
    gproj = jnp.concatenate([gq.astype(BF), gk.astype(BF), gv.astype(BF), ggate], axis=-1)
    gproj = gproj.reshape(N, NI)

    gnormed = nt(gproj, w_in).astype(BF).reshape(C, T, Q, W)
    gt, dgain1, dbias1 = pl.pallas_call(
        functools.partial(last_kernel, dims),
        out_shape=(sds((T, Q, W), BF), sds((1, W), F32), sds((1, W), F32)),
        in_specs=[ANY, VMEM, VMEM, VMEM],
        out_specs=[ANY, VMEM, VMEM],
        scratch_shapes=[pltpu.VMEM((Q, W), BF), pltpu.SemaphoreType.DMA]
        + share_sems()
        + scatter_scratch(C, Q, W),
        compiler_params=params(4),
        name="k_last",
    )(gnormed, gm, mytok, gain1)
    grad_tokens = gt.reshape(tokens.shape)

    grads = jnp.concatenate(
        [
            tn(normed, gproj).astype(BF),
            tn(branch, gated).astype(BF),
            tn(second, gfg).astype(BF),
            tn(second, gfu).astype(BF),
            tn(gout, hidden).astype(BF),
        ],
        axis=1,
    ).reshape(F, C, R, NI + NR)
    vpart = jnp.concatenate([dgain1, dbias1, dgain2, dbias2, jnp.zeros((4, W), F32)], axis=0)
    vpart = jnp.transpose(vpart.reshape(8, F, C, R), (1, 2, 0, 3))
    NG = NI + NR
    gsum, vsum = pl.pallas_call(
        functools.partial(grads_kernel, dims),
        out_shape=(sds((C, R, NG), BF), sds((8, R), F32)),
        in_specs=[ANY, VMEM],
        out_specs=[ANY, VMEM],
        scratch_shapes=[
            pltpu.VMEM((C, R, NG), BF),
            pltpu.VMEM((F - 1, C, R, NG), BF),
            pltpu.VMEM((C, R, NG), BF),
            pltpu.VMEM((F, C, 8, R), F32),
            pltpu.VMEM((F, C, 8, R), F32),
            pltpu.VMEM((F, C, 8, R), F32),
            pltpu.VMEM((F, C, 8, R), F32),
            pltpu.VMEM((F - 1, C, 8, R), F32),
            pltpu.VMEM((2, C, 8, R), F32),
            sem(C),
            pltpu.SemaphoreType.DMA,
            sem(C, F),
            sem(C, F),
            sem(C),
            sem(C),
            sem(2),
            sem(2),
            sem(F),
            sem(F),
            sem(C),
            sem(C),
        ],
        compiler_params=params(5),
        name="k_grads",
    )(grads, vpart)

    def by_head(lo):
        x = gsum[:, :, lo : lo + KEY].astype(F32).reshape(heads, halves, R, KEY).sum(axis=1)
        return jnp.transpose(x, (1, 0, 2)).reshape(R, heads * KEY)

    def side(lo, n):
        return jnp.transpose(gsum[:, :, lo : lo + n].astype(F32), (1, 0, 2)).reshape(R, C * n)

    return (
        output,
        grad_tokens,
        by_head(0),
        by_head(KEY),
        side(2 * KEY, HV),
        side(2 * KEY + HV, HV),
        side(NI, HV),
        vsum[0],
        vsum[1],
        side(NI + HV, U),
        side(NI + HV + U, U),
        side(NI + HV + 2 * U, U),
        vsum[2],
        vsum[3],
    )


def solution(mesh):
    dims = (mesh.shape["fsdp"], mesh.shape["ctx"], mesh.shape["tp"])
    rows, vec = P(("fsdp", "ctx"), "tp"), P(("fsdp", "ctx"))
    acts = P("fsdp", "ctx", None)
    return jax.shard_map(
        functools.partial(shards, dims),
        mesh=mesh,
        in_specs=(acts, P("fsdp", "ctx", "tp"), rows, rows, rows, rows, rows, vec, vec, rows, rows, rows, vec, vec, acts),
        out_specs=(acts, acts, rows, rows, rows, rows, rows, vec, vec, rows, rows, rows, vec, vec),
        check_vma=False,
    )
```

```python
import functools

import jax
import jax.numpy as jnp
from jax import lax
from jax.experimental import pallas as pl
from jax.experimental.pallas import tpu as pltpu
from jax.sharding import PartitionSpec as P

KEY = 256
HEAD_V = 512
EPSILON = 1e-05
MESH = pl.DeviceIdType.MESH
ANY = pl.BlockSpec(memory_space=pl.ANY)
VMEM = pl.BlockSpec(memory_space=pltpu.VMEM)
BF = jnp.bfloat16
F32 = jnp.float32


def dot(a, b, dims):
    return lax.dot_general(a, b, (dims, ((), ())), preferred_element_type=F32)


def nn(a, b):
    return dot(a, b, ((1,), (0,)))


def nt(a, b):
    return dot(a, b, ((1,), (1,)))


def tn(a, b):
    return dot(a, b, ((0,), (0,)))


class Place:
    def __init__(self, F, C, T):
        self.F, self.C, self.T = F, C, T
        self.f = lax.axis_index("fsdp")
        self.z = lax.axis_index("ctx")
        self.t = lax.axis_index("tp")
        self.lo = lax.rem(self.t, 2)
        self.hi = self.t // 2
        self.near = self.t + 1 - 2 * self.lo
        self.far = lax.rem(self.t + 2, 4)

    def ahead(self, d):
        return lax.rem(self.z + d, self.C)

    def behind(self, d):
        return lax.rem(self.z + self.C - d, self.C)

    def fahead(self, d):
        return lax.rem(self.f + d, self.F)

    def fbehind(self, d):
        return lax.rem(self.f + self.F - d, self.F)

    def barrier(self, ctx=True, fsdp=False, tp=True):
        sem = pltpu.get_barrier_semaphore()
        peers = []
        if tp:
            peers += [{"tp": self.near}, {"tp": self.far}]
        if fsdp:
            peers += [{"fsdp": self.fahead(d)} for d in range(1, self.F)]
        if ctx:
            peers += [{"ctx": self.ahead(d)} for d in range(1, self.C)]
        for peer in peers:
            pl.semaphore_signal(sem, inc=1, device_id=peer, device_id_type=MESH)
        pl.semaphore_wait(sem, len(peers))


def remote(src, dst, ssem, rsem, peer):
    return pltpu.make_async_remote_copy(
        src_ref=src, dst_ref=dst, send_sem=ssem, recv_sem=rsem, device_id=peer, device_id_type=MESH
    )


def sem(*shape):
    return pltpu.SemaphoreType.DMA(shape)


def gather_sems(C):
    return [sem(C), sem(C), sem(C), sem(C), sem(C, 2), sem(C, 2)]


def gather_stage(pc, x, out, lsem, sems, owned=False):
    C = pc.C
    zs, zr, ys, yr, cs, cr = sems
    z, t = pc.z, pc.t
    started = []
    local = pltpu.make_async_copy(x, out.at[z, t], lsem)
    local.start()
    zc = [None] * C
    for d in range(1, C):
        zc[d] = remote(x, out.at[z, t], zs.at[d], zr.at[d], {"ctx": pc.ahead(d)})
        zc[d].start()
    yc = [None] * C
    cc = [[None, None] for _ in range(C)]
    for d in range(C):
        c = pc.behind(d)
        src = x if d == 0 else out.at[c, t]
        if d:
            zc[d].wait_recv()
        yc[d] = remote(src, out.at[c, t], ys.at[d], yr.at[d], {"tp": pc.far})
        yc[d].start()
        cc[d][0] = remote(src, out.at[c, t], cs.at[d, 0], cr.at[d, 0], {"tp": pc.near})
        cc[d][0].start()
    for d in range(C):
        c = pc.behind(d)
        yc[d].wait_recv()
        src = out.at[c, pc.far]
        cc[d][1] = remote(src, src, cs.at[d, 1], cr.at[d, 1], {"tp": pc.near})
        cc[d][1].start()
    local.wait()
    for d in range(C):
        if d:
            zc[d].wait_send()
        yc[d].wait_send()
        for j in range(2):
            cc[d][j].wait()


def share_sems():
    return [sem(3), sem(3)]


def share_stage(pc, x, out, lsem, sems):
    ss, rs = sems
    t = pc.t
    local = pltpu.make_async_copy(x, out.at[t], lsem)
    local.start()
    a = remote(x, out.at[t], ss.at[0], rs.at[0], {"tp": pc.far})
    a.start()
    b = remote(x, out.at[t], ss.at[1], rs.at[1], {"tp": pc.near})
    b.start()
    a.wait_recv()
    src = out.at[pc.far]
    c = remote(src, src, ss.at[2], rs.at[2], {"tp": pc.near})
    c.start()
    local.wait()
    a.wait_send()
    b.wait()
    c.wait()


def scatter_scratch(C, Q, W):
    return [
        pltpu.VMEM((C, 2, Q, W), BF),
        pltpu.VMEM((C, 2, Q, W), BF),
        pltpu.VMEM((C, Q, W), BF),
        pltpu.VMEM((C, Q, W), BF),
        pltpu.VMEM((C, Q, W), BF),
        pltpu.VMEM((C, Q, W), BF),
        sem(C, 2),
        sem(C, 2),
        sem(C, 2),
        sem(C),
        sem(C),
        sem(C),
        sem(C),
    ]


class Scatter:
    def __init__(self, pc, p, scratch):
        self.pc, self.p = pc, p
        (self.loc, self.buf1, self.snd2, self.buf2, self.snd3, self.buf3) = scratch[:6]
        self.ls, self.s1, self.r1, self.s2, self.r2, self.s3, self.r3 = scratch[6:]

    def start(self):
        pc, p = self.pc, self.p
        C = pc.C
        self.order = list(range(1, C)) + [0]
        self.lc, self.c1 = {}, {}
        for d in self.order:
            c = pc.ahead(d)
            for j in range(2):
                hi = 1 - pc.hi if j == 0 else pc.hi
                cp = remote(
                    p.at[c, hi * 2 + 1 - pc.lo],
                    self.buf1.at[d, j],
                    self.s1.at[d, j],
                    self.r1.at[d, j],
                    {"tp": pc.near},
                )
                cp.start()
                self.c1[d, j] = cp
                lc = pltpu.make_async_copy(
                    p.at[c, hi * 2 + pc.lo], self.loc.at[d, j], self.ls.at[d, j]
                )
                lc.start()
                self.lc[d, j] = lc

    def finish(self, between=lambda: None):
        pc = self.pc
        c2, c3 = {}, {}
        for d in self.order:
            self.lc[d, 0].wait()
            self.c1[d, 0].wait_recv()
            self.snd2[d] = (self.loc[d, 0].astype(F32) + self.buf1[d, 0].astype(F32)).astype(BF)
            c2[d] = remote(
                self.snd2.at[d], self.buf2.at[d], self.s2.at[d], self.r2.at[d], {"tp": pc.far}
            )
            c2[d].start()
        total = None
        for d in self.order:
            self.lc[d, 1].wait()
            self.c1[d, 1].wait_recv()
            c2[d].wait_recv()
            part = (
                self.loc[d, 1].astype(F32)
                + self.buf1[d, 1].astype(F32)
                + self.buf2[d].astype(F32)
            )
            if d:
                self.snd3[d] = part.astype(BF)
                c3[d] = remote(
                    self.snd3.at[d],
                    self.buf3.at[d],
                    self.s3.at[d],
                    self.r3.at[d],
                    {"ctx": pc.ahead(d)},
                )
                c3[d].start()
            else:
                total = part
            between()
        for d in range(1, pc.C):
            c3[d].wait_recv()
            total = total + self.buf3[d].astype(F32)
        for d in self.order:
            self.c1[d, 0].wait_send()
            self.c1[d, 1].wait_send()
            c2[d].wait_send()
            if d:
                c3[d].wait_send()
        return total


def first_kernel(
    dims, layout, wq, wk, wv, wg, wo, vec, ld, tok, go, owin, ovec, old, otok, ogo, ls, zs, zr, xs, xr, ys, yr, cs, cr
):
    pc = Place(*dims)
    F, C, T = dims
    f, z, t = pc.f, pc.z, pc.t
    pc.barrier(True, True, True)
    weights = (wq, wk, wv, wg, wo)
    pieces = [None, vec, ld]
    outs = [owin, ovec, old]

    def slot(i, ff, c):
        return outs[i].at[ff, c] if i < 2 else outs[i].at[c]

    def columns(dst):
        at = 0
        for w, (share, n) in zip(weights, layout):
            start = pl.multiple_of((dst // share) * n, n)
            yield w.at[:, pl.ds(start, n)], owin.at[f, z, :, pl.ds(at, n)]
            at += n

    acts, oacts = [tok, go], [otok, ogo]
    zc, xc, yc, cc = {}, {}, {}, {}

    def send_piece(i):
        for d in range(1, C):
            dst = pc.ahead(d)
            sems = (zs.at[i, d], zr.at[i, d])
            if i:
                zc[i, d] = remote(pieces[i], slot(i, f, z), *sems, {"ctx": dst})
                zc[i, d].start()
            else:
                for src, to in columns(dst):
                    remote(src, to, *sems, {"ctx": dst}).start()
                c = pc.behind(d)
                zc[i, d] = remote(slot(i, f, c), slot(i, f, c), *sems, {"ctx": dst})

    def send_act(i):
        for d in range(1, C):
            k = 3 + i
            zc[k, d] = remote(
                acts[i].at[t], oacts[i].at[z, t], zs.at[k, d], zr.at[k, d], {"ctx": pc.ahead(d)}
            )
            zc[k, d].start()

    def across(i, d):
        c = pc.behind(d)
        for e in range(1, F):
            sems = (xs.at[i, d, e], xr.at[i, d, e])
            peer = {"fsdp": pc.fahead(e)}
            if i == 0 and d == 0:
                for src, to in columns(z):
                    remote(src, to, *sems, peer).start()
                here = slot(0, pc.fbehind(e), z)
                xc[i, d, e] = remote(here, here, *sems, peer)
            else:
                src = pieces[i] if d == 0 else slot(i, f, c)
                xc[i, d, e] = remote(src, slot(i, f, c), *sems, peer)
                xc[i, d, e].start()

    def spread(i, d):
        c = pc.behind(d)
        src = oacts[i].at[c, t]
        yc[i, d] = remote(src, src, ys.at[i, d], yr.at[i, d], {"tp": pc.far})
        yc[i, d].start()
        cc[i, d, 0] = remote(src, src, cs.at[i, d, 0], cr.at[i, d, 0], {"tp": pc.near})
        cc[i, d, 0].start()

    def spread_on(i, d):
        c = pc.behind(d)
        yc[i, d].wait_recv()
        src = oacts[i].at[c, pc.far]
        cc[i, d, 1] = remote(src, src, cs.at[i, d, 1], cr.at[i, d, 1], {"tp": pc.near})
        cc[i, d, 1].start()

    for i in (1, 2):
        send_piece(i)
    send_act(0)
    send_piece(0)
    for i in (1, 0):
        across(i, 0)
    send_act(1)
    local = [
        pltpu.make_async_copy(src, to, ls.at[i]) for i, (src, to) in enumerate(columns(z))
    ]
    for i in (1, 2):
        local.append(pltpu.make_async_copy(pieces[i], slot(i, f, z), ls.at[4 + i]))
    for i in range(2):
        local.append(pltpu.make_async_copy(acts[i], oacts[i].at[z], ls.at[7 + i]))
    for cp in local:
        cp.start()
    for d in range(1, C):
        zc[1, d].wait_recv()
        across(1, d)
        zc[3, d].wait_recv()
        spread(0, d)
    for d in range(1, C):
        spread_on(0, d)
    for d in range(1, C):
        zc[0, d].wait_recv()
        across(0, d)
    for d in range(1, C):
        zc[4, d].wait_recv()
        spread(1, d)
    for d in range(1, C):
        spread_on(1, d)
        zc[2, d].wait_recv()
    for cp in local:
        cp.wait()
    for cp in zc.values():
        cp.wait_send()
    for cp in xc.values():
        cp.wait()
    for cp in yc.values():
        cp.wait_send()
    for cp in cc.values():
        cp.wait()


def out_kernel(
    dims, p, tok, gain, bias, near, mid, sn, full, x, lsem, ws, wr, wl, *scratch
):
    pc = Place(*dims)
    F, C, T = dims
    pc.barrier(True, True, True)
    n = len(gather_sems(C))
    rs = Scatter(pc, p, scratch[n:])
    rs.start()
    moves = []
    for d in range(C):
        dst = full.at[pc.f, pc.behind(d)]
        for e in range(1, F):
            cp = remote(near.at[d], dst, ws.at[d, e], wr.at[d, e], {"fsdp": pc.fahead(e)})
            cp.start()
            moves.append(cp)
        cp = pltpu.make_async_copy(near.at[d], dst, wl.at[d])
        cp.start()
        moves.append(cp)
    total = rs.finish() + tok[...].astype(F32)
    mid[...] = total
    center = total - jnp.mean(total, axis=-1, keepdims=True)
    spread = jnp.mean(center * center, axis=-1, keepdims=True)
    x[...] = (center * lax.rsqrt(spread + EPSILON) * gain[...] + bias[...]).astype(BF)
    gather_stage(pc, x, sn, lsem, scratch[:n])
    for cp in moves:
        cp.wait()


def norm_pull(values, gain, grad):
    center = values - jnp.mean(values, axis=-1, keepdims=True)
    spread = jnp.mean(center * center, axis=-1, keepdims=True)
    inv = lax.rsqrt(spread + EPSILON)
    xhat = center * inv
    g = grad * gain
    back = inv * (
        g - jnp.mean(g, axis=-1, keepdims=True) - xhat * jnp.mean(g * xhat, axis=-1, keepdims=True)
    )
    return (
        back,
        jnp.sum(grad * xhat, axis=0, keepdims=True),
        jnp.sum(grad, axis=0, keepdims=True),
    )


def mlp_kernel(
    dims, pg, pd, mid, go, gain, g0, g1, g2, gm, gb, out, dgain, dbias, xg, x, y, lsem, gxs, gxr, *scratch
):
    pc = Place(*dims)
    pc.barrier(True, True, True)
    n = len(gather_sems(pc.C))
    m = (len(scratch) - n - 2) // 2
    gs, ss = scratch[:n], scratch[n : n + 2]
    rg = Scatter(pc, pg, scratch[n + 2 : n + 2 + m])
    rd = Scatter(pc, pd, scratch[n + 2 + m :])
    rg.start()
    moves = []
    u = g0.shape[3]
    for i, g in enumerate((g0, g1, g2)):
        for e in range(1, pc.F):
            cp = remote(
                g.at[pc.fahead(e)],
                xg.at[e - 1, :, :, pl.ds(i * u, u)],
                gxs.at[i, e],
                gxr.at[i, e],
                {"fsdp": pc.fahead(e)},
            )
            cp.start()
            moves.append(cp)
    rd.start()
    back, dg, db = norm_pull(mid[...], gain[...], rg.finish())
    dgain[...] = dg
    dbias[...] = db
    grad_middle = go[...].astype(F32) + back
    gm[...] = grad_middle
    x[...] = grad_middle.astype(BF)
    gather_stage(pc, x, gb, lsem.at[0], gs)
    y[...] = (mid[...] + rd.finish()).astype(BF)
    share_stage(pc, y, out, lsem.at[1], ss)
    for cp in moves:
        cp.wait()


class GradScatter:
    def __init__(self, pc, grads, out, own, xbuf, zsnd, ls, os, xs, xr, zs, zr):
        self.pc, self.grads, self.out = pc, grads, out
        self.own, self.xbuf, self.zsnd = own, xbuf, zsnd
        self.sems = (ls, os, xs, xr, zs, zr)
        C = pc.C
        self.H = os.shape[0]
        self.rows = own.shape[1] // self.H
        far = sorted(range(1, C), key=lambda d: abs(d - C // 2))
        self.order = [(d, h) for d in far + [0] for h in range(self.H)]

    def start(self):
        pc = self.pc
        ls, os, xs, xr, zs, zr = self.sems
        self.loc, self.xc, self.zc, self.keep, self.sent = {}, {}, {}, {}, []
        for d, h in self.order:
            c = pc.ahead(d)
            part = pl.ds(h * self.rows, self.rows)
            at = 0
            for g in self.grads:
                n = g.shape[3]
                for e in range(1, pc.F):
                    remote(
                        g.at[pc.fahead(e), c, part],
                        self.xbuf.at[e - 1, d, part, pl.ds(at, n)],
                        xs.at[d, h, e],
                        xr.at[d, h, e],
                        {"fsdp": pc.fahead(e)},
                    ).start()
                pltpu.make_async_copy(
                    g.at[pc.f, c, part], self.own.at[d, part, pl.ds(at, n)], ls.at[d, h]
                ).start()
                at += n
            here = self.own.at[d, part]
            self.loc[d, h] = pltpu.make_async_copy(here, here, ls.at[d, h])
            for e in range(1, pc.F):
                there = self.xbuf.at[e - 1, d, part]
                self.xc[d, h, e] = remote(
                    there, there, xs.at[d, h, e], xr.at[d, h, e], {"fsdp": pc.fahead(e)}
                )
        self.todo = list(self.order)

    def step(self, count=1):
        pc = self.pc
        ls, os, xs, xr, zs, zr = self.sems
        for _ in range(count):
            if not self.todo:
                return
            d, h = self.todo.pop(0)
            part = pl.ds(h * self.rows, self.rows)
            self.loc[d, h].wait()
            total = self.own[d, part].astype(F32)
            for e in range(1, pc.F):
                self.xc[d, h, e].wait_recv()
                total = total + self.xbuf[e - 1, d, part].astype(F32)
            self.zsnd[d, part] = total.astype(BF)
            src, dst = self.zsnd.at[d, part], self.out.at[pc.z, part]
            if d:
                self.zc[d, h] = remote(src, dst, zs.at[d, h], zr.at[d, h], {"ctx": pc.ahead(d)})
                self.zc[d, h].start()
            else:
                self.keep[h] = pltpu.make_async_copy(src, dst, os.at[h])
                self.keep[h].start()

    def finish(self):
        for cp in self.keep.values():
            cp.wait()
        for cp in self.zc.values():
            cp.wait()
        for cp in self.xc.values():
            cp.wait_send()


def vector_stage(pc, v, vout, va, vb, vc, vd, vx, vz, ts, tr, vxs, vxr, vzs, vzr):
    F, C = pc.F, pc.C
    t0 = remote(v, vb, ts.at[0], tr.at[0], {"tp": pc.near})
    t0.start()
    t0.wait_recv()
    va[...] = v[...] + vb[...]
    t1 = remote(va, vc, ts.at[1], tr.at[1], {"tp": pc.far})
    t1.start()
    t1.wait_recv()
    vd[...] = va[...] + vc[...]
    vxc, vzc = {}, {}
    for e in range(1, F):
        vxc[e] = remote(
            vd.at[pc.fahead(e)], vx.at[e - 1], vxs.at[e], vxr.at[e], {"fsdp": pc.fahead(e)}
        )
        vxc[e].start()
    vs = vd[pc.f]
    for e in range(1, F):
        vxc[e].wait_recv()
        vs = vs + vx[e - 1]
    vz[0] = vs
    for d in range(1, C):
        vzc[d] = remote(
            vz.at[0, pc.ahead(d)], vz.at[1, d], vzs.at[d], vzr.at[d], {"ctx": pc.ahead(d)}
        )
        vzc[d].start()
    acc = vz[0, pc.z]
    for d in range(1, C):
        vzc[d].wait_recv()
        acc = acc + vz[1, d]
    vout[...] = acc
    for cp in [t0, t1] + list(vxc.values()) + list(vzc.values()):
        cp.wait_send()


def vector_scratch(F, C, R):
    full = pltpu.VMEM((F, C, 8, R), F32)
    return [
        full,
        full,
        full,
        full,
        full,
        pltpu.VMEM((F - 1, C, 8, R), F32),
        pltpu.VMEM((2, C, 8, R), F32),
        sem(2),
        sem(2),
        sem(F),
        sem(F),
        sem(C),
        sem(C),
    ]


def last_kernel(
    dims, p, g0, g1, gm, tok, gain, dg2, db2, gt, gout, vout, y, lsem, s0, s1, *scratch
):
    pc = Place(*dims)
    F, C, T = dims
    pc.barrier(True, True, True)
    gr = GradScatter(pc, (g0, g1), gout, *scratch[:9])
    v, rest = scratch[9], scratch[10:22]
    rs = Scatter(pc, p, scratch[22:])
    rs.start()
    gr.start()
    back, dg, db = norm_pull(tok[...].astype(F32), gain[...], rs.finish(gr.step))
    y[...] = (gm[...] + back).astype(BF)
    R = v.shape[3]
    for i in range(F * C):
        rows = [r[:, i * R : (i + 1) * R] for r in (dg, db)] + [
            r[:, i * R : (i + 1) * R] for r in (dg2, db2)
        ]
        v[i // C, i % C] = jnp.concatenate(rows + [jnp.zeros((4, R), F32)], axis=0)
    gr.step(len(gr.todo))
    share_stage(pc, y, gt, lsem, (s0, s1))
    vector_stage(pc, v, vout, *rest)
    gr.finish()


def assemble_kernel(halves, key, hv, z, a, m, q, k, v, g, o, fg, fu, fd):
    c = pl.program_id(0)
    first = lax.rem(c, halves) == 0
    for i, ref in enumerate((q, k)):
        x = a[0, :, i * key : (i + 1) * key].astype(F32)

        @pl.when(first)
        def _(ref=ref, x=x):
            ref[...] = x

        @pl.when(jnp.logical_not(first))
        def _(ref=ref, x=x):
            ref[...] += x

    v[...] = a[0, :, 2 * key : 2 * key + hv].astype(F32)
    g[...] = a[0, :, 2 * key + hv : 2 * key + 2 * hv].astype(F32)
    o[...] = a[0, :, 2 * key + 2 * hv :].astype(F32)
    u = fg.shape[1]
    for i, ref in enumerate((fg, fu, fd)):
        ref[...] = m[0, :, i * u : (i + 1) * u].astype(F32)


def params(cid):
    return pltpu.CompilerParams(collective_id=cid, has_side_effects=True)


def silu_parts(g):
    s = jax.nn.sigmoid(g)
    return g * s, s * (1.0 + g * (1.0 - s))


def shards(
    dims,
    tokens,
    log_decay,
    w_query,
    w_key,
    w_value,
    w_gate,
    w_out,
    norm1_gain,
    norm1_bias,
    w_ffgate,
    w_ffup,
    w_down,
    norm2_gain,
    norm2_bias,
    grad_out,
):
    F, C, T = dims
    S, B, W = tokens.shape
    L = S * B
    Q = L // T
    N = C * L
    R = w_query.shape[0]
    heads = log_decay.shape[2]
    halves = C // heads
    HV = HEAD_V // halves
    U = w_ffgate.shape[1] // C
    z = lax.axis_index("ctx")
    t = lax.axis_index("tp")
    scale = float(KEY) ** (-0.5)

    f = lax.axis_index("fsdp")

    def hop(x, axis, d):
        n = lax.axis_size(axis)
        return lax.ppermute(x, axis, [(i, (i + d) % n) for i in range(n)])

    def at(x, i, n):
        return lax.dynamic_index_in_dim(x, lax.rem(i, n), 0, False)

    def tied(x, after):
        return lax.optimization_barrier((x, after))[0]

    def part_of(w, i, n):
        return lax.dynamic_slice_in_dim(w, lax.rem(i, C) * n, n, 1)

    NI, NR = 2 * KEY + 2 * HV, 3 * U
    NO = NI + HV
    vec = jnp.stack([norm1_gain, norm1_bias, norm2_gain, norm2_bias]).astype(F32)
    vec = jnp.pad(vec, ((0, 4), (0, 0)))
    ld = jnp.pad(jnp.transpose(log_decay, (2, 0, 1)).reshape(heads, L), ((0, 8 - heads), (0, 0)))
    tok = tokens.reshape(T, Q, W)
    go = grad_out.reshape(T, Q, W)
    sds = jax.ShapeDtypeStruct
    owin, ovec, old, otok, ogo = pl.pallas_call(
        functools.partial(first_kernel, dims, ((halves, KEY), (halves, KEY), (1, HV), (1, HV), (1, HV))),
        out_shape=(
            sds((F, C, R, NO), BF),
            sds((F, C, 8, R), F32),
            sds((C, 8, L), F32),
            sds((C, T, Q, W), BF),
            sds((C, T, Q, W), BF),
        ),
        in_specs=[ANY] * 9,
        out_specs=[ANY] * 5,
        scratch_shapes=[
            sem(9),
            sem(5, C),
            sem(5, C),
            sem(2, C, F),
            sem(2, C, F),
            sem(2, C),
            sem(2, C),
            sem(2, C, 2),
            sem(2, C, 2),
        ],
        compiler_params=params(1),
        name="k_first",
    )(w_query, w_key, w_value, w_gate, w_out, vec, ld, tok, go)

    vecs = jnp.transpose(ovec[:, :, :4], (2, 0, 1, 3)).reshape(4, 1, W)
    gain1, bias1, gain2, bias2 = vecs[0], vecs[1], vecs[2], vecs[3]
    w_all = owin.reshape(W, NO)
    w_in, w_o = w_all[:, :NI], w_all[:, NI:]
    after = tied((w_ffgate, w_ffup, w_down), ovec)
    near = []
    for d in range(C):
        piece = jnp.concatenate([part_of(w, z + d, U) for w in after], axis=1)
        near.append(hop(piece, "ctx", d) if d else piece)
    near = jnp.stack(near)
    xs = otok.reshape(N, W).astype(F32)
    center = xs - jnp.mean(xs, axis=-1, keepdims=True)
    spread = jnp.mean(center * center, axis=-1, keepdims=True)
    normed = (center * lax.rsqrt(spread + EPSILON) * gain1 + bias1).astype(BF)
    proj = nn(normed, w_in).astype(BF)
    q = proj[:, :KEY].reshape(C, S, B, KEY)
    k = proj[:, KEY : 2 * KEY].reshape(C, S, B, KEY)
    v = proj[:, 2 * KEY : 2 * KEY + HV].reshape(C, S, B, HV)
    g = proj[:, 2 * KEY + HV :].reshape(C, S, B, HV).astype(F32)

    rates = lax.dynamic_index_in_dim(old, z // halves, 1, False).reshape(C, S, B)
    cum = jnp.cumsum(rates, axis=-1)
    total = cum[..., -1]
    positions = jnp.arange(B)
    causal = positions[:, None] >= positions[None, :]
    table = jnp.where(
        causal, jnp.exp(jnp.minimum(cum[..., :, None] - cum[..., None, :], 0.0)), 0.0
    )
    growth = jnp.exp(cum)[..., None]
    keeping = jnp.exp(total[..., None] - cum)[..., None]
    through = jnp.exp(total)[..., None, None]

    def ein(spec, a, b):
        return jnp.einsum(spec, a, b, preferred_element_type=F32)

    weights = (ein("cstd,csud->cstu", q, k) * scale * table).astype(BF)
    q_grown = (q.astype(F32) * growth).astype(BF)
    k_kept = (k.astype(F32) * keeping).astype(BF)
    fresh = ein("csud,csue->csde", k_kept, v)
    state = jnp.zeros_like(fresh[0])
    states = []
    for c in range(C):
        states.append(state.astype(BF))
        state = through[c] * state + fresh[c]
    states = jnp.stack(states)
    mixer = ein("cstu,csue->cste", weights, v) + ein("cstd,csde->cste", q_grown, states)

    def pair(stats):
        got = [stats]
        for j in range(1, halves):
            perm = []
            for c in range(C):
                base = c - c % halves
                perm.append((c, base + (c % halves + j) % halves))
            got.append(lax.ppermute(stats, "ctx", perm))
        return got

    mean_here = jnp.mean(mixer, axis=-1)
    dev = mixer - mean_here[..., None]
    m2_here = jnp.sum(dev * dev, axis=-1)
    got = pair(jnp.stack([mean_here, m2_here]))
    mean = sum(x[0] for x in got) / halves
    m2 = sum(x[1] + HV * (x[0] - mean) ** 2 for x in got)
    inv = lax.rsqrt(m2 / HEAD_V + EPSILON)[..., None]
    normal = (mixer - mean[..., None]) * inv
    silu, dsilu = silu_parts(g)
    gated = (silu * normal).astype(BF).reshape(N, HV)

    part = nt(gated, w_o).astype(BF).reshape(C, T, Q, W)
    mytok = lax.dynamic_index_in_dim(tok, t, 0, False)
    mygo = lax.dynamic_index_in_dim(go, t, 0, False)
    mid, sn, full = pl.pallas_call(
        functools.partial(out_kernel, dims),
        out_shape=(sds((Q, W), F32), sds((C, T, Q, W), BF), sds((F, C, R, NR), BF)),
        in_specs=[ANY, VMEM, VMEM, VMEM, ANY],
        out_specs=[VMEM, ANY, ANY],
        scratch_shapes=[
            pltpu.VMEM((Q, W), BF),
            pltpu.SemaphoreType.DMA,
            sem(C, F),
            sem(C, F),
            sem(C),
        ]
        + gather_sems(C)
        + scatter_scratch(C, Q, W),
        compiler_params=params(2),
        name="k_out",
    )(part, mytok, gain2, bias2, near)
    w_rest = full.reshape(W, NR)
    w_fg, w_fu, w_d = w_rest[:, :U], w_rest[:, U : 2 * U], w_rest[:, 2 * U :]

    second = sn.reshape(N, W)
    ff_gate = nn(second, w_fg).astype(BF)
    ff_up = nn(second, w_fu).astype(BF)
    hidden, gelu_pull = jax.vjp(
        lambda a, b: jax.nn.gelu(a, approximate=True) * b, ff_gate.astype(F32), ff_up.astype(F32)
    )
    hidden = hidden.astype(BF)
    down = nt(hidden, w_d).astype(BF).reshape(C, T, Q, W)
    gout = ogo.reshape(N, W)
    grad_hidden = nn(gout, w_d)
    gfg, gfu = gelu_pull(grad_hidden)
    gfg, gfu = gfg.astype(BF), gfu.astype(BF)
    gsecond = (nt(gfg, w_fg) + nt(gfu, w_fu)).astype(BF).reshape(C, T, Q, W)
    mlp_parts = [
        tn(a, b).astype(BF).reshape(F, C, R, U)
        for a, b in ((second, gfg), (second, gfu), (gout, hidden))
    ]
    gm, gb, out, dgain2, dbias2, mlp_got = pl.pallas_call(
        functools.partial(mlp_kernel, dims),
        out_shape=(
            sds((Q, W), F32),
            sds((C, T, Q, W), BF),
            sds((T, Q, W), BF),
            sds((1, W), F32),
            sds((1, W), F32),
            sds((F - 1, C, R, NR), BF),
        ),
        in_specs=[ANY, ANY, VMEM, VMEM, VMEM, ANY, ANY, ANY],
        out_specs=[VMEM, ANY, ANY, VMEM, VMEM, ANY],
        scratch_shapes=[pltpu.VMEM((Q, W), BF), pltpu.VMEM((Q, W), BF), sem(2), sem(3, F), sem(3, F)]
        + gather_sems(C)
        + share_sems()
        + scatter_scratch(C, Q, W)
        + scatter_scratch(C, Q, W),
        compiler_params=params(3),
        name="k_mlp",
    )(gsecond, down, mid, mygo, gain2, *mlp_parts)
    output = out.reshape(tokens.shape)

    branch = gb.reshape(N, W)
    mlp_sum = jnp.concatenate([at(x, f, F) for x in mlp_parts], axis=2).astype(F32)
    for e in range(F - 1):
        mlp_sum = mlp_sum + mlp_got[e].astype(F32)
    mlp_sum = mlp_sum.astype(BF)
    mlp_grads = [at(mlp_sum, z, C)]
    mlp_grads += [hop(at(mlp_sum, z + d, C), "ctx", d) for d in range(1, C)]
    mlp_grads = jnp.stack(mlp_grads)
    ggated = nn(branch, w_o).reshape(C, S, B, HV)
    ggate = (ggated * normal * dsilu).astype(BF)
    gn = ggated * silu
    sums = pair(jnp.stack([jnp.sum(gn, axis=-1), jnp.sum(gn * normal, axis=-1)]))
    s1 = sum(x[0] for x in sums)[..., None] / HEAD_V
    s2 = sum(x[1] for x in sums)[..., None] / HEAD_V
    gmixer = (inv * (gn - s1 - normal * s2)).astype(BF)
    gscores = (ein("cste,csue->cstu", gmixer, v) * scale * table).astype(BF)
    pulled = ein("cstd,cste->csde", q_grown, gmixer)
    later = jnp.zeros_like(pulled[0])
    laters = [None] * C
    for c in reversed(range(C)):
        laters[c] = later.astype(BF)
        later = through[c] * later + pulled[c]
    laters = jnp.stack(laters)
    gq = ein("cstu,csud->cstd", gscores, k) + growth * ein("cste,csde->cstd", gmixer, states)
    gk = ein("cstu,cstd->csud", gscores, q) + keeping * ein("csue,csde->csud", v, laters)
    gv = ein("cstu,cste->csue", weights, gmixer) + ein("csud,csde->csue", k_kept, laters)
    gproj = jnp.concatenate([gq.astype(BF), gk.astype(BF), gv.astype(BF), ggate], axis=-1)
    gproj = gproj.reshape(N, NI)

    gnormed = nt(gproj, w_in).astype(BF).reshape(C, T, Q, W)
    in_parts = tn(normed, gproj).astype(BF).reshape(F, C, R, NI)
    out_parts = tn(branch, gated).astype(BF).reshape(F, C, R, HV)
    H = 2
    gt, gsum, vsum = pl.pallas_call(
        functools.partial(last_kernel, dims),
        out_shape=(sds((T, Q, W), BF), sds((C, R, NO), BF), sds((8, R), F32)),
        in_specs=[ANY, ANY, ANY, VMEM, VMEM, VMEM, VMEM, VMEM],
        out_specs=[ANY, ANY, VMEM],
        scratch_shapes=[pltpu.VMEM((Q, W), BF), pltpu.SemaphoreType.DMA]
        + share_sems()
        + [
            pltpu.VMEM((C, R, NO), BF),
            pltpu.VMEM((F - 1, C, R, NO), BF),
            pltpu.VMEM((C, R, NO), BF),
            sem(C, H),
            sem(H),
            sem(C, H, F),
            sem(C, H, F),
            sem(C, H),
            sem(C, H),
        ]
        + vector_scratch(F, C, R)
        + scatter_scratch(C, Q, W),
        compiler_params=params(4),
        name="k_last",
    )(gnormed, in_parts, out_parts, gm, mytok, gain1, dgain2, dbias2)
    grad_tokens = gt.reshape(tokens.shape)

    def rel(n):
        return pl.BlockSpec((1, R, n), lambda c, z: (lax.rem(z[0] + C - c, C), 0, 0))

    def quarter(n):
        return pl.BlockSpec((R, n), lambda c, z: (0, c))

    per_head = pl.BlockSpec((R, KEY), lambda c, z: (0, c // halves))
    gq, gk, gv, gg, gw, gfg, gfu, gfd = pl.pallas_call(
        functools.partial(assemble_kernel, halves, KEY, HV),
        out_shape=[sds((R, heads * KEY), F32)] * 2
        + [sds((R, C * HV), F32)] * 3
        + [sds((R, C * U), F32)] * 3,
        grid_spec=pltpu.PrefetchScalarGridSpec(
            num_scalar_prefetch=1,
            grid=(C,),
            in_specs=[
                pl.BlockSpec((1, R, NO), lambda c, z: (c, 0, 0)),
                rel(3 * U),
            ],
            out_specs=[per_head, per_head] + [quarter(HV)] * 3 + [quarter(U)] * 3,
        ),
        name="k_assemble",
    )(jnp.full((1,), z, jnp.int32), gsum, mlp_grads)
    return (
        output,
        grad_tokens,
        gq,
        gk,
        gv,
        gg,
        gw,
        vsum[0],
        vsum[1],
        gfg,
        gfu,
        gfd,
        vsum[2],
        vsum[3],
    )


def solution(mesh):
    dims = (mesh.shape["fsdp"], mesh.shape["ctx"], mesh.shape["tp"])
    rows, vec = P(("fsdp", "ctx"), "tp"), P(("fsdp", "ctx"))
    acts = P("fsdp", "ctx", None)
    return jax.shard_map(
        functools.partial(shards, dims),
        mesh=mesh,
        in_specs=(acts, P("fsdp", "ctx", "tp"), rows, rows, rows, rows, rows, vec, vec, rows, rows, rows, vec, vec, acts),
        out_specs=(acts, acts, rows, rows, rows, rows, rows, vec, vec, rows, rows, rows, vec, vec),
        check_vma=False,
    )
```

```python
import functools

import jax
import jax.numpy as jnp
from jax import lax
from jax.experimental import pallas as pl
from jax.experimental.pallas import tpu as pltpu
from jax.sharding import PartitionSpec as P

KEY = 256
HEAD_V = 512
EPSILON = 1e-05
MESH = pl.DeviceIdType.MESH
ANY = pl.BlockSpec(memory_space=pl.ANY)
VMEM = pl.BlockSpec(memory_space=pltpu.VMEM)
BF = jnp.bfloat16
F32 = jnp.float32


def dot(a, b, dims):
    return lax.dot_general(a, b, (dims, ((), ())), preferred_element_type=F32)


def nn(a, b):
    return dot(a, b, ((1,), (0,)))


def nt(a, b):
    return dot(a, b, ((1,), (1,)))


def tn(a, b):
    return dot(a, b, ((0,), (0,)))


class Place:
    def __init__(self, F, C, T):
        self.F, self.C, self.T = F, C, T
        self.f = lax.axis_index("fsdp")
        self.z = lax.axis_index("ctx")
        self.t = lax.axis_index("tp")
        self.lo = lax.rem(self.t, 2)
        self.hi = self.t // 2
        self.near = self.t + 1 - 2 * self.lo
        self.far = lax.rem(self.t + 2, 4)

    def ahead(self, d):
        return lax.rem(self.z + d, self.C)

    def behind(self, d):
        return lax.rem(self.z + self.C - d, self.C)

    def fahead(self, d):
        return lax.rem(self.f + d, self.F)

    def fbehind(self, d):
        return lax.rem(self.f + self.F - d, self.F)

    def barrier(self, ctx=True, fsdp=False, tp=True):
        sem = pltpu.get_barrier_semaphore()
        peers = []
        if tp:
            peers += [{"tp": self.near}, {"tp": self.far}]
        if fsdp:
            peers += [{"fsdp": self.fahead(d)} for d in range(1, self.F)]
        if ctx:
            peers += [{"ctx": self.ahead(d)} for d in range(1, self.C)]
        for peer in peers:
            pl.semaphore_signal(sem, inc=1, device_id=peer, device_id_type=MESH)
        pl.semaphore_wait(sem, len(peers))


def remote(src, dst, ssem, rsem, peer):
    return pltpu.make_async_remote_copy(
        src_ref=src, dst_ref=dst, send_sem=ssem, recv_sem=rsem, device_id=peer, device_id_type=MESH
    )


def sem(*shape):
    return pltpu.SemaphoreType.DMA(shape)


def gather_sems(C):
    return [sem(C), sem(C), sem(C), sem(C), sem(C, 2), sem(C, 2), pltpu.SemaphoreType.DMA]


class Gather:
    def __init__(self, pc, x, out, rows, sems):
        self.pc, self.x = pc, x
        self.zs, self.zr, self.ys, self.yr, self.cs, self.cr, self.ls = sems
        self.slot = lambda c, t: out.at[c, t, rows]

    def start(self):
        pc, x = self.pc, self.x
        self.here = self.slot(pc.z, pc.t)
        self.local = pltpu.make_async_copy(x, self.here, self.ls)
        self.local.start()
        self.zc, self.yc, self.cc = {}, {}, {}
        for d in range(1, pc.C):
            self.zc[d] = remote(
                x, self.here, self.zs.at[d], self.zr.at[d], {"ctx": pc.ahead(d)}
            )
            self.zc[d].start()
        self.forward(0)

    def forward(self, d):
        pc = self.pc
        dst = self.slot(pc.behind(d), pc.t)
        src = dst if d else self.x
        if d:
            self.zc[d].wait_recv()
        self.yc[d] = remote(src, dst, self.ys.at[d], self.yr.at[d], {"tp": pc.far})
        self.yc[d].start()
        self.cc[d, 0] = remote(src, dst, self.cs.at[d, 0], self.cr.at[d, 0], {"tp": pc.near})
        self.cc[d, 0].start()

    def onward(self, d):
        pc = self.pc
        self.yc[d].wait_recv()
        src = self.slot(pc.behind(d), pc.far)
        self.cc[d, 1] = remote(src, src, self.cs.at[d, 1], self.cr.at[d, 1], {"tp": pc.near})
        self.cc[d, 1].start()

    def finish(self):
        self.local.wait()
        for cp in self.zc.values():
            cp.wait_send()
        for cp in self.yc.values():
            cp.wait_send()
        for cp in self.cc.values():
            cp.wait()


def share_sems():
    return [sem(3), sem(3)]


def share_stage(pc, x, out, lsem, sems):
    ss, rs = sems
    t = pc.t
    local = pltpu.make_async_copy(x, out.at[t], lsem)
    local.start()
    a = remote(x, out.at[t], ss.at[0], rs.at[0], {"tp": pc.far})
    a.start()
    b = remote(x, out.at[t], ss.at[1], rs.at[1], {"tp": pc.near})
    b.start()
    a.wait_recv()
    src = out.at[pc.far]
    c = remote(src, src, ss.at[2], rs.at[2], {"tp": pc.near})
    c.start()
    local.wait()
    a.wait_send()
    b.wait()
    c.wait()


def scatter_scratch(C, Q, W):
    return [
        pltpu.VMEM((C, 2, Q, W), BF),
        pltpu.VMEM((C, 2, Q, W), BF),
        pltpu.VMEM((C, Q, W), BF),
        pltpu.VMEM((C, Q, W), BF),
        pltpu.VMEM((C, Q, W), BF),
        pltpu.VMEM((C, Q, W), BF),
        sem(C, 2),
        sem(C, 2),
        sem(C, 2),
        sem(C),
        sem(C),
        sem(C),
        sem(C),
    ]


class Scatter:
    def __init__(self, pc, p, rows, scratch):
        self.pc, self.p, self.rows = pc, p, rows
        (self.loc, self.buf1, self.snd2, self.buf2, self.snd3, self.buf3) = scratch[:6]
        self.ls, self.s1, self.r1, self.s2, self.r2, self.s3, self.r3 = scratch[6:]
        self.order = list(range(1, pc.C)) + [0]

    def start(self):
        pc, p, rows = self.pc, self.p, self.rows
        self.lc, self.c1, self.c2, self.c3 = {}, {}, {}, {}
        for j in range(2):
            for d in self.order:
                c = pc.ahead(d)
                hi = 1 - pc.hi if j == 0 else pc.hi
                cp = remote(
                    p.at[c, hi * 2 + 1 - pc.lo, rows],
                    self.buf1.at[d, j],
                    self.s1.at[d, j],
                    self.r1.at[d, j],
                    {"tp": pc.near},
                )
                cp.start()
                self.c1[d, j] = cp
                lc = pltpu.make_async_copy(
                    p.at[c, hi * 2 + pc.lo, rows], self.loc.at[d, j], self.ls.at[d, j]
                )
                lc.start()
                self.lc[d, j] = lc

    def far(self):
        for d in self.order:
            self.lc[d, 0].wait()
            self.c1[d, 0].wait_recv()
            self.snd2[d] = (self.loc[d, 0].astype(F32) + self.buf1[d, 0].astype(F32)).astype(BF)
            self.c2[d] = remote(
                self.snd2.at[d],
                self.buf2.at[d],
                self.s2.at[d],
                self.r2.at[d],
                {"tp": self.pc.far},
            )
            self.c2[d].start()

    def along(self, d):
        self.lc[d, 1].wait()
        self.c1[d, 1].wait_recv()
        self.c2[d].wait_recv()
        part = (
            self.loc[d, 1].astype(F32) + self.buf1[d, 1].astype(F32) + self.buf2[d].astype(F32)
        )
        if d:
            self.snd3[d] = part.astype(BF)
            self.c3[d] = remote(
                self.snd3.at[d],
                self.buf3.at[d],
                self.s3.at[d],
                self.r3.at[d],
                {"ctx": self.pc.ahead(d)},
            )
            self.c3[d].start()
        else:
            self.total = part

    def result(self):
        total = self.total
        for d in range(1, self.pc.C):
            self.c3[d].wait_recv()
            total = total + self.buf3[d].astype(F32)
        return total

    def finish(self):
        for copies in (self.c1, self.c2, self.c3):
            for cp in copies.values():
                cp.wait_send()


def first_kernel(
    dims, layout, wq, wk, wv, wg, wo, vec, ld, tok, go, owin, ovec, old, otok, ogo, ls, zs, zr, xs, xr, ys, yr, cs, cr
):
    pc = Place(*dims)
    F, C, T = dims
    f, z, t = pc.f, pc.z, pc.t
    pc.barrier(True, True, True)
    weights = (wq, wk, wv, wg, wo)
    pieces = [None, vec, ld]
    outs = [owin, ovec, old]

    def slot(i, ff, c):
        return outs[i].at[ff, c] if i < 2 else outs[i].at[c]

    def columns(dst):
        at = 0
        for w, (share, n) in zip(weights, layout):
            start = pl.multiple_of((dst // share) * n, n)
            yield w.at[:, pl.ds(start, n)], owin.at[f, z, :, pl.ds(at, n)]
            at += n

    acts, oacts = [tok, go], [otok, ogo]
    zc, xc, yc, cc = {}, {}, {}, {}

    def send_piece(i):
        for d in range(1, C):
            dst = pc.ahead(d)
            sems = (zs.at[i, d], zr.at[i, d])
            if i:
                zc[i, d] = remote(pieces[i], slot(i, f, z), *sems, {"ctx": dst})
                zc[i, d].start()
            else:
                for src, to in columns(dst):
                    remote(src, to, *sems, {"ctx": dst}).start()
                c = pc.behind(d)
                zc[i, d] = remote(slot(i, f, c), slot(i, f, c), *sems, {"ctx": dst})

    def send_act(i):
        for d in range(1, C):
            k = 3 + i
            zc[k, d] = remote(
                acts[i].at[t], oacts[i].at[z, t], zs.at[k, d], zr.at[k, d], {"ctx": pc.ahead(d)}
            )
            zc[k, d].start()

    def across(i, d):
        c = pc.behind(d)
        for e in range(1, F):
            sems = (xs.at[i, d, e], xr.at[i, d, e])
            peer = {"fsdp": pc.fahead(e)}
            if i == 0 and d == 0:
                for src, to in columns(z):
                    remote(src, to, *sems, peer).start()
                here = slot(0, pc.fbehind(e), z)
                xc[i, d, e] = remote(here, here, *sems, peer)
            else:
                src = pieces[i] if d == 0 else slot(i, f, c)
                xc[i, d, e] = remote(src, slot(i, f, c), *sems, peer)
                xc[i, d, e].start()

    def spread(i, d):
        c = pc.behind(d)
        src = oacts[i].at[c, t]
        yc[i, d] = remote(src, src, ys.at[i, d], yr.at[i, d], {"tp": pc.far})
        yc[i, d].start()
        cc[i, d, 0] = remote(src, src, cs.at[i, d, 0], cr.at[i, d, 0], {"tp": pc.near})
        cc[i, d, 0].start()

    def spread_on(i, d):
        c = pc.behind(d)
        yc[i, d].wait_recv()
        src = oacts[i].at[c, pc.far]
        cc[i, d, 1] = remote(src, src, cs.at[i, d, 1], cr.at[i, d, 1], {"tp": pc.near})
        cc[i, d, 1].start()

    for i in (1, 2):
        send_piece(i)
    send_act(0)
    send_piece(0)
    for i in (1, 0):
        across(i, 0)
    send_act(1)
    local = [
        pltpu.make_async_copy(src, to, ls.at[i]) for i, (src, to) in enumerate(columns(z))
    ]
    for i in (1, 2):
        local.append(pltpu.make_async_copy(pieces[i], slot(i, f, z), ls.at[4 + i]))
    for i in range(2):
        local.append(pltpu.make_async_copy(acts[i], oacts[i].at[z], ls.at[7 + i]))
    for cp in local:
        cp.start()
    for d in range(1, C):
        zc[1, d].wait_recv()
        across(1, d)
        zc[3, d].wait_recv()
        spread(0, d)
    for d in range(1, C):
        spread_on(0, d)
    for d in range(1, C):
        zc[0, d].wait_recv()
        across(0, d)
    for d in range(1, C):
        zc[4, d].wait_recv()
        spread(1, d)
    for d in range(1, C):
        spread_on(1, d)
        zc[2, d].wait_recv()
    for cp in local:
        cp.wait()
    for cp in zc.values():
        cp.wait_send()
    for cp in xc.values():
        cp.wait()
    for cp in yc.values():
        cp.wait_send()
    for cp in cc.values():
        cp.wait()


PARTS = 2


def halves_of(rows):
    n = rows // PARTS
    return (lambda h: pl.ds(h * n, n)), PARTS


def out_kernel(
    dims, p, tok, gain, bias, near, mid, sn, full, x, ws, wr, wl, *scratch
):
    pc = Place(*dims)
    F, C, T = dims
    pc.barrier(True, True, True)
    n, m = len(gather_sems(C)), len(scatter_scratch(C, 8, 128))
    cut, parts = halves_of(x.shape[0])
    scatters, gathers = [], []
    for h in range(parts):
        at = h * (n + m)
        gathers.append(Gather(pc, x.at[cut(h)], sn, cut(h), scratch[at : at + n]))
        scatters.append(Scatter(pc, p, cut(h), scratch[at + n : at + n + m]))
    for rs in scatters:
        rs.start()
    moves = []
    for d in range(C):
        dst = full.at[pc.f, pc.behind(d)]
        for e in range(1, F):
            cp = remote(near.at[d], dst, ws.at[d, e], wr.at[d, e], {"fsdp": pc.fahead(e)})
            cp.start()
            moves.append(cp)
        cp = pltpu.make_async_copy(near.at[d], dst, wl.at[d])
        cp.start()
        moves.append(cp)
    for rs in scatters:
        rs.far()
    for h, rs in enumerate(scatters):
        for d in rs.order:
            rs.along(d)
        part = cut(h)
        total = rs.result() + tok[part].astype(F32)
        mid[part] = total
        center = total - jnp.mean(total, axis=-1, keepdims=True)
        spread = jnp.mean(center * center, axis=-1, keepdims=True)
        x[part] = (center * lax.rsqrt(spread + EPSILON) * gain[...] + bias[...]).astype(BF)
        gathers[h].start()
    for ga in gathers:
        for d in range(1, C):
            ga.forward(d)
    for ga in gathers:
        for d in range(C):
            ga.onward(d)
    for job in scatters + gathers:
        job.finish()
    for cp in moves:
        cp.wait()


def norm_pull(values, gain, grad):
    center = values - jnp.mean(values, axis=-1, keepdims=True)
    spread = jnp.mean(center * center, axis=-1, keepdims=True)
    inv = lax.rsqrt(spread + EPSILON)
    xhat = center * inv
    g = grad * gain
    back = inv * (
        g - jnp.mean(g, axis=-1, keepdims=True) - xhat * jnp.mean(g * xhat, axis=-1, keepdims=True)
    )
    return (
        back,
        jnp.sum(grad * xhat, axis=0, keepdims=True),
        jnp.sum(grad, axis=0, keepdims=True),
    )


def mlp_kernel(
    dims, pg, pd, mid, go, gain, g0, g1, g2, gm, gb, out, dgain, dbias, xg, x, y, lsem, gxs, gxr, *scratch
):
    pc = Place(*dims)
    C = pc.C
    pc.barrier(True, True, True)
    n, m = len(gather_sems(C)), len(scatter_scratch(C, 8, 128))
    ss, scratch = scratch[:2], scratch[2:]
    rd = Scatter(pc, pd, pl.ds(0, x.shape[0]), scratch[:m])
    scratch = scratch[m:]
    cut, parts = halves_of(x.shape[0])
    scatters, gathers = [], []
    for h in range(parts):
        at = h * (n + m)
        gathers.append(Gather(pc, x.at[cut(h)], gb, cut(h), scratch[at : at + n]))
        scatters.append(Scatter(pc, pg, cut(h), scratch[at + n : at + n + m]))
    for rs in scatters:
        rs.start()
    rd.start()
    moves = []
    u = g0.shape[3]
    for i, g in enumerate((g0, g1, g2)):
        for e in range(1, pc.F):
            cp = remote(
                g.at[pc.fahead(e)],
                xg.at[e - 1, :, :, pl.ds(i * u, u)],
                gxs.at[i, e],
                gxr.at[i, e],
                {"fsdp": pc.fahead(e)},
            )
            cp.start()
            moves.append(cp)
    for rs in scatters:
        rs.far()
    rd.far()
    for h, rs in enumerate(scatters):
        for d in rs.order:
            rs.along(d)
        part = cut(h)
        back, dg, db = norm_pull(mid[part], gain[...], rs.result())
        dgain[...] = dgain[...] + dg if h else dg
        dbias[...] = dbias[...] + db if h else db
        grad_middle = go[part].astype(F32) + back
        gm[part] = grad_middle
        x[part] = grad_middle.astype(BF)
        gathers[h].start()
    for d in rd.order[:2]:
        rd.along(d)
    for d in range(1, C):
        gathers[0].forward(d)
    for d in rd.order[2:]:
        rd.along(d)
    for ga in gathers[1:]:
        for d in range(1, C):
            ga.forward(d)
    for d in range(C):
        for ga in gathers:
            ga.onward(d)
    y[...] = (mid[...] + rd.result()).astype(BF)
    share_stage(pc, y, out, lsem, ss)
    for job in scatters + gathers + [rd]:
        job.finish()
    for cp in moves:
        cp.wait()


class GradScatter:
    def __init__(self, pc, grads, out, own, xbuf, zsnd, ls, os, xs, xr, zs, zr):
        self.pc, self.grads, self.out = pc, grads, out
        self.own, self.xbuf, self.zsnd = own, xbuf, zsnd
        self.sems = (ls, os, xs, xr, zs, zr)
        C = pc.C
        self.H = os.shape[0]
        self.rows = own.shape[1] // self.H
        far = sorted(range(1, C), key=lambda d: abs(d - C // 2))
        self.order = [(d, h) for d in far + [0] for h in range(self.H)]

    def start(self):
        pc = self.pc
        ls, os, xs, xr, zs, zr = self.sems
        self.loc, self.xc, self.zc, self.keep, self.sent = {}, {}, {}, {}, []
        for d, h in self.order:
            c = pc.ahead(d)
            part = pl.ds(h * self.rows, self.rows)
            at = 0
            for g in self.grads:
                n = g.shape[3]
                for e in range(1, pc.F):
                    remote(
                        g.at[pc.fahead(e), c, part],
                        self.xbuf.at[e - 1, d, part, pl.ds(at, n)],
                        xs.at[d, h, e],
                        xr.at[d, h, e],
                        {"fsdp": pc.fahead(e)},
                    ).start()
                pltpu.make_async_copy(
                    g.at[pc.f, c, part], self.own.at[d, part, pl.ds(at, n)], ls.at[d, h]
                ).start()
                at += n
            here = self.own.at[d, part]
            self.loc[d, h] = pltpu.make_async_copy(here, here, ls.at[d, h])
            for e in range(1, pc.F):
                there = self.xbuf.at[e - 1, d, part]
                self.xc[d, h, e] = remote(
                    there, there, xs.at[d, h, e], xr.at[d, h, e], {"fsdp": pc.fahead(e)}
                )
        self.todo = list(self.order)

    def step(self, count=1):
        pc = self.pc
        ls, os, xs, xr, zs, zr = self.sems
        for _ in range(count):
            if not self.todo:
                return
            d, h = self.todo.pop(0)
            part = pl.ds(h * self.rows, self.rows)
            self.loc[d, h].wait()
            total = self.own[d, part].astype(F32)
            for e in range(1, pc.F):
                self.xc[d, h, e].wait_recv()
                total = total + self.xbuf[e - 1, d, part].astype(F32)
            self.zsnd[d, part] = total.astype(BF)
            src, dst = self.zsnd.at[d, part], self.out.at[pc.z, part]
            if d:
                self.zc[d, h] = remote(src, dst, zs.at[d, h], zr.at[d, h], {"ctx": pc.ahead(d)})
                self.zc[d, h].start()
            else:
                self.keep[h] = pltpu.make_async_copy(src, dst, os.at[h])
                self.keep[h].start()

    def finish(self):
        for cp in self.keep.values():
            cp.wait()
        for cp in self.zc.values():
            cp.wait()
        for cp in self.xc.values():
            cp.wait_send()


def vector_stage(pc, v, vout, va, vb, vc, vd, vx, vz, ts, tr, vxs, vxr, vzs, vzr):
    F, C = pc.F, pc.C
    t0 = remote(v, vb, ts.at[0], tr.at[0], {"tp": pc.near})
    t0.start()
    t0.wait_recv()
    va[...] = v[...] + vb[...]
    t1 = remote(va, vc, ts.at[1], tr.at[1], {"tp": pc.far})
    t1.start()
    t1.wait_recv()
    vd[...] = va[...] + vc[...]
    vxc, vzc = {}, {}
    for e in range(1, F):
        vxc[e] = remote(
            vd.at[pc.fahead(e)], vx.at[e - 1], vxs.at[e], vxr.at[e], {"fsdp": pc.fahead(e)}
        )
        vxc[e].start()
    vs = vd[pc.f]
    for e in range(1, F):
        vxc[e].wait_recv()
        vs = vs + vx[e - 1]
    vz[0] = vs
    for d in range(1, C):
        vzc[d] = remote(
            vz.at[0, pc.ahead(d)], vz.at[1, d], vzs.at[d], vzr.at[d], {"ctx": pc.ahead(d)}
        )
        vzc[d].start()
    acc = vz[0, pc.z]
    for d in range(1, C):
        vzc[d].wait_recv()
        acc = acc + vz[1, d]
    vout[...] = acc
    for cp in [t0, t1] + list(vxc.values()) + list(vzc.values()):
        cp.wait_send()


def vector_scratch(F, C, R):
    full = pltpu.VMEM((F, C, 8, R), F32)
    return [
        full,
        full,
        full,
        full,
        full,
        pltpu.VMEM((F - 1, C, 8, R), F32),
        pltpu.VMEM((2, C, 8, R), F32),
        sem(2),
        sem(2),
        sem(F),
        sem(F),
        sem(C),
        sem(C),
    ]


def last_kernel(
    dims, p, g0, g1, gm, tok, gain, dg2, db2, gt, gout, vout, y, lsem, s0, s1, *scratch
):
    pc = Place(*dims)
    F, C, T = dims
    pc.barrier(True, True, True)
    gr = GradScatter(pc, (g0, g1), gout, *scratch[:9])
    v, rest = scratch[9], scratch[10:22]
    rs = Scatter(pc, p, pl.ds(0, y.shape[0]), scratch[22:])
    rs.start()
    gr.start()
    rs.far()
    for d in rs.order:
        rs.along(d)
        gr.step()
    back, dg, db = norm_pull(tok[...].astype(F32), gain[...], rs.result())
    y[...] = (gm[...] + back).astype(BF)
    R = v.shape[3]
    for i in range(F * C):
        rows = [r[:, i * R : (i + 1) * R] for r in (dg, db)] + [
            r[:, i * R : (i + 1) * R] for r in (dg2, db2)
        ]
        v[i // C, i % C] = jnp.concatenate(rows + [jnp.zeros((4, R), F32)], axis=0)
    gr.step(len(gr.todo))
    share_stage(pc, y, gt, lsem, (s0, s1))
    vector_stage(pc, v, vout, *rest)
    gr.finish()
    rs.finish()


def assemble_kernel(halves, key, hv, z, a, m, q, k, v, g, o, fg, fu, fd):
    c = pl.program_id(0)
    first = lax.rem(c, halves) == 0
    for i, ref in enumerate((q, k)):
        x = a[0, :, i * key : (i + 1) * key].astype(F32)

        @pl.when(first)
        def _(ref=ref, x=x):
            ref[...] = x

        @pl.when(jnp.logical_not(first))
        def _(ref=ref, x=x):
            ref[...] += x

    v[...] = a[0, :, 2 * key : 2 * key + hv].astype(F32)
    g[...] = a[0, :, 2 * key + hv : 2 * key + 2 * hv].astype(F32)
    o[...] = a[0, :, 2 * key + 2 * hv :].astype(F32)
    u = fg.shape[1]
    for i, ref in enumerate((fg, fu, fd)):
        ref[...] = m[0, :, i * u : (i + 1) * u].astype(F32)


def params(cid):
    return pltpu.CompilerParams(collective_id=cid, has_side_effects=True)


def silu_parts(g):
    s = jax.nn.sigmoid(g)
    return g * s, s * (1.0 + g * (1.0 - s))


def shards(
    dims,
    tokens,
    log_decay,
    w_query,
    w_key,
    w_value,
    w_gate,
    w_out,
    norm1_gain,
    norm1_bias,
    w_ffgate,
    w_ffup,
    w_down,
    norm2_gain,
    norm2_bias,
    grad_out,
):
    F, C, T = dims
    S, B, W = tokens.shape
    L = S * B
    Q = L // T
    N = C * L
    R = w_query.shape[0]
    heads = log_decay.shape[2]
    halves = C // heads
    HV = HEAD_V // halves
    U = w_ffgate.shape[1] // C
    z = lax.axis_index("ctx")
    t = lax.axis_index("tp")
    scale = float(KEY) ** (-0.5)

    f = lax.axis_index("fsdp")

    def hop(x, axis, d):
        n = lax.axis_size(axis)
        return lax.ppermute(x, axis, [(i, (i + d) % n) for i in range(n)])

    def at(x, i, n):
        return lax.dynamic_index_in_dim(x, lax.rem(i, n), 0, False)

    def tied(x, after):
        return lax.optimization_barrier((x, after))[0]

    def part_of(w, i, n):
        return lax.dynamic_slice_in_dim(w, lax.rem(i, C) * n, n, 1)

    NI, NR = 2 * KEY + 2 * HV, 3 * U
    NO = NI + HV
    vec = jnp.stack([norm1_gain, norm1_bias, norm2_gain, norm2_bias]).astype(F32)
    vec = jnp.pad(vec, ((0, 4), (0, 0)))
    ld = jnp.pad(jnp.transpose(log_decay, (2, 0, 1)).reshape(heads, L), ((0, 8 - heads), (0, 0)))
    tok = tokens.reshape(T, Q, W)
    go = grad_out.reshape(T, Q, W)
    sds = jax.ShapeDtypeStruct
    owin, ovec, old, otok, ogo = pl.pallas_call(
        functools.partial(first_kernel, dims, ((halves, KEY), (halves, KEY), (1, HV), (1, HV), (1, HV))),
        out_shape=(
            sds((F, C, R, NO), BF),
            sds((F, C, 8, R), F32),
            sds((C, 8, L), F32),
            sds((C, T, Q, W), BF),
            sds((C, T, Q, W), BF),
        ),
        in_specs=[ANY] * 9,
        out_specs=[ANY] * 5,
        scratch_shapes=[
            sem(9),
            sem(5, C),
            sem(5, C),
            sem(2, C, F),
            sem(2, C, F),
            sem(2, C),
            sem(2, C),
            sem(2, C, 2),
            sem(2, C, 2),
        ],
        compiler_params=params(1),
        name="k_first",
    )(w_query, w_key, w_value, w_gate, w_out, vec, ld, tok, go)

    vecs = jnp.transpose(ovec[:, :, :4], (2, 0, 1, 3)).reshape(4, 1, W)
    gain1, bias1, gain2, bias2 = vecs[0], vecs[1], vecs[2], vecs[3]
    w_all = owin.reshape(W, NO)
    w_in, w_o = w_all[:, :NI], w_all[:, NI:]
    after = tied((w_ffgate, w_ffup, w_down), ovec)
    near = []
    for d in range(C):
        piece = jnp.concatenate([part_of(w, z + d, U) for w in after], axis=1)
        near.append(hop(piece, "ctx", d) if d else piece)
    near = jnp.stack(near)
    xs = otok.reshape(N, W).astype(F32)
    center = xs - jnp.mean(xs, axis=-1, keepdims=True)
    spread = jnp.mean(center * center, axis=-1, keepdims=True)
    normed = (center * lax.rsqrt(spread + EPSILON) * gain1 + bias1).astype(BF)
    proj = nn(normed, w_in).astype(BF)
    q = proj[:, :KEY].reshape(C, S, B, KEY)
    k = proj[:, KEY : 2 * KEY].reshape(C, S, B, KEY)
    v = proj[:, 2 * KEY : 2 * KEY + HV].reshape(C, S, B, HV)
    g = proj[:, 2 * KEY + HV :].reshape(C, S, B, HV).astype(F32)

    rates = lax.dynamic_index_in_dim(old, z // halves, 1, False).reshape(C, S, B)
    cum = jnp.cumsum(rates, axis=-1)
    total = cum[..., -1]
    positions = jnp.arange(B)
    causal = positions[:, None] >= positions[None, :]
    table = jnp.where(
        causal, jnp.exp(jnp.minimum(cum[..., :, None] - cum[..., None, :], 0.0)), 0.0
    )
    growth = jnp.exp(cum)[..., None]
    keeping = jnp.exp(total[..., None] - cum)[..., None]
    through = jnp.exp(total)[..., None, None]

    def ein(spec, a, b):
        return jnp.einsum(spec, a, b, preferred_element_type=F32)

    weights = (ein("cstd,csud->cstu", q, k) * scale * table).astype(BF)
    q_grown = (q.astype(F32) * growth).astype(BF)
    k_kept = (k.astype(F32) * keeping).astype(BF)
    fresh = ein("csud,csue->csde", k_kept, v)
    state = jnp.zeros_like(fresh[0])
    states = []
    for c in range(C):
        states.append(state.astype(BF))
        state = through[c] * state + fresh[c]
    states = jnp.stack(states)
    mixer = ein("cstu,csue->cste", weights, v) + ein("cstd,csde->cste", q_grown, states)

    def pair(stats):
        got = [stats]
        for j in range(1, halves):
            perm = []
            for c in range(C):
                base = c - c % halves
                perm.append((c, base + (c % halves + j) % halves))
            got.append(lax.ppermute(stats, "ctx", perm))
        return got

    mean_here = jnp.mean(mixer, axis=-1)
    dev = mixer - mean_here[..., None]
    m2_here = jnp.sum(dev * dev, axis=-1)
    got = pair(jnp.stack([mean_here, m2_here]))
    mean = sum(x[0] for x in got) / halves
    m2 = sum(x[1] + HV * (x[0] - mean) ** 2 for x in got)
    inv = lax.rsqrt(m2 / HEAD_V + EPSILON)[..., None]
    normal = (mixer - mean[..., None]) * inv
    silu, dsilu = silu_parts(g)
    gated = (silu * normal).astype(BF).reshape(N, HV)

    part = nt(gated, w_o).astype(BF).reshape(C, T, Q, W)
    mytok = lax.dynamic_index_in_dim(tok, t, 0, False)
    mygo = lax.dynamic_index_in_dim(go, t, 0, False)
    mid, sn, full = pl.pallas_call(
        functools.partial(out_kernel, dims),
        out_shape=(sds((Q, W), F32), sds((C, T, Q, W), BF), sds((F, C, R, NR), BF)),
        in_specs=[ANY, VMEM, VMEM, VMEM, ANY],
        out_specs=[VMEM, ANY, ANY],
        scratch_shapes=[
            pltpu.VMEM((Q, W), BF),
            sem(C, F),
            sem(C, F),
            sem(C),
        ]
        + (gather_sems(C) + scatter_scratch(C, Q // PARTS, W)) * PARTS,
        compiler_params=params(2),
        name="k_out",
    )(part, mytok, gain2, bias2, near)
    w_rest = full.reshape(W, NR)
    w_fg, w_fu, w_d = w_rest[:, :U], w_rest[:, U : 2 * U], w_rest[:, 2 * U :]

    second = sn.reshape(N, W)
    ff_gate = nn(second, w_fg).astype(BF)
    ff_up = nn(second, w_fu).astype(BF)
    hidden, gelu_pull = jax.vjp(
        lambda a, b: jax.nn.gelu(a, approximate=True) * b, ff_gate.astype(F32), ff_up.astype(F32)
    )
    hidden = hidden.astype(BF)
    down = nt(hidden, w_d).astype(BF).reshape(C, T, Q, W)
    gout = ogo.reshape(N, W)
    grad_hidden = nn(gout, w_d)
    gfg, gfu = gelu_pull(grad_hidden)
    gfg, gfu = gfg.astype(BF), gfu.astype(BF)
    gsecond = (nt(gfg, w_fg) + nt(gfu, w_fu)).astype(BF).reshape(C, T, Q, W)
    mlp_parts = [
        tn(a, b).astype(BF).reshape(F, C, R, U)
        for a, b in ((second, gfg), (second, gfu), (gout, hidden))
    ]
    gm, gb, out, dgain2, dbias2, mlp_got = pl.pallas_call(
        functools.partial(mlp_kernel, dims),
        out_shape=(
            sds((Q, W), F32),
            sds((C, T, Q, W), BF),
            sds((T, Q, W), BF),
            sds((1, W), F32),
            sds((1, W), F32),
            sds((F - 1, C, R, NR), BF),
        ),
        in_specs=[ANY, ANY, VMEM, VMEM, VMEM, ANY, ANY, ANY],
        out_specs=[VMEM, ANY, ANY, VMEM, VMEM, ANY],
        scratch_shapes=[pltpu.VMEM((Q, W), BF), pltpu.VMEM((Q, W), BF), pltpu.SemaphoreType.DMA]
        + [sem(3, F), sem(3, F)]
        + share_sems()
        + scatter_scratch(C, Q, W)
        + (gather_sems(C) + scatter_scratch(C, Q // PARTS, W)) * PARTS,
        compiler_params=params(3),
        name="k_mlp",
    )(gsecond, down, mid, mygo, gain2, *mlp_parts)
    output = out.reshape(tokens.shape)

    branch = gb.reshape(N, W)
    mlp_sum = jnp.concatenate([at(x, f, F) for x in mlp_parts], axis=2).astype(F32)
    for e in range(F - 1):
        mlp_sum = mlp_sum + mlp_got[e].astype(F32)
    mlp_sum = mlp_sum.astype(BF)
    mlp_grads = [at(mlp_sum, z, C)]
    mlp_grads += [hop(at(mlp_sum, z + d, C), "ctx", d) for d in range(1, C)]
    mlp_grads = jnp.stack(mlp_grads)
    ggated = nn(branch, w_o).reshape(C, S, B, HV)
    ggate = (ggated * normal * dsilu).astype(BF)
    gn = ggated * silu
    sums = pair(jnp.stack([jnp.sum(gn, axis=-1), jnp.sum(gn * normal, axis=-1)]))
    s1 = sum(x[0] for x in sums)[..., None] / HEAD_V
    s2 = sum(x[1] for x in sums)[..., None] / HEAD_V
    gmixer = (inv * (gn - s1 - normal * s2)).astype(BF)
    gscores = (ein("cste,csue->cstu", gmixer, v) * scale * table).astype(BF)
    pulled = ein("cstd,cste->csde", q_grown, gmixer)
    later = jnp.zeros_like(pulled[0])
    laters = [None] * C
    for c in reversed(range(C)):
        laters[c] = later.astype(BF)
        later = through[c] * later + pulled[c]
    laters = jnp.stack(laters)
    gq = ein("cstu,csud->cstd", gscores, k) + growth * ein("cste,csde->cstd", gmixer, states)
    gk = ein("cstu,cstd->csud", gscores, q) + keeping * ein("csue,csde->csud", v, laters)
    gv = ein("cstu,cste->csue", weights, gmixer) + ein("csud,csde->csue", k_kept, laters)
    gproj = jnp.concatenate([gq.astype(BF), gk.astype(BF), gv.astype(BF), ggate], axis=-1)
    gproj = gproj.reshape(N, NI)

    gnormed = nt(gproj, w_in).astype(BF).reshape(C, T, Q, W)
    in_parts = tn(normed, gproj).astype(BF).reshape(F, C, R, NI)
    out_parts = tn(branch, gated).astype(BF).reshape(F, C, R, HV)
    H = 2
    gt, gsum, vsum = pl.pallas_call(
        functools.partial(last_kernel, dims),
        out_shape=(sds((T, Q, W), BF), sds((C, R, NO), BF), sds((8, R), F32)),
        in_specs=[ANY, ANY, ANY, VMEM, VMEM, VMEM, VMEM, VMEM],
        out_specs=[ANY, ANY, VMEM],
        scratch_shapes=[pltpu.VMEM((Q, W), BF), pltpu.SemaphoreType.DMA]
        + share_sems()
        + [
            pltpu.VMEM((C, R, NO), BF),
            pltpu.VMEM((F - 1, C, R, NO), BF),
            pltpu.VMEM((C, R, NO), BF),
            sem(C, H),
            sem(H),
            sem(C, H, F),
            sem(C, H, F),
            sem(C, H),
            sem(C, H),
        ]
        + vector_scratch(F, C, R)
        + scatter_scratch(C, Q, W),
        compiler_params=params(4),
        name="k_last",
    )(gnormed, in_parts, out_parts, gm, mytok, gain1, dgain2, dbias2)
    grad_tokens = gt.reshape(tokens.shape)

    def rel(n):
        return pl.BlockSpec((1, R, n), lambda c, z: (lax.rem(z[0] + C - c, C), 0, 0))

    def quarter(n):
        return pl.BlockSpec((R, n), lambda c, z: (0, c))

    per_head = pl.BlockSpec((R, KEY), lambda c, z: (0, c // halves))
    gq, gk, gv, gg, gw, gfg, gfu, gfd = pl.pallas_call(
        functools.partial(assemble_kernel, halves, KEY, HV),
        out_shape=[sds((R, heads * KEY), F32)] * 2
        + [sds((R, C * HV), F32)] * 3
        + [sds((R, C * U), F32)] * 3,
        grid_spec=pltpu.PrefetchScalarGridSpec(
            num_scalar_prefetch=1,
            grid=(C,),
            in_specs=[
                pl.BlockSpec((1, R, NO), lambda c, z: (c, 0, 0)),
                rel(3 * U),
            ],
            out_specs=[per_head, per_head] + [quarter(HV)] * 3 + [quarter(U)] * 3,
        ),
        name="k_assemble",
    )(jnp.full((1,), z, jnp.int32), gsum, mlp_grads)
    return (
        output,
        grad_tokens,
        gq,
        gk,
        gv,
        gg,
        gw,
        vsum[0],
        vsum[1],
        gfg,
        gfu,
        gfd,
        vsum[2],
        vsum[3],
    )


def solution(mesh):
    dims = (mesh.shape["fsdp"], mesh.shape["ctx"], mesh.shape["tp"])
    rows, vec = P(("fsdp", "ctx"), "tp"), P(("fsdp", "ctx"))
    acts = P("fsdp", "ctx", None)
    return jax.shard_map(
        functools.partial(shards, dims),
        mesh=mesh,
        in_specs=(acts, P("fsdp", "ctx", "tp"), rows, rows, rows, rows, rows, vec, vec, rows, rows, rows, vec, vec, acts),
        out_specs=(acts, acts, rows, rows, rows, rows, rows, vec, vec, rows, rows, rows, vec, vec),
        check_vma=False,
    )
```

```python
import functools

import jax
import jax.numpy as jnp
from jax import lax
from jax.experimental import pallas as pl
from jax.experimental.pallas import tpu as pltpu
from jax.sharding import PartitionSpec as P

KEY = 256
HEAD_V = 512
EPSILON = 1e-05
MESH = pl.DeviceIdType.MESH
ANY = pl.BlockSpec(memory_space=pl.ANY)
VMEM = pl.BlockSpec(memory_space=pltpu.VMEM)
BF = jnp.bfloat16
F32 = jnp.float32


def dot(a, b, dims):
    return lax.dot_general(a, b, (dims, ((), ())), preferred_element_type=F32)


def nn(a, b):
    return dot(a, b, ((1,), (0,)))


def nt(a, b):
    return dot(a, b, ((1,), (1,)))


def tn(a, b):
    return dot(a, b, ((0,), (0,)))


class Place:
    def __init__(self, F, C, T):
        self.F, self.C, self.T = F, C, T
        self.f = lax.axis_index("fsdp")
        self.z = lax.axis_index("ctx")
        self.t = lax.axis_index("tp")
        self.lo = lax.rem(self.t, 2)
        self.hi = self.t // 2
        self.near = self.t + 1 - 2 * self.lo
        self.far = lax.rem(self.t + 2, 4)

    def ahead(self, d):
        return lax.rem(self.z + d, self.C)

    def behind(self, d):
        return lax.rem(self.z + self.C - d, self.C)

    def fahead(self, d):
        return lax.rem(self.f + d, self.F)

    def fbehind(self, d):
        return lax.rem(self.f + self.F - d, self.F)

    def barrier(self, ctx=True, fsdp=False, tp=True):
        sem = pltpu.get_barrier_semaphore()
        peers = []
        if tp:
            peers += [{"tp": self.near}, {"tp": self.far}]
        if fsdp:
            peers += [{"fsdp": self.fahead(d)} for d in range(1, self.F)]
        if ctx:
            peers += [{"ctx": self.ahead(d)} for d in range(1, self.C)]
        for peer in peers:
            pl.semaphore_signal(sem, inc=1, device_id=peer, device_id_type=MESH)
        pl.semaphore_wait(sem, len(peers))


def remote(src, dst, ssem, rsem, peer):
    return pltpu.make_async_remote_copy(
        src_ref=src, dst_ref=dst, send_sem=ssem, recv_sem=rsem, device_id=peer, device_id_type=MESH
    )


def sem(*shape):
    return pltpu.SemaphoreType.DMA(shape)


def gather_sems(C):
    return [sem(C), sem(C), sem(C), sem(C), sem(C, 2), sem(C, 2), pltpu.SemaphoreType.DMA]


class Gather:
    def __init__(self, pc, x, out, rows, sems):
        self.pc, self.x = pc, x
        self.zs, self.zr, self.ys, self.yr, self.cs, self.cr, self.ls = sems
        self.slot = lambda c, t: out.at[c, t, rows]

    def start(self):
        pc, x = self.pc, self.x
        self.here = self.slot(pc.z, pc.t)
        self.local = pltpu.make_async_copy(x, self.here, self.ls)
        self.local.start()
        self.zc, self.yc, self.cc = {}, {}, {}
        for d in range(1, pc.C):
            self.zc[d] = remote(
                x, self.here, self.zs.at[d], self.zr.at[d], {"ctx": pc.ahead(d)}
            )
            self.zc[d].start()
        self.forward(0)

    def forward(self, d):
        pc = self.pc
        dst = self.slot(pc.behind(d), pc.t)
        src = dst if d else self.x
        if d:
            self.zc[d].wait_recv()
        self.yc[d] = remote(src, dst, self.ys.at[d], self.yr.at[d], {"tp": pc.far})
        self.yc[d].start()
        self.cc[d, 0] = remote(src, dst, self.cs.at[d, 0], self.cr.at[d, 0], {"tp": pc.near})
        self.cc[d, 0].start()

    def onward(self, d):
        pc = self.pc
        self.yc[d].wait_recv()
        src = self.slot(pc.behind(d), pc.far)
        self.cc[d, 1] = remote(src, src, self.cs.at[d, 1], self.cr.at[d, 1], {"tp": pc.near})
        self.cc[d, 1].start()

    def finish(self):
        self.local.wait()
        for cp in self.zc.values():
            cp.wait_send()
        for cp in self.yc.values():
            cp.wait_send()
        for cp in self.cc.values():
            cp.wait()


def share_sems():
    return [sem(3), sem(3)]


def share_stage(pc, x, out, lsem, sems):
    ss, rs = sems
    t = pc.t
    local = pltpu.make_async_copy(x, out.at[t], lsem)
    local.start()
    a = remote(x, out.at[t], ss.at[0], rs.at[0], {"tp": pc.far})
    a.start()
    b = remote(x, out.at[t], ss.at[1], rs.at[1], {"tp": pc.near})
    b.start()
    a.wait_recv()
    src = out.at[pc.far]
    c = remote(src, src, ss.at[2], rs.at[2], {"tp": pc.near})
    c.start()
    local.wait()
    a.wait_send()
    b.wait()
    c.wait()


def scatter_scratch(C, Q, W):
    return [
        pltpu.VMEM((C, 2, Q, W), BF),
        pltpu.VMEM((C, Q, W), BF),
        pltpu.VMEM((C, Q, W), BF),
        pltpu.VMEM((C, Q, W), BF),
        pltpu.VMEM((C, Q, W), BF),
        sem(C, 2),
        sem(C, 2),
        sem(C),
        sem(C),
        sem(C),
        sem(C),
    ]


def local_scratch(C, Q, W):
    return [pltpu.VMEM((C, 2, Q, W), BF), sem(C, 2)]


class Scatter:
    def __init__(self, pc, p, rows, scratch, local=None):
        self.pc, self.p, self.rows, self.local = pc, p, rows, local
        (self.buf1, self.snd2, self.buf2, self.snd3, self.buf3) = scratch[:5]
        self.s1, self.r1, self.s2, self.r2, self.s3, self.r3 = scratch[5:]
        self.order = list(range(1, pc.C)) + [0]
        self.lc, self.c1, self.c2, self.c3 = {}, {}, {}, {}

    def side(self, j):
        return 1 - self.pc.hi if j == 0 else self.pc.hi

    def begin(self, d):
        pc, p, rows = self.pc, self.p, self.rows
        c = pc.ahead(d)
        for j in range(2):
            self.c1[d, j] = remote(
                p.at[c, self.side(j) * 2 + 1 - pc.lo, rows],
                self.buf1.at[d, j],
                self.s1.at[d, j],
                self.r1.at[d, j],
                {"tp": pc.near},
            )
            self.c1[d, j].start()
            if self.local:
                self.lc[d, j] = pltpu.make_async_copy(
                    p.at[c, self.side(j) * 2 + pc.lo, rows],
                    self.local[0].at[d, j],
                    self.local[1].at[d, j],
                )
                self.lc[d, j].start()

    def start(self):
        for d in self.order:
            self.begin(d)

    def own(self, d, j):
        self.c1[d, j].wait_recv()
        if self.local:
            self.lc[d, j].wait()
            here = self.local[0][d, j]
        else:
            here = self.p[self.pc.ahead(d), self.side(j) * 2 + self.pc.lo, self.rows]
        return here.astype(F32) + self.buf1[d, j].astype(F32)

    def far(self):
        for d in self.order:
            self.snd2[d] = self.own(d, 0).astype(BF)
            self.c2[d] = remote(
                self.snd2.at[d],
                self.buf2.at[d],
                self.s2.at[d],
                self.r2.at[d],
                {"tp": self.pc.far},
            )
            self.c2[d].start()

    def along(self, d):
        part = self.own(d, 1)
        self.c2[d].wait_recv()
        part = part + self.buf2[d].astype(F32)
        if d:
            self.snd3[d] = part.astype(BF)
            self.c3[d] = remote(
                self.snd3.at[d],
                self.buf3.at[d],
                self.s3.at[d],
                self.r3.at[d],
                {"ctx": self.pc.ahead(d)},
            )
            self.c3[d].start()
        else:
            self.total = part

    def result(self):
        total = self.total
        for d in range(1, self.pc.C):
            self.c3[d].wait_recv()
            total = total + self.buf3[d].astype(F32)
        return total

    def finish(self):
        for copies in (self.c1, self.c2, self.c3):
            for cp in copies.values():
                cp.wait_send()


PARTS = 2


def halves_of(rows):
    n = rows // PARTS
    return (lambda h: pl.ds(h * n, n)), PARTS


def layer_norm_rows(values, gain, bias):
    center = values - jnp.mean(values, axis=-1, keepdims=True)
    spread = jnp.mean(center * center, axis=-1, keepdims=True)
    return (center * lax.rsqrt(spread + EPSILON) * gain + bias).astype(BF)


def eye_of(n):
    return lax.broadcasted_iota(jnp.int32, (n, n), 0) == lax.broadcasted_iota(jnp.int32, (n, n), 1)


def as_row(column):
    return jnp.sum(jnp.where(eye_of(column.shape[0]), column, 0.0), axis=0, keepdims=True)


def as_column(row):
    return jnp.sum(jnp.where(eye_of(row.shape[1]), row, 0.0), axis=1, keepdims=True)


def decays(rates):
    B = rates.shape[1]
    causal = lax.broadcasted_iota(jnp.int32, (B, B), 0) >= lax.broadcasted_iota(jnp.int32, (B, B), 1)
    column = jnp.sum(jnp.where(causal, rates, 0.0), axis=1, keepdims=True)
    row = as_row(column)
    table = jnp.where(causal, jnp.exp(jnp.minimum(column - row, 0.0)), 0.0)
    total = column[B - 1 :]
    return table, jnp.exp(column), jnp.exp(total - column), jnp.exp(total)


class Mover:
    def __init__(self, pc, weights, layout, out, zs, zr, xs, xr, ls):
        self.pc, self.weights, self.layout, self.out = pc, weights, layout, out
        self.zs, self.zr, self.xs, self.xr, self.ls = zs, zr, xs, xr, ls
        self.zc, self.xc = {}, {}

    def columns(self, dst):
        at = 0
        for w, (share, n) in zip(self.weights, self.layout):
            start = pl.multiple_of((dst // share) * n, n)
            yield w.at[:, pl.ds(start, n)], self.out.at[self.pc.f, self.pc.z, :, pl.ds(at, n)]
            at += n

    def start(self):
        pc = self.pc
        for d in range(1, pc.C):
            dst = pc.ahead(d)
            sems, peer = (self.zs.at[d], self.zr.at[d]), {"ctx": dst}
            for src, to in self.columns(dst):
                remote(src, to, *sems, peer).start()
            here = self.out.at[pc.f, pc.behind(d)]
            self.zc[d] = remote(here, here, *sems, peer)
        for e in range(1, pc.F):
            sems, peer = (self.xs.at[0, e], self.xr.at[0, e]), {"fsdp": pc.fahead(e)}
            for src, to in self.columns(pc.z):
                remote(src, to, *sems, peer).start()
            here = self.out.at[pc.fbehind(e), pc.z]
            self.xc[0, e] = remote(here, here, *sems, peer)
        for src, to in self.columns(pc.z):
            pltpu.make_async_copy(src, to, self.ls).start()
        here = self.out.at[pc.f, pc.z]
        self.local = pltpu.make_async_copy(here, here, self.ls)

    def forward(self, d):
        pc = self.pc
        self.zc[d].wait_recv()
        here = self.out.at[pc.f, pc.behind(d)]
        for e in range(1, pc.F):
            self.xc[d, e] = remote(
                here, here, self.xs.at[d, e], self.xr.at[d, e], {"fsdp": pc.fahead(e)}
            )
            self.xc[d, e].start()

    def arrived(self, d, e):
        self.xc[d, e].wait_recv()

    def sent(self):
        for cp in list(self.zc.values()) + list(self.xc.values()):
            cp.wait_send()


class Blocks:
    def __init__(self, pc, x, out, zs, zr, ys, yr, cs, cr, ls):
        self.pc, self.x, self.out = pc, x, out
        self.zs, self.zr, self.ys, self.yr, self.cs, self.cr, self.ls = zs, zr, ys, yr, cs, cr, ls
        self.zc, self.yc, self.cc = {}, {}, {}

    def start(self):
        pc = self.pc
        for d in range(1, pc.C):
            self.zc[d] = remote(
                self.x.at[pc.t],
                self.out.at[pc.z, pc.t],
                self.zs.at[d],
                self.zr.at[d],
                {"ctx": pc.ahead(d)},
            )
            self.zc[d].start()
        self.local = pltpu.make_async_copy(self.x, self.out.at[pc.z], self.ls)
        self.local.start()

    def forward(self, d):
        pc = self.pc
        self.zc[d].wait_recv()
        here = self.out.at[pc.behind(d), pc.t]
        self.yc[d] = remote(here, here, self.ys.at[d], self.yr.at[d], {"tp": pc.far})
        self.yc[d].start()
        self.cc[d, 0] = remote(here, here, self.cs.at[d, 0], self.cr.at[d, 0], {"tp": pc.near})
        self.cc[d, 0].start()

    def onward(self, d):
        pc = self.pc
        self.yc[d].wait_recv()
        here = self.out.at[pc.behind(d), pc.far]
        self.cc[d, 1] = remote(here, here, self.cs.at[d, 1], self.cr.at[d, 1], {"tp": pc.near})
        self.cc[d, 1].start()

    def finish(self):
        self.local.wait()
        for cp in list(self.zc.values()) + list(self.yc.values()):
            cp.wait_send()
        for cp in self.cc.values():
            cp.wait()


def mover_sems(F, C):
    return [sem(C), sem(C), sem(C, F), sem(C, F), pltpu.SemaphoreType.DMA]


def blocks_sems(C):
    return [sem(C), sem(C), sem(C), sem(C), sem(C, 2), sem(C, 2), pltpu.SemaphoreType.DMA]


def forward_kernel(dims, cfg, *refs):
    F, C, T = dims
    S, B, halves, HV, in_layout, rest_layout = cfg
    refs = list(refs)

    def take(n):
        out = refs[:n]
        del refs[:n]
        return out

    in_weights, rest_weights = take(5), take(3)
    vec, ld, tok, go = take(4)
    o_win, o_normed, o_proj, o_states, o_normal, o_inv, o_gated, old, vecs, mid, sn, full, ogo = take(13)
    otok, win, ovec, normed, acc, proj, states, state, normal, inv, gated, stats, mytok, x = take(14)
    in_sems, rest_sems = take(5), take(5)
    tok_sems, go_sems = take(7), take(7)
    vzs, vzr, vxs, vxr, lzs, lzr, sts, strr, oses = take(9)
    n, m = len(gather_sems(C)), len(scatter_scratch(C, 8, 128))

    pc = Place(*dims)
    f, z, t = pc.f, pc.z, pc.t
    L = S * B
    R = win.shape[2]
    W = F * C * R
    NI = proj.shape[1]
    N = proj.shape[0]
    units = C * S
    saved = []

    def save(src, dst):
        cp = pltpu.make_async_copy(src, dst, oses.at[len(saved)])
        cp.start()
        saved.append(cp)

    pc.barrier(True, True, True)
    vz, vx, lz = {}, {}, {}
    for d in range(1, C):
        peer = {"ctx": pc.ahead(d)}
        vz[d] = remote(vec, ovec.at[f, z], vzs.at[d], vzr.at[d], peer)
        vz[d].start()
        lz[d] = remote(ld, old.at[z], lzs.at[d], lzr.at[d], peer)
        lz[d].start()
    ovec[f, z] = vec[...]
    old[z] = ld[...]

    def vec_across(d):
        for e in range(1, F):
            src = ovec.at[f, pc.behind(d)] if d else vec
            vx[d, e] = remote(
                src, ovec.at[f, pc.behind(d)], vxs.at[d, e], vxr.at[d, e], {"fsdp": pc.fahead(e)}
            )
            vx[d, e].start()

    vec_across(0)
    tk = Blocks(pc, tok, otok, *tok_sems)
    tk.start()
    wi = Mover(pc, in_weights, in_layout, win, *in_sems)
    wi.start()
    mine = pltpu.make_async_copy(tok.at[t], mytok, oses.at[15])
    mine.start()
    for d in range(1, C):
        vz[d].wait_recv()
        vec_across(d)
        tk.forward(d)
    wr = Mover(pc, rest_weights, rest_layout, full, *rest_sems)
    wr.start()
    gk = Blocks(pc, go, ogo, *go_sems)
    gk.start()
    for d in range(1, C):
        tk.onward(d)
    for cp in vx.values():
        cp.wait()
    for cp in vz.values():
        cp.wait_send()
    for b in range(F * C):
        vecs[:, b * R : (b + 1) * R] = ovec[b // C, b % C]
    tk.finish()
    gain1, bias1 = vecs[0:1], vecs[1:2]

    def norm_unit(i, carry):
        rows = otok[i // T, lax.rem(i, T)].astype(F32)
        q = rows.shape[0]
        normed[pl.ds(pl.multiple_of(i * q, q), q)] = layer_norm_rows(rows, gain1, bias1)
        return carry

    lax.fori_loop(0, C * T, norm_unit, 0)
    save(normed, o_normed)

    tile = min(256, N)

    def project(ff, c, first, last):
        columns = pl.ds(pl.multiple_of((ff * C + c) * R, 128), R)

        def one(i, carry):
            rows = pl.ds(pl.multiple_of(i * tile, tile), tile)
            part = nn(normed[rows, columns], win[ff, c, :, :NI])
            if not first:
                part = part + acc[rows]
            if last:
                proj[rows] = part.astype(BF)
            else:
                acc[rows] = part
            return carry

        lax.fori_loop(0, N // tile, one, 0)

    wi.local.wait()
    project(f, z, True, False)
    for d in range(1, C):
        wi.forward(d)
        for e in range(1, F):
            wi.arrived(d - 1, e)
            project(pc.fbehind(e), pc.behind(d - 1), False, False)
        project(f, pc.behind(d), False, False)
    for e in range(1, F):
        wi.arrived(C - 1, e)
        project(pc.fbehind(e), pc.behind(C - 1), False, e == F - 1)
    save(proj, o_proj)
    save(win, o_win)

    for cp in lz.values():
        cp.wait()
    head = z // halves
    scale = float(KEY) ** (-0.5)
    state[...] = jnp.zeros_like(state)

    def retain(u, carry):
        c, s = u // S, lax.rem(u, S)
        rows = pl.ds(pl.multiple_of(u * B, B), B)
        rates = old[c, pl.ds(head, 1), pl.ds(pl.multiple_of(s * B, B), B)]
        table, growth, keeping, through = decays(rates)
        q, k, v = proj[rows, :KEY], proj[rows, KEY : 2 * KEY], proj[rows, 2 * KEY : 2 * KEY + HV]
        weights = (nt(q, k) * scale * table).astype(BF)
        before = state[s]
        states[u] = before.astype(BF)
        mixed = nn(weights, v) + nn((q.astype(F32) * growth).astype(BF), before.astype(BF))
        state[s] = through * before + tn((k.astype(F32) * keeping).astype(BF), v)
        normal[rows] = mixed
        mean = jnp.mean(mixed, axis=-1, keepdims=True)
        dev = mixed - mean
        stats[0, 0:1, rows] = as_row(mean)
        stats[0, 1:2, rows] = as_row(jnp.sum(dev * dev, axis=-1, keepdims=True))
        return carry

    stats[0] = jnp.zeros(stats.shape[1:], F32)
    lax.fori_loop(0, units, retain, 0)
    save(states, o_states)
    st = []
    place = lax.rem(z, halves)
    for j in range(1, halves):
        peer = {"ctx": z - place + lax.rem(place + j, halves)}
        cp = remote(stats.at[0], stats.at[j], sts.at[j], strr.at[j], peer)
        cp.start()
        st.append(cp)
    for cp in st:
        cp.wait()

    def finish_unit(u, carry):
        rows = pl.ds(pl.multiple_of(u * B, B), B)
        got = [(stats[j, 0:1, rows], stats[j, 1:2, rows]) for j in range(halves)]
        mean = sum(a for a, _ in got) / halves
        m2 = sum(b + HV * (a - mean) * (a - mean) for a, b in got)
        scaled = as_column(lax.rsqrt(m2 / HEAD_V + EPSILON))
        value = (normal[rows] - as_column(mean)) * scaled
        gate = proj[rows, 2 * KEY + HV :].astype(F32)
        normal[rows] = value
        inv[rows] = jnp.broadcast_to(scaled, (B, 128))
        gated[rows] = (gate * jax.nn.sigmoid(gate) * value).astype(BF)
        return carry

    lax.fori_loop(0, units, finish_unit, 0)
    save(normal, o_normal)
    save(inv, o_inv)
    save(gated, o_gated)

    p = otok
    Q = x.shape[0]
    cut, parts = halves_of(Q)
    scatters, gathers = [], []
    for h in range(parts):
        at = h * (n + m)
        gathers.append(Gather(pc, x.at[cut(h)], sn, cut(h), refs[at : at + n]))
        scatters.append(Scatter(pc, p, cut(h), refs[at + n : at + n + m]))
    for d in scatters[0].order:
        c = pc.ahead(d)
        mixed = gated[pl.ds(pl.multiple_of(c * L, L), L)]

        def one(b, carry):
            part = nt(mixed, win[b // C, lax.rem(b, C), :, NI:]).astype(BF)
            columns = pl.ds(pl.multiple_of(b * R, 128), R)
            for i in range(T):
                p[c, i, :, columns] = part[i * Q : (i + 1) * Q]
            return carry

        lax.fori_loop(0, F * C, one, 0)
        for rs in scatters:
            rs.begin(d)
    for rs in scatters:
        rs.far()
    for rs in scatters:
        for d in rs.order:
            rs.along(d)
    for d in range(1, C):
        wr.forward(d)
    mine.wait()
    for h, rs in enumerate(scatters):
        part = cut(h)
        total = rs.result() + mytok[part].astype(F32)
        mid[part] = total
        x[part] = layer_norm_rows(total, vecs[2:3], vecs[3:4])
        gathers[h].start()
    for d in range(1, C):
        gk.forward(d)
    for ga in gathers:
        for d in range(1, C):
            ga.forward(d)
    for d in range(1, C):
        gk.onward(d)
    for ga in gathers:
        for d in range(C):
            ga.onward(d)
    for job in scatters + gathers:
        job.finish()
    gk.finish()
    wi.sent()
    wr.local.wait()
    for d in range(C):
        for e in range(1, F):
            wr.arrived(d, e)
    wr.sent()
    for cp in saved:
        cp.wait()


def norm_pull(values, gain, grad):
    center = values - jnp.mean(values, axis=-1, keepdims=True)
    spread = jnp.mean(center * center, axis=-1, keepdims=True)
    inv = lax.rsqrt(spread + EPSILON)
    xhat = center * inv
    g = grad * gain
    back = inv * (
        g - jnp.mean(g, axis=-1, keepdims=True) - xhat * jnp.mean(g * xhat, axis=-1, keepdims=True)
    )
    return (
        back,
        jnp.sum(grad * xhat, axis=0, keepdims=True),
        jnp.sum(grad, axis=0, keepdims=True),
    )


def mlp_kernel(
    dims, pg, pd, mid, allgo, gain, g0, g1, g2, gm, gb, out, dgain, dbias, xg, x, y, go, lsem, gosem, gxs, gxr, *scratch
):
    pc = Place(*dims)
    C = pc.C
    mine = pltpu.make_async_copy(allgo.at[pc.t], go, gosem)
    mine.start()
    pc.barrier(True, True, True)
    n, m = len(gather_sems(C)), len(scatter_scratch(C, 8, 128))
    ss, scratch = scratch[:2], scratch[2:]
    rd = Scatter(pc, pd, pl.ds(0, x.shape[0]), scratch[:m], scratch[m : m + 2])
    scratch = scratch[m + 2 :]
    cut, parts = halves_of(x.shape[0])
    scatters, gathers = [], []
    for h in range(parts):
        at = h * (n + m + 2)
        gathers.append(Gather(pc, x.at[cut(h)], gb, cut(h), scratch[at : at + n]))
        at += n
        scatters.append(Scatter(pc, pg, cut(h), scratch[at : at + m], scratch[at + m : at + m + 2]))
    for rs in scatters:
        rs.start()
    rd.start()
    moves = []
    u = g0.shape[3]
    for i, g in enumerate((g0, g1, g2)):
        for e in range(1, pc.F):
            cp = remote(
                g.at[pc.fahead(e)],
                xg.at[e - 1, :, :, pl.ds(i * u, u)],
                gxs.at[i, e],
                gxr.at[i, e],
                {"fsdp": pc.fahead(e)},
            )
            cp.start()
            moves.append(cp)
    for rs in scatters:
        rs.far()
    rd.far()
    mine.wait()
    for h, rs in enumerate(scatters):
        for d in rs.order:
            rs.along(d)
        part = cut(h)
        back, dg, db = norm_pull(mid[part], gain[...], rs.result())
        dgain[...] = dgain[...] + dg if h else dg
        dbias[...] = dbias[...] + db if h else db
        grad_middle = go[part].astype(F32) + back
        gm[part] = grad_middle
        x[part] = grad_middle.astype(BF)
        gathers[h].start()
    for d in rd.order[:2]:
        rd.along(d)
    for d in range(1, C):
        gathers[0].forward(d)
    for d in rd.order[2:]:
        rd.along(d)
    for ga in gathers[1:]:
        for d in range(1, C):
            ga.forward(d)
    for d in range(C):
        for ga in gathers:
            ga.onward(d)
    y[...] = (mid[...] + rd.result()).astype(BF)
    share_stage(pc, y, out, lsem, ss)
    for job in scatters + gathers + [rd]:
        job.finish()
    for cp in moves:
        cp.wait()


class GradScatter:
    def __init__(self, pc, grads, out, own, xbuf, zsnd, ls, os, xs, xr, zs, zr):
        self.pc, self.grads, self.out = pc, grads, out
        self.own, self.xbuf, self.zsnd = own, xbuf, zsnd
        self.sems = (ls, os, xs, xr, zs, zr)
        C = pc.C
        self.H = os.shape[0]
        self.rows = own.shape[1] // self.H
        far = sorted(range(1, C), key=lambda d: abs(d - C // 2))
        self.order = [(d, h) for d in far + [0] for h in range(self.H)]

    def start(self):
        pc = self.pc
        ls, os, xs, xr, zs, zr = self.sems
        self.loc, self.xc, self.zc, self.keep, self.sent = {}, {}, {}, {}, []
        for d, h in self.order:
            c = pc.ahead(d)
            part = pl.ds(h * self.rows, self.rows)
            at = 0
            for g in self.grads:
                n = g.shape[3]
                for e in range(1, pc.F):
                    remote(
                        g.at[pc.fahead(e), c, part],
                        self.xbuf.at[e - 1, d, part, pl.ds(at, n)],
                        xs.at[d, h, e],
                        xr.at[d, h, e],
                        {"fsdp": pc.fahead(e)},
                    ).start()
                pltpu.make_async_copy(
                    g.at[pc.f, c, part], self.own.at[d, part, pl.ds(at, n)], ls.at[d, h]
                ).start()
                at += n
            here = self.own.at[d, part]
            self.loc[d, h] = pltpu.make_async_copy(here, here, ls.at[d, h])
            for e in range(1, pc.F):
                there = self.xbuf.at[e - 1, d, part]
                self.xc[d, h, e] = remote(
                    there, there, xs.at[d, h, e], xr.at[d, h, e], {"fsdp": pc.fahead(e)}
                )
        self.todo = list(self.order)

    def step(self, count=1):
        pc = self.pc
        ls, os, xs, xr, zs, zr = self.sems
        for _ in range(count):
            if not self.todo:
                return
            d, h = self.todo.pop(0)
            part = pl.ds(h * self.rows, self.rows)
            self.loc[d, h].wait()
            total = self.own[d, part].astype(F32)
            for e in range(1, pc.F):
                self.xc[d, h, e].wait_recv()
                total = total + self.xbuf[e - 1, d, part].astype(F32)
            self.zsnd[d, part] = total.astype(BF)
            src, dst = self.zsnd.at[d, part], self.out.at[pc.z, part]
            if d:
                self.zc[d, h] = remote(src, dst, zs.at[d, h], zr.at[d, h], {"ctx": pc.ahead(d)})
                self.zc[d, h].start()
            else:
                self.keep[h] = pltpu.make_async_copy(src, dst, os.at[h])
                self.keep[h].start()

    def finish(self):
        for cp in self.keep.values():
            cp.wait()
        for cp in self.zc.values():
            cp.wait()
        for cp in self.xc.values():
            cp.wait_send()


def vector_stage(pc, v, vout, va, vb, vc, vd, vx, vz, ts, tr, vxs, vxr, vzs, vzr):
    F, C = pc.F, pc.C
    t0 = remote(v, vb, ts.at[0], tr.at[0], {"tp": pc.near})
    t0.start()
    t0.wait_recv()
    va[...] = v[...] + vb[...]
    t1 = remote(va, vc, ts.at[1], tr.at[1], {"tp": pc.far})
    t1.start()
    t1.wait_recv()
    vd[...] = va[...] + vc[...]
    vxc, vzc = {}, {}
    for e in range(1, F):
        vxc[e] = remote(
            vd.at[pc.fahead(e)], vx.at[e - 1], vxs.at[e], vxr.at[e], {"fsdp": pc.fahead(e)}
        )
        vxc[e].start()
    vs = vd[pc.f]
    for e in range(1, F):
        vxc[e].wait_recv()
        vs = vs + vx[e - 1]
    vz[0] = vs
    for d in range(1, C):
        vzc[d] = remote(
            vz.at[0, pc.ahead(d)], vz.at[1, d], vzs.at[d], vzr.at[d], {"ctx": pc.ahead(d)}
        )
        vzc[d].start()
    acc = vz[0, pc.z]
    for d in range(1, C):
        vzc[d].wait_recv()
        acc = acc + vz[1, d]
    vout[...] = acc
    for cp in [t0, t1] + list(vxc.values()) + list(vzc.values()):
        cp.wait_send()


def vector_scratch(F, C, R):
    full = pltpu.VMEM((F, C, 8, R), F32)
    return [
        full,
        full,
        full,
        full,
        full,
        pltpu.VMEM((F - 1, C, 8, R), F32),
        pltpu.VMEM((2, C, 8, R), F32),
        sem(2),
        sem(2),
        sem(F),
        sem(F),
        sem(C),
        sem(C),
    ]


def last_kernel(
    dims, p, g0, g1, gm, alltok, gain, dg2, db2, gt, gout, vout, y, tok, lsem, toksem, s0, s1, *scratch
):
    pc = Place(*dims)
    mine = pltpu.make_async_copy(alltok.at[pc.t], tok, toksem)
    mine.start()
    F, C, T = dims
    pc.barrier(True, True, True)
    gr = GradScatter(pc, (g0, g1), gout, *scratch[:9])
    v, rest = scratch[9], scratch[10:22]
    rs = Scatter(pc, p, pl.ds(0, y.shape[0]), scratch[22:-2], scratch[-2:])
    rs.start()
    gr.start()
    rs.far()
    for d in rs.order:
        rs.along(d)
        gr.step()
    mine.wait()
    back, dg, db = norm_pull(tok[...].astype(F32), gain[...], rs.result())
    y[...] = (gm[...] + back).astype(BF)
    R = v.shape[3]
    for i in range(F * C):
        rows = [r[:, i * R : (i + 1) * R] for r in (dg, db)] + [
            r[:, i * R : (i + 1) * R] for r in (dg2, db2)
        ]
        v[i // C, i % C] = jnp.concatenate(rows + [jnp.zeros((4, R), F32)], axis=0)
    gr.step(len(gr.todo))
    share_stage(pc, y, gt, lsem, (s0, s1))
    vector_stage(pc, v, vout, *rest)
    gr.finish()
    rs.finish()


def assemble_kernel(halves, key, hv, z, a, m, q, k, v, g, o, fg, fu, fd):
    c = pl.program_id(0)
    first = lax.rem(c, halves) == 0
    for i, ref in enumerate((q, k)):
        x = a[0, :, i * key : (i + 1) * key].astype(F32)

        @pl.when(first)
        def _(ref=ref, x=x):
            ref[...] = x

        @pl.when(jnp.logical_not(first))
        def _(ref=ref, x=x):
            ref[...] += x

    v[...] = a[0, :, 2 * key : 2 * key + hv].astype(F32)
    g[...] = a[0, :, 2 * key + hv : 2 * key + 2 * hv].astype(F32)
    o[...] = a[0, :, 2 * key + 2 * hv :].astype(F32)
    u = fg.shape[1]
    for i, ref in enumerate((fg, fu, fd)):
        ref[...] = m[0, :, i * u : (i + 1) * u].astype(F32)


def params(cid):
    return pltpu.CompilerParams(collective_id=cid, has_side_effects=True)


def silu_parts(g):
    s = jax.nn.sigmoid(g)
    return g * s, s * (1.0 + g * (1.0 - s))


def shards(
    dims,
    tokens,
    log_decay,
    w_query,
    w_key,
    w_value,
    w_gate,
    w_out,
    norm1_gain,
    norm1_bias,
    w_ffgate,
    w_ffup,
    w_down,
    norm2_gain,
    norm2_bias,
    grad_out,
):
    F, C, T = dims
    S, B, W = tokens.shape
    L = S * B
    Q = L // T
    N = C * L
    R = w_query.shape[0]
    heads = log_decay.shape[2]
    halves = C // heads
    HV = HEAD_V // halves
    U = w_ffgate.shape[1] // C
    z = lax.axis_index("ctx")
    t = lax.axis_index("tp")
    scale = float(KEY) ** (-0.5)

    f = lax.axis_index("fsdp")

    def hop(x, axis, d):
        n = lax.axis_size(axis)
        return lax.ppermute(x, axis, [(i, (i + d) % n) for i in range(n)])

    def at(x, i, n):
        return lax.dynamic_index_in_dim(x, lax.rem(i, n), 0, False)

    NI, NR = 2 * KEY + 2 * HV, 3 * U
    NO = NI + HV
    vec = jnp.stack([norm1_gain, norm1_bias, norm2_gain, norm2_bias]).astype(F32)
    vec = jnp.pad(vec, ((0, 4), (0, 0)))
    ld = jnp.pad(jnp.transpose(log_decay, (2, 0, 1)).reshape(heads, L), ((0, 8 - heads), (0, 0)))
    tok = tokens.reshape(T, Q, W)
    go = grad_out.reshape(T, Q, W)
    sds = jax.ShapeDtypeStruct
    cfg = (
        S,
        B,
        halves,
        HV,
        ((halves, KEY), (halves, KEY), (1, HV), (1, HV), (1, HV)),
        ((1, U), (1, U), (1, U)),
    )
    owin, normed, proj, states, normal, inv, gated, old, vecs, mid, sn, full, ogo = pl.pallas_call(
        functools.partial(forward_kernel, dims, cfg),
        out_shape=(
            sds((F, C, R, NO), BF),
            sds((N, W), BF),
            sds((N, NI), BF),
            sds((C * S, KEY, HV), BF),
            sds((N, HV), F32),
            sds((N, 128), F32),
            sds((N, HV), BF),
            sds((C, 8, L), F32),
            sds((8, W), F32),
            sds((Q, W), F32),
            sds((C, T, Q, W), BF),
            sds((F, C, R, NR), BF),
            sds((C, T, Q, W), BF),
        ),
        in_specs=[ANY] * 8 + [VMEM, VMEM, ANY, ANY],
        out_specs=[ANY] * 7 + [VMEM] * 3 + [ANY] * 3,
        scratch_shapes=[
            pltpu.VMEM((C, T, Q, W), BF),
            pltpu.VMEM((F, C, R, NO), BF),
            pltpu.VMEM((F, C, 8, R), F32),
            pltpu.VMEM((N, W), BF),
            pltpu.VMEM((N, NI), F32),
            pltpu.VMEM((N, NI), BF),
            pltpu.VMEM((C * S, KEY, HV), BF),
            pltpu.VMEM((S, KEY, HV), F32),
            pltpu.VMEM((N, HV), F32),
            pltpu.VMEM((N, 128), F32),
            pltpu.VMEM((N, HV), BF),
            pltpu.VMEM((halves, 8, N), F32),
            pltpu.VMEM((Q, W), BF),
            pltpu.VMEM((Q, W), BF),
        ]
        + mover_sems(F, C) * 2
        + blocks_sems(C) * 2
        + [sem(C), sem(C), sem(C, F), sem(C, F), sem(C), sem(C), sem(halves), sem(halves), sem(16)]
        + (gather_sems(C) + scatter_scratch(C, Q // PARTS, W)) * PARTS,
        compiler_params=params(1),
        name="k_forward",
    )(w_query, w_key, w_value, w_gate, w_out, w_ffgate, w_ffup, w_down, vec, ld, tok, go)
    gain1, gain2 = vecs[0:1], vecs[2:3]
    w_all = owin.reshape(W, NO)
    w_in, w_o = w_all[:, :NI], w_all[:, NI:]
    w_rest = full.reshape(W, NR)
    w_fg, w_fu, w_d = w_rest[:, :U], w_rest[:, U : 2 * U], w_rest[:, 2 * U :]

    q = proj[:, :KEY].reshape(C, S, B, KEY)
    k = proj[:, KEY : 2 * KEY].reshape(C, S, B, KEY)
    v = proj[:, 2 * KEY : 2 * KEY + HV].reshape(C, S, B, HV)
    g = proj[:, 2 * KEY + HV :].reshape(C, S, B, HV).astype(F32)
    rates = lax.dynamic_index_in_dim(old, z // halves, 1, False).reshape(C, S, B)
    cum = jnp.cumsum(rates, axis=-1)
    total = cum[..., -1]
    positions = jnp.arange(B)
    causal = positions[:, None] >= positions[None, :]
    table = jnp.where(
        causal, jnp.exp(jnp.minimum(cum[..., :, None] - cum[..., None, :], 0.0)), 0.0
    )
    growth = jnp.exp(cum)[..., None]
    keeping = jnp.exp(total[..., None] - cum)[..., None]
    through = jnp.exp(total)[..., None, None]

    def ein(spec, a, b):
        return jnp.einsum(spec, a, b, preferred_element_type=F32)

    weights = (ein("cstd,csud->cstu", q, k) * scale * table).astype(BF)
    q_grown = (q.astype(F32) * growth).astype(BF)
    k_kept = (k.astype(F32) * keeping).astype(BF)
    def pair(stats):
        got = [stats]
        for j in range(1, halves):
            perm = []
            for c in range(C):
                base = c - c % halves
                perm.append((c, base + (c % halves + j) % halves))
            got.append(lax.ppermute(stats, "ctx", perm))
        return got

    silu, dsilu = silu_parts(g)
    normal = normal.reshape(C, S, B, HV)
    inv = inv[:, :1].reshape(C, S, B, 1)
    states = states.reshape(C, S, KEY, HV)
    second = sn.reshape(N, W)
    ff_gate = nn(second, w_fg).astype(BF)
    ff_up = nn(second, w_fu).astype(BF)
    hidden, gelu_pull = jax.vjp(
        lambda a, b: jax.nn.gelu(a, approximate=True) * b, ff_gate.astype(F32), ff_up.astype(F32)
    )
    hidden = hidden.astype(BF)
    down = nt(hidden, w_d).astype(BF).reshape(C, T, Q, W)
    gout = ogo.reshape(N, W)
    grad_hidden = nn(gout, w_d)
    gfg, gfu = gelu_pull(grad_hidden)
    gfg, gfu = gfg.astype(BF), gfu.astype(BF)
    gsecond = (nt(gfg, w_fg) + nt(gfu, w_fu)).astype(BF).reshape(C, T, Q, W)
    mlp_parts = [
        tn(a, b).astype(BF).reshape(F, C, R, U)
        for a, b in ((second, gfg), (second, gfu), (gout, hidden))
    ]
    gm, gb, out, dgain2, dbias2, mlp_got = pl.pallas_call(
        functools.partial(mlp_kernel, dims),
        out_shape=(
            sds((Q, W), F32),
            sds((C, T, Q, W), BF),
            sds((T, Q, W), BF),
            sds((1, W), F32),
            sds((1, W), F32),
            sds((F - 1, C, R, NR), BF),
        ),
        in_specs=[ANY, ANY, VMEM, ANY, VMEM, ANY, ANY, ANY],
        out_specs=[VMEM, ANY, ANY, VMEM, VMEM, ANY],
        scratch_shapes=[pltpu.VMEM((Q, W), BF)] * 3
        + [pltpu.SemaphoreType.DMA] * 2
        + [sem(3, F), sem(3, F)]
        + share_sems()
        + scatter_scratch(C, Q, W)
        + local_scratch(C, Q, W)
        + (gather_sems(C) + scatter_scratch(C, Q // PARTS, W) + local_scratch(C, Q // PARTS, W)) * PARTS,
        compiler_params=params(3),
        name="k_mlp",
    )(gsecond, down, mid, go, gain2, *mlp_parts)
    output = out.reshape(tokens.shape)

    branch = gb.reshape(N, W)
    mlp_sum = jnp.concatenate([at(x, f, F) for x in mlp_parts], axis=2).astype(F32)
    for e in range(F - 1):
        mlp_sum = mlp_sum + mlp_got[e].astype(F32)
    mlp_sum = mlp_sum.astype(BF)
    mlp_grads = [at(mlp_sum, z, C)]
    mlp_grads += [hop(at(mlp_sum, z + d, C), "ctx", d) for d in range(1, C)]
    mlp_grads = jnp.stack(mlp_grads)
    ggated = nn(branch, w_o).reshape(C, S, B, HV)
    ggate = (ggated * normal * dsilu).astype(BF)
    gn = ggated * silu
    sums = pair(jnp.stack([jnp.sum(gn, axis=-1), jnp.sum(gn * normal, axis=-1)]))
    s1 = sum(x[0] for x in sums)[..., None] / HEAD_V
    s2 = sum(x[1] for x in sums)[..., None] / HEAD_V
    gmixer = (inv * (gn - s1 - normal * s2)).astype(BF)
    gscores = (ein("cste,csue->cstu", gmixer, v) * scale * table).astype(BF)
    pulled = ein("cstd,cste->csde", q_grown, gmixer)
    later = jnp.zeros_like(pulled[0])
    laters = [None] * C
    for c in reversed(range(C)):
        laters[c] = later.astype(BF)
        later = through[c] * later + pulled[c]
    laters = jnp.stack(laters)
    gq = ein("cstu,csud->cstd", gscores, k) + growth * ein("cste,csde->cstd", gmixer, states)
    gk = ein("cstu,cstd->csud", gscores, q) + keeping * ein("csue,csde->csud", v, laters)
    gv = ein("cstu,cste->csue", weights, gmixer) + ein("csud,csde->csue", k_kept, laters)
    gproj = jnp.concatenate([gq.astype(BF), gk.astype(BF), gv.astype(BF), ggate], axis=-1)
    gproj = gproj.reshape(N, NI)

    gnormed = nt(gproj, w_in).astype(BF).reshape(C, T, Q, W)
    in_parts = tn(normed, gproj).astype(BF).reshape(F, C, R, NI)
    out_parts = tn(branch, gated).astype(BF).reshape(F, C, R, HV)
    H = 2
    gt, gsum, vsum = pl.pallas_call(
        functools.partial(last_kernel, dims),
        out_shape=(sds((T, Q, W), BF), sds((C, R, NO), BF), sds((8, R), F32)),
        in_specs=[ANY, ANY, ANY, VMEM, ANY, VMEM, VMEM, VMEM],
        out_specs=[ANY, ANY, VMEM],
        scratch_shapes=[pltpu.VMEM((Q, W), BF)] * 2
        + [pltpu.SemaphoreType.DMA] * 2
        + share_sems()
        + [
            pltpu.VMEM((C, R, NO), BF),
            pltpu.VMEM((F - 1, C, R, NO), BF),
            pltpu.VMEM((C, R, NO), BF),
            sem(C, H),
            sem(H),
            sem(C, H, F),
            sem(C, H, F),
            sem(C, H),
            sem(C, H),
        ]
        + vector_scratch(F, C, R)
        + scatter_scratch(C, Q, W)
        + local_scratch(C, Q, W),
        compiler_params=params(4),
        name="k_last",
    )(gnormed, in_parts, out_parts, gm, tok, gain1, dgain2, dbias2)
    grad_tokens = gt.reshape(tokens.shape)

    def rel(n):
        return pl.BlockSpec((1, R, n), lambda c, z: (lax.rem(z[0] + C - c, C), 0, 0))

    def quarter(n):
        return pl.BlockSpec((R, n), lambda c, z: (0, c))

    per_head = pl.BlockSpec((R, KEY), lambda c, z: (0, c // halves))
    gq, gk, gv, gg, gw, gfg, gfu, gfd = pl.pallas_call(
        functools.partial(assemble_kernel, halves, KEY, HV),
        out_shape=[sds((R, heads * KEY), F32)] * 2
        + [sds((R, C * HV), F32)] * 3
        + [sds((R, C * U), F32)] * 3,
        grid_spec=pltpu.PrefetchScalarGridSpec(
            num_scalar_prefetch=1,
            grid=(C,),
            in_specs=[
                pl.BlockSpec((1, R, NO), lambda c, z: (c, 0, 0)),
                rel(3 * U),
            ],
            out_specs=[per_head, per_head] + [quarter(HV)] * 3 + [quarter(U)] * 3,
        ),
        name="k_assemble",
    )(jnp.full((1,), z, jnp.int32), gsum, mlp_grads)
    return (
        output,
        grad_tokens,
        gq,
        gk,
        gv,
        gg,
        gw,
        vsum[0],
        vsum[1],
        gfg,
        gfu,
        gfd,
        vsum[2],
        vsum[3],
    )


def solution(mesh):
    dims = (mesh.shape["fsdp"], mesh.shape["ctx"], mesh.shape["tp"])
    rows, vec = P(("fsdp", "ctx"), "tp"), P(("fsdp", "ctx"))
    acts = P("fsdp", "ctx", None)
    return jax.shard_map(
        functools.partial(shards, dims),
        mesh=mesh,
        in_specs=(acts, P("fsdp", "ctx", "tp"), rows, rows, rows, rows, rows, vec, vec, rows, rows, rows, vec, vec, acts),
        out_specs=(acts, acts, rows, rows, rows, rows, rows, vec, vec, rows, rows, rows, vec, vec),
        check_vma=False,
    )
```

```python
import functools

import jax
import jax.numpy as jnp
from jax import lax
from jax.experimental import pallas as pl
from jax.experimental.pallas import tpu as pltpu
from jax.sharding import PartitionSpec as P

KEY = 256
HEAD_V = 512
EPSILON = 1e-05
MESH = pl.DeviceIdType.MESH
ANY = pl.BlockSpec(memory_space=pl.ANY)
VMEM = pl.BlockSpec(memory_space=pltpu.VMEM)
BF = jnp.bfloat16
F32 = jnp.float32


def dot(a, b, dims):
    return lax.dot_general(a, b, (dims, ((), ())), preferred_element_type=F32)


def nn(a, b):
    return dot(a, b, ((1,), (0,)))


def nt(a, b):
    return dot(a, b, ((1,), (1,)))


def tn(a, b):
    return dot(a, b, ((0,), (0,)))


class Place:
    def __init__(self, F, C, T):
        self.F, self.C, self.T = F, C, T
        self.f = lax.axis_index("fsdp")
        self.z = lax.axis_index("ctx")
        self.t = lax.axis_index("tp")
        self.lo = lax.rem(self.t, 2)
        self.hi = self.t // 2
        self.near = self.t + 1 - 2 * self.lo
        self.far = lax.rem(self.t + 2, 4)

    def ahead(self, d):
        return lax.rem(self.z + d, self.C)

    def behind(self, d):
        return lax.rem(self.z + self.C - d, self.C)

    def fahead(self, d):
        return lax.rem(self.f + d, self.F)

    def fbehind(self, d):
        return lax.rem(self.f + self.F - d, self.F)

    def barrier(self, ctx=True, fsdp=False, tp=True):
        sem = pltpu.get_barrier_semaphore()
        peers = []
        if tp:
            peers += [{"tp": self.near}, {"tp": self.far}]
        if fsdp:
            peers += [{"fsdp": self.fahead(d)} for d in range(1, self.F)]
        if ctx:
            peers += [{"ctx": self.ahead(d)} for d in range(1, self.C)]
        for peer in peers:
            pl.semaphore_signal(sem, inc=1, device_id=peer, device_id_type=MESH)
        pl.semaphore_wait(sem, len(peers))


def remote(src, dst, ssem, rsem, peer):
    return pltpu.make_async_remote_copy(
        src_ref=src, dst_ref=dst, send_sem=ssem, recv_sem=rsem, device_id=peer, device_id_type=MESH
    )


def sem(*shape):
    return pltpu.SemaphoreType.DMA(shape)


def gather_sems(C):
    return [sem(2, C), sem(2, C), sem(2, C), sem(2, C), sem(2, C, 2), sem(2, C, 2), pltpu.SemaphoreType.DMA]


class Gather:
    def __init__(self, pc, x, slot, sems, own=None):
        self.pc, self.x, self.slot, self.block = pc, x, slot, own
        self.zs, self.zr, self.ys, self.yr, self.cs, self.cr, self.ls = sems

    def came(self, s, h):
        z = self.pc.z
        return (z >= h, z - h) if s == 0 else (z + h <= self.pc.C - 1, z + h)

    def goes(self, s, h):
        pc = self.pc
        if s == 0:
            return jnp.logical_and(pc.z >= h - 1, pc.z < pc.C - 1)
        return jnp.logical_and(pc.z + h <= pc.C, pc.z > 0)

    def hop(self, s, h, c):
        z = self.pc.z
        here = self.slot(c, self.pc.t)
        src = self.x if h == 1 else here
        return remote(src, here, self.zs.at[s, h], self.zr.at[s, h], {"ctx": z + 1 if s == 0 else z - 1})

    def to_far(self, s, h, c):
        here = self.slot(c, self.pc.t)
        src = here if h else self.x
        return remote(src, here, self.ys.at[s, h], self.yr.at[s, h], {"tp": self.pc.far})

    def to_near(self, s, h, c):
        here = self.slot(c, self.pc.t)
        src = here if h else self.x
        return remote(src, here, self.cs.at[s, h, 0], self.cr.at[s, h, 0], {"tp": self.pc.near})

    def spread(self, s, h, c):
        self.to_far(s, h, c).start()
        self.to_near(s, h, c).start()

    def again(self, s, h, c):
        there = self.slot(c, self.pc.far)
        return remote(there, there, self.cs.at[s, h, 1], self.cr.at[s, h, 1], {"tp": self.pc.near})

    def start(self):
        pc = self.pc
        for s in range(2):
            pl.when(self.goes(s, 1))(lambda s=s: self.hop(s, 1, pc.z).start())
        src, dst = self.block or (self.x, self.slot(pc.z, pc.t))
        self.local = pltpu.make_async_copy(src, dst, self.ls)
        self.local.start()
        if not self.block:
            self.spread(0, 0, pc.z)

    def forward(self, h):
        for s in range(2):
            ok, c = self.came(s, h)

            @pl.when(ok)
            def _(s=s, c=c):
                self.hop(s, h, c).wait_recv()
                if h + 1 < self.pc.C:
                    pl.when(self.goes(s, h + 1))(lambda: self.hop(s, h + 1, c).start())
                self.spread(s, h, c)

    def onward(self, h):
        if h == 0:
            if not self.block:
                self.to_far(0, 0, self.pc.z).wait_recv()
                self.again(0, 0, self.pc.z).start()
            return
        for s in range(2):
            ok, c = self.came(s, h)

            @pl.when(ok)
            def _(s=s, c=c):
                self.to_far(s, h, c).wait_recv()
                self.again(s, h, c).start()

    def settle(self, s, h, c):
        self.to_far(s, h, c).wait_send()
        self.to_near(s, h, c).wait()
        self.again(s, h, c).wait()

    def finish(self):
        pc = self.pc
        self.local.wait()
        if not self.block:
            self.settle(0, 0, pc.z)
        for h in range(1, pc.C):
            for s in range(2):
                ok, c = self.came(s, h)
                first = pc.z - h + 1 if s == 0 else pc.z + h - 1
                pl.when(self.goes(s, h))(lambda s=s, c=first: self.hop(s, h, c).wait_send())
                pl.when(ok)(lambda s=s, c=c: self.settle(s, h, c))


def share_sems():
    return [sem(3), sem(3)]


def share_stage(pc, x, out, lsem, sems):
    ss, rs = sems
    t = pc.t
    local = pltpu.make_async_copy(x, out.at[t], lsem)
    local.start()
    a = remote(x, out.at[t], ss.at[0], rs.at[0], {"tp": pc.far})
    a.start()
    b = remote(x, out.at[t], ss.at[1], rs.at[1], {"tp": pc.near})
    b.start()
    a.wait_recv()
    src = out.at[pc.far]
    c = remote(src, src, ss.at[2], rs.at[2], {"tp": pc.near})
    c.start()
    local.wait()
    a.wait_send()
    b.wait()
    c.wait()


def scatter_scratch(C, Q, W):
    return [
        pltpu.VMEM((C, 2, Q, W), BF),
        pltpu.VMEM((C, Q, W), BF),
        pltpu.VMEM((C, Q, W), BF),
        pltpu.VMEM((C, Q, W), BF),
        pltpu.VMEM((2, C, Q, W), BF),
        pltpu.VMEM((Q, W), F32),
        pltpu.VMEM((Q, W), F32),
        sem(C, 2),
        sem(C, 2),
        sem(C),
        sem(C),
        sem(2, C),
        sem(2, C),
    ]


def local_scratch(C, Q, W):
    return [pltpu.VMEM((C, 2, Q, W), BF), sem(C, 2)]


class Scatter:
    def __init__(self, pc, p, rows, scratch, local=None):
        self.pc, self.p, self.rows, self.local = pc, p, rows, local
        (self.buf1, self.snd2, self.buf2, self.snd3, self.buf3, self.tot, self.keep) = scratch[:7]
        self.s1, self.r1, self.s2, self.r2, self.s3, self.r3 = scratch[7:]
        mid = (pc.C - 1) / 2
        self.order = sorted(range(pc.C), key=lambda c: -abs(c - mid))
        self.lc, self.c1, self.c2 = {}, {}, {}

    def side(self, j):
        return 1 - self.pc.hi if j == 0 else self.pc.hi

    def begin(self, c):
        pc, p, rows = self.pc, self.p, self.rows
        for j in range(2):
            self.c1[c, j] = remote(
                p.at[c, self.side(j) * 2 + 1 - pc.lo, rows],
                self.buf1.at[c, j],
                self.s1.at[c, j],
                self.r1.at[c, j],
                {"tp": pc.near},
            )
            self.c1[c, j].start()
            if self.local:
                self.lc[c, j] = pltpu.make_async_copy(
                    p.at[c, self.side(j) * 2 + pc.lo, rows],
                    self.local[0].at[c, j],
                    self.local[1].at[c, j],
                )
                self.lc[c, j].start()

    def start(self):
        for c in self.order:
            self.begin(c)

    def own(self, c, j):
        self.c1[c, j].wait_recv()
        if self.local:
            self.lc[c, j].wait()
            here = self.local[0][c, j]
        else:
            here = self.p[c, self.side(j) * 2 + self.pc.lo, self.rows]
        return here.astype(F32) + self.buf1[c, j].astype(F32)

    def far_one(self, c):
        self.snd2[c] = self.own(c, 0).astype(BF)
        self.c2[c] = remote(
            self.snd2.at[c],
            self.buf2.at[c],
            self.s2.at[c],
            self.r2.at[c],
            {"tp": self.pc.far},
        )
        self.c2[c].start()

    def far(self):
        for c in self.order:
            self.far_one(c)

    def hop(self, s, c):
        z = self.pc.z
        return remote(
            self.snd3.at[c],
            self.buf3.at[s, c],
            self.s3.at[s, c],
            self.r3.at[s, c],
            {"ctx": z + 1 if s == 0 else z - 1},
        )

    def add(self, s, c):
        self.hop(s, c).wait_recv()
        self.tot[...] += self.buf3[s, c].astype(F32)

    def along(self, c):
        z, C = self.pc.z, self.pc.C
        part = self.own(c, 1)
        self.c2[c].wait_recv()
        part = part + self.buf2[c].astype(F32)

        def send(s):
            self.snd3[c] = self.tot[...].astype(BF)
            self.hop(s, c).start()

        self.tot[...] = part
        if c > 0:

            @pl.when(z < c)
            def _():
                pl.when(z > 0)(lambda: self.add(0, c))
                send(0)

        if c < C - 1:

            @pl.when(z > c)
            def _():
                pl.when(z < C - 1)(lambda: self.add(1, c))
                send(1)

        @pl.when(z == c)
        def _():
            self.keep[...] = part

    def result(self):
        z, C = self.pc.z, self.pc.C
        self.tot[...] = self.keep[...]
        pl.when(z > 0)(lambda: self.add(0, z))
        pl.when(z < C - 1)(lambda: self.add(1, z))
        return self.tot[...]

    def finish(self):
        z, C = self.pc.z, self.pc.C
        for copies in (self.c1, self.c2):
            for cp in copies.values():
                cp.wait_send()
        for c in range(C):
            if c > 0:
                pl.when(z < c)(lambda c=c: self.hop(0, c).wait_send())
            if c < C - 1:
                pl.when(z > c)(lambda c=c: self.hop(1, c).wait_send())


PARTS = 2


def halves_of(rows):
    n = rows // PARTS
    return (lambda h: pl.ds(h * n, n)), PARTS


def layer_norm_rows(values, gain, bias):
    center = values - jnp.mean(values, axis=-1, keepdims=True)
    spread = jnp.mean(center * center, axis=-1, keepdims=True)
    return (center * lax.rsqrt(spread + EPSILON) * gain + bias).astype(BF)


def eye_of(n):
    return lax.broadcasted_iota(jnp.int32, (n, n), 0) == lax.broadcasted_iota(jnp.int32, (n, n), 1)


def as_row(column):
    return jnp.sum(jnp.where(eye_of(column.shape[0]), column, 0.0), axis=0, keepdims=True)


def as_column(row):
    return jnp.sum(jnp.where(eye_of(row.shape[1]), row, 0.0), axis=1, keepdims=True)


def decays(rates):
    B = rates.shape[1]
    causal = lax.broadcasted_iota(jnp.int32, (B, B), 0) >= lax.broadcasted_iota(jnp.int32, (B, B), 1)
    column = jnp.sum(jnp.where(causal, rates, 0.0), axis=1, keepdims=True)
    row = as_row(column)
    table = jnp.where(causal, jnp.exp(jnp.minimum(column - row, 0.0)), 0.0)
    total = column[B - 1 :]
    return table, jnp.exp(column), jnp.exp(total - column), jnp.exp(total)


class Mover:
    def __init__(self, pc, weights, layout, out, zs, zr, xs, xr, ls):
        self.pc, self.weights, self.layout, self.out = pc, weights, layout, out
        self.zs, self.zr, self.xs, self.xr, self.ls = zs, zr, xs, xr, ls
        self.zc, self.xc = {}, {}

    def columns(self, dst):
        at = 0
        for w, (share, n) in zip(self.weights, self.layout):
            start = pl.multiple_of((dst // share) * n, n)
            yield w.at[:, pl.ds(start, n)], self.out.at[self.pc.f, self.pc.z, :, pl.ds(at, n)]
            at += n

    def start(self):
        pc = self.pc
        for d in range(1, pc.C):
            dst = pc.ahead(d)
            sems, peer = (self.zs.at[d], self.zr.at[d]), {"ctx": dst}
            for src, to in self.columns(dst):
                remote(src, to, *sems, peer).start()
            here = self.out.at[pc.f, pc.behind(d)]
            self.zc[d] = remote(here, here, *sems, peer)
        for e in range(1, pc.F):
            sems, peer = (self.xs.at[0, e], self.xr.at[0, e]), {"fsdp": pc.fahead(e)}
            for src, to in self.columns(pc.z):
                remote(src, to, *sems, peer).start()
            here = self.out.at[pc.fbehind(e), pc.z]
            self.xc[0, e] = remote(here, here, *sems, peer)
        for src, to in self.columns(pc.z):
            pltpu.make_async_copy(src, to, self.ls).start()
        here = self.out.at[pc.f, pc.z]
        self.local = pltpu.make_async_copy(here, here, self.ls)

    def forward(self, d):
        pc = self.pc
        self.zc[d].wait_recv()
        here = self.out.at[pc.f, pc.behind(d)]
        for e in range(1, pc.F):
            self.xc[d, e] = remote(
                here, here, self.xs.at[d, e], self.xr.at[d, e], {"fsdp": pc.fahead(e)}
            )
            self.xc[d, e].start()

    def arrived(self, d, e):
        self.xc[d, e].wait_recv()

    def sent(self):
        for cp in list(self.zc.values()) + list(self.xc.values()):
            cp.wait_send()


def mover_sems(F, C):
    return [sem(C), sem(C), sem(C, F), sem(C, F), pltpu.SemaphoreType.DMA]


def forward_kernel(dims, cfg, *refs):
    F, C, T = dims
    S, B, halves, HV, in_layout, rest_layout = cfg
    refs = list(refs)

    def take(n):
        out = refs[:n]
        del refs[:n]
        return out

    in_weights, rest_weights = take(5), take(3)
    vec, ld, tok, go = take(4)
    o_win, o_normed, o_proj, o_states, o_normal, o_inv, o_gated, old, vecs, mid, sn, full, ogo = take(13)
    otok, win, ovec, normed, acc, proj, states, state, normal, inv, gated, stats, mytok, x = take(14)
    in_sems, rest_sems = take(5), take(5)
    tok_sems, go_sems = take(7), take(7)
    vzs, vzr, vxs, vxr, lzs, lzr, sts, strr, oses = take(9)
    n, m = len(gather_sems(C)), len(scatter_scratch(C, 8, 128))

    pc = Place(*dims)
    f, z, t = pc.f, pc.z, pc.t
    L = S * B
    R = win.shape[2]
    W = F * C * R
    NI = proj.shape[1]
    N = proj.shape[0]
    units = C * S
    saved = []

    def save(src, dst):
        cp = pltpu.make_async_copy(src, dst, oses.at[len(saved)])
        cp.start()
        saved.append(cp)

    pc.barrier(True, True, True)
    vz, vx, lz = {}, {}, {}
    for d in range(1, C):
        peer = {"ctx": pc.ahead(d)}
        vz[d] = remote(vec, ovec.at[f, z], vzs.at[d], vzr.at[d], peer)
        vz[d].start()
        lz[d] = remote(ld, old.at[z], lzs.at[d], lzr.at[d], peer)
        lz[d].start()
    ovec[f, z] = vec[...]
    old[z] = ld[...]

    def vec_across(d):
        for e in range(1, F):
            src = ovec.at[f, pc.behind(d)] if d else vec
            vx[d, e] = remote(
                src, ovec.at[f, pc.behind(d)], vxs.at[d, e], vxr.at[d, e], {"fsdp": pc.fahead(e)}
            )
            vx[d, e].start()

    vec_across(0)
    tk = Gather(pc, tok.at[t], lambda c, i: otok.at[c, i], tok_sems, (tok, otok.at[z]))
    tk.start()
    wi = Mover(pc, in_weights, in_layout, win, *in_sems)
    wi.start()
    mine = pltpu.make_async_copy(tok.at[t], mytok, oses.at[15])
    mine.start()
    for d in range(1, C):
        vz[d].wait_recv()
        vec_across(d)
        tk.forward(d)
    gk = Gather(pc, go.at[t], lambda c, i: ogo.at[c, i], go_sems, (go, ogo.at[z]))
    gk.start()
    wr = Mover(pc, rest_weights, rest_layout, full, *rest_sems)
    wr.start()
    for d in range(1, C):
        tk.onward(d)
    for cp in vx.values():
        cp.wait()
    for cp in vz.values():
        cp.wait_send()
    for b in range(F * C):
        vecs[:, b * R : (b + 1) * R] = ovec[b // C, b % C]
    tk.finish()
    gain1, bias1 = vecs[0:1], vecs[1:2]

    def norm_unit(i, carry):
        rows = otok[i // T, lax.rem(i, T)].astype(F32)
        q = rows.shape[0]
        normed[pl.ds(pl.multiple_of(i * q, q), q)] = layer_norm_rows(rows, gain1, bias1)
        return carry

    lax.fori_loop(0, C * T, norm_unit, 0)
    save(normed, o_normed)

    tile = min(256, N)

    def project(ff, c, first, last):
        columns = pl.ds(pl.multiple_of((ff * C + c) * R, 128), R)

        def one(i, carry):
            rows = pl.ds(pl.multiple_of(i * tile, tile), tile)
            part = nn(normed[rows, columns], win[ff, c, :, :NI])
            if not first:
                part = part + acc[rows]
            if last:
                proj[rows] = part.astype(BF)
            else:
                acc[rows] = part
            return carry

        lax.fori_loop(0, N // tile, one, 0)

    wi.local.wait()
    project(f, z, True, False)
    for d in range(1, C):
        wi.forward(d)
        for e in range(1, F):
            wi.arrived(d - 1, e)
            project(pc.fbehind(e), pc.behind(d - 1), False, False)
        project(f, pc.behind(d), False, False)
    for e in range(1, F):
        wi.arrived(C - 1, e)
        project(pc.fbehind(e), pc.behind(C - 1), False, e == F - 1)
    save(proj, o_proj)
    save(win, o_win)

    for cp in lz.values():
        cp.wait()
    head = z // halves
    scale = float(KEY) ** (-0.5)
    state[...] = jnp.zeros_like(state)

    def retain(u, carry):
        c, s = u // S, lax.rem(u, S)
        rows = pl.ds(pl.multiple_of(u * B, B), B)
        rates = old[c, pl.ds(head, 1), pl.ds(pl.multiple_of(s * B, B), B)]
        table, growth, keeping, through = decays(rates)
        q, k, v = proj[rows, :KEY], proj[rows, KEY : 2 * KEY], proj[rows, 2 * KEY : 2 * KEY + HV]
        weights = (nt(q, k) * scale * table).astype(BF)
        before = state[s]
        states[u] = before.astype(BF)
        mixed = nn(weights, v) + nn((q.astype(F32) * growth).astype(BF), before.astype(BF))
        state[s] = through * before + tn((k.astype(F32) * keeping).astype(BF), v)
        normal[rows] = mixed
        mean = jnp.mean(mixed, axis=-1, keepdims=True)
        dev = mixed - mean
        stats[0, 0:1, rows] = as_row(mean)
        stats[0, 1:2, rows] = as_row(jnp.sum(dev * dev, axis=-1, keepdims=True))
        return carry

    stats[0] = jnp.zeros(stats.shape[1:], F32)
    lax.fori_loop(0, units, retain, 0)
    save(states, o_states)
    for d in range(1, C):
        gk.forward(d)
    st = []
    place = lax.rem(z, halves)
    for j in range(1, halves):
        peer = {"ctx": z - place + lax.rem(place + j, halves)}
        cp = remote(stats.at[0], stats.at[j], sts.at[j], strr.at[j], peer)
        cp.start()
        st.append(cp)
    for cp in st:
        cp.wait()

    def finish_unit(u, carry):
        rows = pl.ds(pl.multiple_of(u * B, B), B)
        got = [(stats[j, 0:1, rows], stats[j, 1:2, rows]) for j in range(halves)]
        mean = sum(a for a, _ in got) / halves
        m2 = sum(b + HV * (a - mean) * (a - mean) for a, b in got)
        scaled = as_column(lax.rsqrt(m2 / HEAD_V + EPSILON))
        value = (normal[rows] - as_column(mean)) * scaled
        gate = proj[rows, 2 * KEY + HV :].astype(F32)
        normal[rows] = value
        inv[rows] = jnp.broadcast_to(scaled, (B, 128))
        gated[rows] = (gate * jax.nn.sigmoid(gate) * value).astype(BF)
        return carry

    lax.fori_loop(0, units, finish_unit, 0)
    save(normal, o_normal)
    save(inv, o_inv)
    save(gated, o_gated)

    p = otok
    Q = x.shape[0]
    cut, parts = halves_of(Q)
    scatters, gathers = [], []
    for h in range(parts):
        at = h * (n + m)
        slot = lambda c, i, h=h: sn.at[c, i, cut(h)]
        gathers.append(Gather(pc, x.at[cut(h)], slot, refs[at : at + n]))
        scatters.append(Scatter(pc, p, cut(h), refs[at + n : at + n + m]))
    for c in scatters[0].order:
        mixed = gated[c * L : (c + 1) * L]

        def one(b, carry, c=c, mixed=mixed):
            part = nt(mixed, win[b // C, lax.rem(b, C), :, NI:]).astype(BF)
            columns = pl.ds(pl.multiple_of(b * R, 128), R)
            for i in range(T):
                p[c, i, :, columns] = part[i * Q : (i + 1) * Q]
            return carry

        lax.fori_loop(0, F * C, one, 0)
        for rs in scatters:
            rs.begin(c)
    for rs in scatters:
        rs.far()
    for d in range(1, C):
        gk.onward(d)
    for rs in scatters:
        for d in rs.order:
            rs.along(d)
    for d in range(1, C):
        wr.forward(d)
    mine.wait()
    for h, rs in enumerate(scatters):
        part = cut(h)
        total = rs.result() + mytok[part].astype(F32)
        mid[part] = total
        x[part] = layer_norm_rows(total, vecs[2:3], vecs[3:4])
        gathers[h].start()
    for ga in gathers:
        for d in range(1, C):
            ga.forward(d)
    for ga in gathers:
        for d in range(C):
            ga.onward(d)
    for job in scatters + gathers:
        job.finish()
    gk.finish()
    wi.sent()
    wr.local.wait()
    for d in range(C):
        for e in range(1, F):
            wr.arrived(d, e)
    wr.sent()
    for cp in saved:
        cp.wait()


def norm_pull(values, gain, grad):
    center = values - jnp.mean(values, axis=-1, keepdims=True)
    spread = jnp.mean(center * center, axis=-1, keepdims=True)
    inv = lax.rsqrt(spread + EPSILON)
    xhat = center * inv
    g = grad * gain
    back = inv * (
        g - jnp.mean(g, axis=-1, keepdims=True) - xhat * jnp.mean(g * xhat, axis=-1, keepdims=True)
    )
    return (
        back,
        jnp.sum(grad * xhat, axis=0, keepdims=True),
        jnp.sum(grad, axis=0, keepdims=True),
    )


def mlp_kernel(
    dims, pg, pd, mid, allgo, gain, g0, g1, g2, gm, gb, out, dgain, dbias, xg, x, y, go, lsem, gosem, gxs, gxr, *scratch
):
    pc = Place(*dims)
    C = pc.C
    mine = pltpu.make_async_copy(allgo.at[pc.t], go, gosem)
    mine.start()
    pc.barrier(True, True, True)
    n, m = len(gather_sems(C)), len(scatter_scratch(C, 8, 128))
    ss, scratch = scratch[:2], scratch[2:]
    rd = Scatter(pc, pd, pl.ds(0, x.shape[0]), scratch[:m], scratch[m : m + 2])
    scratch = scratch[m + 2 :]
    cut, parts = halves_of(x.shape[0])
    scatters, gathers = [], []
    for h in range(parts):
        at = h * (n + m + 2)
        slot = lambda c, i, h=h: gb.at[c, i, cut(h)]
        gathers.append(Gather(pc, x.at[cut(h)], slot, scratch[at : at + n]))
        at += n
        scatters.append(Scatter(pc, pg, cut(h), scratch[at : at + m], scratch[at + m : at + m + 2]))
    for rs in scatters:
        rs.start()
    rd.start()
    moves = []
    u = g0.shape[3]
    for i, g in enumerate((g0, g1, g2)):
        for e in range(1, pc.F):
            cp = remote(
                g.at[pc.fahead(e)],
                xg.at[e - 1, :, :, pl.ds(i * u, u)],
                gxs.at[i, e],
                gxr.at[i, e],
                {"fsdp": pc.fahead(e)},
            )
            cp.start()
            moves.append(cp)
    for rs in scatters:
        rs.far()
    rd.far()
    mine.wait()
    for h, rs in enumerate(scatters):
        for d in rs.order:
            rs.along(d)
        part = cut(h)
        back, dg, db = norm_pull(mid[part], gain[...], rs.result())
        dgain[...] = dgain[...] + dg if h else dg
        dbias[...] = dbias[...] + db if h else db
        grad_middle = go[part].astype(F32) + back
        gm[part] = grad_middle
        x[part] = grad_middle.astype(BF)
        gathers[h].start()
    for d in rd.order[:2]:
        rd.along(d)
    for d in range(1, C):
        gathers[0].forward(d)
    for d in rd.order[2:]:
        rd.along(d)
    for ga in gathers[1:]:
        for d in range(1, C):
            ga.forward(d)
    for d in range(C):
        for ga in gathers:
            ga.onward(d)
    y[...] = (mid[...] + rd.result()).astype(BF)
    share_stage(pc, y, out, lsem, ss)
    for job in scatters + gathers + [rd]:
        job.finish()
    for cp in moves:
        cp.wait()


class GradScatter:
    def __init__(self, pc, grads, out, own, xbuf, zsnd, ls, os, xs, xr, zs, zr):
        self.pc, self.grads, self.out = pc, grads, out
        self.own, self.xbuf, self.zsnd = own, xbuf, zsnd
        self.sems = (ls, os, xs, xr, zs, zr)
        C = pc.C
        self.H = os.shape[0]
        self.rows = own.shape[1] // self.H
        far = sorted(range(1, C), key=lambda d: abs(d - C // 2))
        self.order = [(d, h) for d in far + [0] for h in range(self.H)]

    def start(self):
        pc = self.pc
        ls, os, xs, xr, zs, zr = self.sems
        self.loc, self.xc, self.zc, self.keep, self.sent = {}, {}, {}, {}, []
        for d, h in self.order:
            c = pc.ahead(d)
            part = pl.ds(h * self.rows, self.rows)
            at = 0
            for g in self.grads:
                n = g.shape[3]
                for e in range(1, pc.F):
                    remote(
                        g.at[pc.fahead(e), c, part],
                        self.xbuf.at[e - 1, d, part, pl.ds(at, n)],
                        xs.at[d, h, e],
                        xr.at[d, h, e],
                        {"fsdp": pc.fahead(e)},
                    ).start()
                pltpu.make_async_copy(
                    g.at[pc.f, c, part], self.own.at[d, part, pl.ds(at, n)], ls.at[d, h]
                ).start()
                at += n
            here = self.own.at[d, part]
            self.loc[d, h] = pltpu.make_async_copy(here, here, ls.at[d, h])
            for e in range(1, pc.F):
                there = self.xbuf.at[e - 1, d, part]
                self.xc[d, h, e] = remote(
                    there, there, xs.at[d, h, e], xr.at[d, h, e], {"fsdp": pc.fahead(e)}
                )
        self.todo = list(self.order)

    def step(self, count=1):
        pc = self.pc
        ls, os, xs, xr, zs, zr = self.sems
        for _ in range(count):
            if not self.todo:
                return
            d, h = self.todo.pop(0)
            part = pl.ds(h * self.rows, self.rows)
            self.loc[d, h].wait()
            total = self.own[d, part].astype(F32)
            for e in range(1, pc.F):
                self.xc[d, h, e].wait_recv()
                total = total + self.xbuf[e - 1, d, part].astype(F32)
            self.zsnd[d, part] = total.astype(BF)
            src, dst = self.zsnd.at[d, part], self.out.at[pc.z, part]
            if d:
                self.zc[d, h] = remote(src, dst, zs.at[d, h], zr.at[d, h], {"ctx": pc.ahead(d)})
                self.zc[d, h].start()
            else:
                self.keep[h] = pltpu.make_async_copy(src, dst, os.at[h])
                self.keep[h].start()

    def finish(self):
        for cp in self.keep.values():
            cp.wait()
        for cp in self.zc.values():
            cp.wait()
        for cp in self.xc.values():
            cp.wait_send()


def vector_stage(pc, v, vout, va, vb, vc, vd, vx, vz, ts, tr, vxs, vxr, vzs, vzr):
    F, C = pc.F, pc.C
    t0 = remote(v, vb, ts.at[0], tr.at[0], {"tp": pc.near})
    t0.start()
    t0.wait_recv()
    va[...] = v[...] + vb[...]
    t1 = remote(va, vc, ts.at[1], tr.at[1], {"tp": pc.far})
    t1.start()
    t1.wait_recv()
    vd[...] = va[...] + vc[...]
    vxc, vzc = {}, {}
    for e in range(1, F):
        vxc[e] = remote(
            vd.at[pc.fahead(e)], vx.at[e - 1], vxs.at[e], vxr.at[e], {"fsdp": pc.fahead(e)}
        )
        vxc[e].start()
    vs = vd[pc.f]
    for e in range(1, F):
        vxc[e].wait_recv()
        vs = vs + vx[e - 1]
    vz[0] = vs
    for d in range(1, C):
        vzc[d] = remote(
            vz.at[0, pc.ahead(d)], vz.at[1, d], vzs.at[d], vzr.at[d], {"ctx": pc.ahead(d)}
        )
        vzc[d].start()
    acc = vz[0, pc.z]
    for d in range(1, C):
        vzc[d].wait_recv()
        acc = acc + vz[1, d]
    vout[...] = acc
    for cp in [t0, t1] + list(vxc.values()) + list(vzc.values()):
        cp.wait_send()


def vector_scratch(F, C, R):
    full = pltpu.VMEM((F, C, 8, R), F32)
    return [
        full,
        full,
        full,
        full,
        full,
        pltpu.VMEM((F - 1, C, 8, R), F32),
        pltpu.VMEM((2, C, 8, R), F32),
        sem(2),
        sem(2),
        sem(F),
        sem(F),
        sem(C),
        sem(C),
    ]


def last_kernel(
    dims, p, g0, g1, gm, alltok, gain, dg2, db2, gt, gout, vout, y, tok, lsem, toksem, s0, s1, *scratch
):
    pc = Place(*dims)
    mine = pltpu.make_async_copy(alltok.at[pc.t], tok, toksem)
    mine.start()
    F, C, T = dims
    pc.barrier(True, True, True)
    gr = GradScatter(pc, (g0, g1), gout, *scratch[:9])
    v, rest = scratch[9], scratch[10:22]
    rs = Scatter(pc, p, pl.ds(0, y.shape[0]), scratch[22:-2], scratch[-2:])
    rs.start()
    gr.start()
    rs.far()
    for d in rs.order:
        rs.along(d)
        gr.step()
    mine.wait()
    back, dg, db = norm_pull(tok[...].astype(F32), gain[...], rs.result())
    y[...] = (gm[...] + back).astype(BF)
    R = v.shape[3]
    for i in range(F * C):
        rows = [r[:, i * R : (i + 1) * R] for r in (dg, db)] + [
            r[:, i * R : (i + 1) * R] for r in (dg2, db2)
        ]
        v[i // C, i % C] = jnp.concatenate(rows + [jnp.zeros((4, R), F32)], axis=0)
    gr.step(len(gr.todo))
    share_stage(pc, y, gt, lsem, (s0, s1))
    vector_stage(pc, v, vout, *rest)
    gr.finish()
    rs.finish()


def assemble_kernel(halves, key, hv, z, a, m, q, k, v, g, o, fg, fu, fd):
    c = pl.program_id(0)
    first = lax.rem(c, halves) == 0
    for i, ref in enumerate((q, k)):
        x = a[0, :, i * key : (i + 1) * key].astype(F32)

        @pl.when(first)
        def _(ref=ref, x=x):
            ref[...] = x

        @pl.when(jnp.logical_not(first))
        def _(ref=ref, x=x):
            ref[...] += x

    v[...] = a[0, :, 2 * key : 2 * key + hv].astype(F32)
    g[...] = a[0, :, 2 * key + hv : 2 * key + 2 * hv].astype(F32)
    o[...] = a[0, :, 2 * key + 2 * hv :].astype(F32)
    u = fg.shape[1]
    for i, ref in enumerate((fg, fu, fd)):
        ref[...] = m[0, :, i * u : (i + 1) * u].astype(F32)


def params(cid):
    return pltpu.CompilerParams(collective_id=cid, has_side_effects=True)


def silu_parts(g):
    s = jax.nn.sigmoid(g)
    return g * s, s * (1.0 + g * (1.0 - s))


def shards(
    dims,
    tokens,
    log_decay,
    w_query,
    w_key,
    w_value,
    w_gate,
    w_out,
    norm1_gain,
    norm1_bias,
    w_ffgate,
    w_ffup,
    w_down,
    norm2_gain,
    norm2_bias,
    grad_out,
):
    F, C, T = dims
    S, B, W = tokens.shape
    L = S * B
    Q = L // T
    N = C * L
    R = w_query.shape[0]
    heads = log_decay.shape[2]
    halves = C // heads
    HV = HEAD_V // halves
    U = w_ffgate.shape[1] // C
    z = lax.axis_index("ctx")
    t = lax.axis_index("tp")
    scale = float(KEY) ** (-0.5)

    f = lax.axis_index("fsdp")

    def hop(x, axis, d):
        n = lax.axis_size(axis)
        return lax.ppermute(x, axis, [(i, (i + d) % n) for i in range(n)])

    def at(x, i, n):
        return lax.dynamic_index_in_dim(x, lax.rem(i, n), 0, False)

    NI, NR = 2 * KEY + 2 * HV, 3 * U
    NO = NI + HV
    vec = jnp.stack([norm1_gain, norm1_bias, norm2_gain, norm2_bias]).astype(F32)
    vec = jnp.pad(vec, ((0, 4), (0, 0)))
    ld = jnp.pad(jnp.transpose(log_decay, (2, 0, 1)).reshape(heads, L), ((0, 8 - heads), (0, 0)))
    tok = tokens.reshape(T, Q, W)
    go = grad_out.reshape(T, Q, W)
    sds = jax.ShapeDtypeStruct
    cfg = (
        S,
        B,
        halves,
        HV,
        ((halves, KEY), (halves, KEY), (1, HV), (1, HV), (1, HV)),
        ((1, U), (1, U), (1, U)),
    )
    owin, normed, proj, states, normal, inv, gated, old, vecs, mid, sn, full, ogo = pl.pallas_call(
        functools.partial(forward_kernel, dims, cfg),
        out_shape=(
            sds((F, C, R, NO), BF),
            sds((N, W), BF),
            sds((N, NI), BF),
            sds((C * S, KEY, HV), BF),
            sds((N, HV), F32),
            sds((N, 128), F32),
            sds((N, HV), BF),
            sds((C, 8, L), F32),
            sds((8, W), F32),
            sds((Q, W), F32),
            sds((C, T, Q, W), BF),
            sds((F, C, R, NR), BF),
            sds((C, T, Q, W), BF),
        ),
        in_specs=[ANY] * 8 + [VMEM, VMEM, ANY, ANY],
        out_specs=[ANY] * 7 + [VMEM] * 3 + [ANY] * 3,
        scratch_shapes=[
            pltpu.VMEM((C, T, Q, W), BF),
            pltpu.VMEM((F, C, R, NO), BF),
            pltpu.VMEM((F, C, 8, R), F32),
            pltpu.VMEM((N, W), BF),
            pltpu.VMEM((N, NI), F32),
            pltpu.VMEM((N, NI), BF),
            pltpu.VMEM((C * S, KEY, HV), BF),
            pltpu.VMEM((S, KEY, HV), F32),
            pltpu.VMEM((N, HV), F32),
            pltpu.VMEM((N, 128), F32),
            pltpu.VMEM((N, HV), BF),
            pltpu.VMEM((halves, 8, N), F32),
            pltpu.VMEM((Q, W), BF),
            pltpu.VMEM((Q, W), BF),
        ]
        + mover_sems(F, C) * 2
        + gather_sems(C) * 2
        + [sem(C), sem(C), sem(C, F), sem(C, F), sem(C), sem(C), sem(halves), sem(halves), sem(16)]
        + (gather_sems(C) + scatter_scratch(C, Q // PARTS, W)) * PARTS,
        compiler_params=params(1),
        name="k_forward",
    )(w_query, w_key, w_value, w_gate, w_out, w_ffgate, w_ffup, w_down, vec, ld, tok, go)
    gain1, gain2 = vecs[0:1], vecs[2:3]
    w_all = owin.reshape(W, NO)
    w_in, w_o = w_all[:, :NI], w_all[:, NI:]
    w_rest = full.reshape(W, NR)
    w_fg, w_fu, w_d = w_rest[:, :U], w_rest[:, U : 2 * U], w_rest[:, 2 * U :]

    q = proj[:, :KEY].reshape(C, S, B, KEY)
    k = proj[:, KEY : 2 * KEY].reshape(C, S, B, KEY)
    v = proj[:, 2 * KEY : 2 * KEY + HV].reshape(C, S, B, HV)
    g = proj[:, 2 * KEY + HV :].reshape(C, S, B, HV).astype(F32)
    rates = lax.dynamic_index_in_dim(old, z // halves, 1, False).reshape(C, S, B)
    cum = jnp.cumsum(rates, axis=-1)
    total = cum[..., -1]
    positions = jnp.arange(B)
    causal = positions[:, None] >= positions[None, :]
    table = jnp.where(
        causal, jnp.exp(jnp.minimum(cum[..., :, None] - cum[..., None, :], 0.0)), 0.0
    )
    growth = jnp.exp(cum)[..., None]
    keeping = jnp.exp(total[..., None] - cum)[..., None]
    through = jnp.exp(total)[..., None, None]

    def ein(spec, a, b):
        return jnp.einsum(spec, a, b, preferred_element_type=F32)

    weights = (ein("cstd,csud->cstu", q, k) * scale * table).astype(BF)
    q_grown = (q.astype(F32) * growth).astype(BF)
    k_kept = (k.astype(F32) * keeping).astype(BF)
    def pair(stats):
        got = [stats]
        for j in range(1, halves):
            perm = []
            for c in range(C):
                base = c - c % halves
                perm.append((c, base + (c % halves + j) % halves))
            got.append(lax.ppermute(stats, "ctx", perm))
        return got

    silu, dsilu = silu_parts(g)
    normal = normal.reshape(C, S, B, HV)
    inv = inv[:, :1].reshape(C, S, B, 1)
    states = states.reshape(C, S, KEY, HV)
    second = sn.reshape(N, W)
    ff_gate = nn(second, w_fg).astype(BF)
    ff_up = nn(second, w_fu).astype(BF)
    hidden, gelu_pull = jax.vjp(
        lambda a, b: jax.nn.gelu(a, approximate=True) * b, ff_gate.astype(F32), ff_up.astype(F32)
    )
    hidden = hidden.astype(BF)
    down = nt(hidden, w_d).astype(BF).reshape(C, T, Q, W)
    gout = ogo.reshape(N, W)
    grad_hidden = nn(gout, w_d)
    gfg, gfu = gelu_pull(grad_hidden)
    gfg, gfu = gfg.astype(BF), gfu.astype(BF)
    gsecond = (nt(gfg, w_fg) + nt(gfu, w_fu)).astype(BF).reshape(C, T, Q, W)
    mlp_parts = [
        tn(a, b).astype(BF).reshape(F, C, R, U)
        for a, b in ((second, gfg), (second, gfu), (gout, hidden))
    ]
    gm, gb, out, dgain2, dbias2, mlp_got = pl.pallas_call(
        functools.partial(mlp_kernel, dims),
        out_shape=(
            sds((Q, W), F32),
            sds((C, T, Q, W), BF),
            sds((T, Q, W), BF),
            sds((1, W), F32),
            sds((1, W), F32),
            sds((F - 1, C, R, NR), BF),
        ),
        in_specs=[ANY, ANY, VMEM, ANY, VMEM, ANY, ANY, ANY],
        out_specs=[VMEM, ANY, ANY, VMEM, VMEM, ANY],
        scratch_shapes=[pltpu.VMEM((Q, W), BF)] * 3
        + [pltpu.SemaphoreType.DMA] * 2
        + [sem(3, F), sem(3, F)]
        + share_sems()
        + scatter_scratch(C, Q, W)
        + local_scratch(C, Q, W)
        + (gather_sems(C) + scatter_scratch(C, Q // PARTS, W) + local_scratch(C, Q // PARTS, W)) * PARTS,
        compiler_params=params(3),
        name="k_mlp",
    )(gsecond, down, mid, go, gain2, *mlp_parts)
    output = out.reshape(tokens.shape)

    branch = gb.reshape(N, W)
    mlp_sum = jnp.concatenate([at(x, f, F) for x in mlp_parts], axis=2).astype(F32)
    for e in range(F - 1):
        mlp_sum = mlp_sum + mlp_got[e].astype(F32)
    mlp_sum = mlp_sum.astype(BF)
    mlp_grads = [at(mlp_sum, z, C)]
    mlp_grads += [hop(at(mlp_sum, z + d, C), "ctx", d) for d in range(1, C)]
    mlp_grads = jnp.stack(mlp_grads)
    ggated = nn(branch, w_o).reshape(C, S, B, HV)
    ggate = (ggated * normal * dsilu).astype(BF)
    gn = ggated * silu
    sums = pair(jnp.stack([jnp.sum(gn, axis=-1), jnp.sum(gn * normal, axis=-1)]))
    s1 = sum(x[0] for x in sums)[..., None] / HEAD_V
    s2 = sum(x[1] for x in sums)[..., None] / HEAD_V
    gmixer = (inv * (gn - s1 - normal * s2)).astype(BF)
    gscores = (ein("cste,csue->cstu", gmixer, v) * scale * table).astype(BF)
    pulled = ein("cstd,cste->csde", q_grown, gmixer)
    later = jnp.zeros_like(pulled[0])
    laters = [None] * C
    for c in reversed(range(C)):
        laters[c] = later.astype(BF)
        later = through[c] * later + pulled[c]
    laters = jnp.stack(laters)
    gq = ein("cstu,csud->cstd", gscores, k) + growth * ein("cste,csde->cstd", gmixer, states)
    gk = ein("cstu,cstd->csud", gscores, q) + keeping * ein("csue,csde->csud", v, laters)
    gv = ein("cstu,cste->csue", weights, gmixer) + ein("csud,csde->csue", k_kept, laters)
    gproj = jnp.concatenate([gq.astype(BF), gk.astype(BF), gv.astype(BF), ggate], axis=-1)
    gproj = gproj.reshape(N, NI)

    gnormed = nt(gproj, w_in).astype(BF).reshape(C, T, Q, W)
    in_parts = tn(normed, gproj).astype(BF).reshape(F, C, R, NI)
    out_parts = tn(branch, gated).astype(BF).reshape(F, C, R, HV)
    H = 2
    gt, gsum, vsum = pl.pallas_call(
        functools.partial(last_kernel, dims),
        out_shape=(sds((T, Q, W), BF), sds((C, R, NO), BF), sds((8, R), F32)),
        in_specs=[ANY, ANY, ANY, VMEM, ANY, VMEM, VMEM, VMEM],
        out_specs=[ANY, ANY, VMEM],
        scratch_shapes=[pltpu.VMEM((Q, W), BF)] * 2
        + [pltpu.SemaphoreType.DMA] * 2
        + share_sems()
        + [
            pltpu.VMEM((C, R, NO), BF),
            pltpu.VMEM((F - 1, C, R, NO), BF),
            pltpu.VMEM((C, R, NO), BF),
            sem(C, H),
            sem(H),
            sem(C, H, F),
            sem(C, H, F),
            sem(C, H),
            sem(C, H),
        ]
        + vector_scratch(F, C, R)
        + scatter_scratch(C, Q, W)
        + local_scratch(C, Q, W),
        compiler_params=params(4),
        name="k_last",
    )(gnormed, in_parts, out_parts, gm, tok, gain1, dgain2, dbias2)
    grad_tokens = gt.reshape(tokens.shape)

    def rel(n):
        return pl.BlockSpec((1, R, n), lambda c, z: (lax.rem(z[0] + C - c, C), 0, 0))

    def quarter(n):
        return pl.BlockSpec((R, n), lambda c, z: (0, c))

    per_head = pl.BlockSpec((R, KEY), lambda c, z: (0, c // halves))
    gq, gk, gv, gg, gw, gfg, gfu, gfd = pl.pallas_call(
        functools.partial(assemble_kernel, halves, KEY, HV),
        out_shape=[sds((R, heads * KEY), F32)] * 2
        + [sds((R, C * HV), F32)] * 3
        + [sds((R, C * U), F32)] * 3,
        grid_spec=pltpu.PrefetchScalarGridSpec(
            num_scalar_prefetch=1,
            grid=(C,),
            in_specs=[
                pl.BlockSpec((1, R, NO), lambda c, z: (c, 0, 0)),
                rel(3 * U),
            ],
            out_specs=[per_head, per_head] + [quarter(HV)] * 3 + [quarter(U)] * 3,
        ),
        name="k_assemble",
    )(jnp.full((1,), z, jnp.int32), gsum, mlp_grads)
    return (
        output,
        grad_tokens,
        gq,
        gk,
        gv,
        gg,
        gw,
        vsum[0],
        vsum[1],
        gfg,
        gfu,
        gfd,
        vsum[2],
        vsum[3],
    )


def solution(mesh):
    dims = (mesh.shape["fsdp"], mesh.shape["ctx"], mesh.shape["tp"])
    rows, vec = P(("fsdp", "ctx"), "tp"), P(("fsdp", "ctx"))
    acts = P("fsdp", "ctx", None)
    return jax.shard_map(
        functools.partial(shards, dims),
        mesh=mesh,
        in_specs=(acts, P("fsdp", "ctx", "tp"), rows, rows, rows, rows, rows, vec, vec, rows, rows, rows, vec, vec, acts),
        out_specs=(acts, acts, rows, rows, rows, rows, rows, vec, vec, rows, rows, rows, vec, vec),
        check_vma=False,
    )
```

```python
import functools

import jax
import jax.numpy as jnp
from jax import lax
from jax.experimental import pallas as pl
from jax.experimental.pallas import tpu as pltpu
from jax.sharding import PartitionSpec as P

KEY = 256
HEAD_V = 512
EPSILON = 1e-05
MESH = pl.DeviceIdType.MESH
ANY = pl.BlockSpec(memory_space=pl.ANY)
VMEM = pl.BlockSpec(memory_space=pltpu.VMEM)
BF = jnp.bfloat16
F32 = jnp.float32


def dot(a, b, dims):
    return lax.dot_general(a, b, (dims, ((), ())), preferred_element_type=F32)


def nn(a, b):
    return dot(a, b, ((1,), (0,)))


def nt(a, b):
    return dot(a, b, ((1,), (1,)))


def tn(a, b):
    return dot(a, b, ((0,), (0,)))


class Place:
    def __init__(self, F, C, T):
        self.F, self.C, self.T = F, C, T
        self.f = lax.axis_index("fsdp")
        self.z = lax.axis_index("ctx")
        self.t = lax.axis_index("tp")
        self.lo = lax.rem(self.t, 2)
        self.hi = self.t // 2
        self.near = self.t + 1 - 2 * self.lo
        self.far = lax.rem(self.t + 2, 4)

    def near_first(self):
        return [1] + ([self.C - 1] if self.C > 2 else []) + list(range(2, self.C - 1))

    def ahead(self, d):
        return lax.rem(self.z + d, self.C)

    def behind(self, d):
        return lax.rem(self.z + self.C - d, self.C)

    def fahead(self, d):
        return lax.rem(self.f + d, self.F)

    def fbehind(self, d):
        return lax.rem(self.f + self.F - d, self.F)

    def barrier(self, ctx=True, fsdp=False, tp=True):
        sem = pltpu.get_barrier_semaphore()
        peers = []
        if tp:
            peers += [{"tp": self.near}, {"tp": self.far}]
        if fsdp:
            peers += [{"fsdp": self.fahead(d)} for d in range(1, self.F)]
        if ctx:
            peers += [{"ctx": self.ahead(d)} for d in range(1, self.C)]
        for peer in peers:
            pl.semaphore_signal(sem, inc=1, device_id=peer, device_id_type=MESH)
        pl.semaphore_wait(sem, len(peers))


def remote(src, dst, ssem, rsem, peer):
    return pltpu.make_async_remote_copy(
        src_ref=src, dst_ref=dst, send_sem=ssem, recv_sem=rsem, device_id=peer, device_id_type=MESH
    )


def sem(*shape):
    return pltpu.SemaphoreType.DMA(shape)


def gather_sems(C):
    return [sem(C), sem(C), sem(C), sem(C), sem(C, 2), sem(C, 2), pltpu.SemaphoreType.DMA]


class Gather:
    def __init__(self, pc, x, out, rows, sems):
        self.pc, self.x = pc, x
        self.zs, self.zr, self.ys, self.yr, self.cs, self.cr, self.ls = sems
        self.slot = lambda c, t: out.at[c, t, rows]

    def start(self):
        pc, x = self.pc, self.x
        self.here = self.slot(pc.z, pc.t)
        self.local = pltpu.make_async_copy(x, self.here, self.ls)
        self.local.start()
        self.zc, self.yc, self.cc = {}, {}, {}
        self.later = pc.near_first()
        self.forward(0)
        self.send(2)

    def send(self, count=1):
        for d in self.later[:count]:
            self.zc[d] = remote(
                self.x, self.here, self.zs.at[d], self.zr.at[d], {"ctx": self.pc.ahead(d)}
            )
            self.zc[d].start()
        del self.later[:count]

    def forward(self, d):
        pc = self.pc
        dst = self.slot(pc.behind(d), pc.t)
        src = dst if d else self.x
        if d:
            self.zc[d].wait_recv()
            self.send()
        self.yc[d] = remote(src, dst, self.ys.at[d], self.yr.at[d], {"tp": pc.far})
        self.yc[d].start()
        self.cc[d, 0] = remote(src, dst, self.cs.at[d, 0], self.cr.at[d, 0], {"tp": pc.near})
        self.cc[d, 0].start()

    def onward(self, d):
        pc = self.pc
        self.yc[d].wait_recv()
        src = self.slot(pc.behind(d), pc.far)
        self.cc[d, 1] = remote(src, src, self.cs.at[d, 1], self.cr.at[d, 1], {"tp": pc.near})
        self.cc[d, 1].start()

    def finish(self):
        self.local.wait()
        for cp in self.zc.values():
            cp.wait_send()
        for cp in self.yc.values():
            cp.wait_send()
        for cp in self.cc.values():
            cp.wait()


def share_sems():
    return [sem(3), sem(3)]


def share_stage(pc, x, out, lsem, sems):
    ss, rs = sems
    t = pc.t
    local = pltpu.make_async_copy(x, out.at[t], lsem)
    local.start()
    a = remote(x, out.at[t], ss.at[0], rs.at[0], {"tp": pc.far})
    a.start()
    b = remote(x, out.at[t], ss.at[1], rs.at[1], {"tp": pc.near})
    b.start()
    a.wait_recv()
    src = out.at[pc.far]
    c = remote(src, src, ss.at[2], rs.at[2], {"tp": pc.near})
    c.start()
    local.wait()
    a.wait_send()
    b.wait()
    c.wait()


def scatter_scratch(C, Q, W):
    return [
        pltpu.VMEM((C, 2, Q, W), BF),
        pltpu.VMEM((C, Q, W), BF),
        pltpu.VMEM((C, Q, W), BF),
        pltpu.VMEM((C, Q, W), BF),
        pltpu.VMEM((C, Q, W), BF),
        sem(C, 2),
        sem(C, 2),
        sem(C),
        sem(C),
        sem(C),
        sem(C),
    ]


def local_scratch(C, Q, W):
    return [pltpu.VMEM((C, 2, Q, W), BF), sem(C, 2)]


class Scatter:
    def __init__(self, pc, p, rows, scratch, local=None):
        self.pc, self.p, self.rows, self.local = pc, p, rows, local
        (self.buf1, self.snd2, self.buf2, self.snd3, self.buf3) = scratch[:5]
        self.s1, self.r1, self.s2, self.r2, self.s3, self.r3 = scratch[5:]
        self.order = pc.near_first() + [0]
        self.lc, self.c1, self.c2, self.c3 = {}, {}, {}, {}

    def side(self, j):
        return 1 - self.pc.hi if j == 0 else self.pc.hi

    def begin(self, d):
        pc, p, rows = self.pc, self.p, self.rows
        c = pc.ahead(d)
        for j in range(2):
            self.c1[d, j] = remote(
                p.at[c, self.side(j) * 2 + 1 - pc.lo, rows],
                self.buf1.at[d, j],
                self.s1.at[d, j],
                self.r1.at[d, j],
                {"tp": pc.near},
            )
            self.c1[d, j].start()
            if self.local:
                self.lc[d, j] = pltpu.make_async_copy(
                    p.at[c, self.side(j) * 2 + pc.lo, rows],
                    self.local[0].at[d, j],
                    self.local[1].at[d, j],
                )
                self.lc[d, j].start()

    def start(self):
        for d in self.order:
            self.begin(d)

    def own(self, d, j):
        self.c1[d, j].wait_recv()
        if self.local:
            self.lc[d, j].wait()
            here = self.local[0][d, j]
        else:
            here = self.p[self.pc.ahead(d), self.side(j) * 2 + self.pc.lo, self.rows]
        return here.astype(F32) + self.buf1[d, j].astype(F32)

    def far(self, d):
        self.snd2[d] = self.own(d, 0).astype(BF)
        self.c2[d] = remote(
            self.snd2.at[d], self.buf2.at[d], self.s2.at[d], self.r2.at[d], {"tp": self.pc.far}
        )
        self.c2[d].start()

    def along(self, d):
        part = self.own(d, 1)
        self.c2[d].wait_recv()
        part = part + self.buf2[d].astype(F32)
        if d:
            self.snd3[d] = part.astype(BF)
            self.c3[d] = remote(
                self.snd3.at[d],
                self.buf3.at[d],
                self.s3.at[d],
                self.r3.at[d],
                {"ctx": self.pc.ahead(d)},
            )
            self.c3[d].start()
        else:
            self.total = part

    def result(self):
        total = self.total
        for d in range(1, self.pc.C):
            self.c3[d].wait_recv()
            total = total + self.buf3[d].astype(F32)
        return total

    def finish(self):
        for copies in (self.c1, self.c2, self.c3):
            for cp in copies.values():
                cp.wait_send()


class Pump:
    def __init__(self, scatters, begun=0, window=3):
        self.units = [(rs, d) for rs in scatters for d in rs.order]
        self.window, self.begun, self.sent, self.done = window, begun, 0, 0

    def fill(self):
        while self.begun < min(len(self.units), self.done + 2 * self.window):
            rs, d = self.units[self.begun]
            rs.begin(d)
            self.begun += 1
        while self.sent < min(len(self.units), self.done + self.window):
            rs, d = self.units[self.sent]
            rs.far(d)
            self.sent += 1

    def run(self, count):
        for _ in range(count):
            self.fill()
            rs, d = self.units[self.done]
            rs.along(d)
            self.done += 1
        self.fill()


def silu_parts(g):
    s = jax.nn.sigmoid(g)
    return g * s, s * (1.0 + g * (1.0 - s))


PARTS = 2


def halves_of(rows):
    n = rows // PARTS
    return (lambda h: pl.ds(h * n, n)), PARTS


def layer_norm_rows(values, gain, bias):
    center = values - jnp.mean(values, axis=-1, keepdims=True)
    spread = jnp.mean(center * center, axis=-1, keepdims=True)
    return (center * lax.rsqrt(spread + EPSILON) * gain + bias).astype(BF)


def eye_of(n):
    return lax.broadcasted_iota(jnp.int32, (n, n), 0) == lax.broadcasted_iota(jnp.int32, (n, n), 1)


def as_row(column):
    return jnp.sum(jnp.where(eye_of(column.shape[0]), column, 0.0), axis=0, keepdims=True)


def as_column(row):
    return jnp.sum(jnp.where(eye_of(row.shape[1]), row, 0.0), axis=1, keepdims=True)


def decays(rates):
    B = rates.shape[1]
    causal = lax.broadcasted_iota(jnp.int32, (B, B), 0) >= lax.broadcasted_iota(jnp.int32, (B, B), 1)
    column = jnp.sum(jnp.where(causal, rates, 0.0), axis=1, keepdims=True)
    row = as_row(column)
    table = jnp.where(causal, jnp.exp(jnp.minimum(column - row, 0.0)), 0.0)
    total = column[B - 1 :]
    return table, jnp.exp(column), jnp.exp(total - column), jnp.exp(total)


def across_blocks(rows, blocks, i, columns):
    F, C, R, _ = blocks.shape
    group = max(1, 128 // R)
    parts = []
    for g in range(group):
        b = i * group + g
        parts.append(nt(rows, blocks[b // C, lax.rem(b, C), :, columns]))
    part = parts[0] if group == 1 else jnp.concatenate(parts, axis=1)
    return part.astype(BF)


class Mover:
    def __init__(self, pc, weights, layout, out, zs, zr, xs, xr, ls):
        self.pc, self.weights, self.layout, self.out = pc, weights, layout, out
        self.zs, self.zr, self.xs, self.xr, self.ls = zs, zr, xs, xr, ls
        self.zc, self.xc = {}, {}
        rows = out.shape[2]
        near = pc.near_first()
        part = rows // 4
        self.units = [(d, pl.ds(i * part, part)) for d in near for i in range(4)]
        self.later = list(enumerate(self.units))

    def columns(self, dst, part):
        at = 0
        for w, (share, n) in zip(self.weights, self.layout):
            start = pl.multiple_of((dst // share) * n, n)
            yield (
                w.at[part, pl.ds(start, n)],
                self.out.at[self.pc.f, self.pc.z, part, pl.ds(at, n)],
            )
            at += n

    def send(self, count=1):
        pc = self.pc
        for k, (d, part) in self.later[:count]:
            dst = pc.ahead(d)
            sems, peer = (self.zs.at[k], self.zr.at[k]), {"ctx": dst}
            for src, to in self.columns(dst, part):
                remote(src, to, *sems, peer).start()
            here = self.out.at[pc.f, pc.behind(d), part]
            self.zc[k] = remote(here, here, *sems, peer)
        del self.later[:count]

    def start(self, count):
        pc = self.pc
        whole = pl.ds(0, self.out.shape[2])
        own = len(self.units)
        for e in range(1, pc.F):
            sems, peer = (self.xs.at[own, e], self.xr.at[own, e]), {"fsdp": pc.fahead(e)}
            for src, to in self.columns(pc.z, whole):
                remote(src, to, *sems, peer).start()
            here = self.out.at[pc.fbehind(e), pc.z]
            self.xc[own, e] = remote(here, here, *sems, peer)
        for src, to in self.columns(pc.z, whole):
            pltpu.make_async_copy(src, to, self.ls).start()
        here = self.out.at[pc.f, pc.z]
        self.local = pltpu.make_async_copy(here, here, self.ls)
        self.send(count)

    def forward(self, k):
        pc = self.pc
        d, part = self.units[k]
        self.zc[k].wait_recv()
        self.send()
        here = self.out.at[pc.f, pc.behind(d), part]
        for e in range(1, pc.F):
            self.xc[k, e] = remote(
                here, here, self.xs.at[k, e], self.xr.at[k, e], {"fsdp": pc.fahead(e)}
            )
            self.xc[k, e].start()

    def arrived(self, k, e):
        self.xc[k, e].wait_recv()

    def sent(self):
        for cp in list(self.zc.values()) + list(self.xc.values()):
            cp.wait_send()


class Blocks:
    def __init__(self, pc, x, out, zs, zr, ys, yr, cs, cr, ls):
        self.pc, self.x, self.out = pc, x, out
        self.zs, self.zr, self.ys, self.yr, self.cs, self.cr, self.ls = zs, zr, ys, yr, cs, cr, ls
        self.zc, self.yc, self.cc = {}, {}, {}

    def start(self):
        pc = self.pc
        self.later = pc.near_first()
        self.local = pltpu.make_async_copy(self.x, self.out.at[pc.z], self.ls)
        self.local.start()
        self.send(2)

    def send(self, count=1):
        pc = self.pc
        for d in self.later[:count]:
            self.zc[d] = remote(
                self.x.at[pc.t],
                self.out.at[pc.z, pc.t],
                self.zs.at[d],
                self.zr.at[d],
                {"ctx": pc.ahead(d)},
            )
            self.zc[d].start()
        del self.later[:count]

    def forward(self, d):
        pc = self.pc
        self.zc[d].wait_recv()
        self.send()
        here = self.out.at[pc.behind(d), pc.t]
        self.yc[d] = remote(here, here, self.ys.at[d], self.yr.at[d], {"tp": pc.far})
        self.yc[d].start()
        self.cc[d, 0] = remote(here, here, self.cs.at[d, 0], self.cr.at[d, 0], {"tp": pc.near})
        self.cc[d, 0].start()

    def onward(self, d):
        pc = self.pc
        self.yc[d].wait_recv()
        here = self.out.at[pc.behind(d), pc.far]
        self.cc[d, 1] = remote(here, here, self.cs.at[d, 1], self.cr.at[d, 1], {"tp": pc.near})
        self.cc[d, 1].start()

    def finish(self):
        self.local.wait()
        for cp in list(self.zc.values()) + list(self.yc.values()):
            cp.wait_send()
        for cp in self.cc.values():
            cp.wait()


def mover_sems(F, C):
    return [sem(4 * C), sem(4 * C), sem(4 * C, F), sem(4 * C, F), pltpu.SemaphoreType.DMA]


def blocks_sems(C):
    return [sem(C), sem(C), sem(C), sem(C), sem(C, 2), sem(C, 2), pltpu.SemaphoreType.DMA]


def forward_kernel(dims, cfg, *refs):
    F, C, T = dims
    S, B, halves, HV, in_layout, rest_layout = cfg
    refs = list(refs)

    def take(n):
        out = refs[:n]
        del refs[:n]
        return out

    in_weights, rest_weights = take(5), take(3)
    vec, ld, tok, go = take(4)
    o_win, o_normed, o_proj, o_states, o_normal, o_gated, inv, old, vecs, mid, sn, full, ogo = take(13)
    otok, win, ovec, normed, acc, proj, states, state, normal, gated, stats, mytok, x = take(13)
    in_sems, rest_sems = take(5), take(5)
    tok_sems, go_sems = take(7), take(7)
    vzs, vzr, vxs, vxr, lzs, lzr, sts, strr, oses = take(9)
    n, m = len(gather_sems(C)), len(scatter_scratch(C, 8, 128))

    pc = Place(*dims)
    f, z, t = pc.f, pc.z, pc.t
    near = pc.near_first()
    L = S * B
    R = win.shape[2]
    W = F * C * R
    NI = proj.shape[1]
    N = proj.shape[0]
    units = C * S
    saved = []

    def save(src, dst):
        cp = pltpu.make_async_copy(src, dst, oses.at[len(saved)])
        cp.start()
        saved.append(cp)

    pc.barrier(True, True, True)
    vz, vx, lz = {}, {}, {}
    for d in range(1, C):
        peer = {"ctx": pc.ahead(d)}
        vz[d] = remote(vec, ovec.at[f, z], vzs.at[d], vzr.at[d], peer)
        vz[d].start()
        lz[d] = remote(ld, old.at[z], lzs.at[d], lzr.at[d], peer)
        lz[d].start()
    ovec[f, z] = vec[...]
    old[z] = ld[...]

    def vec_across(d):
        for e in range(1, F):
            src = ovec.at[f, pc.behind(d)] if d else vec
            vx[d, e] = remote(
                src, ovec.at[f, pc.behind(d)], vxs.at[d, e], vxr.at[d, e], {"fsdp": pc.fahead(e)}
            )
            vx[d, e].start()

    vec_across(0)
    tk = Blocks(pc, tok, otok, *tok_sems)
    tk.start()
    wi = Mover(pc, in_weights, in_layout, win, *in_sems)
    wi.start(0)
    mine = pltpu.make_async_copy(tok.at[t], mytok, oses.at[15])
    mine.start()
    for d in range(1, C):
        vz[d].wait_recv()
        vec_across(d)
    for d in near:
        tk.forward(d)
        wi.send(4)
    wr = Mover(pc, rest_weights, rest_layout, full, *rest_sems)
    gk = Blocks(pc, go, ogo, *go_sems)
    for d in near:
        tk.onward(d)
    for cp in vx.values():
        cp.wait()
    for cp in vz.values():
        cp.wait_send()
    for b in range(F * C):
        vecs[:, b * R : (b + 1) * R] = ovec[b // C, b % C]
    tk.finish()
    gain1, bias1 = vecs[0:1], vecs[1:2]

    def norm_unit(i, carry):
        rows = otok[i // T, lax.rem(i, T)].astype(F32)
        q = rows.shape[0]
        value = layer_norm_rows(rows, gain1, bias1)
        for b in range(F * C):
            normed[b, pl.ds(pl.multiple_of(i * q, q), q)] = value[:, b * R : (b + 1) * R]
        return carry

    lax.fori_loop(0, C * T, norm_unit, 0)
    save(normed, o_normed)

    tile = min(256, N)

    def project(ff, c, first, last):
        def one(i, carry):
            rows = pl.ds(pl.multiple_of(i * tile, tile), tile)
            part = nn(normed[ff * C + c, rows], win[ff, c, :, :NI])
            if not first:
                part = part + acc[rows]
            if last:
                proj[rows] = part.astype(BF)
            else:
                acc[rows] = part
            return carry

        lax.fori_loop(0, N // tile, one, 0)

    wi.local.wait()
    own = len(wi.units)
    project(f, z, True, False)
    for e in range(1, F):
        wi.arrived(own, e)
        project(pc.fbehind(e), z, False, False)
    gk.start()
    for i, d in enumerate(near):
        keys = [k for k, (dd, _) in enumerate(wi.units) if dd == d]
        for k in keys:
            wi.forward(k)
        project(f, pc.behind(d), False, False)
        if i == 1:
            wr.start(4)
    for i, d in enumerate(near):
        keys = [k for k, (dd, _) in enumerate(wi.units) if dd == d]
        for e in range(1, F):
            for k in keys:
                wi.arrived(k, e)
            project(pc.fbehind(e), pc.behind(d), False, i == C - 2 and e == F - 1)
    gk.send(C)
    wr.send(4)
    save(proj, o_proj)
    save(win, o_win)

    for cp in lz.values():
        cp.wait()
    head = z // halves
    scale = float(KEY) ** (-0.5)
    state[...] = jnp.zeros_like(state)

    def retain(u, carry):
        c, s = u // S, lax.rem(u, S)
        rows = pl.ds(pl.multiple_of(u * B, B), B)
        rates = old[c, pl.ds(head, 1), pl.ds(pl.multiple_of(s * B, B), B)]
        table, growth, keeping, through = decays(rates)
        q, k, v = proj[rows, :KEY], proj[rows, KEY : 2 * KEY], proj[rows, 2 * KEY : 2 * KEY + HV]
        weights = (nt(q, k) * scale * table).astype(BF)
        before = state[s]
        states[u] = before.astype(BF)
        mixed = nn(weights, v) + nn((q.astype(F32) * growth).astype(BF), before.astype(BF))
        state[s] = through * before + tn((k.astype(F32) * keeping).astype(BF), v)
        normal[rows] = mixed
        mean = jnp.mean(mixed, axis=-1, keepdims=True)
        dev = mixed - mean
        stats[0, 0:1, rows] = as_row(mean)
        stats[0, 1:2, rows] = as_row(jnp.sum(dev * dev, axis=-1, keepdims=True))
        return carry

    stats[0] = jnp.zeros(stats.shape[1:], F32)
    lax.fori_loop(0, units, retain, 0)
    save(states, o_states)
    wr.send(4 * C)
    st = []
    place = lax.rem(z, halves)
    for j in range(1, halves):
        peer = {"ctx": z - place + lax.rem(place + j, halves)}
        cp = remote(stats.at[0], stats.at[j], sts.at[j], strr.at[j], peer)
        cp.start()
        st.append(cp)
    for cp in st:
        cp.wait()

    def finish_unit(u, carry):
        rows = pl.ds(pl.multiple_of(u * B, B), B)
        got = [(stats[j, 0:1, rows], stats[j, 1:2, rows]) for j in range(halves)]
        mean = sum(a for a, _ in got) / halves
        m2 = sum(b + HV * (a - mean) * (a - mean) for a, b in got)
        scaled = as_column(lax.rsqrt(m2 / HEAD_V + EPSILON))
        value = (normal[rows] - as_column(mean)) * scaled
        gate = proj[rows, 2 * KEY + HV :].astype(F32)
        normal[rows] = value
        inv[0:1, rows] = lax.rsqrt(m2 / HEAD_V + EPSILON)
        gated[rows] = (gate * jax.nn.sigmoid(gate) * value).astype(BF)
        return carry

    inv[...] = jnp.zeros_like(inv)
    lax.fori_loop(0, units, finish_unit, 0)
    save(normal, o_normal)
    save(gated, o_gated)

    p = otok
    Q = x.shape[0]
    cut, parts = halves_of(Q)
    scatters, gathers = [], []
    for h in range(parts):
        at = h * (n + m)
        gathers.append(Gather(pc, x.at[cut(h)], sn, cut(h), refs[at : at + n]))
        scatters.append(Scatter(pc, p, cut(h), refs[at + n : at + n + m]))
    for d in near + [0]:
        c = pc.ahead(d)
        mixed = gated[pl.ds(pl.multiple_of(c * L, L), L)]

        def one(b, carry):
            part = across_blocks(mixed, win, b, pl.ds(NI, HV))
            columns = pl.ds(pl.multiple_of(b * part.shape[1], 128), part.shape[1])
            for i in range(T):
                p[c, i, :, columns] = part[i * Q : (i + 1) * Q]
            return carry

        lax.fori_loop(0, W // max(R, 128), one, 0)
        scatters[0].begin(d)
    for d in near:
        gk.forward(d)
    pump = Pump(scatters, begun=C)
    pump.run(C)
    for k in range(8):
        wr.forward(k)
    for d in near:
        gk.onward(d)
    mine.wait()
    for h, rs in enumerate(scatters):
        pump.run(min(2, len(pump.units) - pump.done))
        part = cut(h)
        total = rs.result() + mytok[part].astype(F32)
        mid[part] = total
        x[part] = layer_norm_rows(total, vecs[2:3], vecs[3:4])
        gathers[h].start()
        if h == 0:
            pump.run(len(pump.units) - pump.done)
            for k in range(8, len(wr.units)):
                wr.forward(k)
    for ga in gathers:
        for d in near:
            ga.forward(d)
    for ga in gathers:
        for d in [0] + near:
            ga.onward(d)
    for job in scatters + gathers:
        job.finish()
    gk.finish()
    wi.sent()
    wr.local.wait()
    for k in range(len(wr.units) + 1):
        for e in range(1, F):
            wr.arrived(k, e)
    wr.sent()
    for cp in saved:
        cp.wait()


def norm_pull(values, gain, grad):
    center = values - jnp.mean(values, axis=-1, keepdims=True)
    spread = jnp.mean(center * center, axis=-1, keepdims=True)
    inv = lax.rsqrt(spread + EPSILON)
    xhat = center * inv
    g = grad * gain
    back = inv * (
        g - jnp.mean(g, axis=-1, keepdims=True) - xhat * jnp.mean(g * xhat, axis=-1, keepdims=True)
    )
    return (
        back,
        jnp.sum(grad * xhat, axis=0, keepdims=True),
        jnp.sum(grad, axis=0, keepdims=True),
    )


def mlp_kernel(
    dims, pg, pd, mid, allgo, gain, g0, g1, g2, gm, gb, out, dgain, dbias, xg, x, y, go, lsem, gosem, gxs, gxr, *scratch
):
    pc = Place(*dims)
    C = pc.C
    mine = pltpu.make_async_copy(allgo.at[pc.t], go, gosem)
    mine.start()
    pc.barrier(True, True, True)
    n, m = len(gather_sems(C)), len(scatter_scratch(C, 8, 128))
    ss, scratch = scratch[:2], scratch[2:]
    rd = Scatter(pc, pd, pl.ds(0, x.shape[0]), scratch[:m], scratch[m : m + 2])
    scratch = scratch[m + 2 :]
    cut, parts = halves_of(x.shape[0])
    scatters, gathers = [], []
    for h in range(parts):
        at = h * (n + m + 2)
        gathers.append(Gather(pc, x.at[cut(h)], gb, cut(h), scratch[at : at + n]))
        at += n
        scatters.append(Scatter(pc, pg, cut(h), scratch[at : at + m], scratch[at + m : at + m + 2]))
    for rs in scatters:
        rs.start()
    rd.start()
    moves = []
    u = g0.shape[3]
    for i, g in enumerate((g0, g1, g2)):
        for e in range(1, pc.F):
            cp = remote(
                g.at[pc.fahead(e)],
                xg.at[e - 1, :, :, pl.ds(i * u, u)],
                gxs.at[i, e],
                gxr.at[i, e],
                {"fsdp": pc.fahead(e)},
            )
            cp.start()
            moves.append(cp)
    for rs in scatters + [rd]:
        for d in rs.order:
            rs.far(d)
    mine.wait()
    for h, rs in enumerate(scatters):
        for d in rs.order:
            rs.along(d)
        part = cut(h)
        back, dg, db = norm_pull(mid[part], gain[...], rs.result())
        dgain[...] = dgain[...] + dg if h else dg
        dbias[...] = dbias[...] + db if h else db
        grad_middle = go[part].astype(F32) + back
        gm[part] = grad_middle
        x[part] = grad_middle.astype(BF)
        gathers[h].start()
    for d in rd.order[:2]:
        rd.along(d)
    near = pc.near_first()
    for d in near:
        gathers[0].forward(d)
    for d in rd.order[2:]:
        rd.along(d)
    for ga in gathers[1:]:
        for d in near:
            ga.forward(d)
    for d in range(C):
        for ga in gathers:
            ga.onward(d)
    y[...] = (mid[...] + rd.result()).astype(BF)
    share_stage(pc, y, out, lsem, ss)
    for job in scatters + gathers + [rd]:
        job.finish()
    for cp in moves:
        cp.wait()


def vector_stage(pc, v, vout, va, vb, vc, vd, vx, vz, ts, tr, vxs, vxr, vzs, vzr):
    F, C = pc.F, pc.C
    t0 = remote(v, vb, ts.at[0], tr.at[0], {"tp": pc.near})
    t0.start()
    t0.wait_recv()
    va[...] = v[...] + vb[...]
    t1 = remote(va, vc, ts.at[1], tr.at[1], {"tp": pc.far})
    t1.start()
    t1.wait_recv()
    vd[...] = va[...] + vc[...]
    vxc, vzc = {}, {}
    for e in range(1, F):
        vxc[e] = remote(
            vd.at[pc.fahead(e)], vx.at[e - 1], vxs.at[e], vxr.at[e], {"fsdp": pc.fahead(e)}
        )
        vxc[e].start()
    vs = vd[pc.f]
    for e in range(1, F):
        vxc[e].wait_recv()
        vs = vs + vx[e - 1]
    vz[0] = vs
    for d in range(1, C):
        vzc[d] = remote(
            vz.at[0, pc.ahead(d)], vz.at[1, d], vzs.at[d], vzr.at[d], {"ctx": pc.ahead(d)}
        )
        vzc[d].start()
    acc = vz[0, pc.z]
    for d in range(1, C):
        vzc[d].wait_recv()
        acc = acc + vz[1, d]
    vout[...] = acc
    for cp in [t0, t1] + list(vxc.values()) + list(vzc.values()):
        cp.wait_send()


def vector_scratch(F, C, R):
    full = pltpu.VMEM((F, C, 8, R), F32)
    return [
        full,
        full,
        full,
        full,
        full,
        pltpu.VMEM((F - 1, C, 8, R), F32),
        pltpu.VMEM((2, C, 8, R), F32),
        sem(2),
        sem(2),
        sem(F),
        sem(F),
        sem(C),
        sem(C),
    ]


def backward_kernel(dims, cfg, *refs):
    F, C, T = dims
    S, B, halves, HV = cfg
    refs = list(refs)

    def take(n):
        out = refs[:n]
        del refs[:n]
        return out

    branch, normed, win, proj, states, normal, inv, gated, old, vecs, gm, alltok, mlp, dg2, db2 = take(15)
    gt, gout, mout, vout = take(4)
    btile, ntile, cblock, turned, turned2, gn, gproj, later, stats, p = take(10)
    gsend, xbuf, zsnd, tok, y = take(5)
    bsem, nsem, sts, strr, mzs, mzr, xs, xr, zs, zr, keeps, toksem, lsem, msem = take(14)
    shares, vscratch = take(2), take(13)

    pc = Place(*dims)
    f, z, t = pc.f, pc.z, pc.t
    L = S * B
    R = win.shape[2]
    W = F * C * R
    N, NI = gproj.shape
    Q = y.shape[0]
    units = C * S
    pc.barrier(True, True, True)
    mine = pltpu.make_async_copy(alltok.at[t], tok, toksem)
    mine.start()

    moves = [pltpu.make_async_copy(mlp.at[z], mout.at[z], msem)]
    for d in pc.near_first():
        dst = pc.ahead(d)
        moves.append(remote(mlp.at[dst], mout.at[z], mzs.at[d], mzr.at[d], {"ctx": dst}))
    for cp in moves:
        cp.start()

    def rows_in(u, slot):
        rows = pl.ds(pl.multiple_of(u * B, B), B)
        return pltpu.make_async_copy(branch.at[rows], btile.at[slot], bsem.at[slot])

    rows_in(0, 0).start()
    stats[0] = jnp.zeros(stats.shape[1:], F32)

    def pull_gate(u, carry):
        slot = lax.rem(u, 2)
        pl.when(u + 1 < units)(lambda: rows_in(u + 1, 1 - slot).start())
        rows_in(u, slot).wait()
        grad = None
        rows = pl.ds(pl.multiple_of(u * B, B), B)
        for b in range(F * C):
            piece = btile[slot, :, b * R : (b + 1) * R]
            cblock[b, rows] = piece
            part = nn(piece, win[b // C, b % C, :, NI:])
            grad = part if grad is None else grad + part
        gate = proj[rows, 2 * KEY + HV :].astype(F32)
        silu, dsilu = silu_parts(gate)
        value = normal[rows]
        gproj[rows, 2 * KEY + HV :] = (grad * value * dsilu).astype(BF)
        inner = grad * silu
        gn[rows] = inner
        stats[0, 0:1, rows] = as_row(jnp.sum(inner, axis=-1, keepdims=True))
        stats[0, 1:2, rows] = as_row(jnp.sum(inner * value, axis=-1, keepdims=True))
        return carry

    lax.fori_loop(0, units, pull_gate, 0)
    st = []
    place = lax.rem(z, halves)
    for j in range(1, halves):
        peer = {"ctx": z - place + lax.rem(place + j, halves)}
        cp = remote(stats.at[0], stats.at[j], sts.at[j], strr.at[j], peer)
        cp.start()
        st.append(cp)

    blocks = []
    far = sorted(range(1, C), key=lambda d: abs(d - C // 2))
    order = far + [0]
    sends = [("send", d, e) for d in order for e in range(1, F)]
    owns = [("own", d, 0) for d in order]
    lead = 2 * (F - 1)
    blocks = sends[:lead]
    rest = sends[lead:]
    for i, own in enumerate(owns):
        blocks.append(own)
        blocks += rest[i * (F - 1) : (i + 1) * (F - 1)]

    def columns_in(i):
        kind, d, e = blocks[i]
        b = (pc.fahead(e) if kind == "send" else f) * C + pc.ahead(d)
        return b, pltpu.make_async_copy(normed.at[b], ntile.at[i % 2], nsem.at[i % 2])

    def start_columns(i):
        if i < len(blocks):
            columns_in(i)[1].start()

    start_columns(0)
    for cp in st:
        cp.wait()

    head = z // halves
    scale = float(KEY) ** (-0.5)
    later[...] = jnp.zeros_like(later)

    def retain(i, carry):
        u = units - 1 - i
        c, s = u // S, lax.rem(u, S)
        rows = pl.ds(pl.multiple_of(u * B, B), B)
        rates = old[c, pl.ds(head, 1), pl.ds(pl.multiple_of(s * B, B), B)]
        table, growth, keeping, through = decays(rates)
        q, k, v = proj[rows, :KEY], proj[rows, KEY : 2 * KEY], proj[rows, 2 * KEY : 2 * KEY + HV]
        s1 = as_column(sum(stats[j, 0:1, rows] for j in range(halves)) / HEAD_V)
        s2 = as_column(sum(stats[j, 1:2, rows] for j in range(halves)) / HEAD_V)
        mix = (as_column(inv[0:1, rows]) * (gn[rows] - s1 - normal[rows] * s2)).astype(BF)
        weights = (nt(q, k) * scale * table).astype(BF)
        scores = (nt(mix, v) * scale * table).astype(BF)
        after = later[s]
        after_low = after.astype(BF)
        gq = nn(scores, k) + growth * nt(mix, states[u])
        gk = tn(scores, q) + keeping * nt(v, after_low)
        gv = tn(weights, mix) + nn((k.astype(F32) * keeping).astype(BF), after_low)
        later[s] = through * after + tn((q.astype(F32) * growth).astype(BF), mix)
        gproj[rows, :KEY] = gq.astype(BF)
        gproj[rows, KEY : 2 * KEY] = gk.astype(BF)
        gproj[rows, 2 * KEY : 2 * KEY + HV] = gv.astype(BF)
        return carry

    lax.fori_loop(0, units, retain, 0)

    rs = Scatter(pc, p, pl.ds(0, Q), refs)
    for d in rs.order:
        c = pc.ahead(d)
        mixed = gproj[pl.ds(pl.multiple_of(c * L, L), L)]

        def one(b, carry, c=c, mixed=mixed):
            part = across_blocks(mixed, win, b, pl.ds(0, NI))
            columns = pl.ds(pl.multiple_of(b * part.shape[1], 128), part.shape[1])
            for i in range(T):
                p[c, i, :, columns] = part[i * Q : (i + 1) * Q]
            return carry

        lax.fori_loop(0, W // max(R, 128), one, 0)
        rs.begin(d)
    pump = Pump([rs], begun=C)
    pump.fill()

    H = 2
    xc, zc = {}, {}
    kept = []

    def block(i):
        kind, d, e = blocks[i]
        start_columns(i + 1)
        b, cp = columns_in(i)
        cp.wait()
        turned[...] = jnp.transpose(ntile[i % 2])
        turned2[...] = jnp.transpose(cblock[b])
        if kind == "own":
            for g in range(1, F):
                for h in range(H):
                    xc[d, g, h].wait_recv()

        def put(columns, part):
            if kind == "send":
                gsend[e - 1, d, :, columns] = part.astype(BF)
            else:
                for g in range(F - 1):
                    part = part + xbuf[g, d, :, columns].astype(F32)
                zsnd[d, :, columns] = part.astype(BF)

        def one(j, carry):
            columns = pl.ds(pl.multiple_of(j * 256, 256), 256)
            put(columns, nn(turned[...], gproj[:, columns]))
            return carry

        lax.fori_loop(0, NI // 256, one, 0)
        put(pl.ds(NI, HV), nn(turned2[...], gated[...]))
        for h in range(H):
            part = pl.ds(h * (R // H), R // H)
            if kind == "send":
                xc[d, e, h] = remote(
                    gsend.at[e - 1, d, part],
                    xbuf.at[e - 1, d, part],
                    xs.at[d, e, h],
                    xr.at[d, e, h],
                    {"fsdp": pc.fahead(e)},
                )
                xc[d, e, h].start()
            elif d:
                zc[d, h] = remote(
                    zsnd.at[d, part], gout.at[z, part], zs.at[d, h], zr.at[d, h], {"ctx": pc.ahead(d)}
                )
                zc[d, h].start()
            else:
                cp = pltpu.make_async_copy(zsnd.at[0, part], gout.at[z, part], keeps.at[h])
                cp.start()
                kept.append(cp)

    for i in range(len(blocks)):
        block(i)
        if pump.done < len(pump.units):
            pump.run(1)
        elif pump.done == len(pump.units):
            pump.done += 1
            mine.wait()
            back, dg, db = norm_pull(tok[...].astype(F32), vecs[0:1], rs.result())
            y[...] = (gm[...] + back).astype(BF)
            v = vscratch[0]
            for b in range(F * C):
                rows = [r[:, b * R : (b + 1) * R] for r in (dg, db)] + [
                    r[:, b * R : (b + 1) * R] for r in (dg2, db2)
                ]
                v[b // C, b % C] = jnp.concatenate(rows + [jnp.zeros((4, R), F32)], axis=0)
    share_stage(pc, y, gt, lsem, shares)
    vector_stage(pc, vscratch[0], vout, *vscratch[1:])
    rs.finish()
    for cp in kept:
        cp.wait()
    for cp in zc.values():
        cp.wait()
    for cp in xc.values():
        cp.wait_send()
    for cp in moves:
        cp.wait()


def assemble_kernel(halves, key, hv, a, m, q, k, v, g, o, fg, fu, fd):
    c = pl.program_id(0)
    first = lax.rem(c, halves) == 0
    for i, ref in enumerate((q, k)):
        x = a[0, :, i * key : (i + 1) * key].astype(F32)

        @pl.when(first)
        def _(ref=ref, x=x):
            ref[...] = x

        @pl.when(jnp.logical_not(first))
        def _(ref=ref, x=x):
            ref[...] += x

    v[...] = a[0, :, 2 * key : 2 * key + hv].astype(F32)
    g[...] = a[0, :, 2 * key + hv : 2 * key + 2 * hv].astype(F32)
    o[...] = a[0, :, 2 * key + 2 * hv :].astype(F32)
    u = fg.shape[1]
    for i, ref in enumerate((fg, fu, fd)):
        ref[...] = m[0, :, i * u : (i + 1) * u].astype(F32)


def params(cid):
    return pltpu.CompilerParams(collective_id=cid, has_side_effects=True)


def shards(
    dims,
    tokens,
    log_decay,
    w_query,
    w_key,
    w_value,
    w_gate,
    w_out,
    norm1_gain,
    norm1_bias,
    w_ffgate,
    w_ffup,
    w_down,
    norm2_gain,
    norm2_bias,
    grad_out,
):
    F, C, T = dims
    S, B, W = tokens.shape
    L = S * B
    Q = L // T
    N = C * L
    R = w_query.shape[0]
    heads = log_decay.shape[2]
    halves = C // heads
    HV = HEAD_V // halves
    U = w_ffgate.shape[1] // C
    z = lax.axis_index("ctx")
    t = lax.axis_index("tp")
    scale = float(KEY) ** (-0.5)

    f = lax.axis_index("fsdp")

    def hop(x, axis, d):
        n = lax.axis_size(axis)
        return lax.ppermute(x, axis, [(i, (i + d) % n) for i in range(n)])

    def at(x, i, n):
        return lax.dynamic_index_in_dim(x, lax.rem(i, n), 0, False)

    NI, NR = 2 * KEY + 2 * HV, 3 * U
    NO = NI + HV
    vec = jnp.stack([norm1_gain, norm1_bias, norm2_gain, norm2_bias]).astype(F32)
    vec = jnp.pad(vec, ((0, 4), (0, 0)))
    ld = jnp.pad(jnp.transpose(log_decay, (2, 0, 1)).reshape(heads, L), ((0, 8 - heads), (0, 0)))
    tok = tokens.reshape(T, Q, W)
    go = grad_out.reshape(T, Q, W)
    sds = jax.ShapeDtypeStruct
    cfg = (
        S,
        B,
        halves,
        HV,
        ((halves, KEY), (halves, KEY), (1, HV), (1, HV), (1, HV)),
        ((1, U), (1, U), (1, U)),
    )
    owin, normed, proj, states, normal, gated, inv, old, vecs, mid, sn, full, ogo = pl.pallas_call(
        functools.partial(forward_kernel, dims, cfg),
        out_shape=(
            sds((F, C, R, NO), BF),
            sds((F * C, N, R), BF),
            sds((N, NI), BF),
            sds((C * S, KEY, HV), BF),
            sds((N, HV), F32),
            sds((N, HV), BF),
            sds((8, N), F32),
            sds((C, 8, L), F32),
            sds((8, W), F32),
            sds((Q, W), F32),
            sds((C, T, Q, W), BF),
            sds((F, C, R, NR), BF),
            sds((C, T, Q, W), BF),
        ),
        in_specs=[ANY] * 8 + [VMEM, VMEM, ANY, ANY],
        out_specs=[ANY] * 6 + [VMEM] * 4 + [ANY] * 3,
        scratch_shapes=[
            pltpu.VMEM((C, T, Q, W), BF),
            pltpu.VMEM((F, C, R, NO), BF),
            pltpu.VMEM((F, C, 8, R), F32),
            pltpu.VMEM((F * C, N, R), BF),
            pltpu.VMEM((N, NI), F32),
            pltpu.VMEM((N, NI), BF),
            pltpu.VMEM((C * S, KEY, HV), BF),
            pltpu.VMEM((S, KEY, HV), F32),
            pltpu.VMEM((N, HV), F32),
            pltpu.VMEM((N, HV), BF),
            pltpu.VMEM((halves, 8, N), F32),
            pltpu.VMEM((Q, W), BF),
            pltpu.VMEM((Q, W), BF),
        ]
        + mover_sems(F, C) * 2
        + blocks_sems(C) * 2
        + [sem(C), sem(C), sem(C, F), sem(C, F), sem(C), sem(C), sem(halves), sem(halves), sem(16)]
        + (gather_sems(C) + scatter_scratch(C, Q // PARTS, W)) * PARTS,
        compiler_params=params(1),
        name="k_forward",
    )(w_query, w_key, w_value, w_gate, w_out, w_ffgate, w_ffup, w_down, vec, ld, tok, go)
    gain1, gain2 = vecs[0:1], vecs[2:3]
    w_rest = full.reshape(W, NR)
    w_fg, w_fu, w_d = w_rest[:, :U], w_rest[:, U : 2 * U], w_rest[:, 2 * U :]

    second = sn.reshape(N, W)
    ff_gate = nn(second, w_fg).astype(BF)
    ff_up = nn(second, w_fu).astype(BF)
    hidden, gelu_pull = jax.vjp(
        lambda a, b: jax.nn.gelu(a, approximate=True) * b, ff_gate.astype(F32), ff_up.astype(F32)
    )
    hidden = hidden.astype(BF)
    down = nt(hidden, w_d).astype(BF).reshape(C, T, Q, W)
    gout = ogo.reshape(N, W)
    grad_hidden = nn(gout, w_d)
    gfg, gfu = gelu_pull(grad_hidden)
    gfg, gfu = gfg.astype(BF), gfu.astype(BF)
    gsecond = (nt(gfg, w_fg) + nt(gfu, w_fu)).astype(BF).reshape(C, T, Q, W)
    mlp_parts = [
        tn(a, b).astype(BF).reshape(F, C, R, U)
        for a, b in ((second, gfg), (second, gfu), (gout, hidden))
    ]
    gm, gb, out, dgain2, dbias2, mlp_got = pl.pallas_call(
        functools.partial(mlp_kernel, dims),
        out_shape=(
            sds((Q, W), F32),
            sds((C, T, Q, W), BF),
            sds((T, Q, W), BF),
            sds((1, W), F32),
            sds((1, W), F32),
            sds((F - 1, C, R, NR), BF),
        ),
        in_specs=[ANY, ANY, VMEM, ANY, VMEM, ANY, ANY, ANY],
        out_specs=[VMEM, ANY, ANY, VMEM, VMEM, ANY],
        scratch_shapes=[pltpu.VMEM((Q, W), BF)] * 3
        + [pltpu.SemaphoreType.DMA] * 2
        + [sem(3, F), sem(3, F)]
        + share_sems()
        + scatter_scratch(C, Q, W)
        + local_scratch(C, Q, W)
        + (gather_sems(C) + scatter_scratch(C, Q // PARTS, W) + local_scratch(C, Q // PARTS, W)) * PARTS,
        compiler_params=params(3),
        name="k_mlp",
    )(gsecond, down, mid, go, gain2, *mlp_parts)
    output = out.reshape(tokens.shape)

    branch = gb.reshape(N, W)
    mlp_sum = jnp.concatenate([at(x, f, F) for x in mlp_parts], axis=2).astype(F32)
    for e in range(F - 1):
        mlp_sum = mlp_sum + mlp_got[e].astype(F32)
    mlp_sum = mlp_sum.astype(BF)
    H = 2
    gt, gsum, mlp_grads, vsum = pl.pallas_call(
        functools.partial(backward_kernel, dims, (S, B, halves, HV)),
        out_shape=(
            sds((T, Q, W), BF),
            sds((C, R, NO), BF),
            sds((C, R, NR), BF),
            sds((8, R), F32),
        ),
        in_specs=[ANY, ANY] + [VMEM] * 9 + [ANY, ANY, VMEM, VMEM],
        out_specs=[ANY, ANY, ANY, VMEM],
        scratch_shapes=[
            pltpu.VMEM((2, B, W), BF),
            pltpu.VMEM((2, N, R), BF),
            pltpu.VMEM((F * C, N, R), BF),
            pltpu.VMEM((R, N), BF),
            pltpu.VMEM((R, N), BF),
            pltpu.VMEM((N, HV), F32),
            pltpu.VMEM((N, NI), BF),
            pltpu.VMEM((S, KEY, HV), F32),
            pltpu.VMEM((halves, 8, N), F32),
            pltpu.VMEM((C, T, Q, W), BF),
            pltpu.VMEM((F - 1, C, R, NO), BF),
            pltpu.VMEM((F - 1, C, R, NO), BF),
            pltpu.VMEM((C, R, NO), BF),
            pltpu.VMEM((Q, W), BF),
            pltpu.VMEM((Q, W), BF),
            sem(2),
            sem(2),
            sem(halves),
            sem(halves),
            sem(C),
            sem(C),
            sem(C, F, H),
            sem(C, F, H),
            sem(C, H),
            sem(C, H),
            sem(H),
        ]
        + [pltpu.SemaphoreType.DMA] * 3
        + share_sems()
        + vector_scratch(F, C, R)
        + scatter_scratch(C, Q, W),
        compiler_params=params(4),
        name="k_backward",
    )(
        branch,
        normed,
        owin,
        proj,
        states,
        normal,
        inv,
        gated,
        old,
        vecs,
        gm,
        tok,
        mlp_sum,
        dgain2,
        dbias2,
    )
    grad_tokens = gt.reshape(tokens.shape)

    def quarter(n):
        return pl.BlockSpec((R, n), lambda c: (0, c))

    per_head = pl.BlockSpec((R, KEY), lambda c: (0, c // halves))
    gq, gk, gv, gg, gw, gfg, gfu, gfd = pl.pallas_call(
        functools.partial(assemble_kernel, halves, KEY, HV),
        out_shape=[sds((R, heads * KEY), F32)] * 2
        + [sds((R, C * HV), F32)] * 3
        + [sds((R, C * U), F32)] * 3,
        grid=(C,),
        in_specs=[
            pl.BlockSpec((1, R, NO), lambda c: (c, 0, 0)),
            pl.BlockSpec((1, R, NR), lambda c: (c, 0, 0)),
        ],
        out_specs=[per_head, per_head] + [quarter(HV)] * 3 + [quarter(U)] * 3,
        name="k_assemble",
    )(gsum, mlp_grads)
    return (
        output,
        grad_tokens,
        gq,
        gk,
        gv,
        gg,
        gw,
        vsum[0],
        vsum[1],
        gfg,
        gfu,
        gfd,
        vsum[2],
        vsum[3],
    )


def solution(mesh):
    dims = (mesh.shape["fsdp"], mesh.shape["ctx"], mesh.shape["tp"])
    rows, vec = P(("fsdp", "ctx"), "tp"), P(("fsdp", "ctx"))
    acts = P("fsdp", "ctx", None)
    return jax.shard_map(
        functools.partial(shards, dims),
        mesh=mesh,
        in_specs=(acts, P("fsdp", "ctx", "tp"), rows, rows, rows, rows, rows, vec, vec, rows, rows, rows, vec, vec, acts),
        out_specs=(acts, acts, rows, rows, rows, rows, rows, vec, vec, rows, rows, rows, vec, vec),
        check_vma=False,
    )
```

```python
import functools

import jax
import jax.numpy as jnp
from jax import lax
from jax.experimental import pallas as pl
from jax.experimental.pallas import tpu as pltpu
from jax.sharding import PartitionSpec as P

KEY = 256
HEAD_V = 512
EPSILON = 1e-05
MESH = pl.DeviceIdType.MESH
ANY = pl.BlockSpec(memory_space=pl.ANY)
VMEM = pl.BlockSpec(memory_space=pltpu.VMEM)
BF = jnp.bfloat16
F32 = jnp.float32


def dot(a, b, dims):
    return lax.dot_general(a, b, (dims, ((), ())), preferred_element_type=F32)


def nn(a, b):
    return dot(a, b, ((1,), (0,)))


def nt(a, b):
    return dot(a, b, ((1,), (1,)))


def tn(a, b):
    return dot(a, b, ((0,), (0,)))


class Place:
    def __init__(self, F, C, T):
        self.F, self.C, self.T = F, C, T
        self.f = lax.axis_index("fsdp")
        self.z = lax.axis_index("ctx")
        self.t = lax.axis_index("tp")
        self.lo = lax.rem(self.t, 2)
        self.hi = self.t // 2
        self.near = self.t + 1 - 2 * self.lo
        self.far = lax.rem(self.t + 2, 4)

    def near_first(self):
        return [1] + ([self.C - 1] if self.C > 2 else []) + list(range(2, self.C - 1))

    def ahead(self, d):
        return lax.rem(self.z + d, self.C)

    def behind(self, d):
        return lax.rem(self.z + self.C - d, self.C)

    def fahead(self, d):
        return lax.rem(self.f + d, self.F)

    def fbehind(self, d):
        return lax.rem(self.f + self.F - d, self.F)

    def barrier(self, ctx=True, fsdp=False, tp=True):
        sem = pltpu.get_barrier_semaphore()
        peers = []
        if tp:
            peers += [{"tp": self.near}, {"tp": self.far}]
        if fsdp:
            peers += [{"fsdp": self.fahead(d)} for d in range(1, self.F)]
        if ctx:
            peers += [{"ctx": self.ahead(d)} for d in range(1, self.C)]
        for peer in peers:
            pl.semaphore_signal(sem, inc=1, device_id=peer, device_id_type=MESH)
        pl.semaphore_wait(sem, len(peers))


def remote(src, dst, ssem, rsem, peer):
    return pltpu.make_async_remote_copy(
        src_ref=src, dst_ref=dst, send_sem=ssem, recv_sem=rsem, device_id=peer, device_id_type=MESH
    )


def sem(*shape):
    return pltpu.SemaphoreType.DMA(shape)


def gather_sems(C):
    return [sem(C), sem(C), sem(C), sem(C), sem(C, 2), sem(C, 2), pltpu.SemaphoreType.DMA]


class Gather:
    def __init__(self, pc, x, out, rows, sems):
        self.pc, self.x = pc, x
        self.zs, self.zr, self.ys, self.yr, self.cs, self.cr, self.ls = sems
        self.slot = lambda c, t: out.at[c, t, rows]

    def start(self):
        pc, x = self.pc, self.x
        self.here = self.slot(pc.z, pc.t)
        self.local = pltpu.make_async_copy(x, self.here, self.ls)
        self.local.start()
        self.zc, self.yc, self.cc = {}, {}, {}
        self.later = pc.near_first()
        self.forward(0)
        self.send(2)

    def send(self, count=1):
        for d in self.later[:count]:
            self.zc[d] = remote(
                self.x, self.here, self.zs.at[d], self.zr.at[d], {"ctx": self.pc.ahead(d)}
            )
            self.zc[d].start()
        del self.later[:count]

    def forward(self, d):
        pc = self.pc
        dst = self.slot(pc.behind(d), pc.t)
        src = dst if d else self.x
        if d:
            self.zc[d].wait_recv()
            self.send()
        self.yc[d] = remote(src, dst, self.ys.at[d], self.yr.at[d], {"tp": pc.far})
        self.yc[d].start()
        self.cc[d, 0] = remote(src, dst, self.cs.at[d, 0], self.cr.at[d, 0], {"tp": pc.near})
        self.cc[d, 0].start()

    def onward(self, d):
        pc = self.pc
        self.yc[d].wait_recv()
        src = self.slot(pc.behind(d), pc.far)
        self.cc[d, 1] = remote(src, src, self.cs.at[d, 1], self.cr.at[d, 1], {"tp": pc.near})
        self.cc[d, 1].start()

    def finish(self):
        self.local.wait()
        for cp in self.zc.values():
            cp.wait_send()
        for cp in self.yc.values():
            cp.wait_send()
        for cp in self.cc.values():
            cp.wait()


def share_sems():
    return [sem(3), sem(3)]


def share_stage(pc, x, out, lsem, sems):
    ss, rs = sems
    t = pc.t
    local = pltpu.make_async_copy(x, out.at[t], lsem)
    local.start()
    a = remote(x, out.at[t], ss.at[0], rs.at[0], {"tp": pc.far})
    a.start()
    b = remote(x, out.at[t], ss.at[1], rs.at[1], {"tp": pc.near})
    b.start()
    yield
    a.wait_recv()
    src = out.at[pc.far]
    c = remote(src, src, ss.at[2], rs.at[2], {"tp": pc.near})
    c.start()
    yield
    local.wait()
    a.wait_send()
    b.wait()
    c.wait()


def scatter_scratch(C, Q, W):
    return [
        pltpu.VMEM((C, 2, Q, W), BF),
        pltpu.VMEM((C, Q, W), BF),
        pltpu.VMEM((C, Q, W), BF),
        pltpu.VMEM((C, Q, W), BF),
        pltpu.VMEM((C, Q, W), BF),
        sem(C, 2),
        sem(C, 2),
        sem(C),
        sem(C),
        sem(C),
        sem(C),
    ]


def local_scratch(C, Q, W):
    return [pltpu.VMEM((C, 2, Q, W), BF), sem(C, 2)]


class Scatter:
    def __init__(self, pc, p, rows, scratch, local=None):
        self.pc, self.p, self.rows, self.local = pc, p, rows, local
        (self.buf1, self.snd2, self.buf2, self.snd3, self.buf3) = scratch[:5]
        self.s1, self.r1, self.s2, self.r2, self.s3, self.r3 = scratch[5:]
        self.order = pc.near_first() + [0]
        self.lc, self.c1, self.c2, self.c3 = {}, {}, {}, {}

    def side(self, j):
        return 1 - self.pc.hi if j == 0 else self.pc.hi

    def begin(self, d):
        pc, p, rows = self.pc, self.p, self.rows
        c = pc.ahead(d)
        for j in range(2):
            self.c1[d, j] = remote(
                p.at[c, self.side(j) * 2 + 1 - pc.lo, rows],
                self.buf1.at[d, j],
                self.s1.at[d, j],
                self.r1.at[d, j],
                {"tp": pc.near},
            )
            self.c1[d, j].start()
            if self.local:
                self.lc[d, j] = pltpu.make_async_copy(
                    p.at[c, self.side(j) * 2 + pc.lo, rows],
                    self.local[0].at[d, j],
                    self.local[1].at[d, j],
                )
                self.lc[d, j].start()

    def start(self):
        for d in self.order:
            self.begin(d)

    def own(self, d, j):
        self.c1[d, j].wait_recv()
        if self.local:
            self.lc[d, j].wait()
            here = self.local[0][d, j]
        else:
            here = self.p[self.pc.ahead(d), self.side(j) * 2 + self.pc.lo, self.rows]
        return here.astype(F32) + self.buf1[d, j].astype(F32)

    def far(self, d):
        self.snd2[d] = self.own(d, 0).astype(BF)
        self.c2[d] = remote(
            self.snd2.at[d], self.buf2.at[d], self.s2.at[d], self.r2.at[d], {"tp": self.pc.far}
        )
        self.c2[d].start()

    def along(self, d):
        part = self.own(d, 1)
        self.c2[d].wait_recv()
        part = part + self.buf2[d].astype(F32)
        if d:
            self.snd3[d] = part.astype(BF)
            self.c3[d] = remote(
                self.snd3.at[d],
                self.buf3.at[d],
                self.s3.at[d],
                self.r3.at[d],
                {"ctx": self.pc.ahead(d)},
            )
            self.c3[d].start()
        else:
            self.total = part

    def result(self):
        total = self.total
        for d in range(1, self.pc.C):
            self.c3[d].wait_recv()
            total = total + self.buf3[d].astype(F32)
        return total

    def finish(self):
        for copies in (self.c1, self.c2, self.c3):
            for cp in copies.values():
                cp.wait_send()


def drain(stage):
    for _ in stage:
        pass


class Pump:
    def __init__(self, scatters, begun=0, window=3):
        self.units = [(rs, d) for rs in scatters for d in rs.order]
        self.window, self.begun, self.sent, self.done = window, begun, 0, 0

    def fill(self):
        while self.begun < min(len(self.units), self.done + 2 * self.window):
            rs, d = self.units[self.begun]
            rs.begin(d)
            self.begun += 1
        while self.sent < min(len(self.units), self.done + self.window):
            rs, d = self.units[self.sent]
            rs.far(d)
            self.sent += 1

    def run(self, count):
        for _ in range(count):
            self.fill()
            rs, d = self.units[self.done]
            rs.along(d)
            self.done += 1
        self.fill()


def silu_parts(g):
    s = jax.nn.sigmoid(g)
    return g * s, s * (1.0 + g * (1.0 - s))


PARTS = 2


def halves_of(rows):
    n = rows // PARTS
    return (lambda h: pl.ds(h * n, n)), PARTS


def layer_norm_rows(values, gain, bias):
    center = values - jnp.mean(values, axis=-1, keepdims=True)
    spread = jnp.mean(center * center, axis=-1, keepdims=True)
    return (center * lax.rsqrt(spread + EPSILON) * gain + bias).astype(BF)


def eye_of(n):
    return lax.broadcasted_iota(jnp.int32, (n, n), 0) == lax.broadcasted_iota(jnp.int32, (n, n), 1)


def as_row(column):
    return jnp.sum(jnp.where(eye_of(column.shape[0]), column, 0.0), axis=0, keepdims=True)


def as_column(row):
    return jnp.sum(jnp.where(eye_of(row.shape[1]), row, 0.0), axis=1, keepdims=True)


def decays(rates):
    B = rates.shape[1]
    causal = lax.broadcasted_iota(jnp.int32, (B, B), 0) >= lax.broadcasted_iota(jnp.int32, (B, B), 1)
    column = jnp.sum(jnp.where(causal, rates, 0.0), axis=1, keepdims=True)
    row = as_row(column)
    table = jnp.where(causal, jnp.exp(jnp.minimum(column - row, 0.0)), 0.0)
    total = column[B - 1 :]
    return table, jnp.exp(column), jnp.exp(total - column), jnp.exp(total)


def across_blocks(rows, blocks, i, columns):
    F, C, R, _ = blocks.shape
    group = max(1, 128 // R)
    parts = []
    for g in range(group):
        b = i * group + g
        parts.append(nt(rows, blocks[b // C, lax.rem(b, C), :, columns]))
    part = parts[0] if group == 1 else jnp.concatenate(parts, axis=1)
    return part.astype(BF)


class Mover:
    def __init__(self, pc, weights, layout, out, zs, zr, xs, xr, ls):
        self.pc, self.weights, self.layout, self.out = pc, weights, layout, out
        self.zs, self.zr, self.xs, self.xr, self.ls = zs, zr, xs, xr, ls
        self.zc, self.xc = {}, {}
        rows = out.shape[2]
        near = pc.near_first()
        part = rows // 4
        self.units = [(d, pl.ds(i * part, part)) for d in near for i in range(4)]
        self.later = list(enumerate(self.units))

    def columns(self, dst, part):
        at = 0
        for w, (share, n) in zip(self.weights, self.layout):
            start = pl.multiple_of((dst // share) * n, n)
            yield (
                w.at[part, pl.ds(start, n)],
                self.out.at[self.pc.f, self.pc.z, part, pl.ds(at, n)],
            )
            at += n

    def send(self, count=1):
        pc = self.pc
        for k, (d, part) in self.later[:count]:
            dst = pc.ahead(d)
            sems, peer = (self.zs.at[k], self.zr.at[k]), {"ctx": dst}
            for src, to in self.columns(dst, part):
                remote(src, to, *sems, peer).start()
            here = self.out.at[pc.f, pc.behind(d), part]
            self.zc[k] = remote(here, here, *sems, peer)
        del self.later[:count]

    def start(self, count):
        pc = self.pc
        whole = pl.ds(0, self.out.shape[2])
        own = len(self.units)
        for e in range(1, pc.F):
            sems, peer = (self.xs.at[own, e], self.xr.at[own, e]), {"fsdp": pc.fahead(e)}
            for src, to in self.columns(pc.z, whole):
                remote(src, to, *sems, peer).start()
            here = self.out.at[pc.fbehind(e), pc.z]
            self.xc[own, e] = remote(here, here, *sems, peer)
        for src, to in self.columns(pc.z, whole):
            pltpu.make_async_copy(src, to, self.ls).start()
        here = self.out.at[pc.f, pc.z]
        self.local = pltpu.make_async_copy(here, here, self.ls)
        self.send(count)

    def forward(self, k):
        pc = self.pc
        d, part = self.units[k]
        self.zc[k].wait_recv()
        self.send()
        here = self.out.at[pc.f, pc.behind(d), part]
        for e in range(1, pc.F):
            self.xc[k, e] = remote(
                here, here, self.xs.at[k, e], self.xr.at[k, e], {"fsdp": pc.fahead(e)}
            )
            self.xc[k, e].start()

    def arrived(self, k, e):
        self.xc[k, e].wait_recv()

    def sent(self):
        for cp in list(self.zc.values()) + list(self.xc.values()):
            cp.wait_send()


class Blocks:
    def __init__(self, pc, x, out, zs, zr, ys, yr, cs, cr, ls):
        self.pc, self.x, self.out = pc, x, out
        self.zs, self.zr, self.ys, self.yr, self.cs, self.cr, self.ls = zs, zr, ys, yr, cs, cr, ls
        self.zc, self.yc, self.cc = {}, {}, {}

    def start(self):
        pc = self.pc
        self.later = pc.near_first()
        self.local = pltpu.make_async_copy(self.x, self.out.at[pc.z], self.ls)
        self.local.start()
        self.send(3)

    def send(self, count=1):
        pc = self.pc
        for d in self.later[:count]:
            self.zc[d] = remote(
                self.x.at[pc.t],
                self.out.at[pc.z, pc.t],
                self.zs.at[d],
                self.zr.at[d],
                {"ctx": pc.ahead(d)},
            )
            self.zc[d].start()
        del self.later[:count]

    def forward(self, d):
        pc = self.pc
        self.zc[d].wait_recv()
        self.send()
        here = self.out.at[pc.behind(d), pc.t]
        self.yc[d] = remote(here, here, self.ys.at[d], self.yr.at[d], {"tp": pc.far})
        self.yc[d].start()
        self.cc[d, 0] = remote(here, here, self.cs.at[d, 0], self.cr.at[d, 0], {"tp": pc.near})
        self.cc[d, 0].start()

    def onward(self, d):
        pc = self.pc
        self.yc[d].wait_recv()
        here = self.out.at[pc.behind(d), pc.far]
        self.cc[d, 1] = remote(here, here, self.cs.at[d, 1], self.cr.at[d, 1], {"tp": pc.near})
        self.cc[d, 1].start()

    def finish(self):
        self.local.wait()
        for cp in list(self.zc.values()) + list(self.yc.values()):
            cp.wait_send()
        for cp in self.cc.values():
            cp.wait()


def mover_sems(F, C):
    return [sem(4 * C), sem(4 * C), sem(4 * C, F), sem(4 * C, F), pltpu.SemaphoreType.DMA]


def blocks_sems(C):
    return [sem(C), sem(C), sem(C), sem(C), sem(C, 2), sem(C, 2), pltpu.SemaphoreType.DMA]


def forward_kernel(dims, cfg, *refs):
    F, C, T = dims
    S, B, halves, HV, in_layout, rest_layout = cfg
    refs = list(refs)

    def take(n):
        out = refs[:n]
        del refs[:n]
        return out

    in_weights, rest_weights = take(5), take(3)
    vec, ld, tok, go = take(4)
    o_win, o_normed, o_proj, o_states, o_normal, o_gated, inv, old, vecs, mid, sn, full, ogo = take(13)
    otok, win, ovec, normed, acc, proj, states, state, normal, gated, stats, mytok, x = take(13)
    in_sems, rest_sems = take(5), take(5)
    tok_sems, go_sems = take(7), take(7)
    vzs, vzr, vxs, vxr, lzs, lzr, sts, strr, oses = take(9)
    n, m = len(gather_sems(C)), len(scatter_scratch(C, 8, 128))

    pc = Place(*dims)
    f, z, t = pc.f, pc.z, pc.t
    near = pc.near_first()
    L = S * B
    R = win.shape[2]
    W = F * C * R
    NI = proj.shape[1]
    N = proj.shape[0]
    units = C * S
    saved = []

    def save(src, dst):
        cp = pltpu.make_async_copy(src, dst, oses.at[len(saved)])
        cp.start()
        saved.append(cp)

    pc.barrier(True, True, True)
    vz, vx, lz = {}, {}, {}
    for d in range(1, C):
        peer = {"ctx": pc.ahead(d)}
        vz[d] = remote(vec, ovec.at[f, z], vzs.at[d], vzr.at[d], peer)
        vz[d].start()
        lz[d] = remote(ld, old.at[z], lzs.at[d], lzr.at[d], peer)
        lz[d].start()
    ovec[f, z] = vec[...]
    old[z] = ld[...]

    def vec_across(d):
        for e in range(1, F):
            src = ovec.at[f, pc.behind(d)] if d else vec
            vx[d, e] = remote(
                src, ovec.at[f, pc.behind(d)], vxs.at[d, e], vxr.at[d, e], {"fsdp": pc.fahead(e)}
            )
            vx[d, e].start()

    vec_across(0)
    tk = Blocks(pc, tok, otok, *tok_sems)
    tk.start()
    wi = Mover(pc, in_weights, in_layout, win, *in_sems)
    wi.start(0)
    mine = pltpu.make_async_copy(tok.at[t], mytok, oses.at[15])
    mine.start()
    for d in range(1, C):
        vz[d].wait_recv()
        vec_across(d)
    for d in near:
        tk.forward(d)
        wi.send(4)
    wr = Mover(pc, rest_weights, rest_layout, full, *rest_sems)
    gk = Blocks(pc, go, ogo, *go_sems)
    for d in near:
        tk.onward(d)
    for cp in vx.values():
        cp.wait()
    for cp in vz.values():
        cp.wait_send()
    for b in range(F * C):
        vecs[:, b * R : (b + 1) * R] = ovec[b // C, b % C]
    tk.finish()
    gain1, bias1 = vecs[0:1], vecs[1:2]

    def norm_unit(i, carry):
        rows = otok[i // T, lax.rem(i, T)].astype(F32)
        q = rows.shape[0]
        value = layer_norm_rows(rows, gain1, bias1)
        for b in range(F * C):
            normed[b, pl.ds(pl.multiple_of(i * q, q), q)] = value[:, b * R : (b + 1) * R]
        return carry

    lax.fori_loop(0, C * T, norm_unit, 0)
    save(normed, o_normed)

    tile = min(256, N)

    def project(ff, c, first, last):
        def one(i, carry):
            rows = pl.ds(pl.multiple_of(i * tile, tile), tile)
            part = nn(normed[ff * C + c, rows], win[ff, c, :, :NI])
            if not first:
                part = part + acc[rows]
            if last:
                proj[rows] = part.astype(BF)
            else:
                acc[rows] = part
            return carry

        lax.fori_loop(0, N // tile, one, 0)

    wi.local.wait()
    own = len(wi.units)
    project(f, z, True, False)
    for e in range(1, F):
        wi.arrived(own, e)
        project(pc.fbehind(e), z, False, False)
    gk.start()
    for i, d in enumerate(near):
        keys = [k for k, (dd, _) in enumerate(wi.units) if dd == d]
        for k in keys:
            wi.forward(k)
        project(f, pc.behind(d), False, False)
        if i == 1:
            wr.start(4)
    for i, d in enumerate(near):
        keys = [k for k, (dd, _) in enumerate(wi.units) if dd == d]
        for e in range(1, F):
            for k in keys:
                wi.arrived(k, e)
            project(pc.fbehind(e), pc.behind(d), False, i == C - 2 and e == F - 1)
    gk.send(C)
    wr.send(4)
    save(proj, o_proj)
    save(win, o_win)

    for cp in lz.values():
        cp.wait()
    head = z // halves
    scale = float(KEY) ** (-0.5)
    state[...] = jnp.zeros_like(state)

    def retain(u, carry):
        c, s = u // S, lax.rem(u, S)
        rows = pl.ds(pl.multiple_of(u * B, B), B)
        rates = old[c, pl.ds(head, 1), pl.ds(pl.multiple_of(s * B, B), B)]
        table, growth, keeping, through = decays(rates)
        q, k, v = proj[rows, :KEY], proj[rows, KEY : 2 * KEY], proj[rows, 2 * KEY : 2 * KEY + HV]
        weights = (nt(q, k) * scale * table).astype(BF)
        before = state[s]
        states[u] = before.astype(BF)
        mixed = nn(weights, v) + nn((q.astype(F32) * growth).astype(BF), before.astype(BF))
        state[s] = through * before + tn((k.astype(F32) * keeping).astype(BF), v)
        normal[rows] = mixed
        mean = jnp.mean(mixed, axis=-1, keepdims=True)
        dev = mixed - mean
        stats[0, 0:1, rows] = as_row(mean)
        stats[0, 1:2, rows] = as_row(jnp.sum(dev * dev, axis=-1, keepdims=True))
        return carry

    stats[0] = jnp.zeros(stats.shape[1:], F32)
    lax.fori_loop(0, units, retain, 0)
    save(states, o_states)
    wr.send(4 * C)
    st = []
    place = lax.rem(z, halves)
    for j in range(1, halves):
        peer = {"ctx": z - place + lax.rem(place + j, halves)}
        cp = remote(stats.at[0], stats.at[j], sts.at[j], strr.at[j], peer)
        cp.start()
        st.append(cp)
    for cp in st:
        cp.wait()

    def finish_unit(u, carry):
        rows = pl.ds(pl.multiple_of(u * B, B), B)
        got = [(stats[j, 0:1, rows], stats[j, 1:2, rows]) for j in range(halves)]
        mean = sum(a for a, _ in got) / halves
        m2 = sum(b + HV * (a - mean) * (a - mean) for a, b in got)
        scaled = as_column(lax.rsqrt(m2 / HEAD_V + EPSILON))
        value = (normal[rows] - as_column(mean)) * scaled
        gate = proj[rows, 2 * KEY + HV :].astype(F32)
        normal[rows] = value
        inv[0:1, rows] = lax.rsqrt(m2 / HEAD_V + EPSILON)
        gated[rows] = (gate * jax.nn.sigmoid(gate) * value).astype(BF)
        return carry

    inv[...] = jnp.zeros_like(inv)
    lax.fori_loop(0, units, finish_unit, 0)
    save(normal, o_normal)
    save(gated, o_gated)

    p = otok
    Q = x.shape[0]
    cut, parts = halves_of(Q)
    scatters, gathers = [], []
    for h in range(parts):
        at = h * (n + m)
        gathers.append(Gather(pc, x.at[cut(h)], sn, cut(h), refs[at : at + n]))
        scatters.append(Scatter(pc, p, cut(h), refs[at + n : at + n + m]))
    for d in near + [0]:
        c = pc.ahead(d)
        mixed = gated[pl.ds(pl.multiple_of(c * L, L), L)]

        def one(b, carry):
            part = across_blocks(mixed, win, b, pl.ds(NI, HV))
            columns = pl.ds(pl.multiple_of(b * part.shape[1], 128), part.shape[1])
            for i in range(T):
                p[c, i, :, columns] = part[i * Q : (i + 1) * Q]
            return carry

        lax.fori_loop(0, W // max(R, 128), one, 0)
        scatters[0].begin(d)
    for d in near:
        gk.forward(d)
    pump = Pump(scatters, begun=C)
    pump.run(C)
    for k in range(8):
        wr.forward(k)
    for d in near:
        gk.onward(d)
    mine.wait()
    for h, rs in enumerate(scatters):
        pump.run(min(2, len(pump.units) - pump.done))
        part = cut(h)
        total = rs.result() + mytok[part].astype(F32)
        mid[part] = total
        x[part] = layer_norm_rows(total, vecs[2:3], vecs[3:4])
        gathers[h].start()
        if h == 0:
            pump.run(len(pump.units) - pump.done)
            for k in range(8, len(wr.units)):
                wr.forward(k)
    for ga in gathers:
        for d in near:
            ga.forward(d)
    for ga in gathers:
        for d in [0] + near:
            ga.onward(d)
    for job in scatters + gathers:
        job.finish()
    gk.finish()
    wi.sent()
    wr.local.wait()
    for k in range(len(wr.units) + 1):
        for e in range(1, F):
            wr.arrived(k, e)
    wr.sent()
    for cp in saved:
        cp.wait()


def norm_pull(values, gain, grad):
    center = values - jnp.mean(values, axis=-1, keepdims=True)
    spread = jnp.mean(center * center, axis=-1, keepdims=True)
    inv = lax.rsqrt(spread + EPSILON)
    xhat = center * inv
    g = grad * gain
    back = inv * (
        g - jnp.mean(g, axis=-1, keepdims=True) - xhat * jnp.mean(g * xhat, axis=-1, keepdims=True)
    )
    return (
        back,
        jnp.sum(grad * xhat, axis=0, keepdims=True),
        jnp.sum(grad, axis=0, keepdims=True),
    )


def gelu_parts(v):
    c = (2.0 / jnp.pi) ** 0.5
    t = jnp.tanh(c * (v + 0.044715 * v * v * v))
    return 0.5 * v * (1.0 + t), 0.5 * (1.0 + t) + 0.5 * v * (1.0 - t * t) * c * (
        1.0 + 3 * 0.044715 * v * v
    )


def middle_kernel(dims, cfg, *refs):
    F, C, T = dims
    S, B, U = cfg
    refs = list(refs)

    def take(n):
        out = refs[:n]
        del refs[:n]
        return out

    second, gout, wr, mid, allgo, vecs = take(6)
    gm, gb, out, dgain, dbias, msum = take(6)
    stile, gtile, sblk, gblk, acc, gates, hid, pg, pd, turned, turned2 = take(11)
    msend, mgot, mloc, x, y, go = take(6)
    ssem, gsem, gosem, lsem, msem, mxs, mxr = take(7)
    shares, gsems = take(2), take(len(gather_sems(C)))
    half = len(refs) // 2

    pc = Place(*dims)
    f = pc.f
    near = pc.near_first()
    R, N = wr.shape[2], hid.shape[0]
    Q = x.shape[0]
    W = F * C * R
    pc.barrier(True, True, True)
    mine = pltpu.make_async_copy(allgo.at[pc.t], go, gosem)
    mine.start()
    rg = Scatter(pc, pg, pl.ds(0, Q), refs[:half])
    rd = Scatter(pc, pd, pl.ds(0, Q), refs[half:])
    order = rg.order
    units = [(d, s) for d in order for s in range(S)]

    def rows_of(i):
        d, s = units[i]
        return pl.ds(pl.multiple_of((pc.ahead(d) * S + s) * B, B), B)

    def load(i):
        k = i % 2
        return (
            pltpu.make_async_copy(second.at[rows_of(i)], stile.at[k], ssem.at[k]),
            pltpu.make_async_copy(gout.at[rows_of(i)], gtile.at[k], gsem.at[k]),
        )

    for cp in load(0):
        cp.start()

    def unit(i):
        d, s = units[i]
        k = i % 2
        rows = rows_of(i)
        if i + 1 < len(units):
            for cp in load(i + 1):
                cp.start()
        for cp in load(i):
            cp.wait()
        for b in range(F * C):
            sblk[b, rows] = stile[k, :, b * R : (b + 1) * R]
            gblk[b, rows] = gtile[k, :, b * R : (b + 1) * R]
        acc[...] = jnp.zeros_like(acc)

        def forward(b, carry):
            w = wr[b // C, lax.rem(b, C)]
            acc[:, : 2 * U] += nn(sblk[b, rows], w[:, : 2 * U])
            acc[:, 2 * U :] += nn(gblk[b, rows], w[:, 2 * U :])
            return carry

        lax.fori_loop(0, F * C, forward, 0)
        gate = acc[:, :U].astype(BF).astype(F32)
        up = acc[:, U : 2 * U].astype(BF).astype(F32)
        grad = acc[:, 2 * U :]
        value, slope = gelu_parts(gate)
        hid[rows] = (value * up).astype(BF)
        gates[rows, :U] = (grad * up * slope).astype(BF)
        gates[rows, U:] = (grad * value).astype(BF)
        c = pc.ahead(d)
        pull, keep = gates[rows], hid[rows]

        def back(b, carry):
            for p, part in (
                (pg, across_blocks(pull, wr, b, pl.ds(0, 2 * U))),
                (pd, across_blocks(keep, wr, b, pl.ds(2 * U, U))),
            ):
                columns = pl.ds(pl.multiple_of(b * part.shape[1], 128), part.shape[1])
                for j in range(B // Q):
                    p[c, s * (B // Q) + j, :, columns] = part[j * Q : (j + 1) * Q]
            return carry

        lax.fori_loop(0, W // max(R, 128), back, 0)

    for i in range(len(units)):
        unit(i)
        if units[i][1] == S - 1:
            k = i // S
            rg.begin(order[k])
            rd.begin(order[k])
            if k >= 1:
                rg.far(order[k - 1])
            if k >= 2:
                rg.along(order[k - 2])
    rg.far(order[C - 1])
    for d in order[max(C - 2, 0) :]:
        rg.along(d)
    for d in order:
        rd.far(d)

    xc = {}

    def block(d, e):
        b = pc.fahead(e) * C + pc.ahead(d)
        turned[...] = jnp.transpose(sblk[b])
        turned2[...] = jnp.transpose(gblk[b])
        return nn(turned[...], gates[...]), nn(turned2[...], hid[...])

    for d in order:
        for e in range(1, F):
            c = pc.ahead(d)
            first, last = block(d, e)
            msend[e - 1, d, :, : 2 * U] = first.astype(BF)
            msend[e - 1, d, :, 2 * U :] = last.astype(BF)
            xc[d, e] = remote(
                msend.at[e - 1, d], mgot.at[e - 1, d], mxs.at[d, e], mxr.at[d, e], {"fsdp": pc.fahead(e)}
            )
            xc[d, e].start()

    mine.wait()
    back, dg, db = norm_pull(mid[...], vecs[2:3], rg.result())
    dgain[...] = dg
    dbias[...] = db
    grad_middle = go[...].astype(F32) + back
    gm[...] = grad_middle
    x[...] = grad_middle.astype(BF)
    ga = Gather(pc, x, gb, pl.ds(0, Q), gsems)
    ga.start()
    for d in order[:2]:
        rd.along(d)
    for d in near[:1]:
        ga.forward(d)
    for d in order[2:]:
        rd.along(d)
    for d in near[1:]:
        ga.forward(d)
    saved = []
    for d in order:
        first, last = block(d, 0)
        for e in range(1, F):
            xc[d, e].wait_recv()
            first = first + mgot[e - 1, d, :, : 2 * U].astype(F32)
            last = last + mgot[e - 1, d, :, 2 * U :].astype(F32)
        mloc[d, :, : 2 * U] = first.astype(BF)
        mloc[d, :, 2 * U :] = last.astype(BF)
        cp = pltpu.make_async_copy(mloc.at[d], msum.at[pc.ahead(d)], msem.at[d])
        cp.start()
        saved.append(cp)
    for d in [0] + near:
        ga.onward(d)
    y[...] = (mid[...] + rd.result()).astype(BF)
    drain(share_stage(pc, y, out, lsem, shares))
    for job in (rg, rd, ga):
        job.finish()
    for cp in xc.values():
        cp.wait_send()
    for cp in saved:
        cp.wait()


def vector_stage(pc, v, vout, va, vb, vc, vd, vx, vz, ts, tr, vxs, vxr, vzs, vzr):
    F, C = pc.F, pc.C
    t0 = remote(v, vb, ts.at[0], tr.at[0], {"tp": pc.near})
    t0.start()
    yield
    t0.wait_recv()
    va[...] = v[...] + vb[...]
    t1 = remote(va, vc, ts.at[1], tr.at[1], {"tp": pc.far})
    t1.start()
    yield
    t1.wait_recv()
    vd[...] = va[...] + vc[...]
    vxc, vzc = {}, {}
    for e in range(1, F):
        vxc[e] = remote(
            vd.at[pc.fahead(e)], vx.at[e - 1], vxs.at[e], vxr.at[e], {"fsdp": pc.fahead(e)}
        )
        vxc[e].start()
    yield
    vs = vd[pc.f]
    for e in range(1, F):
        vxc[e].wait_recv()
        vs = vs + vx[e - 1]
    vz[0] = vs
    for d in range(1, C):
        vzc[d] = remote(
            vz.at[0, pc.ahead(d)], vz.at[1, d], vzs.at[d], vzr.at[d], {"ctx": pc.ahead(d)}
        )
        vzc[d].start()
    yield
    acc = vz[0, pc.z]
    for d in range(1, C):
        vzc[d].wait_recv()
        acc = acc + vz[1, d]
    vout[...] = acc
    for cp in [t0, t1] + list(vxc.values()) + list(vzc.values()):
        cp.wait_send()


def vector_scratch(F, C, R):
    full = pltpu.VMEM((F, C, 8, R), F32)
    return [
        full,
        full,
        full,
        full,
        full,
        pltpu.VMEM((F - 1, C, 8, R), F32),
        pltpu.VMEM((2, C, 8, R), F32),
        sem(2),
        sem(2),
        sem(F),
        sem(F),
        sem(C),
        sem(C),
    ]


def backward_kernel(dims, cfg, *refs):
    F, C, T = dims
    S, B, halves, HV = cfg
    refs = list(refs)

    def take(n):
        out = refs[:n]
        del refs[:n]
        return out

    branch, normed, win, proj, states, normal, inv, gated, old, vecs, gm, alltok, mlp, dg2, db2 = take(15)
    gt, gout, mout, vout = take(4)
    btile, ntile, cblock, turned, turned2, gn, gproj, later, stats, p = take(10)
    gsend, xbuf, zsnd, tok, y = take(5)
    bsem, nsem, sts, strr, mzs, mzr, xos, xor, xs, xr, zs, zr, keeps, toksem, lsem, msem = take(16)
    shares, vscratch = take(2), take(13)

    pc = Place(*dims)
    f, z, t = pc.f, pc.z, pc.t
    L = S * B
    R = win.shape[2]
    W = F * C * R
    N, NI = gproj.shape
    Q = y.shape[0]
    units = C * S
    pc.barrier(True, True, True)
    mine = pltpu.make_async_copy(alltok.at[t], tok, toksem)
    mine.start()

    moves = [pltpu.make_async_copy(mlp.at[z], mout.at[z], msem)]
    for d in pc.near_first():
        dst = pc.ahead(d)
        moves.append(remote(mlp.at[dst], mout.at[z], mzs.at[d], mzr.at[d], {"ctx": dst}))
    for cp in moves:
        cp.start()

    def rows_in(u, slot):
        rows = pl.ds(pl.multiple_of(u * B, B), B)
        return pltpu.make_async_copy(branch.at[rows], btile.at[slot], bsem.at[slot])

    rows_in(0, 0).start()
    stats[0] = jnp.zeros(stats.shape[1:], F32)

    def pull_gate(u, carry):
        slot = lax.rem(u, 2)
        pl.when(u + 1 < units)(lambda: rows_in(u + 1, 1 - slot).start())
        rows_in(u, slot).wait()
        grad = None
        rows = pl.ds(pl.multiple_of(u * B, B), B)
        for b in range(F * C):
            piece = btile[slot, :, b * R : (b + 1) * R]
            cblock[b, rows] = piece
            part = nn(piece, win[b // C, b % C, :, NI:])
            grad = part if grad is None else grad + part
        gate = proj[rows, 2 * KEY + HV :].astype(F32)
        silu, dsilu = silu_parts(gate)
        value = normal[rows]
        gproj[rows, 2 * KEY + HV :] = (grad * value * dsilu).astype(BF)
        inner = grad * silu
        gn[rows] = inner
        stats[0, 0:1, rows] = as_row(jnp.sum(inner, axis=-1, keepdims=True))
        stats[0, 1:2, rows] = as_row(jnp.sum(inner * value, axis=-1, keepdims=True))
        return carry

    lax.fori_loop(0, units, pull_gate, 0)
    st = []
    place = lax.rem(z, halves)
    for j in range(1, halves):
        peer = {"ctx": z - place + lax.rem(place + j, halves)}
        cp = remote(stats.at[0], stats.at[j], sts.at[j], strr.at[j], peer)
        cp.start()
        st.append(cp)

    far = sorted(range(1, C), key=lambda d: abs(d - C // 2))
    order = far + [0]
    blocks = [(d, e) for d in order for e in range(1, F)] + [(d, 0) for d in order]
    xo, xc, zc = {}, {}, {}

    def columns_in(i):
        d, e = blocks[i]
        b = pc.fahead(e) * C + pc.ahead(d)
        return b, pltpu.make_async_copy(normed.at[b], ntile.at[i % 2], nsem.at[i % 2])

    def start_columns(i):
        if i < len(blocks):
            columns_in(i)[1].start()

    tail = pl.ds(NI, HV)
    for d, e in blocks[: (F - 1) * C]:
        turned2[...] = jnp.transpose(cblock[pc.fahead(e) * C + pc.ahead(d)])
        gsend[e - 1, d, :, tail] = nn(turned2[...], gated[...]).astype(BF)
        xo[d, e] = remote(
            gsend.at[e - 1, d, :, tail],
            xbuf.at[e - 1, d, :, tail],
            xos.at[d, e],
            xor.at[d, e],
            {"fsdp": pc.fahead(e)},
        )
        xo[d, e].start()

    start_columns(0)
    for cp in st:
        cp.wait()

    head = z // halves
    scale = float(KEY) ** (-0.5)
    later[...] = jnp.zeros_like(later)

    def retain(i, carry):
        u = units - 1 - i
        c, s = u // S, lax.rem(u, S)
        rows = pl.ds(pl.multiple_of(u * B, B), B)
        rates = old[c, pl.ds(head, 1), pl.ds(pl.multiple_of(s * B, B), B)]
        table, growth, keeping, through = decays(rates)
        q, k, v = proj[rows, :KEY], proj[rows, KEY : 2 * KEY], proj[rows, 2 * KEY : 2 * KEY + HV]
        s1 = as_column(sum(stats[j, 0:1, rows] for j in range(halves)) / HEAD_V)
        s2 = as_column(sum(stats[j, 1:2, rows] for j in range(halves)) / HEAD_V)
        mix = (as_column(inv[0:1, rows]) * (gn[rows] - s1 - normal[rows] * s2)).astype(BF)
        weights = (nt(q, k) * scale * table).astype(BF)
        scores = (nt(mix, v) * scale * table).astype(BF)
        after = later[s]
        after_low = after.astype(BF)
        gq = nn(scores, k) + growth * nt(mix, states[u])
        gk = tn(scores, q) + keeping * nt(v, after_low)
        gv = tn(weights, mix) + nn((k.astype(F32) * keeping).astype(BF), after_low)
        later[s] = through * after + tn((q.astype(F32) * growth).astype(BF), mix)
        gproj[rows, :KEY] = gq.astype(BF)
        gproj[rows, KEY : 2 * KEY] = gk.astype(BF)
        gproj[rows, 2 * KEY : 2 * KEY + HV] = gv.astype(BF)
        return carry

    lax.fori_loop(0, units, retain, 0)

    rs = Scatter(pc, p, pl.ds(0, Q), refs)
    for d in rs.order:
        c = pc.ahead(d)
        mixed = gproj[pl.ds(pl.multiple_of(c * L, L), L)]

        def one(b, carry, c=c, mixed=mixed):
            part = across_blocks(mixed, win, b, pl.ds(0, NI))
            columns = pl.ds(pl.multiple_of(b * part.shape[1], 128), part.shape[1])
            for i in range(T):
                p[c, i, :, columns] = part[i * Q : (i + 1) * Q]
            return carry

        lax.fori_loop(0, W // max(R, 128), one, 0)
        rs.begin(d)
    pump = Pump([rs], begun=C)
    pump.fill()

    H = 2
    kept = []
    halfs = [pl.ds(h * (R // H), R // H) for h in range(H)]
    main = pl.ds(0, NI)

    def block(i):
        d, e = blocks[i]
        start_columns(i + 1)
        b, cp = columns_in(i)
        cp.wait()
        turned[...] = jnp.transpose(ntile[i % 2])
        if e == 0:
            turned2[...] = jnp.transpose(cblock[b])
            for g in range(1, F):
                xo[d, g].wait_recv()
                for h in range(H):
                    xc[d, g, h].wait_recv()

        def put(columns, part):
            if e:
                gsend[e - 1, d, :, columns] = part.astype(BF)
            else:
                for g in range(F - 1):
                    part = part + xbuf[g, d, :, columns].astype(F32)
                zsnd[d, :, columns] = part.astype(BF)

        def one(j, carry):
            columns = pl.ds(pl.multiple_of(j * 256, 256), 256)
            put(columns, nn(turned[...], gproj[:, columns]))
            return carry

        lax.fori_loop(0, NI // 256, one, 0)
        if e == 0:
            put(tail, nn(turned2[...], gated[...]))
        for h, part in enumerate(halfs):
            if e:
                xc[d, e, h] = remote(
                    gsend.at[e - 1, d, part, main],
                    xbuf.at[e - 1, d, part, main],
                    xs.at[d, e, h],
                    xr.at[d, e, h],
                    {"fsdp": pc.fahead(e)},
                )
                xc[d, e, h].start()
            elif d:
                zc[d, h] = remote(
                    zsnd.at[d, part], gout.at[z, part], zs.at[d, h], zr.at[d, h], {"ctx": pc.ahead(d)}
                )
                zc[d, h].start()
            else:
                cp = pltpu.make_async_copy(zsnd.at[0, part], gout.at[z, part], keeps.at[h])
                cp.start()
                kept.append(cp)

    sends = (F - 1) * C
    for i in range(sends):
        block(i)
        if pump.done < len(pump.units):
            pump.run(1)
    pump.run(len(pump.units) - pump.done)
    stages = []
    for i in range(sends, len(blocks)):
        block(i)
        if i == sends:
            mine.wait()
            back, dg, db = norm_pull(tok[...].astype(F32), vecs[0:1], rs.result())
            y[...] = (gm[...] + back).astype(BF)
            v = vscratch[0]
            for b in range(F * C):
                rows = [r[:, b * R : (b + 1) * R] for r in (dg, db)] + [
                    r[:, b * R : (b + 1) * R] for r in (dg2, db2)
                ]
                v[b // C, b % C] = jnp.concatenate(rows + [jnp.zeros((4, R), F32)], axis=0)
            stages = [
                share_stage(pc, y, gt, lsem, shares),
                vector_stage(pc, v, vout, *vscratch[1:]),
            ]
        for stage in stages:
            next(stage, None)
    for stage in stages:
        drain(stage)
    rs.finish()
    for cp in kept:
        cp.wait()
    for cp in zc.values():
        cp.wait()
    for cp in list(xc.values()) + list(xo.values()):
        cp.wait_send()
    for cp in moves:
        cp.wait()


def assemble_kernel(halves, key, hv, a, m, q, k, v, g, o, fg, fu, fd):
    c = pl.program_id(0)
    first = lax.rem(c, halves) == 0
    for i, ref in enumerate((q, k)):
        x = a[0, :, i * key : (i + 1) * key].astype(F32)

        @pl.when(first)
        def _(ref=ref, x=x):
            ref[...] = x

        @pl.when(jnp.logical_not(first))
        def _(ref=ref, x=x):
            ref[...] += x

    v[...] = a[0, :, 2 * key : 2 * key + hv].astype(F32)
    g[...] = a[0, :, 2 * key + hv : 2 * key + 2 * hv].astype(F32)
    o[...] = a[0, :, 2 * key + 2 * hv :].astype(F32)
    u = fg.shape[1]
    for i, ref in enumerate((fg, fu, fd)):
        ref[...] = m[0, :, i * u : (i + 1) * u].astype(F32)


def params(cid):
    return pltpu.CompilerParams(collective_id=cid, has_side_effects=True)


def shards(
    dims,
    tokens,
    log_decay,
    w_query,
    w_key,
    w_value,
    w_gate,
    w_out,
    norm1_gain,
    norm1_bias,
    w_ffgate,
    w_ffup,
    w_down,
    norm2_gain,
    norm2_bias,
    grad_out,
):
    F, C, T = dims
    S, B, W = tokens.shape
    L = S * B
    Q = L // T
    N = C * L
    R = w_query.shape[0]
    heads = log_decay.shape[2]
    halves = C // heads
    HV = HEAD_V // halves
    U = w_ffgate.shape[1] // C
    z = lax.axis_index("ctx")
    t = lax.axis_index("tp")
    scale = float(KEY) ** (-0.5)

    f = lax.axis_index("fsdp")

    def hop(x, axis, d):
        n = lax.axis_size(axis)
        return lax.ppermute(x, axis, [(i, (i + d) % n) for i in range(n)])

    def at(x, i, n):
        return lax.dynamic_index_in_dim(x, lax.rem(i, n), 0, False)

    NI, NR = 2 * KEY + 2 * HV, 3 * U
    NO = NI + HV
    vec = jnp.stack([norm1_gain, norm1_bias, norm2_gain, norm2_bias]).astype(F32)
    vec = jnp.pad(vec, ((0, 4), (0, 0)))
    ld = jnp.pad(jnp.transpose(log_decay, (2, 0, 1)).reshape(heads, L), ((0, 8 - heads), (0, 0)))
    tok = tokens.reshape(T, Q, W)
    go = grad_out.reshape(T, Q, W)
    sds = jax.ShapeDtypeStruct
    cfg = (
        S,
        B,
        halves,
        HV,
        ((halves, KEY), (halves, KEY), (1, HV), (1, HV), (1, HV)),
        ((1, U), (1, U), (1, U)),
    )
    owin, normed, proj, states, normal, gated, inv, old, vecs, mid, sn, full, ogo = pl.pallas_call(
        functools.partial(forward_kernel, dims, cfg),
        out_shape=(
            sds((F, C, R, NO), BF),
            sds((F * C, N, R), BF),
            sds((N, NI), BF),
            sds((C * S, KEY, HV), BF),
            sds((N, HV), F32),
            sds((N, HV), BF),
            sds((8, N), F32),
            sds((C, 8, L), F32),
            sds((8, W), F32),
            sds((Q, W), F32),
            sds((C, T, Q, W), BF),
            sds((F, C, R, NR), BF),
            sds((C, T, Q, W), BF),
        ),
        in_specs=[ANY] * 8 + [VMEM, VMEM, ANY, ANY],
        out_specs=[ANY] * 6 + [VMEM] * 4 + [ANY] * 3,
        scratch_shapes=[
            pltpu.VMEM((C, T, Q, W), BF),
            pltpu.VMEM((F, C, R, NO), BF),
            pltpu.VMEM((F, C, 8, R), F32),
            pltpu.VMEM((F * C, N, R), BF),
            pltpu.VMEM((N, NI), F32),
            pltpu.VMEM((N, NI), BF),
            pltpu.VMEM((C * S, KEY, HV), BF),
            pltpu.VMEM((S, KEY, HV), F32),
            pltpu.VMEM((N, HV), F32),
            pltpu.VMEM((N, HV), BF),
            pltpu.VMEM((halves, 8, N), F32),
            pltpu.VMEM((Q, W), BF),
            pltpu.VMEM((Q, W), BF),
        ]
        + mover_sems(F, C) * 2
        + blocks_sems(C) * 2
        + [sem(C), sem(C), sem(C, F), sem(C, F), sem(C), sem(C), sem(halves), sem(halves), sem(16)]
        + (gather_sems(C) + scatter_scratch(C, Q // PARTS, W)) * PARTS,
        compiler_params=params(1),
        name="k_forward",
    )(w_query, w_key, w_value, w_gate, w_out, w_ffgate, w_ffup, w_down, vec, ld, tok, go)
    gm, gb, out, dgain2, dbias2, mlp_sum = pl.pallas_call(
        functools.partial(middle_kernel, dims, (S, B, U)),
        out_shape=(
            sds((Q, W), F32),
            sds((C, T, Q, W), BF),
            sds((T, Q, W), BF),
            sds((1, W), F32),
            sds((1, W), F32),
            sds((C, R, NR), BF),
        ),
        in_specs=[ANY, ANY, VMEM, VMEM, ANY, VMEM],
        out_specs=[VMEM, ANY, ANY, VMEM, VMEM, ANY],
        scratch_shapes=[
            pltpu.VMEM((2, B, W), BF),
            pltpu.VMEM((2, B, W), BF),
            pltpu.VMEM((F * C, N, R), BF),
            pltpu.VMEM((F * C, N, R), BF),
            pltpu.VMEM((B, 3 * U), F32),
            pltpu.VMEM((N, 2 * U), BF),
            pltpu.VMEM((N, U), BF),
            pltpu.VMEM((C, T, Q, W), BF),
            pltpu.VMEM((C, T, Q, W), BF),
            pltpu.VMEM((R, N), BF),
            pltpu.VMEM((R, N), BF),
            pltpu.VMEM((F - 1, C, R, NR), BF),
            pltpu.VMEM((F - 1, C, R, NR), BF),
            pltpu.VMEM((C, R, NR), BF),
            pltpu.VMEM((Q, W), BF),
            pltpu.VMEM((Q, W), BF),
            pltpu.VMEM((Q, W), BF),
            sem(2),
            sem(2),
            pltpu.SemaphoreType.DMA,
            pltpu.SemaphoreType.DMA,
            sem(C),
            sem(C, F),
            sem(C, F),
        ]
        + share_sems()
        + gather_sems(C)
        + scatter_scratch(C, Q, W) * 2,
        compiler_params=params(3),
        name="k_middle",
    )(sn.reshape(N, W), ogo.reshape(N, W), full, mid, go, vecs)
    output = out.reshape(tokens.shape)

    branch = gb.reshape(N, W)
    H = 2
    gt, gsum, mlp_grads, vsum = pl.pallas_call(
        functools.partial(backward_kernel, dims, (S, B, halves, HV)),
        out_shape=(
            sds((T, Q, W), BF),
            sds((C, R, NO), BF),
            sds((C, R, NR), BF),
            sds((8, R), F32),
        ),
        in_specs=[ANY, ANY] + [VMEM] * 9 + [ANY, ANY, VMEM, VMEM],
        out_specs=[ANY, ANY, ANY, VMEM],
        scratch_shapes=[
            pltpu.VMEM((2, B, W), BF),
            pltpu.VMEM((2, N, R), BF),
            pltpu.VMEM((F * C, N, R), BF),
            pltpu.VMEM((R, N), BF),
            pltpu.VMEM((R, N), BF),
            pltpu.VMEM((N, HV), F32),
            pltpu.VMEM((N, NI), BF),
            pltpu.VMEM((S, KEY, HV), F32),
            pltpu.VMEM((halves, 8, N), F32),
            pltpu.VMEM((C, T, Q, W), BF),
            pltpu.VMEM((F - 1, C, R, NO), BF),
            pltpu.VMEM((F - 1, C, R, NO), BF),
            pltpu.VMEM((C, R, NO), BF),
            pltpu.VMEM((Q, W), BF),
            pltpu.VMEM((Q, W), BF),
            sem(2),
            sem(2),
            sem(halves),
            sem(halves),
            sem(C),
            sem(C),
            sem(C, F),
            sem(C, F),
            sem(C, F, H),
            sem(C, F, H),
            sem(C, H),
            sem(C, H),
            sem(H),
        ]
        + [pltpu.SemaphoreType.DMA] * 3
        + share_sems()
        + vector_scratch(F, C, R)
        + scatter_scratch(C, Q, W),
        compiler_params=params(4),
        name="k_backward",
    )(
        branch,
        normed,
        owin,
        proj,
        states,
        normal,
        inv,
        gated,
        old,
        vecs,
        gm,
        tok,
        mlp_sum,
        dgain2,
        dbias2,
    )
    grad_tokens = gt.reshape(tokens.shape)

    def quarter(n):
        return pl.BlockSpec((R, n), lambda c: (0, c))

    per_head = pl.BlockSpec((R, KEY), lambda c: (0, c // halves))
    gq, gk, gv, gg, gw, gfg, gfu, gfd = pl.pallas_call(
        functools.partial(assemble_kernel, halves, KEY, HV),
        out_shape=[sds((R, heads * KEY), F32)] * 2
        + [sds((R, C * HV), F32)] * 3
        + [sds((R, C * U), F32)] * 3,
        grid=(C,),
        in_specs=[
            pl.BlockSpec((1, R, NO), lambda c: (c, 0, 0)),
            pl.BlockSpec((1, R, NR), lambda c: (c, 0, 0)),
        ],
        out_specs=[per_head, per_head] + [quarter(HV)] * 3 + [quarter(U)] * 3,
        name="k_assemble",
    )(gsum, mlp_grads)
    return (
        output,
        grad_tokens,
        gq,
        gk,
        gv,
        gg,
        gw,
        vsum[0],
        vsum[1],
        gfg,
        gfu,
        gfd,
        vsum[2],
        vsum[3],
    )


def solution(mesh):
    dims = (mesh.shape["fsdp"], mesh.shape["ctx"], mesh.shape["tp"])
    rows, vec = P(("fsdp", "ctx"), "tp"), P(("fsdp", "ctx"))
    acts = P("fsdp", "ctx", None)
    return jax.shard_map(
        functools.partial(shards, dims),
        mesh=mesh,
        in_specs=(acts, P("fsdp", "ctx", "tp"), rows, rows, rows, rows, rows, vec, vec, rows, rows, rows, vec, vec, acts),
        out_specs=(acts, acts, rows, rows, rows, rows, rows, vec, vec, rows, rows, rows, vec, vec),
        check_vma=False,
    )
```

```python
import functools

import jax
import jax.numpy as jnp
from jax import lax
from jax.experimental import pallas as pl
from jax.experimental.pallas import tpu as pltpu
from jax.sharding import PartitionSpec as P

KEY = 256
HEAD_V = 512
EPSILON = 1e-05
MESH = pl.DeviceIdType.MESH
ANY = pl.BlockSpec(memory_space=pl.ANY)
VMEM = pl.BlockSpec(memory_space=pltpu.VMEM)
BF = jnp.bfloat16
F32 = jnp.float32


def dot(a, b, dims):
    return lax.dot_general(a, b, (dims, ((), ())), preferred_element_type=F32)


def nn(a, b):
    return dot(a, b, ((1,), (0,)))


def nt(a, b):
    return dot(a, b, ((1,), (1,)))


def tn(a, b):
    return dot(a, b, ((0,), (0,)))


class Place:
    def __init__(self, F, C, T):
        self.F, self.C, self.T = F, C, T
        self.f = lax.axis_index("fsdp")
        self.z = lax.axis_index("ctx")
        self.t = lax.axis_index("tp")
        self.lo = lax.rem(self.t, 2)
        self.hi = self.t // 2
        self.near = self.t + 1 - 2 * self.lo
        self.far = lax.rem(self.t + 2, 4)

    def near_first(self):
        return [1] + ([self.C - 1] if self.C > 2 else []) + list(range(2, self.C - 1))

    def ahead(self, d):
        return lax.rem(self.z + d, self.C)

    def behind(self, d):
        return lax.rem(self.z + self.C - d, self.C)

    def fahead(self, d):
        return lax.rem(self.f + d, self.F)

    def fbehind(self, d):
        return lax.rem(self.f + self.F - d, self.F)

    def barrier(self, ctx=True, fsdp=False, tp=True):
        sem = pltpu.get_barrier_semaphore()
        peers = []
        if tp:
            peers += [{"tp": self.near}, {"tp": self.far}]
        if fsdp:
            peers += [{"fsdp": self.fahead(d)} for d in range(1, self.F)]
        if ctx:
            peers += [{"ctx": self.ahead(d)} for d in range(1, self.C)]
        for peer in peers:
            pl.semaphore_signal(sem, inc=1, device_id=peer, device_id_type=MESH)
        pl.semaphore_wait(sem, len(peers))


def remote(src, dst, ssem, rsem, peer):
    return pltpu.make_async_remote_copy(
        src_ref=src, dst_ref=dst, send_sem=ssem, recv_sem=rsem, device_id=peer, device_id_type=MESH
    )


def sem(*shape):
    return pltpu.SemaphoreType.DMA(shape)


def gather_sems(C):
    return [sem(C), sem(C), sem(C), sem(C), sem(C, 2), sem(C, 2), pltpu.SemaphoreType.DMA]


class Gather:
    def __init__(self, pc, x, out, rows, sems):
        self.pc, self.x = pc, x
        self.zs, self.zr, self.ys, self.yr, self.cs, self.cr, self.ls = sems
        self.slot = lambda c, t: out.at[c, t, rows]

    def start(self):
        pc, x = self.pc, self.x
        self.here = self.slot(pc.z, pc.t)
        self.local = pltpu.make_async_copy(x, self.here, self.ls)
        self.local.start()
        self.zc, self.yc, self.cc = {}, {}, {}
        self.later = pc.near_first()
        self.forward(0)
        self.send(2)

    def send(self, count=1):
        for d in self.later[:count]:
            self.zc[d] = remote(
                self.x, self.here, self.zs.at[d], self.zr.at[d], {"ctx": self.pc.ahead(d)}
            )
            self.zc[d].start()
        del self.later[:count]

    def forward(self, d):
        pc = self.pc
        dst = self.slot(pc.behind(d), pc.t)
        src = dst if d else self.x
        if d:
            self.zc[d].wait_recv()
            self.send()
        self.yc[d] = remote(src, dst, self.ys.at[d], self.yr.at[d], {"tp": pc.far})
        self.yc[d].start()
        self.cc[d, 0] = remote(src, dst, self.cs.at[d, 0], self.cr.at[d, 0], {"tp": pc.near})
        self.cc[d, 0].start()

    def onward(self, d):
        pc = self.pc
        self.yc[d].wait_recv()
        src = self.slot(pc.behind(d), pc.far)
        self.cc[d, 1] = remote(src, src, self.cs.at[d, 1], self.cr.at[d, 1], {"tp": pc.near})
        self.cc[d, 1].start()

    def finish(self):
        self.local.wait()
        for cp in self.zc.values():
            cp.wait_send()
        for cp in self.yc.values():
            cp.wait_send()
        for cp in self.cc.values():
            cp.wait()


def chain_sems(C):
    return [sem(2, C), sem(2, C), sem(2, C), sem(2, C), sem(2, C, 2), sem(2, C, 2), pltpu.SemaphoreType.DMA]


class Chain:
    def __init__(self, pc, x, slot, sems, own=None):
        self.pc, self.x, self.slot, self.block = pc, x, slot, own
        self.zs, self.zr, self.ys, self.yr, self.cs, self.cr, self.ls = sems

    def came(self, s, h):
        z = self.pc.z
        return (z >= h, z - h) if s == 0 else (z + h <= self.pc.C - 1, z + h)

    def goes(self, s, h):
        pc = self.pc
        if s == 0:
            return jnp.logical_and(pc.z >= h - 1, pc.z < pc.C - 1)
        return jnp.logical_and(pc.z + h <= pc.C, pc.z > 0)

    def hop(self, s, h, c):
        z = self.pc.z
        here = self.slot(c, self.pc.t)
        src = self.x if h == 1 else here
        return remote(src, here, self.zs.at[s, h], self.zr.at[s, h], {"ctx": z + 1 if s == 0 else z - 1})

    def to_far(self, s, h, c):
        here = self.slot(c, self.pc.t)
        src = here if h else self.x
        return remote(src, here, self.ys.at[s, h], self.yr.at[s, h], {"tp": self.pc.far})

    def to_near(self, s, h, c):
        here = self.slot(c, self.pc.t)
        src = here if h else self.x
        return remote(src, here, self.cs.at[s, h, 0], self.cr.at[s, h, 0], {"tp": self.pc.near})

    def spread(self, s, h, c):
        self.to_far(s, h, c).start()
        self.to_near(s, h, c).start()

    def again(self, s, h, c):
        there = self.slot(c, self.pc.far)
        return remote(there, there, self.cs.at[s, h, 1], self.cr.at[s, h, 1], {"tp": self.pc.near})

    def start(self):
        pc = self.pc
        for s in range(2):
            pl.when(self.goes(s, 1))(lambda s=s: self.hop(s, 1, pc.z).start())
        src, dst = self.block or (self.x, self.slot(pc.z, pc.t))
        self.local = pltpu.make_async_copy(src, dst, self.ls)
        self.local.start()
        if not self.block:
            self.spread(0, 0, pc.z)

    def forward(self, h):
        for s in range(2):
            ok, c = self.came(s, h)

            @pl.when(ok)
            def _(s=s, c=c):
                self.hop(s, h, c).wait_recv()
                if h + 1 < self.pc.C:
                    pl.when(self.goes(s, h + 1))(lambda: self.hop(s, h + 1, c).start())
                self.spread(s, h, c)

    def onward(self, h):
        if h == 0:
            if not self.block:
                self.to_far(0, 0, self.pc.z).wait_recv()
                self.again(0, 0, self.pc.z).start()
            return
        for s in range(2):
            ok, c = self.came(s, h)

            @pl.when(ok)
            def _(s=s, c=c):
                self.to_far(s, h, c).wait_recv()
                self.again(s, h, c).start()

    def settle(self, s, h, c):
        self.to_far(s, h, c).wait_send()
        self.to_near(s, h, c).wait()
        self.again(s, h, c).wait()

    def finish(self):
        pc = self.pc
        self.local.wait()
        if not self.block:
            self.settle(0, 0, pc.z)
        for h in range(1, pc.C):
            for s in range(2):
                ok, c = self.came(s, h)
                first = pc.z - h + 1 if s == 0 else pc.z + h - 1
                pl.when(self.goes(s, h))(lambda s=s, c=first: self.hop(s, h, c).wait_send())
                pl.when(ok)(lambda s=s, c=c: self.settle(s, h, c))


def share_sems():
    return [sem(3), sem(3)]


def share_stage(pc, x, out, lsem, sems):
    ss, rs = sems
    t = pc.t
    local = pltpu.make_async_copy(x, out.at[t], lsem)
    local.start()
    a = remote(x, out.at[t], ss.at[0], rs.at[0], {"tp": pc.far})
    a.start()
    b = remote(x, out.at[t], ss.at[1], rs.at[1], {"tp": pc.near})
    b.start()
    yield
    a.wait_recv()
    src = out.at[pc.far]
    c = remote(src, src, ss.at[2], rs.at[2], {"tp": pc.near})
    c.start()
    yield
    local.wait()
    a.wait_send()
    b.wait()
    c.wait()


def scatter_scratch(C, Q, W):
    return [
        pltpu.VMEM((C, 2, Q, W), BF),
        pltpu.VMEM((C, Q, W), BF),
        pltpu.VMEM((C, Q, W), BF),
        pltpu.VMEM((C, Q, W), BF),
        pltpu.VMEM((C, Q, W), BF),
        sem(C, 2),
        sem(C, 2),
        sem(C),
        sem(C),
        sem(C),
        sem(C),
    ]


def local_scratch(C, Q, W):
    return [pltpu.VMEM((C, 2, Q, W), BF), sem(C, 2)]


class Scatter:
    def __init__(self, pc, p, rows, scratch, local=None):
        self.pc, self.p, self.rows, self.local = pc, p, rows, local
        (self.buf1, self.snd2, self.buf2, self.snd3, self.buf3) = scratch[:5]
        self.s1, self.r1, self.s2, self.r2, self.s3, self.r3 = scratch[5:]
        self.order = pc.near_first() + [0]
        self.lc, self.c1, self.c2, self.c3 = {}, {}, {}, {}

    def side(self, j):
        return 1 - self.pc.hi if j == 0 else self.pc.hi

    def begin(self, d):
        pc, p, rows = self.pc, self.p, self.rows
        c = pc.ahead(d)
        for j in range(2):
            self.c1[d, j] = remote(
                p.at[c, self.side(j) * 2 + 1 - pc.lo, rows],
                self.buf1.at[d, j],
                self.s1.at[d, j],
                self.r1.at[d, j],
                {"tp": pc.near},
            )
            self.c1[d, j].start()
            if self.local:
                self.lc[d, j] = pltpu.make_async_copy(
                    p.at[c, self.side(j) * 2 + pc.lo, rows],
                    self.local[0].at[d, j],
                    self.local[1].at[d, j],
                )
                self.lc[d, j].start()

    def start(self):
        for d in self.order:
            self.begin(d)

    def own(self, d, j):
        self.c1[d, j].wait_recv()
        if self.local:
            self.lc[d, j].wait()
            here = self.local[0][d, j]
        else:
            here = self.p[self.pc.ahead(d), self.side(j) * 2 + self.pc.lo, self.rows]
        return here.astype(F32) + self.buf1[d, j].astype(F32)

    def far(self, d):
        self.snd2[d] = self.own(d, 0).astype(BF)
        self.c2[d] = remote(
            self.snd2.at[d], self.buf2.at[d], self.s2.at[d], self.r2.at[d], {"tp": self.pc.far}
        )
        self.c2[d].start()

    def along(self, d):
        part = self.own(d, 1)
        self.c2[d].wait_recv()
        part = part + self.buf2[d].astype(F32)
        if d:
            self.snd3[d] = part.astype(BF)
            self.c3[d] = remote(
                self.snd3.at[d],
                self.buf3.at[d],
                self.s3.at[d],
                self.r3.at[d],
                {"ctx": self.pc.ahead(d)},
            )
            self.c3[d].start()
        else:
            self.total = part

    def result(self):
        total = self.total
        for d in range(1, self.pc.C):
            self.c3[d].wait_recv()
            total = total + self.buf3[d].astype(F32)
        return total

    def finish(self):
        for copies in (self.c1, self.c2, self.c3):
            for cp in copies.values():
                cp.wait_send()


def drain(stage):
    for _ in stage:
        pass


class Pump:
    def __init__(self, scatters, begun=0, window=3):
        self.units = [(rs, d) for rs in scatters for d in rs.order]
        self.window, self.begun, self.sent, self.done = window, begun, 0, 0

    def fill(self):
        while self.begun < min(len(self.units), self.done + 2 * self.window):
            rs, d = self.units[self.begun]
            rs.begin(d)
            self.begun += 1
        while self.sent < min(len(self.units), self.done + self.window):
            rs, d = self.units[self.sent]
            rs.far(d)
            self.sent += 1

    def run(self, count):
        for _ in range(count):
            self.fill()
            rs, d = self.units[self.done]
            rs.along(d)
            self.done += 1
        self.fill()


def silu_parts(g):
    s = jax.nn.sigmoid(g)
    return g * s, s * (1.0 + g * (1.0 - s))


PARTS = 2


def halves_of(rows):
    n = rows // PARTS
    return (lambda h: pl.ds(h * n, n)), PARTS


def layer_norm_rows(values, gain, bias):
    center = values - jnp.mean(values, axis=-1, keepdims=True)
    spread = jnp.mean(center * center, axis=-1, keepdims=True)
    return (center * lax.rsqrt(spread + EPSILON) * gain + bias).astype(BF)


def eye_of(n):
    return lax.broadcasted_iota(jnp.int32, (n, n), 0) == lax.broadcasted_iota(jnp.int32, (n, n), 1)


def as_row(column):
    return jnp.sum(jnp.where(eye_of(column.shape[0]), column, 0.0), axis=0, keepdims=True)


def as_column(row):
    return jnp.sum(jnp.where(eye_of(row.shape[1]), row, 0.0), axis=1, keepdims=True)


def decays(rates):
    B = rates.shape[1]
    causal = lax.broadcasted_iota(jnp.int32, (B, B), 0) >= lax.broadcasted_iota(jnp.int32, (B, B), 1)
    column = jnp.sum(jnp.where(causal, rates, 0.0), axis=1, keepdims=True)
    row = as_row(column)
    table = jnp.where(causal, jnp.exp(jnp.minimum(column - row, 0.0)), 0.0)
    total = column[B - 1 :]
    return table, jnp.exp(column), jnp.exp(total - column), jnp.exp(total)


def across_blocks(rows, blocks, i, columns):
    F, C, R, _ = blocks.shape
    group = max(1, 128 // R)
    parts = []
    for g in range(group):
        b = i * group + g
        parts.append(nt(rows, blocks[b // C, lax.rem(b, C), :, columns]))
    part = parts[0] if group == 1 else jnp.concatenate(parts, axis=1)
    return part.astype(BF)


class Mover:
    def __init__(self, pc, weights, layout, out, zs, zr, xs, xr, ls):
        self.pc, self.weights, self.layout, self.out = pc, weights, layout, out
        self.zs, self.zr, self.xs, self.xr, self.ls = zs, zr, xs, xr, ls
        self.zc, self.xc = {}, {}
        rows = out.shape[2]
        near = pc.near_first()
        part = rows // 4
        self.units = [(d, pl.ds(i * part, part)) for d in near for i in range(4)]
        self.later = list(enumerate(self.units))

    def columns(self, dst, part):
        at = 0
        for w, (share, n) in zip(self.weights, self.layout):
            start = pl.multiple_of((dst // share) * n, n)
            yield (
                w.at[part, pl.ds(start, n)],
                self.out.at[self.pc.f, self.pc.z, part, pl.ds(at, n)],
            )
            at += n

    def send(self, count=1):
        pc = self.pc
        for k, (d, part) in self.later[:count]:
            dst = pc.ahead(d)
            sems, peer = (self.zs.at[k], self.zr.at[k]), {"ctx": dst}
            for src, to in self.columns(dst, part):
                remote(src, to, *sems, peer).start()
            here = self.out.at[pc.f, pc.behind(d), part]
            self.zc[k] = remote(here, here, *sems, peer)
        del self.later[:count]

    def start(self, count):
        pc = self.pc
        whole = pl.ds(0, self.out.shape[2])
        own = len(self.units)
        for e in range(1, pc.F):
            sems, peer = (self.xs.at[own, e], self.xr.at[own, e]), {"fsdp": pc.fahead(e)}
            for src, to in self.columns(pc.z, whole):
                remote(src, to, *sems, peer).start()
            here = self.out.at[pc.fbehind(e), pc.z]
            self.xc[own, e] = remote(here, here, *sems, peer)
        for src, to in self.columns(pc.z, whole):
            pltpu.make_async_copy(src, to, self.ls).start()
        here = self.out.at[pc.f, pc.z]
        self.local = pltpu.make_async_copy(here, here, self.ls)
        self.send(count)

    def forward(self, k):
        pc = self.pc
        d, part = self.units[k]
        self.zc[k].wait_recv()
        self.send()
        here = self.out.at[pc.f, pc.behind(d), part]
        for e in range(1, pc.F):
            self.xc[k, e] = remote(
                here, here, self.xs.at[k, e], self.xr.at[k, e], {"fsdp": pc.fahead(e)}
            )
            self.xc[k, e].start()

    def arrived(self, k, e):
        self.xc[k, e].wait_recv()

    def sent(self):
        for cp in list(self.zc.values()) + list(self.xc.values()):
            cp.wait_send()


class Blocks:
    def __init__(self, pc, x, out, zs, zr, ys, yr, cs, cr, ls):
        self.pc, self.x, self.out = pc, x, out
        self.zs, self.zr, self.ys, self.yr, self.cs, self.cr, self.ls = zs, zr, ys, yr, cs, cr, ls
        self.zc, self.yc, self.cc = {}, {}, {}

    def start(self):
        pc = self.pc
        self.later = pc.near_first()
        self.local = pltpu.make_async_copy(self.x, self.out.at[pc.z], self.ls)
        self.local.start()
        self.send(3)

    def send(self, count=1):
        pc = self.pc
        for d in self.later[:count]:
            self.zc[d] = remote(
                self.x.at[pc.t],
                self.out.at[pc.z, pc.t],
                self.zs.at[d],
                self.zr.at[d],
                {"ctx": pc.ahead(d)},
            )
            self.zc[d].start()
        del self.later[:count]

    def forward(self, d):
        pc = self.pc
        self.zc[d].wait_recv()
        self.send()
        here = self.out.at[pc.behind(d), pc.t]
        self.yc[d] = remote(here, here, self.ys.at[d], self.yr.at[d], {"tp": pc.far})
        self.yc[d].start()
        self.cc[d, 0] = remote(here, here, self.cs.at[d, 0], self.cr.at[d, 0], {"tp": pc.near})
        self.cc[d, 0].start()

    def onward(self, d):
        pc = self.pc
        self.yc[d].wait_recv()
        here = self.out.at[pc.behind(d), pc.far]
        self.cc[d, 1] = remote(here, here, self.cs.at[d, 1], self.cr.at[d, 1], {"tp": pc.near})
        self.cc[d, 1].start()

    def finish(self):
        self.local.wait()
        for cp in list(self.zc.values()) + list(self.yc.values()):
            cp.wait_send()
        for cp in self.cc.values():
            cp.wait()


def mover_sems(F, C):
    return [sem(4 * C), sem(4 * C), sem(4 * C, F), sem(4 * C, F), pltpu.SemaphoreType.DMA]


def blocks_sems(C):
    return [sem(C), sem(C), sem(C), sem(C), sem(C, 2), sem(C, 2), pltpu.SemaphoreType.DMA]


def forward_kernel(dims, cfg, *refs):
    F, C, T = dims
    S, B, halves, HV, in_layout, rest_layout = cfg
    refs = list(refs)

    def take(n):
        out = refs[:n]
        del refs[:n]
        return out

    in_weights, rest_weights = take(5), take(3)
    norms, rates_in, tok, go = take(4), take(1)[0], *take(2)
    o_win, o_normed, o_proj, o_states, o_normal, o_gated, inv, old, vecs, mid, sn, full, ogo = take(13)
    otok, win, ovec, normed, acc, proj, states, state, normal, gated, stats, mytok, x = take(13)
    in_sems, rest_sems = take(5), take(5)
    tok_sems, go_sems = take(7), take(7)
    vzs, vzr, vxs, vxr, lzs, lzr, sts, strr, oses = take(9)
    vec, ld = take(2)
    n, m = len(chain_sems(C)), len(scatter_scratch(C, 8, 128))

    pc = Place(*dims)
    f, z, t = pc.f, pc.z, pc.t
    near = pc.near_first()
    L = S * B
    R = win.shape[2]
    W = F * C * R
    NI = proj.shape[1]
    N = proj.shape[0]
    units = C * S
    saved = []

    def save(src, dst):
        cp = pltpu.make_async_copy(src, dst, oses.at[len(saved)])
        cp.start()
        saved.append(cp)

    R = vec.shape[1]
    vec[...] = jnp.zeros_like(vec)
    for i, ref in enumerate(norms):
        vec[i : i + 1] = ref[...].astype(F32).reshape(1, R)
    ld[...] = jnp.zeros_like(ld)
    for s in range(S):
        for i in range(rates_in.shape[2]):
            ld[i : i + 1, s * B : (s + 1) * B] = as_row(rates_in[s, :, i : i + 1])
    pc.barrier(True, True, True)
    vz, vx, lz = {}, {}, {}
    for d in range(1, C):
        peer = {"ctx": pc.ahead(d)}
        vz[d] = remote(vec, ovec.at[f, z], vzs.at[d], vzr.at[d], peer)
        vz[d].start()
        lz[d] = remote(ld, old.at[z], lzs.at[d], lzr.at[d], peer)
        lz[d].start()
    ovec[f, z] = vec[...]
    old[z] = ld[...]

    def vec_across(d):
        for e in range(1, F):
            src = ovec.at[f, pc.behind(d)] if d else vec
            vx[d, e] = remote(
                src, ovec.at[f, pc.behind(d)], vxs.at[d, e], vxr.at[d, e], {"fsdp": pc.fahead(e)}
            )
            vx[d, e].start()

    vec_across(0)
    tk = Blocks(pc, tok, otok, *tok_sems)
    tk.start()
    wi = Mover(pc, in_weights, in_layout, win, *in_sems)
    wi.start(0)
    mine = pltpu.make_async_copy(tok.at[t], mytok, oses.at[15])
    mine.start()
    for d in range(1, C):
        vz[d].wait_recv()
        vec_across(d)
    for d in near:
        tk.forward(d)
        wi.send(4)
    wr = Mover(pc, rest_weights, rest_layout, full, *rest_sems)
    gk = Blocks(pc, go, ogo, *go_sems)
    for d in near:
        tk.onward(d)
    for cp in vx.values():
        cp.wait()
    for cp in vz.values():
        cp.wait_send()
    for b in range(F * C):
        vecs[:, b * R : (b + 1) * R] = ovec[b // C, b % C]
    tk.finish()
    gain1, bias1 = vecs[0:1], vecs[1:2]

    def norm_unit(i, carry):
        rows = otok[i // T, lax.rem(i, T)].astype(F32)
        q = rows.shape[0]
        value = layer_norm_rows(rows, gain1, bias1)
        for b in range(F * C):
            normed[b, pl.ds(pl.multiple_of(i * q, q), q)] = value[:, b * R : (b + 1) * R]
        return carry

    lax.fori_loop(0, C * T, norm_unit, 0)
    save(normed, o_normed)

    tile = min(256, N)

    def project(ff, c, first, last):
        def one(i, carry):
            rows = pl.ds(pl.multiple_of(i * tile, tile), tile)
            part = nn(normed[ff * C + c, rows], win[ff, c, :, :NI])
            if not first:
                part = part + acc[rows]
            if last:
                proj[rows] = part.astype(BF)
            else:
                acc[rows] = part
            return carry

        lax.fori_loop(0, N // tile, one, 0)

    wi.local.wait()
    own = len(wi.units)
    project(f, z, True, False)
    for e in range(1, F):
        wi.arrived(own, e)
        project(pc.fbehind(e), z, False, False)
    gk.start()
    for i, d in enumerate(near):
        keys = [k for k, (dd, _) in enumerate(wi.units) if dd == d]
        for k in keys:
            wi.forward(k)
        project(f, pc.behind(d), False, False)
        if i == 1:
            wr.start(4)
    for i, d in enumerate(near):
        keys = [k for k, (dd, _) in enumerate(wi.units) if dd == d]
        for e in range(1, F):
            for k in keys:
                wi.arrived(k, e)
            project(pc.fbehind(e), pc.behind(d), False, i == C - 2 and e == F - 1)
    gk.send(C)
    wr.send(4)
    save(proj, o_proj)
    save(win, o_win)

    for cp in lz.values():
        cp.wait()
    head = z // halves
    scale = float(KEY) ** (-0.5)
    state[...] = jnp.zeros_like(state)

    def retain(u, carry):
        c, s = u // S, lax.rem(u, S)
        rows = pl.ds(pl.multiple_of(u * B, B), B)
        rates = old[c, pl.ds(head, 1), pl.ds(pl.multiple_of(s * B, B), B)]
        table, growth, keeping, through = decays(rates)
        q, k, v = proj[rows, :KEY], proj[rows, KEY : 2 * KEY], proj[rows, 2 * KEY : 2 * KEY + HV]
        weights = (nt(q, k) * scale * table).astype(BF)
        before = state[s]
        states[u] = before.astype(BF)
        mixed = nn(weights, v) + nn((q.astype(F32) * growth).astype(BF), before.astype(BF))
        state[s] = through * before + tn((k.astype(F32) * keeping).astype(BF), v)
        normal[rows] = mixed
        mean = jnp.mean(mixed, axis=-1, keepdims=True)
        dev = mixed - mean
        stats[0, 0:1, rows] = as_row(mean)
        stats[0, 1:2, rows] = as_row(jnp.sum(dev * dev, axis=-1, keepdims=True))
        return carry

    stats[0] = jnp.zeros(stats.shape[1:], F32)
    lax.fori_loop(0, units, retain, 0)
    save(states, o_states)
    wr.send(4 * C)
    st = []
    place = lax.rem(z, halves)
    for j in range(1, halves):
        peer = {"ctx": z - place + lax.rem(place + j, halves)}
        cp = remote(stats.at[0], stats.at[j], sts.at[j], strr.at[j], peer)
        cp.start()
        st.append(cp)
    for cp in st:
        cp.wait()

    def finish_unit(u, carry):
        rows = pl.ds(pl.multiple_of(u * B, B), B)
        got = [(stats[j, 0:1, rows], stats[j, 1:2, rows]) for j in range(halves)]
        mean = sum(a for a, _ in got) / halves
        m2 = sum(b + HV * (a - mean) * (a - mean) for a, b in got)
        scaled = as_column(lax.rsqrt(m2 / HEAD_V + EPSILON))
        value = (normal[rows] - as_column(mean)) * scaled
        gate = proj[rows, 2 * KEY + HV :].astype(F32)
        normal[rows] = value
        inv[0:1, rows] = lax.rsqrt(m2 / HEAD_V + EPSILON)
        gated[rows] = (gate * jax.nn.sigmoid(gate) * value).astype(BF)
        return carry

    inv[...] = jnp.zeros_like(inv)
    lax.fori_loop(0, units, finish_unit, 0)
    save(normal, o_normal)
    save(gated, o_gated)

    p = otok
    Q = x.shape[0]
    cut, parts = halves_of(Q)
    scatters, gathers = [], []
    for h in range(parts):
        at = h * (n + m)
        slot = lambda c, i, h=h: sn.at[c, i, cut(h)]
        gathers.append(Chain(pc, x.at[cut(h)], slot, refs[at : at + n]))
        scatters.append(Scatter(pc, p, cut(h), refs[at + n : at + n + m]))
    for d in near + [0]:
        c = pc.ahead(d)
        mixed = gated[pl.ds(pl.multiple_of(c * L, L), L)]

        def one(b, carry):
            part = across_blocks(mixed, win, b, pl.ds(NI, HV))
            columns = pl.ds(pl.multiple_of(b * part.shape[1], 128), part.shape[1])
            for i in range(T):
                p[c, i, :, columns] = part[i * Q : (i + 1) * Q]
            return carry

        lax.fori_loop(0, W // max(R, 128), one, 0)
        scatters[0].begin(d)
    for d in near:
        gk.forward(d)
    pump = Pump(scatters, begun=C)
    pump.run(C)
    for k in range(8):
        wr.forward(k)
    for d in near:
        gk.onward(d)
    mine.wait()
    for h, rs in enumerate(scatters):
        pump.run(min(2, len(pump.units) - pump.done))
        part = cut(h)
        total = rs.result() + mytok[part].astype(F32)
        mid[part] = total
        x[part] = layer_norm_rows(total, vecs[2:3], vecs[3:4])
        gathers[h].start()
        if h == 0:
            pump.run(len(pump.units) - pump.done)
            for k in range(8, len(wr.units)):
                wr.forward(k)
    for d in range(1, C):
        for ga in gathers:
            ga.forward(d)
    for ga in gathers:
        for d in range(C):
            ga.onward(d)
    for job in scatters + gathers:
        job.finish()
    gk.finish()
    wi.sent()
    wr.local.wait()
    for k in range(len(wr.units) + 1):
        for e in range(1, F):
            wr.arrived(k, e)
    wr.sent()
    for cp in saved:
        cp.wait()


def norm_pull(values, gain, grad):
    center = values - jnp.mean(values, axis=-1, keepdims=True)
    spread = jnp.mean(center * center, axis=-1, keepdims=True)
    inv = lax.rsqrt(spread + EPSILON)
    xhat = center * inv
    g = grad * gain
    back = inv * (
        g - jnp.mean(g, axis=-1, keepdims=True) - xhat * jnp.mean(g * xhat, axis=-1, keepdims=True)
    )
    return (
        back,
        jnp.sum(grad * xhat, axis=0, keepdims=True),
        jnp.sum(grad, axis=0, keepdims=True),
    )


def gelu_parts(v):
    c = (2.0 / jnp.pi) ** 0.5
    t = jnp.tanh(c * (v + 0.044715 * v * v * v))
    return 0.5 * v * (1.0 + t), 0.5 * (1.0 + t) + 0.5 * v * (1.0 - t * t) * c * (
        1.0 + 3 * 0.044715 * v * v
    )


def middle_kernel(dims, cfg, *refs):
    F, C, T = dims
    S, B, U = cfg
    refs = list(refs)

    def take(n):
        out = refs[:n]
        del refs[:n]
        return out

    second, gout, wr, mid, allgo, vecs = take(6)
    gm, gb, down, dgain, dbias, msum = take(6)
    stile, gtile, sblk, gblk, acc, gates, hid, pg, pd, turned, turned2 = take(11)
    msend, mgot, mloc, x, go = take(5)
    ssem, gsem, gosem, dsem, msem, mxs, mxr = take(7)
    gsems = take(len(gather_sems(C)))

    pc = Place(*dims)
    f = pc.f
    near = pc.near_first()
    R, N = wr.shape[2], hid.shape[0]
    Q = x.shape[0]
    W = F * C * R
    pc.barrier(True, True, True)
    mine = pltpu.make_async_copy(allgo.at[pc.t], go, gosem)
    mine.start()
    rg = Scatter(pc, pg, pl.ds(0, Q), refs)
    saved = []
    order = rg.order
    units = [(d, s) for d in order for s in range(S)]

    def rows_of(i):
        d, s = units[i]
        return pl.ds(pl.multiple_of((pc.ahead(d) * S + s) * B, B), B)

    def load(i):
        k = i % 2
        return (
            pltpu.make_async_copy(second.at[rows_of(i)], stile.at[k], ssem.at[k]),
            pltpu.make_async_copy(gout.at[rows_of(i)], gtile.at[k], gsem.at[k]),
        )

    for cp in load(0):
        cp.start()

    def unit(i):
        d, s = units[i]
        k = i % 2
        rows = rows_of(i)
        if i + 1 < len(units):
            for cp in load(i + 1):
                cp.start()
        for cp in load(i):
            cp.wait()
        for b in range(F * C):
            sblk[b, rows] = stile[k, :, b * R : (b + 1) * R]
            gblk[b, rows] = gtile[k, :, b * R : (b + 1) * R]
        acc[...] = jnp.zeros_like(acc)

        def forward(b, carry):
            w = wr[b // C, lax.rem(b, C)]
            acc[:, : 2 * U] += nn(sblk[b, rows], w[:, : 2 * U])
            acc[:, 2 * U :] += nn(gblk[b, rows], w[:, 2 * U :])
            return carry

        lax.fori_loop(0, F * C, forward, 0)
        gate = acc[:, :U].astype(BF).astype(F32)
        up = acc[:, U : 2 * U].astype(BF).astype(F32)
        grad = acc[:, 2 * U :]
        value, slope = gelu_parts(gate)
        hid[rows] = (value * up).astype(BF)
        gates[rows, :U] = (grad * up * slope).astype(BF)
        gates[rows, U:] = (grad * value).astype(BF)
        c = pc.ahead(d)
        pull, keep = gates[rows], hid[rows]

        def back(b, carry):
            for p, part in (
                (pg, across_blocks(pull, wr, b, pl.ds(0, 2 * U))),
                (pd, across_blocks(keep, wr, b, pl.ds(2 * U, U))),
            ):
                columns = pl.ds(pl.multiple_of(b * part.shape[1], 128), part.shape[1])
                for j in range(B // Q):
                    p[c, s * (B // Q) + j, :, columns] = part[j * Q : (j + 1) * Q]
            return carry

        lax.fori_loop(0, W // max(R, 128), back, 0)

    for i in range(len(units)):
        unit(i)
        if units[i][1] == S - 1:
            k = i // S
            rg.begin(order[k])
            c = pc.ahead(order[k])
            cp = pltpu.make_async_copy(pd.at[c], down.at[c], dsem.at[k])
            cp.start()
            saved.append(cp)
            if k >= 1:
                rg.far(order[k - 1])
            if k >= 2:
                rg.along(order[k - 2])
    rg.far(order[C - 1])
    for d in order[max(C - 2, 0) :]:
        rg.along(d)

    xc = {}

    def block(d, e):
        b = pc.fahead(e) * C + pc.ahead(d)
        turned[...] = jnp.transpose(sblk[b])
        turned2[...] = jnp.transpose(gblk[b])
        return nn(turned[...], gates[...]), nn(turned2[...], hid[...])

    for d in order:
        for e in range(1, F):
            c = pc.ahead(d)
            first, last = block(d, e)
            msend[e - 1, d, :, : 2 * U] = first.astype(BF)
            msend[e - 1, d, :, 2 * U :] = last.astype(BF)
            xc[d, e] = remote(
                msend.at[e - 1, d], mgot.at[e - 1, d], mxs.at[d, e], mxr.at[d, e], {"fsdp": pc.fahead(e)}
            )
            xc[d, e].start()

    mine.wait()
    back, dg, db = norm_pull(mid[...], vecs[2:3], rg.result())
    dgain[...] = dg
    dbias[...] = db
    grad_middle = go[...].astype(F32) + back
    gm[...] = grad_middle
    x[...] = grad_middle.astype(BF)
    ga = Gather(pc, x, gb, pl.ds(0, Q), gsems)
    ga.start()
    for d in near[:2]:
        ga.forward(d)
    for k, d in enumerate(order):
        if k == 1:
            for far in near[2:]:
                ga.forward(far)
        first, last = block(d, 0)
        for e in range(1, F):
            xc[d, e].wait_recv()
            first = first + mgot[e - 1, d, :, : 2 * U].astype(F32)
            last = last + mgot[e - 1, d, :, 2 * U :].astype(F32)
        mloc[d, :, : 2 * U] = first.astype(BF)
        mloc[d, :, 2 * U :] = last.astype(BF)
        cp = pltpu.make_async_copy(mloc.at[d], msum.at[pc.ahead(d)], msem.at[d])
        cp.start()
        saved.append(cp)
    for d in [0] + near:
        ga.onward(d)
    for job in (rg, ga):
        job.finish()
    for cp in xc.values():
        cp.wait_send()
    for cp in saved:
        cp.wait()


def vector_stage(pc, v, vout, va, vb, vc, vd, vx, vz, ts, tr, vxs, vxr, vzs, vzr):
    F, C = pc.F, pc.C
    t0 = remote(v, vb, ts.at[0], tr.at[0], {"tp": pc.near})
    t0.start()
    yield
    t0.wait_recv()
    va[...] = v[...] + vb[...]
    t1 = remote(va, vc, ts.at[1], tr.at[1], {"tp": pc.far})
    t1.start()
    yield
    t1.wait_recv()
    vd[...] = va[...] + vc[...]
    vxc, vzc = {}, {}
    for e in range(1, F):
        vxc[e] = remote(
            vd.at[pc.fahead(e)], vx.at[e - 1], vxs.at[e], vxr.at[e], {"fsdp": pc.fahead(e)}
        )
        vxc[e].start()
    yield
    vs = vd[pc.f]
    for e in range(1, F):
        vxc[e].wait_recv()
        vs = vs + vx[e - 1]
    vz[0] = vs
    for d in range(1, C):
        vzc[d] = remote(
            vz.at[0, pc.ahead(d)], vz.at[1, d], vzs.at[d], vzr.at[d], {"ctx": pc.ahead(d)}
        )
        vzc[d].start()
    yield
    acc = vz[0, pc.z]
    for d in range(1, C):
        vzc[d].wait_recv()
        acc = acc + vz[1, d]
    vout[...] = acc
    for cp in [t0, t1] + list(vxc.values()) + list(vzc.values()):
        cp.wait_send()


def vector_scratch(F, C, R):
    full = pltpu.VMEM((F, C, 8, R), F32)
    return [
        full,
        full,
        full,
        full,
        full,
        pltpu.VMEM((F - 1, C, 8, R), F32),
        pltpu.VMEM((2, C, 8, R), F32),
        sem(2),
        sem(2),
        sem(F),
        sem(F),
        sem(C),
        sem(C),
    ]


def backward_kernel(dims, cfg, *refs):
    F, C, T = dims
    S, B, halves, HV = cfg
    refs = list(refs)

    def take(n):
        out = refs[:n]
        del refs[:n]
        return out

    branch, normed, win, proj, states, normal, inv, gated, old, vecs, gm, alltok, mlp, dg2, db2, down, mid = take(17)
    gt, result, gout, mout, vout = take(5)
    btile, ntile, cblock, turned, turned2, gn, gproj, later, stats, p = take(10)
    gsend, xbuf, zsnd, tok, y = take(5)
    bsem, nsem, sts, strr, mzs, mzr, xos, xor, xs, xr, zs, zr, keeps, toksem, lsem, msem = take(16)
    shares, shares2, vscratch = take(2), take(2), take(13)
    y2, lsem2, local = take(1)[0], take(1)[0], take(2)
    half = len(refs) // 2

    pc = Place(*dims)
    f, z, t = pc.f, pc.z, pc.t
    L = S * B
    R = win.shape[2]
    W = F * C * R
    N, NI = gproj.shape
    Q = y.shape[0]
    units = C * S
    pc.barrier(True, True, True)
    mine = pltpu.make_async_copy(alltok.at[t], tok, toksem)
    mine.start()

    moves = [pltpu.make_async_copy(mlp.at[z], mout.at[z], msem)]
    for d in pc.near_first():
        dst = pc.ahead(d)
        moves.append(remote(mlp.at[dst], mout.at[z], mzs.at[d], mzr.at[d], {"ctx": dst}))
    for cp in moves:
        cp.start()

    rd = Scatter(pc, down, pl.ds(0, Q), refs[half:], local)
    rd.start()

    def rows_in(u, slot):
        rows = pl.ds(pl.multiple_of(u * B, B), B)
        return pltpu.make_async_copy(branch.at[rows], btile.at[slot], bsem.at[slot])

    rows_in(0, 0).start()
    stats[0] = jnp.zeros(stats.shape[1:], F32)

    def pull_gate(u, carry):
        slot = lax.rem(u, 2)
        pl.when(u + 1 < units)(lambda: rows_in(u + 1, 1 - slot).start())
        rows_in(u, slot).wait()
        grad = None
        rows = pl.ds(pl.multiple_of(u * B, B), B)
        for b in range(F * C):
            piece = btile[slot, :, b * R : (b + 1) * R]
            cblock[b, rows] = piece
            part = nn(piece, win[b // C, b % C, :, NI:])
            grad = part if grad is None else grad + part
        gate = proj[rows, 2 * KEY + HV :].astype(F32)
        silu, dsilu = silu_parts(gate)
        value = normal[rows]
        gproj[rows, 2 * KEY + HV :] = (grad * value * dsilu).astype(BF)
        inner = grad * silu
        gn[rows] = inner
        stats[0, 0:1, rows] = as_row(jnp.sum(inner, axis=-1, keepdims=True))
        stats[0, 1:2, rows] = as_row(jnp.sum(inner * value, axis=-1, keepdims=True))
        return carry

    lax.fori_loop(0, units, pull_gate, 0)
    st = []
    place = lax.rem(z, halves)
    for j in range(1, halves):
        peer = {"ctx": z - place + lax.rem(place + j, halves)}
        cp = remote(stats.at[0], stats.at[j], sts.at[j], strr.at[j], peer)
        cp.start()
        st.append(cp)

    for d in rd.order:
        rd.far(d)

    far = sorted(range(1, C), key=lambda d: abs(d - C // 2))
    order = far + [0]
    blocks = [(d, e) for d in order for e in range(1, F)] + [(d, 0) for d in order]
    xo, xc, zc = {}, {}, {}

    def columns_in(i):
        d, e = blocks[i]
        b = pc.fahead(e) * C + pc.ahead(d)
        return b, pltpu.make_async_copy(normed.at[b], ntile.at[i % 2], nsem.at[i % 2])

    def start_columns(i):
        if i < len(blocks):
            columns_in(i)[1].start()

    tail = pl.ds(NI, HV)
    for d, e in blocks[: (F - 1) * C]:
        turned2[...] = jnp.transpose(cblock[pc.fahead(e) * C + pc.ahead(d)])
        gsend[e - 1, d, :, tail] = nn(turned2[...], gated[...]).astype(BF)
        xo[d, e] = remote(
            gsend.at[e - 1, d, :, tail],
            xbuf.at[e - 1, d, :, tail],
            xos.at[d, e],
            xor.at[d, e],
            {"fsdp": pc.fahead(e)},
        )
        xo[d, e].start()

    start_columns(0)
    for cp in st:
        cp.wait()

    head = z // halves
    scale = float(KEY) ** (-0.5)
    later[...] = jnp.zeros_like(later)

    def retain(i, carry):
        u = units - 1 - i
        c, s = u // S, lax.rem(u, S)
        rows = pl.ds(pl.multiple_of(u * B, B), B)
        rates = old[c, pl.ds(head, 1), pl.ds(pl.multiple_of(s * B, B), B)]
        table, growth, keeping, through = decays(rates)
        q, k, v = proj[rows, :KEY], proj[rows, KEY : 2 * KEY], proj[rows, 2 * KEY : 2 * KEY + HV]
        s1 = as_column(sum(stats[j, 0:1, rows] for j in range(halves)) / HEAD_V)
        s2 = as_column(sum(stats[j, 1:2, rows] for j in range(halves)) / HEAD_V)
        mix = (as_column(inv[0:1, rows]) * (gn[rows] - s1 - normal[rows] * s2)).astype(BF)
        weights = (nt(q, k) * scale * table).astype(BF)
        scores = (nt(mix, v) * scale * table).astype(BF)
        after = later[s]
        after_low = after.astype(BF)
        gq = nn(scores, k) + growth * nt(mix, states[u])
        gk = tn(scores, q) + keeping * nt(v, after_low)
        gv = tn(weights, mix) + nn((k.astype(F32) * keeping).astype(BF), after_low)
        later[s] = through * after + tn((q.astype(F32) * growth).astype(BF), mix)
        gproj[rows, :KEY] = gq.astype(BF)
        gproj[rows, KEY : 2 * KEY] = gk.astype(BF)
        gproj[rows, 2 * KEY : 2 * KEY + HV] = gv.astype(BF)
        return carry

    lax.fori_loop(0, units, retain, 0)

    rs = Scatter(pc, p, pl.ds(0, Q), refs[:half])
    for d in rs.order:
        c = pc.ahead(d)
        mixed = gproj[pl.ds(pl.multiple_of(c * L, L), L)]

        def one(b, carry, c=c, mixed=mixed):
            part = across_blocks(mixed, win, b, pl.ds(0, NI))
            columns = pl.ds(pl.multiple_of(b * part.shape[1], 128), part.shape[1])
            for i in range(T):
                p[c, i, :, columns] = part[i * Q : (i + 1) * Q]
            return carry

        lax.fori_loop(0, W // max(R, 128), one, 0)
        rs.begin(d)
    pump = Pump([rs], begun=C)
    pump.fill()
    for d in rd.order[:2]:
        rd.along(d)

    H = 2
    kept = []
    halfs = [pl.ds(h * (R // H), R // H) for h in range(H)]
    main = pl.ds(0, NI)

    def block(i):
        d, e = blocks[i]
        start_columns(i + 1)
        b, cp = columns_in(i)
        cp.wait()
        turned[...] = jnp.transpose(ntile[i % 2])
        if e == 0:
            turned2[...] = jnp.transpose(cblock[b])
            for g in range(1, F):
                xo[d, g].wait_recv()
                for h in range(H):
                    xc[d, g, h].wait_recv()

        def put(columns, part):
            if e:
                gsend[e - 1, d, :, columns] = part.astype(BF)
            else:
                for g in range(F - 1):
                    part = part + xbuf[g, d, :, columns].astype(F32)
                zsnd[d, :, columns] = part.astype(BF)

        def one(j, carry):
            columns = pl.ds(pl.multiple_of(j * 256, 256), 256)
            put(columns, nn(turned[...], gproj[:, columns]))
            return carry

        lax.fori_loop(0, NI // 256, one, 0)
        if e == 0:
            put(tail, nn(turned2[...], gated[...]))
        for h, part in enumerate(halfs):
            if e:
                xc[d, e, h] = remote(
                    gsend.at[e - 1, d, part, main],
                    xbuf.at[e - 1, d, part, main],
                    xs.at[d, e, h],
                    xr.at[d, e, h],
                    {"fsdp": pc.fahead(e)},
                )
                xc[d, e, h].start()
            elif d:
                zc[d, h] = remote(
                    zsnd.at[d, part], gout.at[z, part], zs.at[d, h], zr.at[d, h], {"ctx": pc.ahead(d)}
                )
                zc[d, h].start()
            else:
                cp = pltpu.make_async_copy(zsnd.at[0, part], gout.at[z, part], keeps.at[h])
                cp.start()
                kept.append(cp)

    sends = (F - 1) * C
    for i in range(sends):
        block(i)
        if i < len(rd.order[2:]):
            rd.along(rd.order[2 + i])
        if pump.done < len(pump.units):
            pump.run(1)
    for d in rd.order[2 + sends :]:
        rd.along(d)
    pump.run(len(pump.units) - pump.done)
    stages = []
    for i in range(sends, len(blocks)):
        block(i)
        if i == sends:
            mine.wait()
            back, dg, db = norm_pull(tok[...].astype(F32), vecs[0:1], rs.result())
            y[...] = (gm[...] + back).astype(BF)
            v = vscratch[0]
            for b in range(F * C):
                rows = [r[:, b * R : (b + 1) * R] for r in (dg, db)] + [
                    r[:, b * R : (b + 1) * R] for r in (dg2, db2)
                ]
                v[b // C, b % C] = jnp.concatenate(rows + [jnp.zeros((4, R), F32)], axis=0)
            y2[...] = (mid[...] + rd.result()).astype(BF)
            stages = [
                share_stage(pc, y, gt, lsem, shares),
                share_stage(pc, y2, result, lsem2, shares2),
                vector_stage(pc, v, vout, *vscratch[1:]),
            ]
        for stage in stages:
            next(stage, None)
    for stage in stages:
        drain(stage)
    rs.finish()
    rd.finish()
    for cp in kept:
        cp.wait()
    for cp in zc.values():
        cp.wait()
    for cp in list(xc.values()) + list(xo.values()):
        cp.wait_send()
    for cp in moves:
        cp.wait()


def assemble_kernel(halves, key, hv, a, m, q, k, v, g, o, fg, fu, fd):
    c = pl.program_id(0)
    first = lax.rem(c, halves) == 0
    for i, ref in enumerate((q, k)):
        x = a[0, :, i * key : (i + 1) * key].astype(F32)

        @pl.when(first)
        def _(ref=ref, x=x):
            ref[...] = x

        @pl.when(jnp.logical_not(first))
        def _(ref=ref, x=x):
            ref[...] += x

    v[...] = a[0, :, 2 * key : 2 * key + hv].astype(F32)
    g[...] = a[0, :, 2 * key + hv : 2 * key + 2 * hv].astype(F32)
    o[...] = a[0, :, 2 * key + 2 * hv :].astype(F32)
    u = fg.shape[1]
    for i, ref in enumerate((fg, fu, fd)):
        ref[...] = m[0, :, i * u : (i + 1) * u].astype(F32)


def params(cid):
    return pltpu.CompilerParams(collective_id=cid, has_side_effects=True)


def shards(
    dims,
    tokens,
    log_decay,
    w_query,
    w_key,
    w_value,
    w_gate,
    w_out,
    norm1_gain,
    norm1_bias,
    w_ffgate,
    w_ffup,
    w_down,
    norm2_gain,
    norm2_bias,
    grad_out,
):
    F, C, T = dims
    S, B, W = tokens.shape
    L = S * B
    Q = L // T
    N = C * L
    R = w_query.shape[0]
    heads = log_decay.shape[2]
    halves = C // heads
    HV = HEAD_V // halves
    U = w_ffgate.shape[1] // C
    z = lax.axis_index("ctx")
    t = lax.axis_index("tp")
    scale = float(KEY) ** (-0.5)

    f = lax.axis_index("fsdp")

    def hop(x, axis, d):
        n = lax.axis_size(axis)
        return lax.ppermute(x, axis, [(i, (i + d) % n) for i in range(n)])

    def at(x, i, n):
        return lax.dynamic_index_in_dim(x, lax.rem(i, n), 0, False)

    NI, NR = 2 * KEY + 2 * HV, 3 * U
    NO = NI + HV
    norms = (norm1_gain, norm1_bias, norm2_gain, norm2_bias)
    tok = tokens.reshape(T, Q, W)
    go = grad_out.reshape(T, Q, W)
    sds = jax.ShapeDtypeStruct
    cfg = (
        S,
        B,
        halves,
        HV,
        ((halves, KEY), (halves, KEY), (1, HV), (1, HV), (1, HV)),
        ((1, U), (1, U), (1, U)),
    )
    owin, normed, proj, states, normal, gated, inv, old, vecs, mid, sn, full, ogo = pl.pallas_call(
        functools.partial(forward_kernel, dims, cfg),
        out_shape=(
            sds((F, C, R, NO), BF),
            sds((F * C, N, R), BF),
            sds((N, NI), BF),
            sds((C * S, KEY, HV), BF),
            sds((N, HV), F32),
            sds((N, HV), BF),
            sds((8, N), F32),
            sds((C, 8, L), F32),
            sds((8, W), F32),
            sds((Q, W), F32),
            sds((C, T, Q, W), BF),
            sds((F, C, R, NR), BF),
            sds((C, T, Q, W), BF),
        ),
        in_specs=[ANY] * 8 + [VMEM] * 5 + [ANY, ANY],
        out_specs=[ANY] * 6 + [VMEM] * 4 + [ANY] * 3,
        scratch_shapes=[
            pltpu.VMEM((C, T, Q, W), BF),
            pltpu.VMEM((F, C, R, NO), BF),
            pltpu.VMEM((F, C, 8, R), F32),
            pltpu.VMEM((F * C, N, R), BF),
            pltpu.VMEM((N, NI), F32),
            pltpu.VMEM((N, NI), BF),
            pltpu.VMEM((C * S, KEY, HV), BF),
            pltpu.VMEM((S, KEY, HV), F32),
            pltpu.VMEM((N, HV), F32),
            pltpu.VMEM((N, HV), BF),
            pltpu.VMEM((halves, 8, N), F32),
            pltpu.VMEM((Q, W), BF),
            pltpu.VMEM((Q, W), BF),
        ]
        + mover_sems(F, C) * 2
        + blocks_sems(C) * 2
        + [sem(C), sem(C), sem(C, F), sem(C, F), sem(C), sem(C), sem(halves), sem(halves), sem(16)]
        + [pltpu.VMEM((8, R), F32), pltpu.VMEM((8, L), F32)]
        + (chain_sems(C) + scatter_scratch(C, Q // PARTS, W)) * PARTS,
        compiler_params=params(1),
        name="k_forward",
    )(w_query, w_key, w_value, w_gate, w_out, w_ffgate, w_ffup, w_down, *norms, log_decay, tok, go)
    gm, gb, down, dgain2, dbias2, mlp_sum = pl.pallas_call(
        functools.partial(middle_kernel, dims, (S, B, U)),
        out_shape=(
            sds((Q, W), F32),
            sds((C, T, Q, W), BF),
            sds((C, T, Q, W), BF),
            sds((1, W), F32),
            sds((1, W), F32),
            sds((C, R, NR), BF),
        ),
        in_specs=[ANY, ANY, VMEM, VMEM, ANY, VMEM],
        out_specs=[VMEM, ANY, ANY, VMEM, VMEM, ANY],
        scratch_shapes=[
            pltpu.VMEM((2, B, W), BF),
            pltpu.VMEM((2, B, W), BF),
            pltpu.VMEM((F * C, N, R), BF),
            pltpu.VMEM((F * C, N, R), BF),
            pltpu.VMEM((B, 3 * U), F32),
            pltpu.VMEM((N, 2 * U), BF),
            pltpu.VMEM((N, U), BF),
            pltpu.VMEM((C, T, Q, W), BF),
            pltpu.VMEM((C, T, Q, W), BF),
            pltpu.VMEM((R, N), BF),
            pltpu.VMEM((R, N), BF),
            pltpu.VMEM((F - 1, C, R, NR), BF),
            pltpu.VMEM((F - 1, C, R, NR), BF),
            pltpu.VMEM((C, R, NR), BF),
            pltpu.VMEM((Q, W), BF),
            pltpu.VMEM((Q, W), BF),
            sem(2),
            sem(2),
            pltpu.SemaphoreType.DMA,
            sem(C),
            sem(C),
            sem(C, F),
            sem(C, F),
        ]
        + gather_sems(C)
        + scatter_scratch(C, Q, W),
        compiler_params=params(3),
        name="k_middle",
    )(sn.reshape(N, W), ogo.reshape(N, W), full, mid, go, vecs)

    branch = gb.reshape(N, W)
    H = 2
    gt, out, gsum, mlp_grads, vsum = pl.pallas_call(
        functools.partial(backward_kernel, dims, (S, B, halves, HV)),
        out_shape=(
            sds((T, Q, W), BF),
            sds((T, Q, W), BF),
            sds((C, R, NO), BF),
            sds((C, R, NR), BF),
            sds((8, R), F32),
        ),
        in_specs=[ANY, ANY] + [VMEM] * 9 + [ANY, ANY, VMEM, VMEM, ANY, VMEM],
        out_specs=[ANY] * 4 + [VMEM],
        scratch_shapes=[
            pltpu.VMEM((2, B, W), BF),
            pltpu.VMEM((2, N, R), BF),
            pltpu.VMEM((F * C, N, R), BF),
            pltpu.VMEM((R, N), BF),
            pltpu.VMEM((R, N), BF),
            pltpu.VMEM((N, HV), F32),
            pltpu.VMEM((N, NI), BF),
            pltpu.VMEM((S, KEY, HV), F32),
            pltpu.VMEM((halves, 8, N), F32),
            pltpu.VMEM((C, T, Q, W), BF),
            pltpu.VMEM((F - 1, C, R, NO), BF),
            pltpu.VMEM((F - 1, C, R, NO), BF),
            pltpu.VMEM((C, R, NO), BF),
            pltpu.VMEM((Q, W), BF),
            pltpu.VMEM((Q, W), BF),
            sem(2),
            sem(2),
            sem(halves),
            sem(halves),
            sem(C),
            sem(C),
            sem(C, F),
            sem(C, F),
            sem(C, F, H),
            sem(C, F, H),
            sem(C, H),
            sem(C, H),
            sem(H),
        ]
        + [pltpu.SemaphoreType.DMA] * 3
        + share_sems() * 2
        + vector_scratch(F, C, R)
        + [pltpu.VMEM((Q, W), BF), pltpu.SemaphoreType.DMA]
        + local_scratch(C, Q, W)
        + scatter_scratch(C, Q, W) * 2,
        compiler_params=params(4),
        name="k_backward",
    )(
        branch,
        normed,
        owin,
        proj,
        states,
        normal,
        inv,
        gated,
        old,
        vecs,
        gm,
        tok,
        mlp_sum,
        dgain2,
        dbias2,
        down,
        mid,
    )
    output = out.reshape(tokens.shape)
    grad_tokens = gt.reshape(tokens.shape)

    def quarter(n):
        return pl.BlockSpec((R, n), lambda c: (0, c))

    per_head = pl.BlockSpec((R, KEY), lambda c: (0, c // halves))
    gq, gk, gv, gg, gw, gfg, gfu, gfd = pl.pallas_call(
        functools.partial(assemble_kernel, halves, KEY, HV),
        out_shape=[sds((R, heads * KEY), F32)] * 2
        + [sds((R, C * HV), F32)] * 3
        + [sds((R, C * U), F32)] * 3,
        grid=(C,),
        in_specs=[
            pl.BlockSpec((1, R, NO), lambda c: (c, 0, 0)),
            pl.BlockSpec((1, R, NR), lambda c: (c, 0, 0)),
        ],
        out_specs=[per_head, per_head] + [quarter(HV)] * 3 + [quarter(U)] * 3,
        name="k_assemble",
    )(gsum, mlp_grads)
    return (
        output,
        grad_tokens,
        gq,
        gk,
        gv,
        gg,
        gw,
        vsum[0],
        vsum[1],
        gfg,
        gfu,
        gfd,
        vsum[2],
        vsum[3],
    )


def solution(mesh):
    dims = (mesh.shape["fsdp"], mesh.shape["ctx"], mesh.shape["tp"])
    rows, vec = P(("fsdp", "ctx"), "tp"), P(("fsdp", "ctx"))
    acts = P("fsdp", "ctx", None)
    return jax.shard_map(
        functools.partial(shards, dims),
        mesh=mesh,
        in_specs=(acts, P("fsdp", "ctx", "tp"), rows, rows, rows, rows, rows, vec, vec, rows, rows, rows, vec, vec, acts),
        out_specs=(acts, acts, rows, rows, rows, rows, rows, vec, vec, rows, rows, rows, vec, vec),
        check_vma=False,
    )
```

```python
import functools

import jax
import jax.numpy as jnp
from jax import lax
from jax.experimental import pallas as pl
from jax.experimental.pallas import tpu as pltpu
from jax.sharding import PartitionSpec as P

KEY = 256
HEAD_V = 512
EPSILON = 1e-05
MESH = pl.DeviceIdType.MESH
ANY = pl.BlockSpec(memory_space=pl.ANY)
VMEM = pl.BlockSpec(memory_space=pltpu.VMEM)
BF = jnp.bfloat16
F32 = jnp.float32


def dot(a, b, dims):
    return lax.dot_general(a, b, (dims, ((), ())), preferred_element_type=F32)


def nn(a, b):
    return dot(a, b, ((1,), (0,)))


def nt(a, b):
    return dot(a, b, ((1,), (1,)))


def tn(a, b):
    return dot(a, b, ((0,), (0,)))


class Place:
    def __init__(self, F, C, T):
        self.F, self.C, self.T = F, C, T
        self.f = lax.axis_index("fsdp")
        self.z = lax.axis_index("ctx")
        self.t = lax.axis_index("tp")
        self.lo = lax.rem(self.t, 2)
        self.hi = self.t // 2
        self.near = self.t + 1 - 2 * self.lo
        self.far = lax.rem(self.t + 2, 4)

    def near_first(self):
        return [1] + ([self.C - 1] if self.C > 2 else []) + list(range(2, self.C - 1))

    def ahead(self, d):
        return lax.rem(self.z + d, self.C)

    def behind(self, d):
        return lax.rem(self.z + self.C - d, self.C)

    def fahead(self, d):
        return lax.rem(self.f + d, self.F)

    def fbehind(self, d):
        return lax.rem(self.f + self.F - d, self.F)

    def barrier(self, ctx=True, fsdp=False, tp=True):
        sem = pltpu.get_barrier_semaphore()
        peers = []
        if tp:
            peers += [{"tp": self.near}, {"tp": self.far}]
        if fsdp:
            peers += [{"fsdp": self.fahead(d)} for d in range(1, self.F)]
        if ctx:
            peers += [{"ctx": self.ahead(d)} for d in range(1, self.C)]
        for peer in peers:
            pl.semaphore_signal(sem, inc=1, device_id=peer, device_id_type=MESH)
        pl.semaphore_wait(sem, len(peers))


def remote(src, dst, ssem, rsem, peer):
    return pltpu.make_async_remote_copy(
        src_ref=src, dst_ref=dst, send_sem=ssem, recv_sem=rsem, device_id=peer, device_id_type=MESH
    )


def sem(*shape):
    return pltpu.SemaphoreType.DMA(shape)


def chain_sems(C):
    return [sem(2, C), sem(2, C), sem(2, C), sem(2, C), sem(2, C, 2), sem(2, C, 2), pltpu.SemaphoreType.DMA]


class Chain:
    def __init__(self, pc, x, slot, sems, own=None):
        self.pc, self.x, self.slot, self.block = pc, x, slot, own
        self.zs, self.zr, self.ys, self.yr, self.cs, self.cr, self.ls = sems

    def came(self, s, h):
        z = self.pc.z
        return (z >= h, z - h) if s == 0 else (z + h <= self.pc.C - 1, z + h)

    def goes(self, s, h):
        pc = self.pc
        if s == 0:
            return jnp.logical_and(pc.z >= h - 1, pc.z < pc.C - 1)
        return jnp.logical_and(pc.z + h <= pc.C, pc.z > 0)

    def hop(self, s, h, c):
        z = self.pc.z
        here = self.slot(c, self.pc.t)
        src = self.x if h == 1 else here
        return remote(src, here, self.zs.at[s, h], self.zr.at[s, h], {"ctx": z + 1 if s == 0 else z - 1})

    def to_far(self, s, h, c):
        here = self.slot(c, self.pc.t)
        src = here if h else self.x
        return remote(src, here, self.ys.at[s, h], self.yr.at[s, h], {"tp": self.pc.far})

    def to_near(self, s, h, c):
        here = self.slot(c, self.pc.t)
        src = here if h else self.x
        return remote(src, here, self.cs.at[s, h, 0], self.cr.at[s, h, 0], {"tp": self.pc.near})

    def spread(self, s, h, c):
        self.to_far(s, h, c).start()
        self.to_near(s, h, c).start()

    def again(self, s, h, c):
        there = self.slot(c, self.pc.far)
        return remote(there, there, self.cs.at[s, h, 1], self.cr.at[s, h, 1], {"tp": self.pc.near})

    def start(self):
        pc = self.pc
        for s in range(2):
            pl.when(self.goes(s, 1))(lambda s=s: self.hop(s, 1, pc.z).start())
        src, dst = self.block or (self.x, self.slot(pc.z, pc.t))
        self.local = pltpu.make_async_copy(src, dst, self.ls)
        self.local.start()
        if not self.block:
            self.spread(0, 0, pc.z)

    def forward(self, h):
        for s in range(2):
            ok, c = self.came(s, h)

            @pl.when(ok)
            def _(s=s, c=c):
                self.hop(s, h, c).wait_recv()
                if h + 1 < self.pc.C:
                    pl.when(self.goes(s, h + 1))(lambda: self.hop(s, h + 1, c).start())
                self.spread(s, h, c)

    def onward(self, h):
        if h == 0:
            if not self.block:
                self.to_far(0, 0, self.pc.z).wait_recv()
                self.again(0, 0, self.pc.z).start()
            return
        for s in range(2):
            ok, c = self.came(s, h)

            @pl.when(ok)
            def _(s=s, c=c):
                self.to_far(s, h, c).wait_recv()
                self.again(s, h, c).start()

    def settle(self, s, h, c):
        self.to_far(s, h, c).wait_send()
        self.to_near(s, h, c).wait()
        self.again(s, h, c).wait()

    def finish(self):
        pc = self.pc
        self.local.wait()
        if not self.block:
            self.settle(0, 0, pc.z)
        for h in range(1, pc.C):
            for s in range(2):
                ok, c = self.came(s, h)
                first = pc.z - h + 1 if s == 0 else pc.z + h - 1
                pl.when(self.goes(s, h))(lambda s=s, c=first: self.hop(s, h, c).wait_send())
                pl.when(ok)(lambda s=s, c=c: self.settle(s, h, c))


def share_sems():
    return [sem(3), sem(3)]


def share_stage(pc, x, out, lsem, sems):
    ss, rs = sems
    t = pc.t
    local = pltpu.make_async_copy(x, out.at[t], lsem)
    local.start()
    a = remote(x, out.at[t], ss.at[0], rs.at[0], {"tp": pc.far})
    a.start()
    b = remote(x, out.at[t], ss.at[1], rs.at[1], {"tp": pc.near})
    b.start()
    yield
    a.wait_recv()
    src = out.at[pc.far]
    c = remote(src, src, ss.at[2], rs.at[2], {"tp": pc.near})
    c.start()
    yield
    local.wait()
    a.wait_send()
    b.wait()
    c.wait()


def scatter_scratch(C, Q, W):
    return [
        pltpu.VMEM((C, 2, Q, W), BF),
        pltpu.VMEM((C, Q, W), BF),
        pltpu.VMEM((C, Q, W), BF),
        pltpu.VMEM((C, Q, W), BF),
        pltpu.VMEM((C, Q, W), BF),
        sem(C, 2),
        sem(C, 2),
        sem(C),
        sem(C),
        sem(C),
        sem(C),
    ]


def local_scratch(C, Q, W):
    return [pltpu.VMEM((C, 2, Q, W), BF), sem(C, 2)]


class Scatter:
    def __init__(self, pc, p, rows, scratch, local=None):
        self.pc, self.p, self.rows, self.local = pc, p, rows, local
        (self.buf1, self.snd2, self.buf2, self.snd3, self.buf3) = scratch[:5]
        self.s1, self.r1, self.s2, self.r2, self.s3, self.r3 = scratch[5:]
        self.order = pc.near_first() + [0]
        self.lc, self.c1, self.c2, self.c3 = {}, {}, {}, {}

    def side(self, j):
        return 1 - self.pc.hi if j == 0 else self.pc.hi

    def begin(self, d):
        pc, p, rows = self.pc, self.p, self.rows
        c = pc.ahead(d)
        for j in range(2):
            self.c1[d, j] = remote(
                p.at[c, self.side(j) * 2 + 1 - pc.lo, rows],
                self.buf1.at[d, j],
                self.s1.at[d, j],
                self.r1.at[d, j],
                {"tp": pc.near},
            )
            self.c1[d, j].start()
            if self.local:
                self.lc[d, j] = pltpu.make_async_copy(
                    p.at[c, self.side(j) * 2 + pc.lo, rows],
                    self.local[0].at[d, j],
                    self.local[1].at[d, j],
                )
                self.lc[d, j].start()

    def start(self):
        for d in self.order:
            self.begin(d)

    def own(self, d, j):
        self.c1[d, j].wait_recv()
        if self.local:
            self.lc[d, j].wait()
            here = self.local[0][d, j]
        else:
            here = self.p[self.pc.ahead(d), self.side(j) * 2 + self.pc.lo, self.rows]
        return here.astype(F32) + self.buf1[d, j].astype(F32)

    def far(self, d):
        self.snd2[d] = self.own(d, 0).astype(BF)
        self.c2[d] = remote(
            self.snd2.at[d], self.buf2.at[d], self.s2.at[d], self.r2.at[d], {"tp": self.pc.far}
        )
        self.c2[d].start()

    def along(self, d):
        part = self.own(d, 1)
        self.c2[d].wait_recv()
        part = part + self.buf2[d].astype(F32)
        if d:
            self.snd3[d] = part.astype(BF)
            self.c3[d] = remote(
                self.snd3.at[d],
                self.buf3.at[d],
                self.s3.at[d],
                self.r3.at[d],
                {"ctx": self.pc.ahead(d)},
            )
            self.c3[d].start()
        else:
            self.total = part

    def result(self):
        total = self.total
        for d in range(1, self.pc.C):
            self.c3[d].wait_recv()
            total = total + self.buf3[d].astype(F32)
        return total

    def finish(self):
        for copies in (self.c1, self.c2, self.c3):
            for cp in copies.values():
                cp.wait_send()


def drain(stage):
    for _ in stage:
        pass


class Pump:
    def __init__(self, scatters, begun=0, window=3):
        self.units = [(rs, d) for rs in scatters for d in rs.order]
        self.window, self.begun, self.sent, self.done = window, begun, 0, 0

    def fill(self):
        while self.begun < min(len(self.units), self.done + 2 * self.window):
            rs, d = self.units[self.begun]
            rs.begin(d)
            self.begun += 1
        while self.sent < min(len(self.units), self.done + self.window):
            rs, d = self.units[self.sent]
            rs.far(d)
            self.sent += 1

    def run(self, count):
        for _ in range(count):
            self.fill()
            rs, d = self.units[self.done]
            rs.along(d)
            self.done += 1
        self.fill()


def silu_parts(g):
    s = jax.nn.sigmoid(g)
    return g * s, s * (1.0 + g * (1.0 - s))


PARTS = 2


def halves_of(rows):
    n = rows // PARTS
    return (lambda h: pl.ds(h * n, n)), PARTS


def layer_norm_rows(values, gain, bias):
    center = values - jnp.mean(values, axis=-1, keepdims=True)
    spread = jnp.mean(center * center, axis=-1, keepdims=True)
    return (center * lax.rsqrt(spread + EPSILON) * gain + bias).astype(BF)


def eye_of(n):
    return lax.broadcasted_iota(jnp.int32, (n, n), 0) == lax.broadcasted_iota(jnp.int32, (n, n), 1)


def as_row(column):
    return jnp.sum(jnp.where(eye_of(column.shape[0]), column, 0.0), axis=0, keepdims=True)


def as_column(row):
    return jnp.sum(jnp.where(eye_of(row.shape[1]), row, 0.0), axis=1, keepdims=True)


def decays(rates):
    B = rates.shape[1]
    causal = lax.broadcasted_iota(jnp.int32, (B, B), 0) >= lax.broadcasted_iota(jnp.int32, (B, B), 1)
    column = jnp.sum(jnp.where(causal, rates, 0.0), axis=1, keepdims=True)
    row = as_row(column)
    table = jnp.where(causal, jnp.exp(jnp.minimum(column - row, 0.0)), 0.0)
    total = column[B - 1 :]
    return table, jnp.exp(column), jnp.exp(total - column), jnp.exp(total)


def across_blocks(rows, blocks, i, columns):
    F, C, R, _ = blocks.shape
    group = max(1, 128 // R)
    parts = []
    for g in range(group):
        b = i * group + g
        parts.append(nt(rows, blocks[b // C, lax.rem(b, C), :, columns]))
    part = parts[0] if group == 1 else jnp.concatenate(parts, axis=1)
    return part.astype(BF)


class Mover:
    def __init__(self, pc, weights, layout, out, zs, zr, xs, xr, ls):
        self.pc, self.weights, self.layout, self.out = pc, weights, layout, out
        self.zs, self.zr, self.xs, self.xr, self.ls = zs, zr, xs, xr, ls
        self.zc, self.xc = {}, {}
        rows = out.shape[2]
        near = pc.near_first()
        part = rows // 4
        self.units = [(d, pl.ds(i * part, part)) for d in near for i in range(4)]
        self.later = list(enumerate(self.units))

    def columns(self, dst, part):
        at = 0
        for w, (share, n) in zip(self.weights, self.layout):
            start = pl.multiple_of((dst // share) * n, n)
            yield (
                w.at[part, pl.ds(start, n)],
                self.out.at[self.pc.f, self.pc.z, part, pl.ds(at, n)],
            )
            at += n

    def send(self, count=1):
        pc = self.pc
        for k, (d, part) in self.later[:count]:
            dst = pc.ahead(d)
            sems, peer = (self.zs.at[k], self.zr.at[k]), {"ctx": dst}
            for src, to in self.columns(dst, part):
                remote(src, to, *sems, peer).start()
            here = self.out.at[pc.f, pc.behind(d), part]
            self.zc[k] = remote(here, here, *sems, peer)
        del self.later[:count]

    def start(self, count):
        pc = self.pc
        whole = pl.ds(0, self.out.shape[2])
        own = len(self.units)
        for e in range(1, pc.F):
            sems, peer = (self.xs.at[own, e], self.xr.at[own, e]), {"fsdp": pc.fahead(e)}
            for src, to in self.columns(pc.z, whole):
                remote(src, to, *sems, peer).start()
            here = self.out.at[pc.fbehind(e), pc.z]
            self.xc[own, e] = remote(here, here, *sems, peer)
        for src, to in self.columns(pc.z, whole):
            pltpu.make_async_copy(src, to, self.ls).start()
        here = self.out.at[pc.f, pc.z]
        self.local = pltpu.make_async_copy(here, here, self.ls)
        self.send(count)

    def forward(self, k):
        pc = self.pc
        d, part = self.units[k]
        self.zc[k].wait_recv()
        self.send()
        here = self.out.at[pc.f, pc.behind(d), part]
        for e in range(1, pc.F):
            self.xc[k, e] = remote(
                here, here, self.xs.at[k, e], self.xr.at[k, e], {"fsdp": pc.fahead(e)}
            )
            self.xc[k, e].start()

    def arrived(self, k, e):
        self.xc[k, e].wait_recv()

    def sent(self):
        for cp in list(self.zc.values()) + list(self.xc.values()):
            cp.wait_send()


class Blocks:
    def __init__(self, pc, x, out, zs, zr, ys, yr, cs, cr, ls):
        self.pc, self.x, self.out = pc, x, out
        self.zs, self.zr, self.ys, self.yr, self.cs, self.cr, self.ls = zs, zr, ys, yr, cs, cr, ls
        self.zc, self.yc, self.cc = {}, {}, {}

    def start(self):
        pc = self.pc
        self.later = pc.near_first()
        self.local = pltpu.make_async_copy(self.x, self.out.at[pc.z], self.ls)
        self.local.start()
        self.send(3)

    def send(self, count=1):
        pc = self.pc
        for d in self.later[:count]:
            self.zc[d] = remote(
                self.x.at[pc.t],
                self.out.at[pc.z, pc.t],
                self.zs.at[d],
                self.zr.at[d],
                {"ctx": pc.ahead(d)},
            )
            self.zc[d].start()
        del self.later[:count]

    def forward(self, d):
        pc = self.pc
        self.zc[d].wait_recv()
        self.send()
        here = self.out.at[pc.behind(d), pc.t]
        self.yc[d] = remote(here, here, self.ys.at[d], self.yr.at[d], {"tp": pc.far})
        self.yc[d].start()
        self.cc[d, 0] = remote(here, here, self.cs.at[d, 0], self.cr.at[d, 0], {"tp": pc.near})
        self.cc[d, 0].start()

    def onward(self, d):
        pc = self.pc
        self.yc[d].wait_recv()
        here = self.out.at[pc.behind(d), pc.far]
        self.cc[d, 1] = remote(here, here, self.cs.at[d, 1], self.cr.at[d, 1], {"tp": pc.near})
        self.cc[d, 1].start()

    def finish(self):
        self.local.wait()
        for cp in list(self.zc.values()) + list(self.yc.values()):
            cp.wait_send()
        for cp in self.cc.values():
            cp.wait()


def mover_sems(F, C):
    return [sem(4 * C), sem(4 * C), sem(4 * C, F), sem(4 * C, F), pltpu.SemaphoreType.DMA]


def blocks_sems(C):
    return [sem(C), sem(C), sem(C), sem(C), sem(C, 2), sem(C, 2), pltpu.SemaphoreType.DMA]


def forward_kernel(dims, cfg, *refs):
    F, C, T = dims
    S, B, halves, HV, in_layout, rest_layout = cfg
    refs = list(refs)

    def take(n):
        out = refs[:n]
        del refs[:n]
        return out

    in_weights, rest_weights = take(5), take(3)
    norms, rates_in, tok, go = take(4), take(1)[0], *take(2)
    o_win, o_normed, o_proj, o_states, o_normal, o_gated, inv, old, vecs, mid, sn, full, ogo = take(13)
    otok, win, ovec, normed, acc, proj, states, state, normal, gated, stats, mytok, x = take(13)
    in_sems, rest_sems = take(5), take(5)
    tok_sems, go_sems = take(7), take(7)
    vzs, vzr, vxs, vxr, lzs, lzr, sts, strr, oses = take(9)
    vec, ld = take(2)
    n, m = len(chain_sems(C)), len(scatter_scratch(C, 8, 128))

    pc = Place(*dims)
    f, z, t = pc.f, pc.z, pc.t
    near = pc.near_first()
    L = S * B
    R = win.shape[2]
    W = F * C * R
    NI = proj.shape[1]
    N = proj.shape[0]
    units = C * S
    saved = []

    def save(src, dst):
        cp = pltpu.make_async_copy(src, dst, oses.at[len(saved)])
        cp.start()
        saved.append(cp)

    R = vec.shape[1]
    vec[...] = jnp.zeros_like(vec)
    for i, ref in enumerate(norms):
        vec[i : i + 1] = ref[...].astype(F32).reshape(1, R)
    ld[...] = jnp.zeros_like(ld)
    for s in range(S):
        for i in range(rates_in.shape[2]):
            ld[i : i + 1, s * B : (s + 1) * B] = as_row(rates_in[s, :, i : i + 1])
    pc.barrier(True, True, True)
    vz, vx, lz = {}, {}, {}
    for d in range(1, C):
        peer = {"ctx": pc.ahead(d)}
        vz[d] = remote(vec, ovec.at[f, z], vzs.at[d], vzr.at[d], peer)
        vz[d].start()
        lz[d] = remote(ld, old.at[z], lzs.at[d], lzr.at[d], peer)
        lz[d].start()
    ovec[f, z] = vec[...]
    old[z] = ld[...]

    def vec_across(d):
        for e in range(1, F):
            src = ovec.at[f, pc.behind(d)] if d else vec
            vx[d, e] = remote(
                src, ovec.at[f, pc.behind(d)], vxs.at[d, e], vxr.at[d, e], {"fsdp": pc.fahead(e)}
            )
            vx[d, e].start()

    vec_across(0)
    tk = Blocks(pc, tok, otok, *tok_sems)
    tk.start()
    wi = Mover(pc, in_weights, in_layout, win, *in_sems)
    wi.start(0)
    mine = pltpu.make_async_copy(tok.at[t], mytok, oses.at[15])
    mine.start()
    for d in range(1, C):
        vz[d].wait_recv()
        vec_across(d)
    for d in near:
        tk.forward(d)
        wi.send(4)
    wr = Mover(pc, rest_weights, rest_layout, full, *rest_sems)
    gk = Blocks(pc, go, ogo, *go_sems)
    for d in near:
        tk.onward(d)
    for cp in vx.values():
        cp.wait()
    for cp in vz.values():
        cp.wait_send()
    for b in range(F * C):
        vecs[:, b * R : (b + 1) * R] = ovec[b // C, b % C]
    tk.finish()
    gain1, bias1 = vecs[0:1], vecs[1:2]

    def norm_unit(i, carry):
        rows = otok[i // T, lax.rem(i, T)].astype(F32)
        q = rows.shape[0]
        value = layer_norm_rows(rows, gain1, bias1)
        for b in range(F * C):
            normed[b, pl.ds(pl.multiple_of(i * q, q), q)] = value[:, b * R : (b + 1) * R]
        return carry

    lax.fori_loop(0, C * T, norm_unit, 0)
    save(normed, o_normed)

    tile = min(256, N)

    def project(ff, c, first, last):
        def one(i, carry):
            rows = pl.ds(pl.multiple_of(i * tile, tile), tile)
            part = nn(normed[ff * C + c, rows], win[ff, c, :, :NI])
            if not first:
                part = part + acc[rows]
            if last:
                proj[rows] = part.astype(BF)
            else:
                acc[rows] = part
            return carry

        lax.fori_loop(0, N // tile, one, 0)

    wi.local.wait()
    own = len(wi.units)
    project(f, z, True, False)
    for e in range(1, F):
        wi.arrived(own, e)
        project(pc.fbehind(e), z, False, False)
    gk.start()
    for i, d in enumerate(near):
        keys = [k for k, (dd, _) in enumerate(wi.units) if dd == d]
        for k in keys:
            wi.forward(k)
        project(f, pc.behind(d), False, False)
        if i == 1:
            wr.start(8)
    for i, d in enumerate(near):
        keys = [k for k, (dd, _) in enumerate(wi.units) if dd == d]
        for e in range(1, F):
            for k in keys:
                wi.arrived(k, e)
            project(pc.fbehind(e), pc.behind(d), False, i == C - 2 and e == F - 1)
    gk.send(C)
    wr.send(4)
    save(proj, o_proj)
    save(win, o_win)

    for cp in lz.values():
        cp.wait()
    head = z // halves
    scale = float(KEY) ** (-0.5)
    state[...] = jnp.zeros_like(state)

    def retain(u, carry):
        c, s = u // S, lax.rem(u, S)
        rows = pl.ds(pl.multiple_of(u * B, B), B)
        rates = old[c, pl.ds(head, 1), pl.ds(pl.multiple_of(s * B, B), B)]
        table, growth, keeping, through = decays(rates)
        q, k, v = proj[rows, :KEY], proj[rows, KEY : 2 * KEY], proj[rows, 2 * KEY : 2 * KEY + HV]
        weights = (nt(q, k) * scale * table).astype(BF)
        before = state[s]
        states[u] = before.astype(BF)
        mixed = nn(weights, v) + nn((q.astype(F32) * growth).astype(BF), before.astype(BF))
        state[s] = through * before + tn((k.astype(F32) * keeping).astype(BF), v)
        normal[rows] = mixed
        mean = jnp.mean(mixed, axis=-1, keepdims=True)
        dev = mixed - mean
        stats[0, 0:1, rows] = as_row(mean)
        stats[0, 1:2, rows] = as_row(jnp.sum(dev * dev, axis=-1, keepdims=True))
        return carry

    stats[0] = jnp.zeros(stats.shape[1:], F32)
    lax.fori_loop(0, units, retain, 0)
    save(states, o_states)
    wr.send(4 * C)
    st = []
    place = lax.rem(z, halves)
    for j in range(1, halves):
        peer = {"ctx": z - place + lax.rem(place + j, halves)}
        cp = remote(stats.at[0], stats.at[j], sts.at[j], strr.at[j], peer)
        cp.start()
        st.append(cp)
    for cp in st:
        cp.wait()

    def finish_unit(u, carry):
        rows = pl.ds(pl.multiple_of(u * B, B), B)
        got = [(stats[j, 0:1, rows], stats[j, 1:2, rows]) for j in range(halves)]
        mean = sum(a for a, _ in got) / halves
        m2 = sum(b + HV * (a - mean) * (a - mean) for a, b in got)
        scaled = as_column(lax.rsqrt(m2 / HEAD_V + EPSILON))
        value = (normal[rows] - as_column(mean)) * scaled
        gate = proj[rows, 2 * KEY + HV :].astype(F32)
        normal[rows] = value
        inv[0:1, rows] = lax.rsqrt(m2 / HEAD_V + EPSILON)
        gated[rows] = (gate * jax.nn.sigmoid(gate) * value).astype(BF)
        return carry

    inv[...] = jnp.zeros_like(inv)
    lax.fori_loop(0, units, finish_unit, 0)
    save(normal, o_normal)
    save(gated, o_gated)

    p = otok
    Q = x.shape[0]
    cut, parts = halves_of(Q)
    scatters, gathers = [], []
    for h in range(parts):
        at = h * (n + m)
        slot = lambda c, i, h=h: sn.at[c, i, cut(h)]
        gathers.append(Chain(pc, x.at[cut(h)], slot, refs[at : at + n]))
        scatters.append(Scatter(pc, p, cut(h), refs[at + n : at + n + m]))
    for d in near + [0]:
        c = pc.ahead(d)
        mixed = gated[pl.ds(pl.multiple_of(c * L, L), L)]

        def one(b, carry):
            part = across_blocks(mixed, win, b, pl.ds(NI, HV))
            columns = pl.ds(pl.multiple_of(b * part.shape[1], 128), part.shape[1])
            for i in range(T):
                p[c, i, :, columns] = part[i * Q : (i + 1) * Q]
            return carry

        lax.fori_loop(0, W // max(R, 128), one, 0)
        scatters[0].begin(d)
    for d in near:
        gk.forward(d)
    pump = Pump(scatters, begun=C)
    pump.run(C)
    for k in range(8):
        wr.forward(k)
    for d in near:
        gk.onward(d)
    mine.wait()
    for h, rs in enumerate(scatters):
        pump.run(min(2, len(pump.units) - pump.done))
        part = cut(h)
        total = rs.result() + mytok[part].astype(F32)
        mid[part] = total
        x[part] = layer_norm_rows(total, vecs[2:3], vecs[3:4])
        gathers[h].start()
        if h == 0:
            pump.run(len(pump.units) - pump.done)
            for k in range(8, len(wr.units)):
                wr.forward(k)
    for d in range(1, C):
        for ga in gathers:
            ga.forward(d)
    for ga in gathers:
        for d in range(C):
            ga.onward(d)
    for job in scatters + gathers:
        job.finish()
    gk.finish()
    wi.sent()
    wr.local.wait()
    for k in range(len(wr.units) + 1):
        for e in range(1, F):
            wr.arrived(k, e)
    wr.sent()
    for cp in saved:
        cp.wait()


def norm_pull(values, gain, grad):
    center = values - jnp.mean(values, axis=-1, keepdims=True)
    spread = jnp.mean(center * center, axis=-1, keepdims=True)
    inv = lax.rsqrt(spread + EPSILON)
    xhat = center * inv
    g = grad * gain
    back = inv * (
        g - jnp.mean(g, axis=-1, keepdims=True) - xhat * jnp.mean(g * xhat, axis=-1, keepdims=True)
    )
    return (
        back,
        jnp.sum(grad * xhat, axis=0, keepdims=True),
        jnp.sum(grad, axis=0, keepdims=True),
    )


def gelu_parts(v):
    c = (2.0 / jnp.pi) ** 0.5
    t = jnp.tanh(c * (v + 0.044715 * v * v * v))
    return 0.5 * v * (1.0 + t), 0.5 * (1.0 + t) + 0.5 * v * (1.0 - t * t) * c * (
        1.0 + 3 * 0.044715 * v * v
    )


def middle_kernel(dims, cfg, *refs):
    F, C, T = dims
    S, B, U = cfg
    refs = list(refs)

    def take(n):
        out = refs[:n]
        del refs[:n]
        return out

    second, gout, wr, mid, allgo, vecs = take(6)
    gm, gb, down, dgain, dbias, msum = take(6)
    stile, gtile, sblk, gblk, acc, gates, hid, pg, pd, turned, turned2 = take(11)
    msend, mgot, mloc, x, go = take(5)
    ssem, gsem, gosem, dsem, msem, mxs, mxr = take(7)
    gsems = take(len(chain_sems(C)))

    pc = Place(*dims)
    f = pc.f
    R, N = wr.shape[2], hid.shape[0]
    Q = x.shape[0]
    W = F * C * R
    pc.barrier(True, True, True)
    mine = pltpu.make_async_copy(allgo.at[pc.t], go, gosem)
    mine.start()
    rg = Scatter(pc, pg, pl.ds(0, Q), refs)
    saved = []
    order = rg.order
    units = [(d, s) for d in order for s in range(S)]

    def rows_of(i):
        d, s = units[i]
        return pl.ds(pl.multiple_of((pc.ahead(d) * S + s) * B, B), B)

    def load(i):
        k = i % 2
        return (
            pltpu.make_async_copy(second.at[rows_of(i)], stile.at[k], ssem.at[k]),
            pltpu.make_async_copy(gout.at[rows_of(i)], gtile.at[k], gsem.at[k]),
        )

    for cp in load(0):
        cp.start()

    def unit(i):
        d, s = units[i]
        k = i % 2
        rows = rows_of(i)
        if i + 1 < len(units):
            for cp in load(i + 1):
                cp.start()
        for cp in load(i):
            cp.wait()
        for b in range(F * C):
            sblk[b, rows] = stile[k, :, b * R : (b + 1) * R]
            gblk[b, rows] = gtile[k, :, b * R : (b + 1) * R]
        acc[...] = jnp.zeros_like(acc)

        def forward(b, carry):
            w = wr[b // C, lax.rem(b, C)]
            acc[:, : 2 * U] += nn(sblk[b, rows], w[:, : 2 * U])
            acc[:, 2 * U :] += nn(gblk[b, rows], w[:, 2 * U :])
            return carry

        lax.fori_loop(0, F * C, forward, 0)
        gate = acc[:, :U].astype(BF).astype(F32)
        up = acc[:, U : 2 * U].astype(BF).astype(F32)
        grad = acc[:, 2 * U :]
        value, slope = gelu_parts(gate)
        hid[rows] = (value * up).astype(BF)
        gates[rows, :U] = (grad * up * slope).astype(BF)
        gates[rows, U:] = (grad * value).astype(BF)
        c = pc.ahead(d)
        pull, keep = gates[rows], hid[rows]

        def back(b, carry):
            for p, part in (
                (pg, across_blocks(pull, wr, b, pl.ds(0, 2 * U))),
                (pd, across_blocks(keep, wr, b, pl.ds(2 * U, U))),
            ):
                columns = pl.ds(pl.multiple_of(b * part.shape[1], 128), part.shape[1])
                for j in range(B // Q):
                    p[c, s * (B // Q) + j, :, columns] = part[j * Q : (j + 1) * Q]
            return carry

        lax.fori_loop(0, W // max(R, 128), back, 0)

    for i in range(len(units)):
        unit(i)
        if units[i][1] == S - 1:
            k = i // S
            rg.begin(order[k])
            c = pc.ahead(order[k])
            cp = pltpu.make_async_copy(pd.at[c], down.at[c], dsem.at[k])
            cp.start()
            saved.append(cp)
            if k >= 1:
                rg.far(order[k - 1])
            if k >= 2:
                rg.along(order[k - 2])
    rg.far(order[C - 1])
    for d in order[max(C - 2, 0) :]:
        rg.along(d)

    xc = {}

    def block(d, e):
        b = pc.fahead(e) * C + pc.ahead(d)
        turned[...] = jnp.transpose(sblk[b])
        turned2[...] = jnp.transpose(gblk[b])
        return nn(turned[...], gates[...]), nn(turned2[...], hid[...])

    for d in order:
        for e in range(1, F):
            c = pc.ahead(d)
            first, last = block(d, e)
            msend[e - 1, d, :, : 2 * U] = first.astype(BF)
            msend[e - 1, d, :, 2 * U :] = last.astype(BF)
            xc[d, e] = remote(
                msend.at[e - 1, d], mgot.at[e - 1, d], mxs.at[d, e], mxr.at[d, e], {"fsdp": pc.fahead(e)}
            )
            xc[d, e].start()

    mine.wait()
    back, dg, db = norm_pull(mid[...], vecs[2:3], rg.result())
    dgain[...] = dg
    dbias[...] = db
    grad_middle = go[...].astype(F32) + back
    gm[...] = grad_middle
    x[...] = grad_middle.astype(BF)
    ga = Chain(pc, x, lambda c, i: gb.at[c, i], gsems)
    ga.start()
    for h in range(1, min(3, C)):
        ga.forward(h)
    for k, d in enumerate(order):
        if k == 1:
            for h in range(3, C):
                ga.forward(h)
        first, last = block(d, 0)
        for e in range(1, F):
            xc[d, e].wait_recv()
            first = first + mgot[e - 1, d, :, : 2 * U].astype(F32)
            last = last + mgot[e - 1, d, :, 2 * U :].astype(F32)
        mloc[d, :, : 2 * U] = first.astype(BF)
        mloc[d, :, 2 * U :] = last.astype(BF)
        cp = pltpu.make_async_copy(mloc.at[d], msum.at[pc.ahead(d)], msem.at[d])
        cp.start()
        saved.append(cp)
    for h in range(C):
        ga.onward(h)
    for job in (rg, ga):
        job.finish()
    for cp in xc.values():
        cp.wait_send()
    for cp in saved:
        cp.wait()


def vector_stage(pc, v, vout, va, vb, vc, vd, vx, vz, ts, tr, vxs, vxr, vzs, vzr):
    F, C = pc.F, pc.C
    t0 = remote(v, vb, ts.at[0], tr.at[0], {"tp": pc.near})
    t0.start()
    yield
    t0.wait_recv()
    va[...] = v[...] + vb[...]
    t1 = remote(va, vc, ts.at[1], tr.at[1], {"tp": pc.far})
    t1.start()
    yield
    t1.wait_recv()
    vd[...] = va[...] + vc[...]
    vxc, vzc = {}, {}
    for e in range(1, F):
        vxc[e] = remote(
            vd.at[pc.fahead(e)], vx.at[e - 1], vxs.at[e], vxr.at[e], {"fsdp": pc.fahead(e)}
        )
        vxc[e].start()
    yield
    vs = vd[pc.f]
    for e in range(1, F):
        vxc[e].wait_recv()
        vs = vs + vx[e - 1]
    vz[0] = vs
    for d in range(1, C):
        vzc[d] = remote(
            vz.at[0, pc.ahead(d)], vz.at[1, d], vzs.at[d], vzr.at[d], {"ctx": pc.ahead(d)}
        )
        vzc[d].start()
    yield
    acc = vz[0, pc.z]
    for d in range(1, C):
        vzc[d].wait_recv()
        acc = acc + vz[1, d]
    vout[...] = acc
    for cp in [t0, t1] + list(vxc.values()) + list(vzc.values()):
        cp.wait_send()


def vector_scratch(F, C, R):
    full = pltpu.VMEM((F, C, 8, R), F32)
    return [
        full,
        full,
        full,
        full,
        full,
        pltpu.VMEM((F - 1, C, 8, R), F32),
        pltpu.VMEM((2, C, 8, R), F32),
        sem(2),
        sem(2),
        sem(F),
        sem(F),
        sem(C),
        sem(C),
    ]


def backward_kernel(dims, cfg, *refs):
    F, C, T = dims
    S, B, halves, HV = cfg
    refs = list(refs)

    def take(n):
        out = refs[:n]
        del refs[:n]
        return out

    branch, normed, win, proj, states, normal, inv, gated, old, vecs, gm, alltok, mlp, dg2, db2, down, mid = take(17)
    gt, result, gout, mout, vout = take(5)
    btile, ntile, cblock, turned, turned2, gn, gproj, later, stats, p = take(10)
    gsend, xbuf, zsnd, tok, y = take(5)
    bsem, nsem, sts, strr, mzs, mzr, xos, xor, xs, xr, zs, zr, keeps, toksem, lsem, msem = take(16)
    shares, shares2, vscratch = take(2), take(2), take(13)
    y2, lsem2, local = take(1)[0], take(1)[0], take(2)
    half = len(refs) // 2

    pc = Place(*dims)
    f, z, t = pc.f, pc.z, pc.t
    L = S * B
    R = win.shape[2]
    W = F * C * R
    N, NI = gproj.shape
    Q = y.shape[0]
    units = C * S
    pc.barrier(True, True, True)
    mine = pltpu.make_async_copy(alltok.at[t], tok, toksem)
    mine.start()

    moves = [pltpu.make_async_copy(mlp.at[z], mout.at[z], msem)]
    for d in pc.near_first():
        dst = pc.ahead(d)
        moves.append(remote(mlp.at[dst], mout.at[z], mzs.at[d], mzr.at[d], {"ctx": dst}))
    for cp in moves:
        cp.start()

    rd = Scatter(pc, down, pl.ds(0, Q), refs[half:], local)
    rd.start()

    def rows_in(u, slot):
        rows = pl.ds(pl.multiple_of(u * B, B), B)
        return pltpu.make_async_copy(branch.at[rows], btile.at[slot], bsem.at[slot])

    rows_in(0, 0).start()
    stats[0] = jnp.zeros(stats.shape[1:], F32)

    def pull_gate(u, carry):
        slot = lax.rem(u, 2)
        pl.when(u + 1 < units)(lambda: rows_in(u + 1, 1 - slot).start())
        rows_in(u, slot).wait()
        grad = None
        rows = pl.ds(pl.multiple_of(u * B, B), B)
        for b in range(F * C):
            piece = btile[slot, :, b * R : (b + 1) * R]
            cblock[b, rows] = piece
            part = nn(piece, win[b // C, b % C, :, NI:])
            grad = part if grad is None else grad + part
        gate = proj[rows, 2 * KEY + HV :].astype(F32)
        silu, dsilu = silu_parts(gate)
        value = normal[rows]
        gproj[rows, 2 * KEY + HV :] = (grad * value * dsilu).astype(BF)
        inner = grad * silu
        gn[rows] = inner
        stats[0, 0:1, rows] = as_row(jnp.sum(inner, axis=-1, keepdims=True))
        stats[0, 1:2, rows] = as_row(jnp.sum(inner * value, axis=-1, keepdims=True))
        return carry

    lax.fori_loop(0, units, pull_gate, 0)
    st = []
    place = lax.rem(z, halves)
    for j in range(1, halves):
        peer = {"ctx": z - place + lax.rem(place + j, halves)}
        cp = remote(stats.at[0], stats.at[j], sts.at[j], strr.at[j], peer)
        cp.start()
        st.append(cp)

    for d in rd.order:
        rd.far(d)

    far = sorted(range(1, C), key=lambda d: abs(d - C // 2))
    order = far + [0]
    blocks = [(d, e) for d in order for e in range(1, F)] + [(d, 0) for d in order]
    xo, xc, zc = {}, {}, {}

    def columns_in(i):
        d, e = blocks[i]
        b = pc.fahead(e) * C + pc.ahead(d)
        return b, pltpu.make_async_copy(normed.at[b], ntile.at[i % 2], nsem.at[i % 2])

    def start_columns(i):
        if i < len(blocks):
            columns_in(i)[1].start()

    tail = pl.ds(NI, HV)
    for d, e in blocks[: (F - 1) * C]:
        turned2[...] = jnp.transpose(cblock[pc.fahead(e) * C + pc.ahead(d)])
        gsend[e - 1, d, :, tail] = nn(turned2[...], gated[...]).astype(BF)
        xo[d, e] = remote(
            gsend.at[e - 1, d, :, tail],
            xbuf.at[e - 1, d, :, tail],
            xos.at[d, e],
            xor.at[d, e],
            {"fsdp": pc.fahead(e)},
        )
        xo[d, e].start()

    start_columns(0)
    for cp in st:
        cp.wait()

    head = z // halves
    scale = float(KEY) ** (-0.5)
    later[...] = jnp.zeros_like(later)

    def retain(i, carry):
        u = units - 1 - i
        c, s = u // S, lax.rem(u, S)
        rows = pl.ds(pl.multiple_of(u * B, B), B)
        rates = old[c, pl.ds(head, 1), pl.ds(pl.multiple_of(s * B, B), B)]
        table, growth, keeping, through = decays(rates)
        q, k, v = proj[rows, :KEY], proj[rows, KEY : 2 * KEY], proj[rows, 2 * KEY : 2 * KEY + HV]
        s1 = as_column(sum(stats[j, 0:1, rows] for j in range(halves)) / HEAD_V)
        s2 = as_column(sum(stats[j, 1:2, rows] for j in range(halves)) / HEAD_V)
        mix = (as_column(inv[0:1, rows]) * (gn[rows] - s1 - normal[rows] * s2)).astype(BF)
        weights = (nt(q, k) * scale * table).astype(BF)
        scores = (nt(mix, v) * scale * table).astype(BF)
        after = later[s]
        after_low = after.astype(BF)
        gq = nn(scores, k) + growth * nt(mix, states[u])
        gk = tn(scores, q) + keeping * nt(v, after_low)
        gv = tn(weights, mix) + nn((k.astype(F32) * keeping).astype(BF), after_low)
        later[s] = through * after + tn((q.astype(F32) * growth).astype(BF), mix)
        gproj[rows, :KEY] = gq.astype(BF)
        gproj[rows, KEY : 2 * KEY] = gk.astype(BF)
        gproj[rows, 2 * KEY : 2 * KEY + HV] = gv.astype(BF)
        return carry

    lax.fori_loop(0, units, retain, 0)

    rs = Scatter(pc, p, pl.ds(0, Q), refs[:half])
    for d in rs.order:
        c = pc.ahead(d)
        mixed = gproj[pl.ds(pl.multiple_of(c * L, L), L)]

        def one(b, carry, c=c, mixed=mixed):
            part = across_blocks(mixed, win, b, pl.ds(0, NI))
            columns = pl.ds(pl.multiple_of(b * part.shape[1], 128), part.shape[1])
            for i in range(T):
                p[c, i, :, columns] = part[i * Q : (i + 1) * Q]
            return carry

        lax.fori_loop(0, W // max(R, 128), one, 0)
        rs.begin(d)
    pump = Pump([rs], begun=C)
    pump.fill()
    for d in rd.order[:2]:
        rd.along(d)

    H = 2
    kept = []
    halfs = [pl.ds(h * (R // H), R // H) for h in range(H)]
    main = pl.ds(0, NI)

    def block(i):
        d, e = blocks[i]
        start_columns(i + 1)
        b, cp = columns_in(i)
        cp.wait()
        turned[...] = jnp.transpose(ntile[i % 2])
        if e == 0:
            turned2[...] = jnp.transpose(cblock[b])
            for g in range(1, F):
                xo[d, g].wait_recv()
                for h in range(H):
                    xc[d, g, h].wait_recv()

        def put(columns, part):
            if e:
                gsend[e - 1, d, :, columns] = part.astype(BF)
            else:
                for g in range(F - 1):
                    part = part + xbuf[g, d, :, columns].astype(F32)
                zsnd[d, :, columns] = part.astype(BF)

        def one(j, carry):
            columns = pl.ds(pl.multiple_of(j * 256, 256), 256)
            put(columns, nn(turned[...], gproj[:, columns]))
            return carry

        lax.fori_loop(0, NI // 256, one, 0)
        if e == 0:
            put(tail, nn(turned2[...], gated[...]))
        for h, part in enumerate(halfs):
            if e:
                xc[d, e, h] = remote(
                    gsend.at[e - 1, d, part, main],
                    xbuf.at[e - 1, d, part, main],
                    xs.at[d, e, h],
                    xr.at[d, e, h],
                    {"fsdp": pc.fahead(e)},
                )
                xc[d, e, h].start()
            elif d:
                zc[d, h] = remote(
                    zsnd.at[d, part], gout.at[z, part], zs.at[d, h], zr.at[d, h], {"ctx": pc.ahead(d)}
                )
                zc[d, h].start()
            else:
                cp = pltpu.make_async_copy(zsnd.at[0, part], gout.at[z, part], keeps.at[h])
                cp.start()
                kept.append(cp)

    sends = (F - 1) * C
    for i in range(sends):
        block(i)
        if i < len(rd.order[2:]):
            rd.along(rd.order[2 + i])
        if pump.done < len(pump.units):
            pump.run(1)
    for d in rd.order[2 + sends :]:
        rd.along(d)
    pump.run(len(pump.units) - pump.done)
    stages = []
    for i in range(sends, len(blocks)):
        block(i)
        if i == sends:
            mine.wait()
            back, dg, db = norm_pull(tok[...].astype(F32), vecs[0:1], rs.result())
            y[...] = (gm[...] + back).astype(BF)
            v = vscratch[0]
            for b in range(F * C):
                rows = [r[:, b * R : (b + 1) * R] for r in (dg, db)] + [
                    r[:, b * R : (b + 1) * R] for r in (dg2, db2)
                ]
                v[b // C, b % C] = jnp.concatenate(rows + [jnp.zeros((4, R), F32)], axis=0)
            y2[...] = (mid[...] + rd.result()).astype(BF)
            stages = [
                share_stage(pc, y, gt, lsem, shares),
                share_stage(pc, y2, result, lsem2, shares2),
                vector_stage(pc, v, vout, *vscratch[1:]),
            ]
        for stage in stages:
            next(stage, None)
    for stage in stages:
        drain(stage)
    rs.finish()
    rd.finish()
    for cp in kept:
        cp.wait()
    for cp in zc.values():
        cp.wait()
    for cp in list(xc.values()) + list(xo.values()):
        cp.wait_send()
    for cp in moves:
        cp.wait()


def assemble_kernel(halves, key, hv, a, m, q, k, v, g, o, fg, fu, fd):
    c = pl.program_id(0)
    first = lax.rem(c, halves) == 0
    for i, ref in enumerate((q, k)):
        x = a[0, :, i * key : (i + 1) * key].astype(F32)

        @pl.when(first)
        def _(ref=ref, x=x):
            ref[...] = x

        @pl.when(jnp.logical_not(first))
        def _(ref=ref, x=x):
            ref[...] += x

    v[...] = a[0, :, 2 * key : 2 * key + hv].astype(F32)
    g[...] = a[0, :, 2 * key + hv : 2 * key + 2 * hv].astype(F32)
    o[...] = a[0, :, 2 * key + 2 * hv :].astype(F32)
    u = fg.shape[1]
    for i, ref in enumerate((fg, fu, fd)):
        ref[...] = m[0, :, i * u : (i + 1) * u].astype(F32)


def params(cid):
    return pltpu.CompilerParams(collective_id=cid, has_side_effects=True)


def shards(
    dims,
    tokens,
    log_decay,
    w_query,
    w_key,
    w_value,
    w_gate,
    w_out,
    norm1_gain,
    norm1_bias,
    w_ffgate,
    w_ffup,
    w_down,
    norm2_gain,
    norm2_bias,
    grad_out,
):
    F, C, T = dims
    S, B, W = tokens.shape
    L = S * B
    Q = L // T
    N = C * L
    R = w_query.shape[0]
    heads = log_decay.shape[2]
    halves = C // heads
    HV = HEAD_V // halves
    U = w_ffgate.shape[1] // C
    z = lax.axis_index("ctx")
    t = lax.axis_index("tp")
    scale = float(KEY) ** (-0.5)

    f = lax.axis_index("fsdp")

    def hop(x, axis, d):
        n = lax.axis_size(axis)
        return lax.ppermute(x, axis, [(i, (i + d) % n) for i in range(n)])

    def at(x, i, n):
        return lax.dynamic_index_in_dim(x, lax.rem(i, n), 0, False)

    NI, NR = 2 * KEY + 2 * HV, 3 * U
    NO = NI + HV
    norms = (norm1_gain, norm1_bias, norm2_gain, norm2_bias)
    tok = tokens.reshape(T, Q, W)
    go = grad_out.reshape(T, Q, W)
    sds = jax.ShapeDtypeStruct
    cfg = (
        S,
        B,
        halves,
        HV,
        ((halves, KEY), (halves, KEY), (1, HV), (1, HV), (1, HV)),
        ((1, U), (1, U), (1, U)),
    )
    owin, normed, proj, states, normal, gated, inv, old, vecs, mid, sn, full, ogo = pl.pallas_call(
        functools.partial(forward_kernel, dims, cfg),
        out_shape=(
            sds((F, C, R, NO), BF),
            sds((F * C, N, R), BF),
            sds((N, NI), BF),
            sds((C * S, KEY, HV), BF),
            sds((N, HV), F32),
            sds((N, HV), BF),
            sds((8, N), F32),
            sds((C, 8, L), F32),
            sds((8, W), F32),
            sds((Q, W), F32),
            sds((C, T, Q, W), BF),
            sds((F, C, R, NR), BF),
            sds((C, T, Q, W), BF),
        ),
        in_specs=[ANY] * 8 + [VMEM] * 5 + [ANY, ANY],
        out_specs=[ANY] * 6 + [VMEM] * 4 + [ANY] * 3,
        scratch_shapes=[
            pltpu.VMEM((C, T, Q, W), BF),
            pltpu.VMEM((F, C, R, NO), BF),
            pltpu.VMEM((F, C, 8, R), F32),
            pltpu.VMEM((F * C, N, R), BF),
            pltpu.VMEM((N, NI), F32),
            pltpu.VMEM((N, NI), BF),
            pltpu.VMEM((C * S, KEY, HV), BF),
            pltpu.VMEM((S, KEY, HV), F32),
            pltpu.VMEM((N, HV), F32),
            pltpu.VMEM((N, HV), BF),
            pltpu.VMEM((halves, 8, N), F32),
            pltpu.VMEM((Q, W), BF),
            pltpu.VMEM((Q, W), BF),
        ]
        + mover_sems(F, C) * 2
        + blocks_sems(C) * 2
        + [sem(C), sem(C), sem(C, F), sem(C, F), sem(C), sem(C), sem(halves), sem(halves), sem(16)]
        + [pltpu.VMEM((8, R), F32), pltpu.VMEM((8, L), F32)]
        + (chain_sems(C) + scatter_scratch(C, Q // PARTS, W)) * PARTS,
        compiler_params=params(1),
        name="k_forward",
    )(w_query, w_key, w_value, w_gate, w_out, w_ffgate, w_ffup, w_down, *norms, log_decay, tok, go)
    gm, gb, down, dgain2, dbias2, mlp_sum = pl.pallas_call(
        functools.partial(middle_kernel, dims, (S, B, U)),
        out_shape=(
            sds((Q, W), F32),
            sds((C, T, Q, W), BF),
            sds((C, T, Q, W), BF),
            sds((1, W), F32),
            sds((1, W), F32),
            sds((C, R, NR), BF),
        ),
        in_specs=[ANY, ANY, VMEM, VMEM, ANY, VMEM],
        out_specs=[VMEM, ANY, ANY, VMEM, VMEM, ANY],
        scratch_shapes=[
            pltpu.VMEM((2, B, W), BF),
            pltpu.VMEM((2, B, W), BF),
            pltpu.VMEM((F * C, N, R), BF),
            pltpu.VMEM((F * C, N, R), BF),
            pltpu.VMEM((B, 3 * U), F32),
            pltpu.VMEM((N, 2 * U), BF),
            pltpu.VMEM((N, U), BF),
            pltpu.VMEM((C, T, Q, W), BF),
            pltpu.VMEM((C, T, Q, W), BF),
            pltpu.VMEM((R, N), BF),
            pltpu.VMEM((R, N), BF),
            pltpu.VMEM((F - 1, C, R, NR), BF),
            pltpu.VMEM((F - 1, C, R, NR), BF),
            pltpu.VMEM((C, R, NR), BF),
            pltpu.VMEM((Q, W), BF),
            pltpu.VMEM((Q, W), BF),
            sem(2),
            sem(2),
            pltpu.SemaphoreType.DMA,
            sem(C),
            sem(C),
            sem(C, F),
            sem(C, F),
        ]
        + chain_sems(C)
        + scatter_scratch(C, Q, W),
        compiler_params=params(3),
        name="k_middle",
    )(sn.reshape(N, W), ogo.reshape(N, W), full, mid, go, vecs)

    branch = gb.reshape(N, W)
    H = 2
    gt, out, gsum, mlp_grads, vsum = pl.pallas_call(
        functools.partial(backward_kernel, dims, (S, B, halves, HV)),
        out_shape=(
            sds((T, Q, W), BF),
            sds((T, Q, W), BF),
            sds((C, R, NO), BF),
            sds((C, R, NR), BF),
            sds((8, R), F32),
        ),
        in_specs=[ANY, ANY] + [VMEM] * 9 + [ANY, ANY, VMEM, VMEM, ANY, VMEM],
        out_specs=[ANY] * 4 + [VMEM],
        scratch_shapes=[
            pltpu.VMEM((2, B, W), BF),
            pltpu.VMEM((2, N, R), BF),
            pltpu.VMEM((F * C, N, R), BF),
            pltpu.VMEM((R, N), BF),
            pltpu.VMEM((R, N), BF),
            pltpu.VMEM((N, HV), F32),
            pltpu.VMEM((N, NI), BF),
            pltpu.VMEM((S, KEY, HV), F32),
            pltpu.VMEM((halves, 8, N), F32),
            pltpu.VMEM((C, T, Q, W), BF),
            pltpu.VMEM((F - 1, C, R, NO), BF),
            pltpu.VMEM((F - 1, C, R, NO), BF),
            pltpu.VMEM((C, R, NO), BF),
            pltpu.VMEM((Q, W), BF),
            pltpu.VMEM((Q, W), BF),
            sem(2),
            sem(2),
            sem(halves),
            sem(halves),
            sem(C),
            sem(C),
            sem(C, F),
            sem(C, F),
            sem(C, F, H),
            sem(C, F, H),
            sem(C, H),
            sem(C, H),
            sem(H),
        ]
        + [pltpu.SemaphoreType.DMA] * 3
        + share_sems() * 2
        + vector_scratch(F, C, R)
        + [pltpu.VMEM((Q, W), BF), pltpu.SemaphoreType.DMA]
        + local_scratch(C, Q, W)
        + scatter_scratch(C, Q, W) * 2,
        compiler_params=params(4),
        name="k_backward",
    )(
        branch,
        normed,
        owin,
        proj,
        states,
        normal,
        inv,
        gated,
        old,
        vecs,
        gm,
        tok,
        mlp_sum,
        dgain2,
        dbias2,
        down,
        mid,
    )
    output = out.reshape(tokens.shape)
    grad_tokens = gt.reshape(tokens.shape)

    def quarter(n):
        return pl.BlockSpec((R, n), lambda c: (0, c))

    per_head = pl.BlockSpec((R, KEY), lambda c: (0, c // halves))
    gq, gk, gv, gg, gw, gfg, gfu, gfd = pl.pallas_call(
        functools.partial(assemble_kernel, halves, KEY, HV),
        out_shape=[sds((R, heads * KEY), F32)] * 2
        + [sds((R, C * HV), F32)] * 3
        + [sds((R, C * U), F32)] * 3,
        grid=(C,),
        in_specs=[
            pl.BlockSpec((1, R, NO), lambda c: (c, 0, 0)),
            pl.BlockSpec((1, R, NR), lambda c: (c, 0, 0)),
        ],
        out_specs=[per_head, per_head] + [quarter(HV)] * 3 + [quarter(U)] * 3,
        name="k_assemble",
    )(gsum, mlp_grads)
    return (
        output,
        grad_tokens,
        gq,
        gk,
        gv,
        gg,
        gw,
        vsum[0],
        vsum[1],
        gfg,
        gfu,
        gfd,
        vsum[2],
        vsum[3],
    )


def solution(mesh):
    dims = (mesh.shape["fsdp"], mesh.shape["ctx"], mesh.shape["tp"])
    rows, vec = P(("fsdp", "ctx"), "tp"), P(("fsdp", "ctx"))
    acts = P("fsdp", "ctx", None)
    return jax.shard_map(
        functools.partial(shards, dims),
        mesh=mesh,
        in_specs=(acts, P("fsdp", "ctx", "tp"), rows, rows, rows, rows, rows, vec, vec, rows, rows, rows, vec, vec, acts),
        out_specs=(acts, acts, rows, rows, rows, rows, rows, vec, vec, rows, rows, rows, vec, vec),
        check_vma=False,
    )
```

```python
import functools

import jax
import jax.numpy as jnp
from jax import lax
from jax.experimental import pallas as pl
from jax.experimental.pallas import tpu as pltpu
from jax.sharding import PartitionSpec as P

KEY = 256
HEAD_V = 512
EPSILON = 1e-05
MESH = pl.DeviceIdType.MESH
ANY = pl.BlockSpec(memory_space=pl.ANY)
VMEM = pl.BlockSpec(memory_space=pltpu.VMEM)
BF = jnp.bfloat16
F32 = jnp.float32


def dot(a, b, dims):
    return lax.dot_general(a, b, (dims, ((), ())), preferred_element_type=F32)


def nn(a, b):
    return dot(a, b, ((1,), (0,)))


def nt(a, b):
    return dot(a, b, ((1,), (1,)))


def tn(a, b):
    return dot(a, b, ((0,), (0,)))


class Place:
    def __init__(self, F, C, T):
        self.F, self.C, self.T = F, C, T
        self.f = lax.axis_index("fsdp")
        self.z = lax.axis_index("ctx")
        self.t = lax.axis_index("tp")
        self.lo = lax.rem(self.t, 2)
        self.hi = self.t // 2
        self.near = self.t + 1 - 2 * self.lo
        self.far = lax.rem(self.t + 2, 4)

    def near_first(self):
        return [1] + ([self.C - 1] if self.C > 2 else []) + list(range(2, self.C - 1))

    def ahead(self, d):
        return lax.rem(self.z + d, self.C)

    def behind(self, d):
        return lax.rem(self.z + self.C - d, self.C)

    def fahead(self, d):
        return lax.rem(self.f + d, self.F)

    def fbehind(self, d):
        return lax.rem(self.f + self.F - d, self.F)

    def barrier(self, ctx=True, fsdp=False, tp=True):
        sem = pltpu.get_barrier_semaphore()
        peers = []
        if tp:
            peers += [{"tp": self.near}, {"tp": self.far}]
        if fsdp:
            peers += [{"fsdp": self.fahead(d)} for d in range(1, self.F)]
        if ctx:
            peers += [{"ctx": self.ahead(d)} for d in range(1, self.C)]
        for peer in peers:
            pl.semaphore_signal(sem, inc=1, device_id=peer, device_id_type=MESH)
        pl.semaphore_wait(sem, len(peers))


def remote(src, dst, ssem, rsem, peer):
    return pltpu.make_async_remote_copy(
        src_ref=src, dst_ref=dst, send_sem=ssem, recv_sem=rsem, device_id=peer, device_id_type=MESH
    )


def sem(*shape):
    return pltpu.SemaphoreType.DMA(shape)


def chain_sems(C):
    return [sem(2, C), sem(2, C), sem(2, C), sem(2, C), sem(2, C, 2), sem(2, C, 2), pltpu.SemaphoreType.DMA]


class Chain:
    def __init__(self, pc, x, slot, sems, own=None):
        self.pc, self.x, self.slot, self.block = pc, x, slot, own
        self.zs, self.zr, self.ys, self.yr, self.cs, self.cr, self.ls = sems

    def came(self, s, h):
        z = self.pc.z
        return (z >= h, z - h) if s == 0 else (z + h <= self.pc.C - 1, z + h)

    def goes(self, s, h):
        pc = self.pc
        if s == 0:
            return jnp.logical_and(pc.z >= h - 1, pc.z < pc.C - 1)
        return jnp.logical_and(pc.z + h <= pc.C, pc.z > 0)

    def hop(self, s, h, c):
        z = self.pc.z
        here = self.slot(c, self.pc.t)
        src = self.x if h == 1 else here
        return remote(src, here, self.zs.at[s, h], self.zr.at[s, h], {"ctx": z + 1 if s == 0 else z - 1})

    def to_far(self, s, h, c):
        here = self.slot(c, self.pc.t)
        src = here if h else self.x
        return remote(src, here, self.ys.at[s, h], self.yr.at[s, h], {"tp": self.pc.far})

    def to_near(self, s, h, c):
        here = self.slot(c, self.pc.t)
        src = here if h else self.x
        return remote(src, here, self.cs.at[s, h, 0], self.cr.at[s, h, 0], {"tp": self.pc.near})

    def spread(self, s, h, c):
        self.to_far(s, h, c).start()
        self.to_near(s, h, c).start()

    def again(self, s, h, c):
        there = self.slot(c, self.pc.far)
        return remote(there, there, self.cs.at[s, h, 1], self.cr.at[s, h, 1], {"tp": self.pc.near})

    def start(self):
        pc = self.pc
        for s in range(2):
            pl.when(self.goes(s, 1))(lambda s=s: self.hop(s, 1, pc.z).start())
        src, dst = self.block or (self.x, self.slot(pc.z, pc.t))
        self.local = pltpu.make_async_copy(src, dst, self.ls)
        self.local.start()
        if not self.block:
            self.spread(0, 0, pc.z)

    def forward(self, h):
        for s in range(2):
            ok, c = self.came(s, h)

            @pl.when(ok)
            def _(s=s, c=c):
                self.hop(s, h, c).wait_recv()
                if h + 1 < self.pc.C:
                    pl.when(self.goes(s, h + 1))(lambda: self.hop(s, h + 1, c).start())
                self.spread(s, h, c)

    def onward(self, h):
        if h == 0:
            if not self.block:
                self.to_far(0, 0, self.pc.z).wait_recv()
                self.again(0, 0, self.pc.z).start()
            return
        for s in range(2):
            ok, c = self.came(s, h)

            @pl.when(ok)
            def _(s=s, c=c):
                self.to_far(s, h, c).wait_recv()
                self.again(s, h, c).start()

    def settle(self, s, h, c):
        self.to_far(s, h, c).wait_send()
        self.to_near(s, h, c).wait()
        self.again(s, h, c).wait()

    def finish(self):
        pc = self.pc
        self.local.wait()
        if not self.block:
            self.settle(0, 0, pc.z)
        for h in range(1, pc.C):
            for s in range(2):
                ok, c = self.came(s, h)
                first = pc.z - h + 1 if s == 0 else pc.z + h - 1
                pl.when(self.goes(s, h))(lambda s=s, c=first: self.hop(s, h, c).wait_send())
                pl.when(ok)(lambda s=s, c=c: self.settle(s, h, c))


def share_sems():
    return [sem(3), sem(3)]


def share_stage(pc, x, out, lsem, sems):
    ss, rs = sems
    t = pc.t
    local = pltpu.make_async_copy(x, out.at[t], lsem)
    local.start()
    a = remote(x, out.at[t], ss.at[0], rs.at[0], {"tp": pc.far})
    a.start()
    b = remote(x, out.at[t], ss.at[1], rs.at[1], {"tp": pc.near})
    b.start()
    yield
    a.wait_recv()
    src = out.at[pc.far]
    c = remote(src, src, ss.at[2], rs.at[2], {"tp": pc.near})
    c.start()
    yield
    local.wait()
    a.wait_send()
    b.wait()
    c.wait()


def scatter_scratch(C, Q, W):
    return [
        pltpu.VMEM((C, 2, Q, W), BF),
        pltpu.VMEM((C, Q, W), BF),
        pltpu.VMEM((C, Q, W), BF),
        pltpu.VMEM((C, Q, W), BF),
        pltpu.VMEM((C, Q, W), BF),
        sem(C, 2),
        sem(C, 2),
        sem(C),
        sem(C),
        sem(C),
        sem(C),
    ]


def local_scratch(C, Q, W):
    return [pltpu.VMEM((C, 2, Q, W), BF), sem(C, 2)]


class Scatter:
    def __init__(self, pc, p, rows, scratch, local=None):
        self.pc, self.p, self.rows, self.local = pc, p, rows, local
        (self.buf1, self.snd2, self.buf2, self.snd3, self.buf3) = scratch[:5]
        self.s1, self.r1, self.s2, self.r2, self.s3, self.r3 = scratch[5:]
        self.order = pc.near_first() + [0]
        self.lc, self.c1, self.c2, self.c3 = {}, {}, {}, {}

    def side(self, j):
        return 1 - self.pc.hi if j == 0 else self.pc.hi

    def begin(self, d):
        pc, p, rows = self.pc, self.p, self.rows
        c = pc.ahead(d)
        for j in range(2):
            self.c1[d, j] = remote(
                p.at[c, self.side(j) * 2 + 1 - pc.lo, rows],
                self.buf1.at[d, j],
                self.s1.at[d, j],
                self.r1.at[d, j],
                {"tp": pc.near},
            )
            self.c1[d, j].start()
            if self.local:
                self.lc[d, j] = pltpu.make_async_copy(
                    p.at[c, self.side(j) * 2 + pc.lo, rows],
                    self.local[0].at[d, j],
                    self.local[1].at[d, j],
                )
                self.lc[d, j].start()

    def start(self):
        for d in self.order:
            self.begin(d)

    def own(self, d, j):
        self.c1[d, j].wait_recv()
        if self.local:
            self.lc[d, j].wait()
            here = self.local[0][d, j]
        else:
            here = self.p[self.pc.ahead(d), self.side(j) * 2 + self.pc.lo, self.rows]
        return here.astype(F32) + self.buf1[d, j].astype(F32)

    def far(self, d):
        self.snd2[d] = self.own(d, 0).astype(BF)
        self.c2[d] = remote(
            self.snd2.at[d], self.buf2.at[d], self.s2.at[d], self.r2.at[d], {"tp": self.pc.far}
        )
        self.c2[d].start()

    def along(self, d):
        part = self.own(d, 1)
        self.c2[d].wait_recv()
        part = part + self.buf2[d].astype(F32)
        if d:
            self.snd3[d] = part.astype(BF)
            self.c3[d] = remote(
                self.snd3.at[d],
                self.buf3.at[d],
                self.s3.at[d],
                self.r3.at[d],
                {"ctx": self.pc.ahead(d)},
            )
            self.c3[d].start()
        else:
            self.total = part

    def result(self):
        total = self.total
        for d in range(1, self.pc.C):
            self.c3[d].wait_recv()
            total = total + self.buf3[d].astype(F32)
        return total

    def finish(self):
        for copies in (self.c1, self.c2, self.c3):
            for cp in copies.values():
                cp.wait_send()


def drain(stage):
    for _ in stage:
        pass


class Pump:
    def __init__(self, scatters, begun=0, window=3):
        self.units = [(rs, d) for rs in scatters for d in rs.order]
        self.window, self.begun, self.sent, self.done = window, begun, 0, 0

    def fill(self):
        while self.begun < min(len(self.units), self.done + 2 * self.window):
            rs, d = self.units[self.begun]
            rs.begin(d)
            self.begun += 1
        while self.sent < min(len(self.units), self.done + self.window):
            rs, d = self.units[self.sent]
            rs.far(d)
            self.sent += 1

    def run(self, count):
        for _ in range(count):
            self.fill()
            rs, d = self.units[self.done]
            rs.along(d)
            self.done += 1
        self.fill()


def silu_parts(g):
    s = jax.nn.sigmoid(g)
    return g * s, s * (1.0 + g * (1.0 - s))


PARTS = 2


def halves_of(rows):
    n = rows // PARTS
    return (lambda h: pl.ds(h * n, n)), PARTS


def layer_norm_rows(values, gain, bias):
    center = values - jnp.mean(values, axis=-1, keepdims=True)
    spread = jnp.mean(center * center, axis=-1, keepdims=True)
    return (center * lax.rsqrt(spread + EPSILON) * gain + bias).astype(BF)


def eye_of(n):
    return lax.broadcasted_iota(jnp.int32, (n, n), 0) == lax.broadcasted_iota(jnp.int32, (n, n), 1)


def as_row(column):
    return jnp.sum(jnp.where(eye_of(column.shape[0]), column, 0.0), axis=0, keepdims=True)


def as_column(row):
    return jnp.sum(jnp.where(eye_of(row.shape[1]), row, 0.0), axis=1, keepdims=True)


def decays(rates):
    B = rates.shape[1]
    causal = lax.broadcasted_iota(jnp.int32, (B, B), 0) >= lax.broadcasted_iota(jnp.int32, (B, B), 1)
    column = jnp.sum(jnp.where(causal, rates, 0.0), axis=1, keepdims=True)
    row = as_row(column)
    table = jnp.where(causal, jnp.exp(jnp.minimum(column - row, 0.0)), 0.0)
    total = column[B - 1 :]
    return table, jnp.exp(column), jnp.exp(total - column), jnp.exp(total)


def across_blocks(rows, blocks, i, columns):
    F, C, R, _ = blocks.shape
    group = max(1, 128 // R)
    parts = []
    for g in range(group):
        b = i * group + g
        parts.append(nt(rows, blocks[b // C, lax.rem(b, C), :, columns]))
    part = parts[0] if group == 1 else jnp.concatenate(parts, axis=1)
    return part.astype(BF)


class Mover:
    def __init__(self, pc, weights, layout, out, zs, zr, xs, xr, ls):
        self.pc, self.weights, self.layout, self.out = pc, weights, layout, out
        self.zs, self.zr, self.xs, self.xr, self.ls = zs, zr, xs, xr, ls
        self.zc, self.xc = {}, {}
        rows = out.shape[2]
        near = pc.near_first()
        part = rows // 4
        self.units = [(d, pl.ds(i * part, part)) for d in near for i in range(4)]
        self.later = list(enumerate(self.units))

    def columns(self, dst, part):
        at = 0
        for w, (share, n) in zip(self.weights, self.layout):
            start = pl.multiple_of((dst // share) * n, n)
            yield (
                w.at[part, pl.ds(start, n)],
                self.out.at[self.pc.f, self.pc.z, part, pl.ds(at, n)],
            )
            at += n

    def send(self, count=1):
        pc = self.pc
        for k, (d, part) in self.later[:count]:
            dst = pc.ahead(d)
            sems, peer = (self.zs.at[k], self.zr.at[k]), {"ctx": dst}
            for src, to in self.columns(dst, part):
                remote(src, to, *sems, peer).start()
            here = self.out.at[pc.f, pc.behind(d), part]
            self.zc[k] = remote(here, here, *sems, peer)
        del self.later[:count]

    def start(self, count):
        pc = self.pc
        whole = pl.ds(0, self.out.shape[2])
        own = len(self.units)
        for e in range(1, pc.F):
            sems, peer = (self.xs.at[own, e], self.xr.at[own, e]), {"fsdp": pc.fahead(e)}
            for src, to in self.columns(pc.z, whole):
                remote(src, to, *sems, peer).start()
            here = self.out.at[pc.fbehind(e), pc.z]
            self.xc[own, e] = remote(here, here, *sems, peer)
        for src, to in self.columns(pc.z, whole):
            pltpu.make_async_copy(src, to, self.ls).start()
        here = self.out.at[pc.f, pc.z]
        self.local = pltpu.make_async_copy(here, here, self.ls)
        self.send(count)

    def forward(self, k):
        pc = self.pc
        d, part = self.units[k]
        self.zc[k].wait_recv()
        self.send()
        here = self.out.at[pc.f, pc.behind(d), part]
        for e in range(1, pc.F):
            self.xc[k, e] = remote(
                here, here, self.xs.at[k, e], self.xr.at[k, e], {"fsdp": pc.fahead(e)}
            )
            self.xc[k, e].start()

    def arrived(self, k, e):
        self.xc[k, e].wait_recv()

    def sent(self):
        for cp in list(self.zc.values()) + list(self.xc.values()):
            cp.wait_send()


class Blocks:
    def __init__(self, pc, x, out, zs, zr, ys, yr, cs, cr, ls):
        self.pc, self.x, self.out = pc, x, out
        self.zs, self.zr, self.ys, self.yr, self.cs, self.cr, self.ls = zs, zr, ys, yr, cs, cr, ls
        self.zc, self.yc, self.cc = {}, {}, {}

    def start(self):
        pc = self.pc
        self.later = pc.near_first()
        self.local = pltpu.make_async_copy(self.x, self.out.at[pc.z], self.ls)
        self.local.start()
        self.send(3)

    def send(self, count=1):
        pc = self.pc
        for d in self.later[:count]:
            self.zc[d] = remote(
                self.x.at[pc.t],
                self.out.at[pc.z, pc.t],
                self.zs.at[d],
                self.zr.at[d],
                {"ctx": pc.ahead(d)},
            )
            self.zc[d].start()
        del self.later[:count]

    def forward(self, d):
        pc = self.pc
        self.zc[d].wait_recv()
        self.send()
        here = self.out.at[pc.behind(d), pc.t]
        self.yc[d] = remote(here, here, self.ys.at[d], self.yr.at[d], {"tp": pc.far})
        self.yc[d].start()
        self.cc[d, 0] = remote(here, here, self.cs.at[d, 0], self.cr.at[d, 0], {"tp": pc.near})
        self.cc[d, 0].start()

    def onward(self, d):
        pc = self.pc
        self.yc[d].wait_recv()
        here = self.out.at[pc.behind(d), pc.far]
        self.cc[d, 1] = remote(here, here, self.cs.at[d, 1], self.cr.at[d, 1], {"tp": pc.near})
        self.cc[d, 1].start()

    def finish(self):
        self.local.wait()
        for cp in list(self.zc.values()) + list(self.yc.values()):
            cp.wait_send()
        for cp in self.cc.values():
            cp.wait()


def mover_sems(F, C):
    return [sem(4 * C), sem(4 * C), sem(4 * C, F), sem(4 * C, F), pltpu.SemaphoreType.DMA]


def blocks_sems(C):
    return [sem(C), sem(C), sem(C), sem(C), sem(C, 2), sem(C, 2), pltpu.SemaphoreType.DMA]


def forward_kernel(dims, cfg, *refs):
    F, C, T = dims
    S, B, halves, HV, in_layout, rest_layout = cfg
    refs = list(refs)

    def take(n):
        out = refs[:n]
        del refs[:n]
        return out

    in_weights, rest_weights = take(5), take(3)
    norms, rates_in, tok, go = take(4), take(1)[0], *take(2)
    o_win, o_normed, o_proj, o_states, o_normal, o_gated, inv, old, vecs, mid, sn, full, ogo = take(13)
    otok, win, ovec, normed, acc, proj, states, state, normal, gated, stats, mytok, x = take(13)
    in_sems, rest_sems = take(5), take(5)
    tok_sems, go_sems = take(7), take(7)
    vzs, vzr, vxs, vxr, lzs, lzr, sts, strr, oses = take(9)
    vec, ld = take(2)
    n, m = len(chain_sems(C)), len(scatter_scratch(C, 8, 128))

    pc = Place(*dims)
    f, z, t = pc.f, pc.z, pc.t
    near = pc.near_first()
    L = S * B
    R = win.shape[2]
    W = F * C * R
    NI = proj.shape[1]
    N = proj.shape[0]
    units = C * S
    saved = []

    def save(src, dst):
        cp = pltpu.make_async_copy(src, dst, oses.at[len(saved)])
        cp.start()
        saved.append(cp)

    R = vec.shape[1]
    vec[...] = jnp.zeros_like(vec)
    for i, ref in enumerate(norms):
        vec[i : i + 1] = ref[...].astype(F32).reshape(1, R)
    ld[...] = jnp.zeros_like(ld)
    for s in range(S):
        for i in range(rates_in.shape[2]):
            ld[i : i + 1, s * B : (s + 1) * B] = as_row(rates_in[s, :, i : i + 1])
    pc.barrier(True, True, True)
    vz, vx, lz = {}, {}, {}
    for d in range(1, C):
        peer = {"ctx": pc.ahead(d)}
        vz[d] = remote(vec, ovec.at[f, z], vzs.at[d], vzr.at[d], peer)
        vz[d].start()
        lz[d] = remote(ld, old.at[z], lzs.at[d], lzr.at[d], peer)
        lz[d].start()
    ovec[f, z] = vec[...]
    old[z] = ld[...]

    def vec_across(d):
        for e in range(1, F):
            src = ovec.at[f, pc.behind(d)] if d else vec
            vx[d, e] = remote(
                src, ovec.at[f, pc.behind(d)], vxs.at[d, e], vxr.at[d, e], {"fsdp": pc.fahead(e)}
            )
            vx[d, e].start()

    vec_across(0)
    tk = Blocks(pc, tok, otok, *tok_sems)
    tk.start()
    wi = Mover(pc, in_weights, in_layout, win, *in_sems)
    wi.start(0)
    mine = pltpu.make_async_copy(tok.at[t], mytok, oses.at[15])
    mine.start()
    for d in range(1, C):
        vz[d].wait_recv()
        vec_across(d)
    for d in near:
        tk.forward(d)
        wi.send(4)
    wr = Mover(pc, rest_weights, rest_layout, full, *rest_sems)
    gk = Blocks(pc, go, ogo, *go_sems)
    for d in near:
        tk.onward(d)
    for cp in vx.values():
        cp.wait()
    for cp in vz.values():
        cp.wait_send()
    for b in range(F * C):
        vecs[:, b * R : (b + 1) * R] = ovec[b // C, b % C]
    tk.finish()
    gain1, bias1 = vecs[0:1], vecs[1:2]

    def norm_unit(i, carry):
        rows = otok[i // T, lax.rem(i, T)].astype(F32)
        q = rows.shape[0]
        value = layer_norm_rows(rows, gain1, bias1)
        for b in range(F * C):
            normed[b, pl.ds(pl.multiple_of(i * q, q), q)] = value[:, b * R : (b + 1) * R]
        return carry

    lax.fori_loop(0, C * T, norm_unit, 0)
    save(normed, o_normed)

    tile = min(256, N)

    def project(ff, c, first, last):
        def one(i, carry):
            rows = pl.ds(pl.multiple_of(i * tile, tile), tile)
            part = nn(normed[ff * C + c, rows], win[ff, c, :, :NI])
            if not first:
                part = part + acc[rows]
            if last:
                proj[rows] = part.astype(BF)
            else:
                acc[rows] = part
            return carry

        lax.fori_loop(0, N // tile, one, 0)

    wi.local.wait()
    own = len(wi.units)
    project(f, z, True, False)
    for e in range(1, F):
        wi.arrived(own, e)
        project(pc.fbehind(e), z, False, False)
    gk.start()
    for i, d in enumerate(near):
        keys = [k for k, (dd, _) in enumerate(wi.units) if dd == d]
        for k in keys:
            wi.forward(k)
        project(f, pc.behind(d), False, False)
        if i == 1:
            wr.start(8)
    for i, d in enumerate(near):
        keys = [k for k, (dd, _) in enumerate(wi.units) if dd == d]
        for e in range(1, F):
            for k in keys:
                wi.arrived(k, e)
            project(pc.fbehind(e), pc.behind(d), False, i == C - 2 and e == F - 1)
    gk.send(C)
    wr.send(4)
    save(proj, o_proj)
    save(win, o_win)

    for cp in lz.values():
        cp.wait()
    head = z // halves
    scale = float(KEY) ** (-0.5)
    state[...] = jnp.zeros_like(state)

    def retain(u, carry):
        c, s = u // S, lax.rem(u, S)
        rows = pl.ds(pl.multiple_of(u * B, B), B)
        rates = old[c, pl.ds(head, 1), pl.ds(pl.multiple_of(s * B, B), B)]
        table, growth, keeping, through = decays(rates)
        q, k, v = proj[rows, :KEY], proj[rows, KEY : 2 * KEY], proj[rows, 2 * KEY : 2 * KEY + HV]
        weights = (nt(q, k) * scale * table).astype(BF)
        before = state[s]
        states[u] = before.astype(BF)
        mixed = nn(weights, v) + nn((q.astype(F32) * growth).astype(BF), before.astype(BF))
        state[s] = through * before + tn((k.astype(F32) * keeping).astype(BF), v)
        normal[rows] = mixed
        mean = jnp.mean(mixed, axis=-1, keepdims=True)
        dev = mixed - mean
        stats[0, 0:1, rows] = as_row(mean)
        stats[0, 1:2, rows] = as_row(jnp.sum(dev * dev, axis=-1, keepdims=True))
        return carry

    stats[0] = jnp.zeros(stats.shape[1:], F32)
    lax.fori_loop(0, units, retain, 0)
    save(states, o_states)
    wr.send(4 * C)
    st = []
    place = lax.rem(z, halves)
    for j in range(1, halves):
        peer = {"ctx": z - place + lax.rem(place + j, halves)}
        cp = remote(stats.at[0], stats.at[j], sts.at[j], strr.at[j], peer)
        cp.start()
        st.append(cp)
    for cp in st:
        cp.wait()

    def finish_unit(u, carry):
        rows = pl.ds(pl.multiple_of(u * B, B), B)
        got = [(stats[j, 0:1, rows], stats[j, 1:2, rows]) for j in range(halves)]
        mean = sum(a for a, _ in got) / halves
        m2 = sum(b + HV * (a - mean) * (a - mean) for a, b in got)
        scaled = as_column(lax.rsqrt(m2 / HEAD_V + EPSILON))
        value = (normal[rows] - as_column(mean)) * scaled
        gate = proj[rows, 2 * KEY + HV :].astype(F32)
        normal[rows] = value
        inv[0:1, rows] = lax.rsqrt(m2 / HEAD_V + EPSILON)
        gated[rows] = (gate * jax.nn.sigmoid(gate) * value).astype(BF)
        return carry

    inv[...] = jnp.zeros_like(inv)
    lax.fori_loop(0, units, finish_unit, 0)
    save(normal, o_normal)
    save(gated, o_gated)

    p = otok
    Q = x.shape[0]
    cut, parts = halves_of(Q)
    scatters, gathers = [], []
    for h in range(parts):
        at = h * (n + m)
        slot = lambda c, i, h=h: sn.at[c, i, cut(h)]
        gathers.append(Chain(pc, x.at[cut(h)], slot, refs[at : at + n]))
        scatters.append(Scatter(pc, p, cut(h), refs[at + n : at + n + m]))
    for d in near + [0]:
        c = pc.ahead(d)
        mixed = gated[pl.ds(pl.multiple_of(c * L, L), L)]

        def one(b, carry):
            part = across_blocks(mixed, win, b, pl.ds(NI, HV))
            columns = pl.ds(pl.multiple_of(b * part.shape[1], 128), part.shape[1])
            for i in range(T):
                p[c, i, :, columns] = part[i * Q : (i + 1) * Q]
            return carry

        lax.fori_loop(0, W // max(R, 128), one, 0)
        scatters[0].begin(d)
    for d in near:
        gk.forward(d)
    pump = Pump(scatters, begun=C)
    pump.run(C)
    for k in range(8):
        wr.forward(k)
    for d in near:
        gk.onward(d)
    mine.wait()
    for h, rs in enumerate(scatters):
        pump.run(min(2, len(pump.units) - pump.done))
        part = cut(h)
        total = rs.result() + mytok[part].astype(F32)
        mid[part] = total
        x[part] = layer_norm_rows(total, vecs[2:3], vecs[3:4])
        gathers[h].start()
        if h == 0:
            pump.run(len(pump.units) - pump.done)
            for k in range(8, len(wr.units)):
                wr.forward(k)
    for d in range(1, C):
        for ga in gathers:
            ga.forward(d)
    for ga in gathers:
        for d in range(C):
            ga.onward(d)
    for job in scatters + gathers:
        job.finish()
    gk.finish()
    wi.sent()
    wr.local.wait()
    for k in range(len(wr.units) + 1):
        for e in range(1, F):
            wr.arrived(k, e)
    wr.sent()
    for cp in saved:
        cp.wait()


def norm_pull(values, gain, grad):
    center = values - jnp.mean(values, axis=-1, keepdims=True)
    spread = jnp.mean(center * center, axis=-1, keepdims=True)
    inv = lax.rsqrt(spread + EPSILON)
    xhat = center * inv
    g = grad * gain
    back = inv * (
        g - jnp.mean(g, axis=-1, keepdims=True) - xhat * jnp.mean(g * xhat, axis=-1, keepdims=True)
    )
    return (
        back,
        jnp.sum(grad * xhat, axis=0, keepdims=True),
        jnp.sum(grad, axis=0, keepdims=True),
    )


def gelu_parts(v):
    c = (2.0 / jnp.pi) ** 0.5
    t = jnp.tanh(c * (v + 0.044715 * v * v * v))
    return 0.5 * v * (1.0 + t), 0.5 * (1.0 + t) + 0.5 * v * (1.0 - t * t) * c * (
        1.0 + 3 * 0.044715 * v * v
    )


def middle_kernel(dims, cfg, *refs):
    F, C, T = dims
    S, B, U = cfg
    refs = list(refs)

    def take(n):
        out = refs[:n]
        del refs[:n]
        return out

    second, gout, wr, mid, allgo, vecs = take(6)
    gm, gb, down, dgain, dbias, msum = take(6)
    stile, gtile, sblk, gblk, acc, gates, hid, pg, pd, turned, turned2 = take(11)
    msend, mgot, mloc, x, go = take(5)
    ssem, gsem, gosem, dsem, msem, mxs, mxr = take(7)
    gsems = take(len(chain_sems(C)))

    pc = Place(*dims)
    f = pc.f
    R, N = wr.shape[2], hid.shape[0]
    Q = x.shape[0]
    W = F * C * R
    pc.barrier(True, True, True)
    mine = pltpu.make_async_copy(allgo.at[pc.t], go, gosem)
    mine.start()
    rg = Scatter(pc, pg, pl.ds(0, Q), refs)
    saved = []
    order = rg.order
    units = [(d, s) for d in order for s in range(S)]

    def rows_of(i):
        d, s = units[i]
        return pl.ds(pl.multiple_of((pc.ahead(d) * S + s) * B, B), B)

    def load(i):
        k = i % 2
        return (
            pltpu.make_async_copy(second.at[rows_of(i)], stile.at[k], ssem.at[k]),
            pltpu.make_async_copy(gout.at[rows_of(i)], gtile.at[k], gsem.at[k]),
        )

    for cp in load(0):
        cp.start()

    def unit(i):
        d, s = units[i]
        k = i % 2
        rows = rows_of(i)
        if i + 1 < len(units):
            for cp in load(i + 1):
                cp.start()
        for cp in load(i):
            cp.wait()
        for b in range(F * C):
            sblk[b, rows] = stile[k, :, b * R : (b + 1) * R]
            gblk[b, rows] = gtile[k, :, b * R : (b + 1) * R]
        acc[...] = jnp.zeros_like(acc)

        def forward(b, carry):
            w = wr[b // C, lax.rem(b, C)]
            acc[:, : 2 * U] += nn(sblk[b, rows], w[:, : 2 * U])
            acc[:, 2 * U :] += nn(gblk[b, rows], w[:, 2 * U :])
            return carry

        lax.fori_loop(0, F * C, forward, 0)
        gate = acc[:, :U].astype(BF).astype(F32)
        up = acc[:, U : 2 * U].astype(BF).astype(F32)
        grad = acc[:, 2 * U :]
        value, slope = gelu_parts(gate)
        hid[rows] = (value * up).astype(BF)
        gates[rows, :U] = (grad * up * slope).astype(BF)
        gates[rows, U:] = (grad * value).astype(BF)
        c = pc.ahead(d)
        pull, keep = gates[rows], hid[rows]

        def back(b, carry):
            for p, part in (
                (pg, across_blocks(pull, wr, b, pl.ds(0, 2 * U))),
                (pd, across_blocks(keep, wr, b, pl.ds(2 * U, U))),
            ):
                columns = pl.ds(pl.multiple_of(b * part.shape[1], 128), part.shape[1])
                for j in range(B // Q):
                    p[c, s * (B // Q) + j, :, columns] = part[j * Q : (j + 1) * Q]
            return carry

        lax.fori_loop(0, W // max(R, 128), back, 0)

    for i in range(len(units)):
        unit(i)
        if units[i][1] == S - 1:
            k = i // S
            rg.begin(order[k])
            c = pc.ahead(order[k])
            cp = pltpu.make_async_copy(pd.at[c], down.at[c], dsem.at[k])
            cp.start()
            saved.append(cp)
            if k >= 1:
                rg.far(order[k - 1])
            if k >= 2:
                rg.along(order[k - 2])
    rg.far(order[C - 1])
    for d in order[max(C - 2, 0) :]:
        rg.along(d)

    xc = {}

    def block(d, e):
        b = pc.fahead(e) * C + pc.ahead(d)
        turned[...] = jnp.transpose(sblk[b])
        turned2[...] = jnp.transpose(gblk[b])
        return nn(turned[...], gates[...]), nn(turned2[...], hid[...])

    for d in order:
        for e in range(1, F):
            c = pc.ahead(d)
            first, last = block(d, e)
            msend[e - 1, d, :, : 2 * U] = first.astype(BF)
            msend[e - 1, d, :, 2 * U :] = last.astype(BF)
            xc[d, e] = remote(
                msend.at[e - 1, d], mgot.at[e - 1, d], mxs.at[d, e], mxr.at[d, e], {"fsdp": pc.fahead(e)}
            )
            xc[d, e].start()

    mine.wait()
    back, dg, db = norm_pull(mid[...], vecs[2:3], rg.result())
    dgain[...] = dg
    dbias[...] = db
    grad_middle = go[...].astype(F32) + back
    gm[...] = grad_middle
    x[...] = grad_middle.astype(BF)
    ga = Chain(pc, x, lambda c, i: gb.at[c, i], gsems)
    ga.start()
    for h in range(1, min(3, C)):
        ga.forward(h)
    for k, d in enumerate(order):
        if k == 1:
            for h in range(3, C):
                ga.forward(h)
        first, last = block(d, 0)
        for e in range(1, F):
            xc[d, e].wait_recv()
            first = first + mgot[e - 1, d, :, : 2 * U].astype(F32)
            last = last + mgot[e - 1, d, :, 2 * U :].astype(F32)
        mloc[d, :, : 2 * U] = first.astype(BF)
        mloc[d, :, 2 * U :] = last.astype(BF)
        cp = pltpu.make_async_copy(mloc.at[d], msum.at[pc.ahead(d)], msem.at[d])
        cp.start()
        saved.append(cp)
    for h in range(C):
        ga.onward(h)
    for job in (rg, ga):
        job.finish()
    for cp in xc.values():
        cp.wait_send()
    for cp in saved:
        cp.wait()


def vector_stage(pc, v, vout, va, vb, vc, vd, vx, vz, ts, tr, vxs, vxr, vzs, vzr):
    F, C = pc.F, pc.C
    t0 = remote(v, vb, ts.at[0], tr.at[0], {"tp": pc.near})
    t0.start()
    yield
    t0.wait_recv()
    va[...] = v[...] + vb[...]
    t1 = remote(va, vc, ts.at[1], tr.at[1], {"tp": pc.far})
    t1.start()
    yield
    t1.wait_recv()
    vd[...] = va[...] + vc[...]
    vxc, vzc = {}, {}
    for e in range(1, F):
        vxc[e] = remote(
            vd.at[pc.fahead(e)], vx.at[e - 1], vxs.at[e], vxr.at[e], {"fsdp": pc.fahead(e)}
        )
        vxc[e].start()
    yield
    vs = vd[pc.f]
    for e in range(1, F):
        vxc[e].wait_recv()
        vs = vs + vx[e - 1]
    vz[0] = vs
    for d in range(1, C):
        vzc[d] = remote(
            vz.at[0, pc.ahead(d)], vz.at[1, d], vzs.at[d], vzr.at[d], {"ctx": pc.ahead(d)}
        )
        vzc[d].start()
    yield
    acc = vz[0, pc.z]
    for d in range(1, C):
        vzc[d].wait_recv()
        acc = acc + vz[1, d]
    vout[...] = acc
    for cp in [t0, t1] + list(vxc.values()) + list(vzc.values()):
        cp.wait_send()


def vector_scratch(F, C, R):
    full = pltpu.VMEM((F, C, 8, R), F32)
    return [
        full,
        full,
        full,
        full,
        full,
        pltpu.VMEM((F - 1, C, 8, R), F32),
        pltpu.VMEM((2, C, 8, R), F32),
        sem(2),
        sem(2),
        sem(F),
        sem(F),
        sem(C),
        sem(C),
    ]


def backward_kernel(dims, cfg, *refs):
    F, C, T = dims
    S, B, halves, HV = cfg
    refs = list(refs)

    def take(n):
        out = refs[:n]
        del refs[:n]
        return out

    branch, normed, win, proj, states, normal, inv, gated, old, vecs, gm, alltok, mlp, dg2, db2, down, mid = take(17)
    gt, result, gout, mout, vout = take(5)
    btile, ntile, cblock, turned, turned2, gn, gproj, later, stats, p = take(10)
    gsend, xbuf, zsnd, tok, y = take(5)
    bsem, nsem, sts, strr, mzs, mzr, xos, xor, xs, xr, zs, zr, keeps, toksem, lsem, msem = take(16)
    shares, shares2, vscratch = take(2), take(2), take(13)
    y2, lsem2, local = take(1)[0], take(1)[0], take(2)
    half = len(refs) // 2

    pc = Place(*dims)
    f, z, t = pc.f, pc.z, pc.t
    L = S * B
    R = win.shape[2]
    W = F * C * R
    N, NI = gproj.shape
    Q = y.shape[0]
    units = C * S
    pc.barrier(True, True, True)
    mine = pltpu.make_async_copy(alltok.at[t], tok, toksem)
    mine.start()

    moves = [pltpu.make_async_copy(mlp.at[z], mout.at[z], msem)]
    for d in pc.near_first():
        dst = pc.ahead(d)
        moves.append(remote(mlp.at[dst], mout.at[z], mzs.at[d], mzr.at[d], {"ctx": dst}))
    for cp in moves:
        cp.start()

    rd = Scatter(pc, down, pl.ds(0, Q), refs[half:], local)
    rd.start()

    def rows_in(u, slot):
        rows = pl.ds(pl.multiple_of(u * B, B), B)
        return pltpu.make_async_copy(branch.at[rows], btile.at[slot], bsem.at[slot])

    rows_in(0, 0).start()
    stats[0] = jnp.zeros(stats.shape[1:], F32)

    def pull_gate(u, carry):
        slot = lax.rem(u, 2)
        pl.when(u + 1 < units)(lambda: rows_in(u + 1, 1 - slot).start())
        rows_in(u, slot).wait()
        grad = None
        rows = pl.ds(pl.multiple_of(u * B, B), B)
        for b in range(F * C):
            piece = btile[slot, :, b * R : (b + 1) * R]
            cblock[b, rows] = piece
            part = nn(piece, win[b // C, b % C, :, NI:])
            grad = part if grad is None else grad + part
        gate = proj[rows, 2 * KEY + HV :].astype(F32)
        silu, dsilu = silu_parts(gate)
        value = normal[rows]
        gproj[rows, 2 * KEY + HV :] = (grad * value * dsilu).astype(BF)
        inner = grad * silu
        gn[rows] = inner
        stats[0, 0:1, rows] = as_row(jnp.sum(inner, axis=-1, keepdims=True))
        stats[0, 1:2, rows] = as_row(jnp.sum(inner * value, axis=-1, keepdims=True))
        return carry

    lax.fori_loop(0, units, pull_gate, 0)
    st = []
    place = lax.rem(z, halves)
    for j in range(1, halves):
        peer = {"ctx": z - place + lax.rem(place + j, halves)}
        cp = remote(stats.at[0], stats.at[j], sts.at[j], strr.at[j], peer)
        cp.start()
        st.append(cp)

    for d in rd.order:
        rd.far(d)

    far = sorted(range(1, C), key=lambda d: abs(d - C // 2))
    order = far + [0]
    blocks = [(d, e) for d in order for e in range(1, F)] + [(d, 0) for d in order]
    xo, xc, zc = {}, {}, {}

    def columns_in(i):
        d, e = blocks[i]
        b = pc.fahead(e) * C + pc.ahead(d)
        return b, pltpu.make_async_copy(normed.at[b], ntile.at[i % 2], nsem.at[i % 2])

    def start_columns(i):
        if i < len(blocks):
            columns_in(i)[1].start()

    tail = pl.ds(NI, HV)
    for d, e in blocks[: (F - 1) * C]:
        turned2[...] = jnp.transpose(cblock[pc.fahead(e) * C + pc.ahead(d)])
        gsend[e - 1, d, :, tail] = nn(turned2[...], gated[...]).astype(BF)
        xo[d, e] = remote(
            gsend.at[e - 1, d, :, tail],
            xbuf.at[e - 1, d, :, tail],
            xos.at[d, e],
            xor.at[d, e],
            {"fsdp": pc.fahead(e)},
        )
        xo[d, e].start()

    start_columns(0)
    for cp in st:
        cp.wait()

    head = z // halves
    scale = float(KEY) ** (-0.5)
    later[...] = jnp.zeros_like(later)

    def retain(i, carry):
        u = units - 1 - i
        c, s = u // S, lax.rem(u, S)
        rows = pl.ds(pl.multiple_of(u * B, B), B)
        rates = old[c, pl.ds(head, 1), pl.ds(pl.multiple_of(s * B, B), B)]
        table, growth, keeping, through = decays(rates)
        q, k, v = proj[rows, :KEY], proj[rows, KEY : 2 * KEY], proj[rows, 2 * KEY : 2 * KEY + HV]
        s1 = as_column(sum(stats[j, 0:1, rows] for j in range(halves)) / HEAD_V)
        s2 = as_column(sum(stats[j, 1:2, rows] for j in range(halves)) / HEAD_V)
        mix = (as_column(inv[0:1, rows]) * (gn[rows] - s1 - normal[rows] * s2)).astype(BF)
        weights = (nt(q, k) * scale * table).astype(BF)
        scores = (nt(mix, v) * scale * table).astype(BF)
        after = later[s]
        after_low = after.astype(BF)
        gq = nn(scores, k) + growth * nt(mix, states[u])
        gk = tn(scores, q) + keeping * nt(v, after_low)
        gv = tn(weights, mix) + nn((k.astype(F32) * keeping).astype(BF), after_low)
        later[s] = through * after + tn((q.astype(F32) * growth).astype(BF), mix)
        gproj[rows, :KEY] = gq.astype(BF)
        gproj[rows, KEY : 2 * KEY] = gk.astype(BF)
        gproj[rows, 2 * KEY : 2 * KEY + HV] = gv.astype(BF)
        return carry

    lax.fori_loop(0, units, retain, 0)

    rs = Scatter(pc, p, pl.ds(0, Q), refs[:half])
    for d in rs.order:
        c = pc.ahead(d)
        mixed = gproj[pl.ds(pl.multiple_of(c * L, L), L)]

        def one(b, carry, c=c, mixed=mixed):
            part = across_blocks(mixed, win, b, pl.ds(0, NI))
            columns = pl.ds(pl.multiple_of(b * part.shape[1], 128), part.shape[1])
            for i in range(T):
                p[c, i, :, columns] = part[i * Q : (i + 1) * Q]
            return carry

        lax.fori_loop(0, W // max(R, 128), one, 0)
        rs.begin(d)
    pump = Pump([rs], begun=C)
    pump.fill()
    for d in rd.order[:2]:
        rd.along(d)

    H = 2
    kept = []
    halfs = [pl.ds(h * (R // H), R // H) for h in range(H)]
    main = pl.ds(0, NI)

    def block(i):
        d, e = blocks[i]
        start_columns(i + 1)
        b, cp = columns_in(i)
        cp.wait()
        turned[...] = jnp.transpose(ntile[i % 2])
        if e == 0:
            turned2[...] = jnp.transpose(cblock[b])
            for g in range(1, F):
                xo[d, g].wait_recv()
                for h in range(H):
                    xc[d, g, h].wait_recv()

        def put(columns, part):
            if e:
                gsend[e - 1, d, :, columns] = part.astype(BF)
            else:
                for g in range(F - 1):
                    part = part + xbuf[g, d, :, columns].astype(F32)
                zsnd[d, :, columns] = part.astype(BF)

        def one(j, carry):
            columns = pl.ds(pl.multiple_of(j * 256, 256), 256)
            put(columns, nn(turned[...], gproj[:, columns]))
            return carry

        lax.fori_loop(0, NI // 256, one, 0)
        if e == 0:
            put(tail, nn(turned2[...], gated[...]))
        for h, part in enumerate(halfs):
            if e:
                xc[d, e, h] = remote(
                    gsend.at[e - 1, d, part, main],
                    xbuf.at[e - 1, d, part, main],
                    xs.at[d, e, h],
                    xr.at[d, e, h],
                    {"fsdp": pc.fahead(e)},
                )
                xc[d, e, h].start()
            elif d:
                zc[d, h] = remote(
                    zsnd.at[d, part], gout.at[z, part], zs.at[d, h], zr.at[d, h], {"ctx": pc.ahead(d)}
                )
                zc[d, h].start()
            else:
                cp = pltpu.make_async_copy(zsnd.at[0, part], gout.at[z, part], keeps.at[h])
                cp.start()
                kept.append(cp)

    sends = (F - 1) * C
    for i in range(sends):
        block(i)
        if i < len(rd.order[2:]):
            rd.along(rd.order[2 + i])
        if pump.done < len(pump.units):
            pump.run(1)
    for d in rd.order[2 + sends :]:
        rd.along(d)
    pump.run(len(pump.units) - pump.done)
    stages = []
    for i in range(sends, len(blocks)):
        block(i)
        if i == sends:
            mine.wait()
            back, dg, db = norm_pull(tok[...].astype(F32), vecs[0:1], rs.result())
            y[...] = (gm[...] + back).astype(BF)
            v = vscratch[0]
            for b in range(F * C):
                rows = [r[:, b * R : (b + 1) * R] for r in (dg, db)] + [
                    r[:, b * R : (b + 1) * R] for r in (dg2, db2)
                ]
                v[b // C, b % C] = jnp.concatenate(rows + [jnp.zeros((4, R), F32)], axis=0)
            y2[...] = (mid[...] + rd.result()).astype(BF)
            stages = [
                share_stage(pc, y, gt, lsem, shares),
                share_stage(pc, y2, result, lsem2, shares2),
                vector_stage(pc, v, vout, *vscratch[1:]),
            ]
        for stage in stages:
            next(stage, None)
    for stage in stages:
        drain(stage)
    rs.finish()
    rd.finish()
    for cp in kept:
        cp.wait()
    for cp in zc.values():
        cp.wait()
    for cp in list(xc.values()) + list(xo.values()):
        cp.wait_send()
    for cp in moves:
        cp.wait()


def assemble_kernel(halves, key, hv, a, m, x0, x1, vec, q, k, v, g, o, fg, fu, fd, y0, y1, *vecs):
    c = pl.program_id(1)
    y0[...] = x0[...]
    y1[...] = x1[...]
    for i, ref in enumerate(vecs):
        ref[...] = vec[i]
    first = lax.rem(c, halves) == 0
    for i, ref in enumerate((q, k)):
        x = a[0, :, i * key : (i + 1) * key].astype(F32)

        @pl.when(first)
        def _(ref=ref, x=x):
            ref[...] = x

        @pl.when(jnp.logical_not(first))
        def _(ref=ref, x=x):
            ref[...] += x

    v[...] = a[0, :, 2 * key : 2 * key + hv].astype(F32)
    g[...] = a[0, :, 2 * key + hv : 2 * key + 2 * hv].astype(F32)
    o[...] = a[0, :, 2 * key + 2 * hv :].astype(F32)
    u = fg.shape[1]
    for i, ref in enumerate((fg, fu, fd)):
        ref[...] = m[0, :, i * u : (i + 1) * u].astype(F32)


def params(cid):
    return pltpu.CompilerParams(collective_id=cid, has_side_effects=True)


def shards(
    dims,
    tokens,
    log_decay,
    w_query,
    w_key,
    w_value,
    w_gate,
    w_out,
    norm1_gain,
    norm1_bias,
    w_ffgate,
    w_ffup,
    w_down,
    norm2_gain,
    norm2_bias,
    grad_out,
):
    F, C, T = dims
    S, B, W = tokens.shape
    L = S * B
    Q = L // T
    N = C * L
    R = w_query.shape[0]
    heads = log_decay.shape[2]
    halves = C // heads
    HV = HEAD_V // halves
    U = w_ffgate.shape[1] // C
    z = lax.axis_index("ctx")
    t = lax.axis_index("tp")
    scale = float(KEY) ** (-0.5)

    f = lax.axis_index("fsdp")

    def hop(x, axis, d):
        n = lax.axis_size(axis)
        return lax.ppermute(x, axis, [(i, (i + d) % n) for i in range(n)])

    def at(x, i, n):
        return lax.dynamic_index_in_dim(x, lax.rem(i, n), 0, False)

    NI, NR = 2 * KEY + 2 * HV, 3 * U
    NO = NI + HV
    norms = (norm1_gain, norm1_bias, norm2_gain, norm2_bias)
    tok = tokens.reshape(T, Q, W)
    go = grad_out.reshape(T, Q, W)
    sds = jax.ShapeDtypeStruct
    cfg = (
        S,
        B,
        halves,
        HV,
        ((halves, KEY), (halves, KEY), (1, HV), (1, HV), (1, HV)),
        ((1, U), (1, U), (1, U)),
    )
    owin, normed, proj, states, normal, gated, inv, old, vecs, mid, sn, full, ogo = pl.pallas_call(
        functools.partial(forward_kernel, dims, cfg),
        out_shape=(
            sds((F, C, R, NO), BF),
            sds((F * C, N, R), BF),
            sds((N, NI), BF),
            sds((C * S, KEY, HV), BF),
            sds((N, HV), F32),
            sds((N, HV), BF),
            sds((8, N), F32),
            sds((C, 8, L), F32),
            sds((8, W), F32),
            sds((Q, W), F32),
            sds((C, T, Q, W), BF),
            sds((F, C, R, NR), BF),
            sds((C, T, Q, W), BF),
        ),
        in_specs=[ANY] * 8 + [VMEM] * 5 + [ANY, ANY],
        out_specs=[ANY] * 6 + [VMEM] * 4 + [ANY] * 3,
        scratch_shapes=[
            pltpu.VMEM((C, T, Q, W), BF),
            pltpu.VMEM((F, C, R, NO), BF),
            pltpu.VMEM((F, C, 8, R), F32),
            pltpu.VMEM((F * C, N, R), BF),
            pltpu.VMEM((N, NI), F32),
            pltpu.VMEM((N, NI), BF),
            pltpu.VMEM((C * S, KEY, HV), BF),
            pltpu.VMEM((S, KEY, HV), F32),
            pltpu.VMEM((N, HV), F32),
            pltpu.VMEM((N, HV), BF),
            pltpu.VMEM((halves, 8, N), F32),
            pltpu.VMEM((Q, W), BF),
            pltpu.VMEM((Q, W), BF),
        ]
        + mover_sems(F, C) * 2
        + blocks_sems(C) * 2
        + [sem(C), sem(C), sem(C, F), sem(C, F), sem(C), sem(C), sem(halves), sem(halves), sem(16)]
        + [pltpu.VMEM((8, R), F32), pltpu.VMEM((8, L), F32)]
        + (chain_sems(C) + scatter_scratch(C, Q // PARTS, W)) * PARTS,
        compiler_params=params(1),
        name="k_forward",
    )(w_query, w_key, w_value, w_gate, w_out, w_ffgate, w_ffup, w_down, *norms, log_decay, tok, go)
    gm, gb, down, dgain2, dbias2, mlp_sum = pl.pallas_call(
        functools.partial(middle_kernel, dims, (S, B, U)),
        out_shape=(
            sds((Q, W), F32),
            sds((C, T, Q, W), BF),
            sds((C, T, Q, W), BF),
            sds((1, W), F32),
            sds((1, W), F32),
            sds((C, R, NR), BF),
        ),
        in_specs=[ANY, ANY, VMEM, VMEM, ANY, VMEM],
        out_specs=[VMEM, ANY, ANY, VMEM, VMEM, ANY],
        scratch_shapes=[
            pltpu.VMEM((2, B, W), BF),
            pltpu.VMEM((2, B, W), BF),
            pltpu.VMEM((F * C, N, R), BF),
            pltpu.VMEM((F * C, N, R), BF),
            pltpu.VMEM((B, 3 * U), F32),
            pltpu.VMEM((N, 2 * U), BF),
            pltpu.VMEM((N, U), BF),
            pltpu.VMEM((C, T, Q, W), BF),
            pltpu.VMEM((C, T, Q, W), BF),
            pltpu.VMEM((R, N), BF),
            pltpu.VMEM((R, N), BF),
            pltpu.VMEM((F - 1, C, R, NR), BF),
            pltpu.VMEM((F - 1, C, R, NR), BF),
            pltpu.VMEM((C, R, NR), BF),
            pltpu.VMEM((Q, W), BF),
            pltpu.VMEM((Q, W), BF),
            sem(2),
            sem(2),
            pltpu.SemaphoreType.DMA,
            sem(C),
            sem(C),
            sem(C, F),
            sem(C, F),
        ]
        + chain_sems(C)
        + scatter_scratch(C, Q, W),
        compiler_params=params(3),
        name="k_middle",
    )(sn.reshape(N, W), ogo.reshape(N, W), full, mid, go, vecs)

    branch = gb.reshape(N, W)
    H = 2
    gt, out, gsum, mlp_grads, vsum = pl.pallas_call(
        functools.partial(backward_kernel, dims, (S, B, halves, HV)),
        out_shape=(
            sds((T, Q, W), BF),
            sds((T, Q, W), BF),
            sds((C, R, NO), BF),
            sds((C, R, NR), BF),
            sds((8, R), F32),
        ),
        in_specs=[ANY, ANY] + [VMEM] * 9 + [ANY, ANY, VMEM, VMEM, ANY, VMEM],
        out_specs=[ANY] * 4 + [VMEM],
        scratch_shapes=[
            pltpu.VMEM((2, B, W), BF),
            pltpu.VMEM((2, N, R), BF),
            pltpu.VMEM((F * C, N, R), BF),
            pltpu.VMEM((R, N), BF),
            pltpu.VMEM((R, N), BF),
            pltpu.VMEM((N, HV), F32),
            pltpu.VMEM((N, NI), BF),
            pltpu.VMEM((S, KEY, HV), F32),
            pltpu.VMEM((halves, 8, N), F32),
            pltpu.VMEM((C, T, Q, W), BF),
            pltpu.VMEM((F - 1, C, R, NO), BF),
            pltpu.VMEM((F - 1, C, R, NO), BF),
            pltpu.VMEM((C, R, NO), BF),
            pltpu.VMEM((Q, W), BF),
            pltpu.VMEM((Q, W), BF),
            sem(2),
            sem(2),
            sem(halves),
            sem(halves),
            sem(C),
            sem(C),
            sem(C, F),
            sem(C, F),
            sem(C, F, H),
            sem(C, F, H),
            sem(C, H),
            sem(C, H),
            sem(H),
        ]
        + [pltpu.SemaphoreType.DMA] * 3
        + share_sems() * 2
        + vector_scratch(F, C, R)
        + [pltpu.VMEM((Q, W), BF), pltpu.SemaphoreType.DMA]
        + local_scratch(C, Q, W)
        + scatter_scratch(C, Q, W) * 2,
        compiler_params=params(4),
        name="k_backward",
    )(
        branch,
        normed,
        owin,
        proj,
        states,
        normal,
        inv,
        gated,
        old,
        vecs,
        gm,
        tok,
        mlp_sum,
        dgain2,
        dbias2,
        down,
        mid,
    )

    steps = 2

    def quarter(n):
        return pl.BlockSpec((R // steps, n), lambda h, c: (h, c))

    def piece(n):
        return pl.BlockSpec((1, R // steps, n), lambda h, c: (c, h, 0))

    rows = pl.BlockSpec((L // (steps * C), W), lambda h, c: (h * C + c, 0))
    per_head = pl.BlockSpec((R // steps, KEY), lambda h, c: (h, c // halves))
    gq, gk, gv, gg, gw, gfg, gfu, gfd, output, grad_tokens, *gvecs = pl.pallas_call(
        functools.partial(assemble_kernel, halves, KEY, HV),
        out_shape=[sds((R, heads * KEY), F32)] * 2
        + [sds((R, C * HV), F32)] * 3
        + [sds((R, C * U), F32)] * 3
        + [sds((L, W), BF)] * 2
        + [sds((R,), F32)] * 4,
        grid=(steps, C),
        in_specs=[piece(NO), piece(NR), rows, rows, pl.BlockSpec((8, R), lambda h, c: (0, 0))],
        out_specs=[per_head, per_head]
        + [quarter(HV)] * 3
        + [quarter(U)] * 3
        + [rows, rows]
        + [pl.BlockSpec((R,), lambda h, c: (0,))] * 4,
        name="k_assemble",
    )(gsum, mlp_grads, out.reshape(L, W), gt.reshape(L, W), vsum)
    return (
        output.reshape(tokens.shape),
        grad_tokens.reshape(tokens.shape),
        gq,
        gk,
        gv,
        gg,
        gw,
        gvecs[0],
        gvecs[1],
        gfg,
        gfu,
        gfd,
        gvecs[2],
        gvecs[3],
    )


def solution(mesh):
    dims = (mesh.shape["fsdp"], mesh.shape["ctx"], mesh.shape["tp"])
    rows, vec = P(("fsdp", "ctx"), "tp"), P(("fsdp", "ctx"))
    acts = P("fsdp", "ctx", None)
    return jax.shard_map(
        functools.partial(shards, dims),
        mesh=mesh,
        in_specs=(acts, P("fsdp", "ctx", "tp"), rows, rows, rows, rows, rows, vec, vec, rows, rows, rows, vec, vec, acts),
        out_specs=(acts, acts, rows, rows, rows, rows, rows, vec, vec, rows, rows, rows, vec, vec),
        check_vma=False,
    )
```

```python
import functools

import jax
import jax.numpy as jnp
from jax import lax
from jax.experimental import pallas as pl
from jax.experimental.pallas import tpu as pltpu
from jax.sharding import PartitionSpec as P

KEY = 256
HEAD_V = 512
EPSILON = 1e-05
MESH = pl.DeviceIdType.MESH
ANY = pl.BlockSpec(memory_space=pl.ANY)
VMEM = pl.BlockSpec(memory_space=pltpu.VMEM)
BF = jnp.bfloat16
F32 = jnp.float32


def dot(a, b, dims):
    return lax.dot_general(a, b, (dims, ((), ())), preferred_element_type=F32)


def nn(a, b):
    return dot(a, b, ((1,), (0,)))


def nt(a, b):
    return dot(a, b, ((1,), (1,)))


def tn(a, b):
    return dot(a, b, ((0,), (0,)))


class Place:
    def __init__(self, F, C, T):
        self.F, self.C, self.T = F, C, T
        self.f = lax.axis_index("fsdp")
        self.z = lax.axis_index("ctx")
        self.t = lax.axis_index("tp")
        self.lo = lax.rem(self.t, 2)
        self.hi = self.t // 2
        self.near = self.t + 1 - 2 * self.lo
        self.far = lax.rem(self.t + 2, 4)

    def near_first(self):
        return [1] + ([self.C - 1] if self.C > 2 else []) + list(range(2, self.C - 1))

    def ahead(self, d):
        return lax.rem(self.z + d, self.C)

    def behind(self, d):
        return lax.rem(self.z + self.C - d, self.C)

    def fahead(self, d):
        return lax.rem(self.f + d, self.F)

    def fbehind(self, d):
        return lax.rem(self.f + self.F - d, self.F)

    def barrier(self, ctx=True, fsdp=False, tp=True):
        sem = pltpu.get_barrier_semaphore()
        peers = []
        if tp:
            peers += [{"tp": self.near}, {"tp": self.far}]
        if fsdp:
            peers += [{"fsdp": self.fahead(d)} for d in range(1, self.F)]
        if ctx:
            peers += [{"ctx": self.ahead(d)} for d in range(1, self.C)]
        for peer in peers:
            pl.semaphore_signal(sem, inc=1, device_id=peer, device_id_type=MESH)
        pl.semaphore_wait(sem, len(peers))


def remote(src, dst, ssem, rsem, peer):
    return pltpu.make_async_remote_copy(
        src_ref=src, dst_ref=dst, send_sem=ssem, recv_sem=rsem, device_id=peer, device_id_type=MESH
    )


def sem(*shape):
    return pltpu.SemaphoreType.DMA(shape)


def chain_sems(C):
    return [sem(2, C), sem(2, C), sem(2, C), sem(2, C), sem(2, C, 2), sem(2, C, 2), pltpu.SemaphoreType.DMA]


class Chain:
    def __init__(self, pc, x, slot, sems, own=None):
        self.pc, self.x, self.slot, self.block = pc, x, slot, own
        self.zs, self.zr, self.ys, self.yr, self.cs, self.cr, self.ls = sems

    def came(self, s, h):
        z = self.pc.z
        return (z >= h, z - h) if s == 0 else (z + h <= self.pc.C - 1, z + h)

    def goes(self, s, h):
        pc = self.pc
        if s == 0:
            return jnp.logical_and(pc.z >= h - 1, pc.z < pc.C - 1)
        return jnp.logical_and(pc.z + h <= pc.C, pc.z > 0)

    def hop(self, s, h, c):
        z = self.pc.z
        here = self.slot(c, self.pc.t)
        src = self.x if h == 1 else here
        return remote(src, here, self.zs.at[s, h], self.zr.at[s, h], {"ctx": z + 1 if s == 0 else z - 1})

    def to_far(self, s, h, c):
        here = self.slot(c, self.pc.t)
        src = here if h else self.x
        return remote(src, here, self.ys.at[s, h], self.yr.at[s, h], {"tp": self.pc.far})

    def to_near(self, s, h, c):
        here = self.slot(c, self.pc.t)
        src = here if h else self.x
        return remote(src, here, self.cs.at[s, h, 0], self.cr.at[s, h, 0], {"tp": self.pc.near})

    def spread(self, s, h, c):
        self.to_far(s, h, c).start()
        self.to_near(s, h, c).start()

    def again(self, s, h, c):
        there = self.slot(c, self.pc.far)
        return remote(there, there, self.cs.at[s, h, 1], self.cr.at[s, h, 1], {"tp": self.pc.near})

    def start(self):
        pc = self.pc
        for s in range(2):
            pl.when(self.goes(s, 1))(lambda s=s: self.hop(s, 1, pc.z).start())
        src, dst = self.block or (self.x, self.slot(pc.z, pc.t))
        self.local = pltpu.make_async_copy(src, dst, self.ls)
        self.local.start()
        if not self.block:
            self.spread(0, 0, pc.z)

    def forward(self, h):
        for s in range(2):
            ok, c = self.came(s, h)

            @pl.when(ok)
            def _(s=s, c=c):
                self.hop(s, h, c).wait_recv()
                if h + 1 < self.pc.C:
                    pl.when(self.goes(s, h + 1))(lambda: self.hop(s, h + 1, c).start())
                self.spread(s, h, c)

    def onward(self, h):
        if h == 0:
            if not self.block:
                self.to_far(0, 0, self.pc.z).wait_recv()
                self.again(0, 0, self.pc.z).start()
            return
        for s in range(2):
            ok, c = self.came(s, h)

            @pl.when(ok)
            def _(s=s, c=c):
                self.to_far(s, h, c).wait_recv()
                self.again(s, h, c).start()

    def settle(self, s, h, c):
        self.to_far(s, h, c).wait_send()
        self.to_near(s, h, c).wait()
        self.again(s, h, c).wait()

    def finish(self):
        pc = self.pc
        self.local.wait()
        if not self.block:
            self.settle(0, 0, pc.z)
        for h in range(1, pc.C):
            for s in range(2):
                ok, c = self.came(s, h)
                first = pc.z - h + 1 if s == 0 else pc.z + h - 1
                pl.when(self.goes(s, h))(lambda s=s, c=first: self.hop(s, h, c).wait_send())
                pl.when(ok)(lambda s=s, c=c: self.settle(s, h, c))


def share_sems():
    return [sem(3), sem(3)]


def share_stage(pc, x, out, lsem, sems):
    ss, rs = sems
    t = pc.t
    local = pltpu.make_async_copy(x, out.at[t], lsem)
    local.start()
    a = remote(x, out.at[t], ss.at[0], rs.at[0], {"tp": pc.far})
    a.start()
    b = remote(x, out.at[t], ss.at[1], rs.at[1], {"tp": pc.near})
    b.start()
    yield
    a.wait_recv()
    src = out.at[pc.far]
    c = remote(src, src, ss.at[2], rs.at[2], {"tp": pc.near})
    c.start()
    yield
    local.wait()
    a.wait_send()
    b.wait()
    c.wait()


def scatter_scratch(C, Q, W):
    return [
        pltpu.VMEM((C, 2, Q, W), BF),
        pltpu.VMEM((C, Q, W), BF),
        pltpu.VMEM((C, Q, W), BF),
        pltpu.VMEM((C, Q, W), BF),
        pltpu.VMEM((C, Q, W), BF),
        sem(C, 2),
        sem(C, 2),
        sem(C),
        sem(C),
        sem(C),
        sem(C),
    ]


def local_scratch(C, Q, W):
    return [pltpu.VMEM((C, 2, Q, W), BF), sem(C, 2)]


class Scatter:
    def __init__(self, pc, p, rows, scratch, local=None):
        self.pc, self.p, self.rows, self.local = pc, p, rows, local
        (self.buf1, self.snd2, self.buf2, self.snd3, self.buf3) = scratch[:5]
        self.s1, self.r1, self.s2, self.r2, self.s3, self.r3 = scratch[5:]
        self.order = pc.near_first() + [0]
        self.lc, self.c1, self.c2, self.c3 = {}, {}, {}, {}

    def side(self, j):
        return 1 - self.pc.hi if j == 0 else self.pc.hi

    def begin(self, d):
        pc, p, rows = self.pc, self.p, self.rows
        c = pc.ahead(d)
        for j in range(2):
            self.c1[d, j] = remote(
                p.at[c, self.side(j) * 2 + 1 - pc.lo, rows],
                self.buf1.at[d, j],
                self.s1.at[d, j],
                self.r1.at[d, j],
                {"tp": pc.near},
            )
            self.c1[d, j].start()
            if self.local:
                self.lc[d, j] = pltpu.make_async_copy(
                    p.at[c, self.side(j) * 2 + pc.lo, rows],
                    self.local[0].at[d, j],
                    self.local[1].at[d, j],
                )
                self.lc[d, j].start()

    def start(self):
        for d in self.order:
            self.begin(d)

    def own(self, d, j):
        self.c1[d, j].wait_recv()
        if self.local:
            self.lc[d, j].wait()
            here = self.local[0][d, j]
        else:
            here = self.p[self.pc.ahead(d), self.side(j) * 2 + self.pc.lo, self.rows]
        return here.astype(F32) + self.buf1[d, j].astype(F32)

    def far(self, d):
        self.snd2[d] = self.own(d, 0).astype(BF)
        self.c2[d] = remote(
            self.snd2.at[d], self.buf2.at[d], self.s2.at[d], self.r2.at[d], {"tp": self.pc.far}
        )
        self.c2[d].start()

    def along(self, d):
        part = self.own(d, 1)
        self.c2[d].wait_recv()
        part = part + self.buf2[d].astype(F32)
        if d:
            self.snd3[d] = part.astype(BF)
            self.c3[d] = remote(
                self.snd3.at[d],
                self.buf3.at[d],
                self.s3.at[d],
                self.r3.at[d],
                {"ctx": self.pc.ahead(d)},
            )
            self.c3[d].start()
        else:
            self.total = part

    def result(self):
        total = self.total
        for d in range(1, self.pc.C):
            self.c3[d].wait_recv()
            total = total + self.buf3[d].astype(F32)
        return total

    def finish(self):
        for copies in (self.c1, self.c2, self.c3):
            for cp in copies.values():
                cp.wait_send()


def drain(stage):
    for _ in stage:
        pass


class Pump:
    def __init__(self, scatters, begun=0, window=3):
        self.units = [(rs, d) for rs in scatters for d in rs.order]
        self.window, self.begun, self.sent, self.done = window, begun, 0, 0

    def fill(self):
        while self.begun < min(len(self.units), self.done + 2 * self.window):
            rs, d = self.units[self.begun]
            rs.begin(d)
            self.begun += 1
        while self.sent < min(len(self.units), self.done + self.window):
            rs, d = self.units[self.sent]
            rs.far(d)
            self.sent += 1

    def run(self, count):
        for _ in range(count):
            self.fill()
            rs, d = self.units[self.done]
            rs.along(d)
            self.done += 1
        self.fill()


def silu_parts(g):
    s = jax.nn.sigmoid(g)
    return g * s, s * (1.0 + g * (1.0 - s))


PARTS = 2


def halves_of(rows):
    n = rows // PARTS
    return (lambda h: pl.ds(h * n, n)), PARTS


def layer_norm_rows(values, gain, bias):
    center = values - jnp.mean(values, axis=-1, keepdims=True)
    spread = jnp.mean(center * center, axis=-1, keepdims=True)
    return (center * lax.rsqrt(spread + EPSILON) * gain + bias).astype(BF)


def eye_of(n):
    return lax.broadcasted_iota(jnp.int32, (n, n), 0) == lax.broadcasted_iota(jnp.int32, (n, n), 1)


def as_row(column):
    return jnp.sum(jnp.where(eye_of(column.shape[0]), column, 0.0), axis=0, keepdims=True)


def as_column(row):
    return jnp.sum(jnp.where(eye_of(row.shape[1]), row, 0.0), axis=1, keepdims=True)


def decays(rates):
    B = rates.shape[1]
    causal = lax.broadcasted_iota(jnp.int32, (B, B), 0) >= lax.broadcasted_iota(jnp.int32, (B, B), 1)
    column = jnp.sum(jnp.where(causal, rates, 0.0), axis=1, keepdims=True)
    row = as_row(column)
    table = jnp.where(causal, jnp.exp(jnp.minimum(column - row, 0.0)), 0.0)
    total = column[B - 1 :]
    return table, jnp.exp(column), jnp.exp(total - column), jnp.exp(total)


def across_blocks(rows, blocks, i, columns):
    F, C, R, _ = blocks.shape
    group = max(1, 128 // R)
    parts = []
    for g in range(group):
        b = i * group + g
        parts.append(nt(rows, blocks[b // C, lax.rem(b, C), :, columns]))
    part = parts[0] if group == 1 else jnp.concatenate(parts, axis=1)
    return part.astype(BF)


class Mover:
    def __init__(self, pc, weights, layout, out, zs, zr, xs, xr, ls):
        self.pc, self.weights, self.layout, self.out = pc, weights, layout, out
        self.zs, self.zr, self.xs, self.xr, self.ls = zs, zr, xs, xr, ls
        self.zc, self.xc = {}, {}
        rows = out.shape[2]
        near = pc.near_first()
        part = rows // 4
        self.units = [(d, pl.ds(i * part, part)) for d in near for i in range(4)]
        self.later = list(enumerate(self.units))

    def columns(self, dst, part):
        at = 0
        for w, (share, n) in zip(self.weights, self.layout):
            start = pl.multiple_of((dst // share) * n, n)
            yield (
                w.at[part, pl.ds(start, n)],
                self.out.at[self.pc.f, self.pc.z, part, pl.ds(at, n)],
            )
            at += n

    def send(self, count=1):
        pc = self.pc
        for k, (d, part) in self.later[:count]:
            dst = pc.ahead(d)
            sems, peer = (self.zs.at[k], self.zr.at[k]), {"ctx": dst}
            for src, to in self.columns(dst, part):
                remote(src, to, *sems, peer).start()
            here = self.out.at[pc.f, pc.behind(d), part]
            self.zc[k] = remote(here, here, *sems, peer)
        del self.later[:count]

    def start(self, count):
        pc = self.pc
        whole = pl.ds(0, self.out.shape[2])
        own = len(self.units)
        for e in range(1, pc.F):
            sems, peer = (self.xs.at[own, e], self.xr.at[own, e]), {"fsdp": pc.fahead(e)}
            for src, to in self.columns(pc.z, whole):
                remote(src, to, *sems, peer).start()
            here = self.out.at[pc.fbehind(e), pc.z]
            self.xc[own, e] = remote(here, here, *sems, peer)
        for src, to in self.columns(pc.z, whole):
            pltpu.make_async_copy(src, to, self.ls).start()
        here = self.out.at[pc.f, pc.z]
        self.local = pltpu.make_async_copy(here, here, self.ls)
        self.send(count)

    def forward(self, k):
        pc = self.pc
        d, part = self.units[k]
        self.zc[k].wait_recv()
        self.send()
        here = self.out.at[pc.f, pc.behind(d), part]
        for e in range(1, pc.F):
            self.xc[k, e] = remote(
                here, here, self.xs.at[k, e], self.xr.at[k, e], {"fsdp": pc.fahead(e)}
            )
            self.xc[k, e].start()

    def arrived(self, k, e):
        self.xc[k, e].wait_recv()

    def sent(self):
        for cp in list(self.zc.values()) + list(self.xc.values()):
            cp.wait_send()


class Blocks:
    def __init__(self, pc, x, out, zs, zr, ys, yr, cs, cr, ls):
        self.pc, self.x, self.out = pc, x, out
        self.zs, self.zr, self.ys, self.yr, self.cs, self.cr, self.ls = zs, zr, ys, yr, cs, cr, ls
        self.zc, self.yc, self.cc = {}, {}, {}

    def start(self):
        pc = self.pc
        self.later = pc.near_first()
        self.local = pltpu.make_async_copy(self.x, self.out.at[pc.z], self.ls)
        self.local.start()
        self.send(3)

    def send(self, count=1):
        pc = self.pc
        for d in self.later[:count]:
            self.zc[d] = remote(
                self.x.at[pc.t],
                self.out.at[pc.z, pc.t],
                self.zs.at[d],
                self.zr.at[d],
                {"ctx": pc.ahead(d)},
            )
            self.zc[d].start()
        del self.later[:count]

    def forward(self, d):
        pc = self.pc
        self.zc[d].wait_recv()
        self.send()
        here = self.out.at[pc.behind(d), pc.t]
        self.yc[d] = remote(here, here, self.ys.at[d], self.yr.at[d], {"tp": pc.far})
        self.yc[d].start()
        self.cc[d, 0] = remote(here, here, self.cs.at[d, 0], self.cr.at[d, 0], {"tp": pc.near})
        self.cc[d, 0].start()

    def onward(self, d):
        pc = self.pc
        self.yc[d].wait_recv()
        here = self.out.at[pc.behind(d), pc.far]
        self.cc[d, 1] = remote(here, here, self.cs.at[d, 1], self.cr.at[d, 1], {"tp": pc.near})
        self.cc[d, 1].start()

    def finish(self):
        self.local.wait()
        for cp in list(self.zc.values()) + list(self.yc.values()):
            cp.wait_send()
        for cp in self.cc.values():
            cp.wait()


def mover_sems(F, C):
    return [sem(4 * C), sem(4 * C), sem(4 * C, F), sem(4 * C, F), pltpu.SemaphoreType.DMA]


def blocks_sems(C):
    return [sem(C), sem(C), sem(C), sem(C), sem(C, 2), sem(C, 2), pltpu.SemaphoreType.DMA]


def forward_kernel(dims, cfg, *refs):
    F, C, T = dims
    S, B, halves, HV, in_layout, rest_layout = cfg
    refs = list(refs)

    def take(n):
        out = refs[:n]
        del refs[:n]
        return out

    in_weights, rest_weights = take(5), take(3)
    norms, rates_in, tok, go = take(4), take(1)[0], *take(2)
    o_win, o_normed, o_proj, o_states, o_normal, o_gated, inv, old, vecs, mid, sn, full, ogo = take(13)
    otok, win, ovec, normed, acc, proj, states, state, normal, gated, stats, mytok, x = take(13)
    in_sems, rest_sems = take(5), take(5)
    tok_sems, go_sems = take(7), take(7)
    vzs, vzr, vxs, vxr, lzs, lzr, sts, strr, oses = take(9)
    vec, ld = take(2)
    n, m = len(chain_sems(C)), len(scatter_scratch(C, 8, 128))

    pc = Place(*dims)
    f, z, t = pc.f, pc.z, pc.t
    near = pc.near_first()
    L = S * B
    R = win.shape[2]
    W = F * C * R
    NI = proj.shape[1]
    N = proj.shape[0]
    units = C * S
    saved = []

    def save(src, dst):
        cp = pltpu.make_async_copy(src, dst, oses.at[len(saved)])
        cp.start()
        saved.append(cp)

    R = vec.shape[1]
    vec[...] = jnp.zeros_like(vec)
    for i, ref in enumerate(norms):
        vec[i : i + 1] = ref[...].astype(F32).reshape(1, R)
    ld[...] = jnp.zeros_like(ld)
    for s in range(S):
        for i in range(rates_in.shape[2]):
            ld[i : i + 1, s * B : (s + 1) * B] = as_row(rates_in[s, :, i : i + 1])
    pc.barrier(True, True, True)
    vz, vx, lz = {}, {}, {}
    for d in range(1, C):
        peer = {"ctx": pc.ahead(d)}
        vz[d] = remote(vec, ovec.at[f, z], vzs.at[d], vzr.at[d], peer)
        vz[d].start()
        lz[d] = remote(ld, old.at[z], lzs.at[d], lzr.at[d], peer)
        lz[d].start()
    ovec[f, z] = vec[...]
    old[z] = ld[...]

    def vec_across(d):
        for e in range(1, F):
            src = ovec.at[f, pc.behind(d)] if d else vec
            vx[d, e] = remote(
                src, ovec.at[f, pc.behind(d)], vxs.at[d, e], vxr.at[d, e], {"fsdp": pc.fahead(e)}
            )
            vx[d, e].start()

    vec_across(0)
    tk = Blocks(pc, tok, otok, *tok_sems)
    tk.start()
    wi = Mover(pc, in_weights, in_layout, win, *in_sems)
    wi.start(0)
    mine = pltpu.make_async_copy(tok.at[t], mytok, oses.at[15])
    mine.start()
    for d in range(1, C):
        vz[d].wait_recv()
        vec_across(d)
    for d in near:
        tk.forward(d)
        wi.send(4)
    wr = Mover(pc, rest_weights, rest_layout, full, *rest_sems)
    gk = Blocks(pc, go, ogo, *go_sems)
    for d in near:
        tk.onward(d)
    for cp in vx.values():
        cp.wait()
    for cp in vz.values():
        cp.wait_send()
    for b in range(F * C):
        vecs[:, b * R : (b + 1) * R] = ovec[b // C, b % C]
    tk.finish()
    gain1, bias1 = vecs[0:1], vecs[1:2]

    def norm_unit(i, carry):
        rows = otok[i // T, lax.rem(i, T)].astype(F32)
        q = rows.shape[0]
        value = layer_norm_rows(rows, gain1, bias1)
        for b in range(F * C):
            normed[b, pl.ds(pl.multiple_of(i * q, q), q)] = value[:, b * R : (b + 1) * R]
        return carry

    lax.fori_loop(0, C * T, norm_unit, 0)
    save(normed, o_normed)

    tile = min(256, N)

    def project(ff, c, first, last):
        def one(i, carry):
            rows = pl.ds(pl.multiple_of(i * tile, tile), tile)
            part = nn(normed[ff * C + c, rows], win[ff, c, :, :NI])
            if not first:
                part = part + acc[rows]
            if last:
                proj[rows] = part.astype(BF)
            else:
                acc[rows] = part
            return carry

        lax.fori_loop(0, N // tile, one, 0)

    wi.local.wait()
    own = len(wi.units)
    project(f, z, True, False)
    for e in range(1, F):
        wi.arrived(own, e)
        project(pc.fbehind(e), z, False, False)
    gk.start()
    for i, d in enumerate(near):
        keys = [k for k, (dd, _) in enumerate(wi.units) if dd == d]
        for k in keys:
            wi.forward(k)
        project(f, pc.behind(d), False, False)
        if i == 1:
            wr.start(8)
    for i, d in enumerate(near):
        keys = [k for k, (dd, _) in enumerate(wi.units) if dd == d]
        for e in range(1, F):
            for k in keys:
                wi.arrived(k, e)
            project(pc.fbehind(e), pc.behind(d), False, i == C - 2 and e == F - 1)
    gk.send(C)
    wr.send(4)
    save(proj, o_proj)
    save(win, o_win)

    for cp in lz.values():
        cp.wait()
    head = z // halves
    scale = float(KEY) ** (-0.5)
    state[...] = jnp.zeros_like(state)

    def retain(u, carry):
        c, s = u // S, lax.rem(u, S)
        rows = pl.ds(pl.multiple_of(u * B, B), B)
        rates = old[c, pl.ds(head, 1), pl.ds(pl.multiple_of(s * B, B), B)]
        table, growth, keeping, through = decays(rates)
        q, k, v = proj[rows, :KEY], proj[rows, KEY : 2 * KEY], proj[rows, 2 * KEY : 2 * KEY + HV]
        weights = (nt(q, k) * scale * table).astype(BF)
        before = state[s]
        states[u] = before.astype(BF)
        mixed = nn(weights, v) + nn((q.astype(F32) * growth).astype(BF), before.astype(BF))
        state[s] = through * before + tn((k.astype(F32) * keeping).astype(BF), v)
        normal[rows] = mixed
        mean = jnp.mean(mixed, axis=-1, keepdims=True)
        dev = mixed - mean
        stats[0, 0:1, rows] = as_row(mean)
        stats[0, 1:2, rows] = as_row(jnp.sum(dev * dev, axis=-1, keepdims=True))
        return carry

    stats[0] = jnp.zeros(stats.shape[1:], F32)
    lax.fori_loop(0, units, retain, 0)
    save(states, o_states)
    wr.send(4 * C)
    st = []
    place = lax.rem(z, halves)
    for j in range(1, halves):
        peer = {"ctx": z - place + lax.rem(place + j, halves)}
        cp = remote(stats.at[0], stats.at[j], sts.at[j], strr.at[j], peer)
        cp.start()
        st.append(cp)
    for cp in st:
        cp.wait()

    def finish_unit(u, carry):
        rows = pl.ds(pl.multiple_of(u * B, B), B)
        got = [(stats[j, 0:1, rows], stats[j, 1:2, rows]) for j in range(halves)]
        mean = sum(a for a, _ in got) / halves
        m2 = sum(b + HV * (a - mean) * (a - mean) for a, b in got)
        scaled = as_column(lax.rsqrt(m2 / HEAD_V + EPSILON))
        value = (normal[rows] - as_column(mean)) * scaled
        gate = proj[rows, 2 * KEY + HV :].astype(F32)
        normal[rows] = value
        inv[0:1, rows] = lax.rsqrt(m2 / HEAD_V + EPSILON)
        gated[rows] = (gate * jax.nn.sigmoid(gate) * value).astype(BF)
        return carry

    inv[...] = jnp.zeros_like(inv)
    lax.fori_loop(0, units, finish_unit, 0)
    save(normal, o_normal)
    save(gated, o_gated)

    p = otok
    Q = x.shape[0]
    cut, parts = halves_of(Q)
    scatters, gathers = [], []
    for h in range(parts):
        at = h * (n + m)
        slot = lambda c, i, h=h: sn.at[c, i, cut(h)]
        gathers.append(Chain(pc, x.at[cut(h)], slot, refs[at : at + n]))
        scatters.append(Scatter(pc, p, cut(h), refs[at + n : at + n + m]))
    for d in near + [0]:
        c = pc.ahead(d)
        mixed = gated[pl.ds(pl.multiple_of(c * L, L), L)]

        def one(b, carry):
            part = across_blocks(mixed, win, b, pl.ds(NI, HV))
            columns = pl.ds(pl.multiple_of(b * part.shape[1], 128), part.shape[1])
            for i in range(T):
                p[c, i, :, columns] = part[i * Q : (i + 1) * Q]
            return carry

        lax.fori_loop(0, W // max(R, 128), one, 0)
        scatters[0].begin(d)
    for d in near:
        gk.forward(d)
    pump = Pump(scatters, begun=C)
    pump.run(C)
    for k in range(8):
        wr.forward(k)
    for d in near:
        gk.onward(d)
    mine.wait()
    for h, rs in enumerate(scatters):
        pump.run(min(2, len(pump.units) - pump.done))
        part = cut(h)
        total = rs.result() + mytok[part].astype(F32)
        mid[part] = total
        x[part] = layer_norm_rows(total, vecs[2:3], vecs[3:4])
        gathers[h].start()
        if h == 0:
            pump.run(len(pump.units) - pump.done)
            for k in range(8, len(wr.units)):
                wr.forward(k)
    for d in range(1, C):
        for ga in gathers:
            ga.forward(d)
    for ga in gathers:
        for d in range(C):
            ga.onward(d)
    for job in scatters + gathers:
        job.finish()
    gk.finish()
    wi.sent()
    wr.local.wait()
    for k in range(len(wr.units) + 1):
        for e in range(1, F):
            wr.arrived(k, e)
    wr.sent()
    for cp in saved:
        cp.wait()


def norm_pull(values, gain, grad):
    center = values - jnp.mean(values, axis=-1, keepdims=True)
    spread = jnp.mean(center * center, axis=-1, keepdims=True)
    inv = lax.rsqrt(spread + EPSILON)
    xhat = center * inv
    g = grad * gain
    back = inv * (
        g - jnp.mean(g, axis=-1, keepdims=True) - xhat * jnp.mean(g * xhat, axis=-1, keepdims=True)
    )
    return (
        back,
        jnp.sum(grad * xhat, axis=0, keepdims=True),
        jnp.sum(grad, axis=0, keepdims=True),
    )


def gelu_parts(v):
    c = (2.0 / jnp.pi) ** 0.5
    t = jnp.tanh(c * (v + 0.044715 * v * v * v))
    return 0.5 * v * (1.0 + t), 0.5 * (1.0 + t) + 0.5 * v * (1.0 - t * t) * c * (
        1.0 + 3 * 0.044715 * v * v
    )


def middle_kernel(dims, cfg, *refs):
    F, C, T = dims
    S, B, U = cfg
    refs = list(refs)

    def take(n):
        out = refs[:n]
        del refs[:n]
        return out

    second, gout, wr, mid, allgo, vecs = take(6)
    gm, gb, down, dgain, dbias, msum = take(6)
    stile, gtile, sblk, gblk, acc, gates, hid, pg, pd, turned, turned2 = take(11)
    msend, mgot, mloc, x, go = take(5)
    ssem, gsem, gosem, dsem, msem, mxs, mxr = take(7)
    gsems = take(len(chain_sems(C)))

    pc = Place(*dims)
    f = pc.f
    R, N = wr.shape[2], hid.shape[0]
    Q = x.shape[0]
    W = F * C * R
    pc.barrier(True, True, True)
    mine = pltpu.make_async_copy(allgo.at[pc.t], go, gosem)
    mine.start()
    rg = Scatter(pc, pg, pl.ds(0, Q), refs)
    saved = []
    order = rg.order
    units = [(d, s) for d in order for s in range(S)]

    def rows_of(i):
        d, s = units[i]
        return pl.ds(pl.multiple_of((pc.ahead(d) * S + s) * B, B), B)

    def load(i):
        k = i % 2
        return (
            pltpu.make_async_copy(second.at[rows_of(i)], stile.at[k], ssem.at[k]),
            pltpu.make_async_copy(gout.at[rows_of(i)], gtile.at[k], gsem.at[k]),
        )

    for cp in load(0):
        cp.start()

    def unit(i):
        d, s = units[i]
        k = i % 2
        rows = rows_of(i)
        if i + 1 < len(units):
            for cp in load(i + 1):
                cp.start()
        for cp in load(i):
            cp.wait()
        for b in range(F * C):
            sblk[b, rows] = stile[k, :, b * R : (b + 1) * R]
            gblk[b, rows] = gtile[k, :, b * R : (b + 1) * R]
        acc[...] = jnp.zeros_like(acc)

        def forward(b, carry):
            w = wr[b // C, lax.rem(b, C)]
            acc[:, : 2 * U] += nn(sblk[b, rows], w[:, : 2 * U])
            acc[:, 2 * U :] += nn(gblk[b, rows], w[:, 2 * U :])
            return carry

        lax.fori_loop(0, F * C, forward, 0)
        gate = acc[:, :U].astype(BF).astype(F32)
        up = acc[:, U : 2 * U].astype(BF).astype(F32)
        grad = acc[:, 2 * U :]
        value, slope = gelu_parts(gate)
        hid[rows] = (value * up).astype(BF)
        gates[rows, :U] = (grad * up * slope).astype(BF)
        gates[rows, U:] = (grad * value).astype(BF)
        c = pc.ahead(d)
        pull, keep = gates[rows], hid[rows]

        def back(b, carry):
            for p, part in (
                (pg, across_blocks(pull, wr, b, pl.ds(0, 2 * U))),
                (pd, across_blocks(keep, wr, b, pl.ds(2 * U, U))),
            ):
                columns = pl.ds(pl.multiple_of(b * part.shape[1], 128), part.shape[1])
                for j in range(B // Q):
                    p[c, s * (B // Q) + j, :, columns] = part[j * Q : (j + 1) * Q]
            return carry

        lax.fori_loop(0, W // max(R, 128), back, 0)

    for i in range(len(units)):
        unit(i)
        if units[i][1] == S - 1:
            k = i // S
            rg.begin(order[k])
            c = pc.ahead(order[k])
            cp = pltpu.make_async_copy(pd.at[c], down.at[c], dsem.at[k])
            cp.start()
            saved.append(cp)
            if k >= 1:
                rg.far(order[k - 1])
            if k >= 2:
                rg.along(order[k - 2])
    rg.far(order[C - 1])
    for d in order[max(C - 2, 0) :]:
        rg.along(d)

    xc = {}

    def block(d, e):
        b = pc.fahead(e) * C + pc.ahead(d)
        turned[...] = jnp.transpose(sblk[b])
        turned2[...] = jnp.transpose(gblk[b])
        return nn(turned[...], gates[...]), nn(turned2[...], hid[...])

    for d in order:
        for e in range(1, F):
            c = pc.ahead(d)
            first, last = block(d, e)
            msend[e - 1, d, :, : 2 * U] = first.astype(BF)
            msend[e - 1, d, :, 2 * U :] = last.astype(BF)
            xc[d, e] = remote(
                msend.at[e - 1, d], mgot.at[e - 1, d], mxs.at[d, e], mxr.at[d, e], {"fsdp": pc.fahead(e)}
            )
            xc[d, e].start()

    mine.wait()
    back, dg, db = norm_pull(mid[...], vecs[2:3], rg.result())
    dgain[...] = dg
    dbias[...] = db
    grad_middle = go[...].astype(F32) + back
    gm[...] = grad_middle
    x[...] = grad_middle.astype(BF)
    ga = Chain(pc, x, lambda c, i: gb.at[c, i], gsems)
    ga.start()
    for h in range(1, min(3, C)):
        ga.forward(h)
    for k, d in enumerate(order):
        if k == 1:
            for h in range(3, C):
                ga.forward(h)
        first, last = block(d, 0)
        for e in range(1, F):
            xc[d, e].wait_recv()
            first = first + mgot[e - 1, d, :, : 2 * U].astype(F32)
            last = last + mgot[e - 1, d, :, 2 * U :].astype(F32)
        mloc[d, :, : 2 * U] = first.astype(BF)
        mloc[d, :, 2 * U :] = last.astype(BF)
        cp = pltpu.make_async_copy(mloc.at[d], msum.at[pc.ahead(d)], msem.at[d])
        cp.start()
        saved.append(cp)
    for h in range(C):
        ga.onward(h)
    for job in (rg, ga):
        job.finish()
    for cp in xc.values():
        cp.wait_send()
    for cp in saved:
        cp.wait()


def vector_stage(pc, v, vout, va, vb, vc, vd, vx, vz, ts, tr, vxs, vxr, vzs, vzr):
    F, C = pc.F, pc.C
    t0 = remote(v, vb, ts.at[0], tr.at[0], {"tp": pc.near})
    t0.start()
    yield
    t0.wait_recv()
    va[...] = v[...] + vb[...]
    t1 = remote(va, vc, ts.at[1], tr.at[1], {"tp": pc.far})
    t1.start()
    yield
    t1.wait_recv()
    vd[...] = va[...] + vc[...]
    vxc, vzc = {}, {}
    for e in range(1, F):
        vxc[e] = remote(
            vd.at[pc.fahead(e)], vx.at[e - 1], vxs.at[e], vxr.at[e], {"fsdp": pc.fahead(e)}
        )
        vxc[e].start()
    yield
    vs = vd[pc.f]
    for e in range(1, F):
        vxc[e].wait_recv()
        vs = vs + vx[e - 1]
    vz[0] = vs
    for d in range(1, C):
        vzc[d] = remote(
            vz.at[0, pc.ahead(d)], vz.at[1, d], vzs.at[d], vzr.at[d], {"ctx": pc.ahead(d)}
        )
        vzc[d].start()
    yield
    acc = vz[0, pc.z]
    for d in range(1, C):
        vzc[d].wait_recv()
        acc = acc + vz[1, d]
    vout[...] = acc
    for cp in [t0, t1] + list(vxc.values()) + list(vzc.values()):
        cp.wait_send()


def vector_scratch(F, C, R):
    full = pltpu.VMEM((F, C, 8, R), F32)
    return [
        full,
        full,
        full,
        full,
        full,
        pltpu.VMEM((F - 1, C, 8, R), F32),
        pltpu.VMEM((2, C, 8, R), F32),
        sem(2),
        sem(2),
        sem(F),
        sem(F),
        sem(C),
        sem(C),
    ]


def backward_kernel(dims, cfg, *refs):
    F, C, T = dims
    S, B, halves, HV = cfg
    refs = list(refs)

    def take(n):
        out = refs[:n]
        del refs[:n]
        return out

    branch, normed, win, proj, states, normal, inv, gated, old, vecs, gm, alltok, mlp, dg2, db2, down, mid = take(17)
    gt, result, gout, mout, vout = take(5)
    btile, ntile, cblock, turned, turned2, gn, gproj, later, stats, p = take(10)
    gsend, xbuf, zsnd, tok, y = take(5)
    bsem, nsem, sts, strr, mzs, mzr, xos, xor, xs, xr, zs, zr, keeps, toksem, lsem, msem = take(16)
    shares, shares2, vscratch = take(2), take(2), take(13)
    y2, lsem2, local = take(1)[0], take(1)[0], take(2)
    half = len(refs) // 2

    pc = Place(*dims)
    f, z, t = pc.f, pc.z, pc.t
    L = S * B
    R = win.shape[2]
    W = F * C * R
    N, NI = gproj.shape
    Q = y.shape[0]
    units = C * S
    pc.barrier(True, True, True)
    mine = pltpu.make_async_copy(alltok.at[t], tok, toksem)
    mine.start()

    moves = [pltpu.make_async_copy(mlp.at[z], mout.at[z], msem)]
    for d in pc.near_first():
        dst = pc.ahead(d)
        moves.append(remote(mlp.at[dst], mout.at[z], mzs.at[d], mzr.at[d], {"ctx": dst}))
    for cp in moves:
        cp.start()

    rd = Scatter(pc, down, pl.ds(0, Q), refs[half:], local)
    rd.start()

    def rows_in(u, slot):
        rows = pl.ds(pl.multiple_of(u * B, B), B)
        return pltpu.make_async_copy(branch.at[rows], btile.at[slot], bsem.at[slot])

    rows_in(0, 0).start()
    stats[0] = jnp.zeros(stats.shape[1:], F32)

    def pull_gate(u, carry):
        slot = lax.rem(u, 2)
        pl.when(u + 1 < units)(lambda: rows_in(u + 1, 1 - slot).start())
        rows_in(u, slot).wait()
        grad = None
        rows = pl.ds(pl.multiple_of(u * B, B), B)
        for b in range(F * C):
            piece = btile[slot, :, b * R : (b + 1) * R]
            cblock[b, rows] = piece
            part = nn(piece, win[b // C, b % C, :, NI:])
            grad = part if grad is None else grad + part
        gate = proj[rows, 2 * KEY + HV :].astype(F32)
        silu, dsilu = silu_parts(gate)
        value = normal[rows]
        gproj[rows, 2 * KEY + HV :] = (grad * value * dsilu).astype(BF)
        inner = grad * silu
        gn[rows] = inner
        stats[0, 0:1, rows] = as_row(jnp.sum(inner, axis=-1, keepdims=True))
        stats[0, 1:2, rows] = as_row(jnp.sum(inner * value, axis=-1, keepdims=True))
        return carry

    lax.fori_loop(0, units, pull_gate, 0)
    st = []
    place = lax.rem(z, halves)
    for j in range(1, halves):
        peer = {"ctx": z - place + lax.rem(place + j, halves)}
        cp = remote(stats.at[0], stats.at[j], sts.at[j], strr.at[j], peer)
        cp.start()
        st.append(cp)

    for d in rd.order:
        rd.far(d)

    far = sorted(range(1, C), key=lambda d: abs(d - C // 2))
    order = far + [0]
    blocks = [(d, e) for d in order for e in range(1, F)] + [(d, 0) for d in order]
    xo, xc, zc = {}, {}, {}

    def columns_in(i):
        d, e = blocks[i]
        b = pc.fahead(e) * C + pc.ahead(d)
        return b, pltpu.make_async_copy(normed.at[b], ntile.at[i % 2], nsem.at[i % 2])

    def start_columns(i):
        if i < len(blocks):
            columns_in(i)[1].start()

    tail = pl.ds(NI, HV)
    for d, e in blocks[: (F - 1) * C]:
        turned2[...] = jnp.transpose(cblock[pc.fahead(e) * C + pc.ahead(d)])
        gsend[e - 1, d, :, tail] = nn(turned2[...], gated[...]).astype(BF)
        xo[d, e] = remote(
            gsend.at[e - 1, d, :, tail],
            xbuf.at[e - 1, d, :, tail],
            xos.at[d, e],
            xor.at[d, e],
            {"fsdp": pc.fahead(e)},
        )
        xo[d, e].start()

    start_columns(0)
    for cp in st:
        cp.wait()

    head = z // halves
    scale = float(KEY) ** (-0.5)
    later[...] = jnp.zeros_like(later)

    def retain(i, carry):
        u = units - 1 - i
        c, s = u // S, lax.rem(u, S)
        rows = pl.ds(pl.multiple_of(u * B, B), B)
        rates = old[c, pl.ds(head, 1), pl.ds(pl.multiple_of(s * B, B), B)]
        table, growth, keeping, through = decays(rates)
        q, k, v = proj[rows, :KEY], proj[rows, KEY : 2 * KEY], proj[rows, 2 * KEY : 2 * KEY + HV]
        s1 = as_column(sum(stats[j, 0:1, rows] for j in range(halves)) / HEAD_V)
        s2 = as_column(sum(stats[j, 1:2, rows] for j in range(halves)) / HEAD_V)
        mix = (as_column(inv[0:1, rows]) * (gn[rows] - s1 - normal[rows] * s2)).astype(BF)
        weights = (nt(q, k) * scale * table).astype(BF)
        scores = (nt(mix, v) * scale * table).astype(BF)
        after = later[s]
        after_low = after.astype(BF)
        gq = nn(scores, k) + growth * nt(mix, states[u])
        gk = tn(scores, q) + keeping * nt(v, after_low)
        gv = tn(weights, mix) + nn((k.astype(F32) * keeping).astype(BF), after_low)
        later[s] = through * after + tn((q.astype(F32) * growth).astype(BF), mix)
        gproj[rows, :KEY] = gq.astype(BF)
        gproj[rows, KEY : 2 * KEY] = gk.astype(BF)
        gproj[rows, 2 * KEY : 2 * KEY + HV] = gv.astype(BF)
        return carry

    lax.fori_loop(0, units, retain, 0)

    rs = Scatter(pc, p, pl.ds(0, Q), refs[:half])
    for d in rs.order:
        c = pc.ahead(d)
        mixed = gproj[pl.ds(pl.multiple_of(c * L, L), L)]

        def one(b, carry, c=c, mixed=mixed):
            part = across_blocks(mixed, win, b, pl.ds(0, NI))
            columns = pl.ds(pl.multiple_of(b * part.shape[1], 128), part.shape[1])
            for i in range(T):
                p[c, i, :, columns] = part[i * Q : (i + 1) * Q]
            return carry

        lax.fori_loop(0, W // max(R, 128), one, 0)
        rs.begin(d)
    pump = Pump([rs], begun=C)
    pump.fill()
    for d in rd.order[:2]:
        rd.along(d)

    H = 2
    kept = []
    halfs = [pl.ds(h * (R // H), R // H) for h in range(H)]
    main = pl.ds(0, NI)

    def block(i):
        d, e = blocks[i]
        start_columns(i + 1)
        b, cp = columns_in(i)
        cp.wait()
        turned[...] = jnp.transpose(ntile[i % 2])
        if e == 0:
            turned2[...] = jnp.transpose(cblock[b])
            for g in range(1, F):
                xo[d, g].wait_recv()
                for h in range(H):
                    xc[d, g, h].wait_recv()

        def put(columns, part):
            if e:
                gsend[e - 1, d, :, columns] = part.astype(BF)
            else:
                for g in range(F - 1):
                    part = part + xbuf[g, d, :, columns].astype(F32)
                zsnd[d, :, columns] = part.astype(BF)

        def one(j, carry):
            columns = pl.ds(pl.multiple_of(j * 256, 256), 256)
            put(columns, nn(turned[...], gproj[:, columns]))
            return carry

        lax.fori_loop(0, NI // 256, one, 0)
        if e == 0:
            put(tail, nn(turned2[...], gated[...]))
        for h, part in enumerate(halfs):
            if e:
                xc[d, e, h] = remote(
                    gsend.at[e - 1, d, part, main],
                    xbuf.at[e - 1, d, part, main],
                    xs.at[d, e, h],
                    xr.at[d, e, h],
                    {"fsdp": pc.fahead(e)},
                )
                xc[d, e, h].start()
            elif d:
                zc[d, h] = remote(
                    zsnd.at[d, part], gout.at[z, part], zs.at[d, h], zr.at[d, h], {"ctx": pc.ahead(d)}
                )
                zc[d, h].start()
            else:
                cp = pltpu.make_async_copy(zsnd.at[0, part], gout.at[z, part], keeps.at[h])
                cp.start()
                kept.append(cp)

    sends = (F - 1) * C
    for i in range(sends):
        block(i)
        if i < len(rd.order[2:]):
            rd.along(rd.order[2 + i])
        if pump.done < len(pump.units):
            pump.run(1)
    for d in rd.order[2 + sends :]:
        rd.along(d)
    pump.run(len(pump.units) - pump.done)
    stages = []
    for i in range(sends, len(blocks)):
        block(i)
        if i == sends:
            mine.wait()
            back, dg, db = norm_pull(tok[...].astype(F32), vecs[0:1], rs.result())
            y[...] = (gm[...] + back).astype(BF)
            v = vscratch[0]
            for b in range(F * C):
                rows = [r[:, b * R : (b + 1) * R] for r in (dg, db)] + [
                    r[:, b * R : (b + 1) * R] for r in (dg2, db2)
                ]
                v[b // C, b % C] = jnp.concatenate(rows + [jnp.zeros((4, R), F32)], axis=0)
            y2[...] = (mid[...] + rd.result()).astype(BF)
            stages = [
                share_stage(pc, y, gt, lsem, shares),
                share_stage(pc, y2, result, lsem2, shares2),
                vector_stage(pc, v, vout, *vscratch[1:]),
            ]
        for stage in stages:
            next(stage, None)
    for stage in stages:
        drain(stage)
    rs.finish()
    rd.finish()
    for cp in kept:
        cp.wait()
    for cp in zc.values():
        cp.wait()
    for cp in list(xc.values()) + list(xo.values()):
        cp.wait_send()
    for cp in moves:
        cp.wait()


def assemble_kernel(halves, key, hv, a, m, x0, x1, vec, q, k, v, g, o, fg, fu, fd, y0, y1, *vecs):
    c = pl.program_id(1)
    y0[...] = x0[...]
    y1[...] = x1[...]
    for i, ref in enumerate(vecs):
        ref[...] = vec[i]
    first = lax.rem(c, halves) == 0
    for i, ref in enumerate((q, k)):
        x = a[0, :, i * key : (i + 1) * key].astype(F32)

        @pl.when(first)
        def _(ref=ref, x=x):
            ref[...] = x

        @pl.when(jnp.logical_not(first))
        def _(ref=ref, x=x):
            ref[...] += x

    v[...] = a[0, :, 2 * key : 2 * key + hv].astype(F32)
    g[...] = a[0, :, 2 * key + hv : 2 * key + 2 * hv].astype(F32)
    o[...] = a[0, :, 2 * key + 2 * hv :].astype(F32)
    u = fg.shape[1]
    for i, ref in enumerate((fg, fu, fd)):
        ref[...] = m[0, :, i * u : (i + 1) * u].astype(F32)


def params(cid):
    return pltpu.CompilerParams(collective_id=cid, has_side_effects=True)


def shards(
    dims,
    tokens,
    log_decay,
    w_query,
    w_key,
    w_value,
    w_gate,
    w_out,
    norm1_gain,
    norm1_bias,
    w_ffgate,
    w_ffup,
    w_down,
    norm2_gain,
    norm2_bias,
    grad_out,
):
    F, C, T = dims
    S, B, W = tokens.shape
    L = S * B
    Q = L // T
    N = C * L
    R = w_query.shape[0]
    heads = log_decay.shape[2]
    halves = C // heads
    HV = HEAD_V // halves
    U = w_ffgate.shape[1] // C
    z = lax.axis_index("ctx")
    t = lax.axis_index("tp")
    scale = float(KEY) ** (-0.5)

    f = lax.axis_index("fsdp")

    def hop(x, axis, d):
        n = lax.axis_size(axis)
        return lax.ppermute(x, axis, [(i, (i + d) % n) for i in range(n)])

    def at(x, i, n):
        return lax.dynamic_index_in_dim(x, lax.rem(i, n), 0, False)

    NI, NR = 2 * KEY + 2 * HV, 3 * U
    NO = NI + HV
    norms = (norm1_gain, norm1_bias, norm2_gain, norm2_bias)
    tok = tokens.reshape(T, Q, W)
    go = grad_out.reshape(T, Q, W)
    sds = jax.ShapeDtypeStruct
    cfg = (
        S,
        B,
        halves,
        HV,
        ((halves, KEY), (halves, KEY), (1, HV), (1, HV), (1, HV)),
        ((1, U), (1, U), (1, U)),
    )
    owin, normed, proj, states, normal, gated, inv, old, vecs, mid, sn, full, ogo = pl.pallas_call(
        functools.partial(forward_kernel, dims, cfg),
        out_shape=(
            sds((F, C, R, NO), BF),
            sds((F * C, N, R), BF),
            sds((N, NI), BF),
            sds((C * S, KEY, HV), BF),
            sds((N, HV), F32),
            sds((N, HV), BF),
            sds((8, N), F32),
            sds((C, 8, L), F32),
            sds((8, W), F32),
            sds((Q, W), F32),
            sds((C, T, Q, W), BF),
            sds((F, C, R, NR), BF),
            sds((C, T, Q, W), BF),
        ),
        in_specs=[ANY] * 8 + [VMEM] * 5 + [ANY, ANY],
        out_specs=[ANY] * 6 + [VMEM] * 4 + [ANY] * 3,
        scratch_shapes=[
            pltpu.VMEM((C, T, Q, W), BF),
            pltpu.VMEM((F, C, R, NO), BF),
            pltpu.VMEM((F, C, 8, R), F32),
            pltpu.VMEM((F * C, N, R), BF),
            pltpu.VMEM((N, NI), F32),
            pltpu.VMEM((N, NI), BF),
            pltpu.VMEM((C * S, KEY, HV), BF),
            pltpu.VMEM((S, KEY, HV), F32),
            pltpu.VMEM((N, HV), F32),
            pltpu.VMEM((N, HV), BF),
            pltpu.VMEM((halves, 8, N), F32),
            pltpu.VMEM((Q, W), BF),
            pltpu.VMEM((Q, W), BF),
        ]
        + mover_sems(F, C) * 2
        + blocks_sems(C) * 2
        + [sem(C), sem(C), sem(C, F), sem(C, F), sem(C), sem(C), sem(halves), sem(halves), sem(16)]
        + [pltpu.VMEM((8, R), F32), pltpu.VMEM((8, L), F32)]
        + (chain_sems(C) + scatter_scratch(C, Q // PARTS, W)) * PARTS,
        compiler_params=params(1),
        name="k_forward",
    )(w_query, w_key, w_value, w_gate, w_out, w_ffgate, w_ffup, w_down, *norms, log_decay, tok, go)
    gm, gb, down, dgain2, dbias2, mlp_sum = pl.pallas_call(
        functools.partial(middle_kernel, dims, (S, B, U)),
        out_shape=(
            sds((Q, W), F32),
            sds((C, T, Q, W), BF),
            sds((C, T, Q, W), BF),
            sds((1, W), F32),
            sds((1, W), F32),
            sds((C, R, NR), BF),
        ),
        in_specs=[ANY, ANY, VMEM, VMEM, ANY, VMEM],
        out_specs=[VMEM, ANY, ANY, VMEM, VMEM, ANY],
        scratch_shapes=[
            pltpu.VMEM((2, B, W), BF),
            pltpu.VMEM((2, B, W), BF),
            pltpu.VMEM((F * C, N, R), BF),
            pltpu.VMEM((F * C, N, R), BF),
            pltpu.VMEM((B, 3 * U), F32),
            pltpu.VMEM((N, 2 * U), BF),
            pltpu.VMEM((N, U), BF),
            pltpu.VMEM((C, T, Q, W), BF),
            pltpu.VMEM((C, T, Q, W), BF),
            pltpu.VMEM((R, N), BF),
            pltpu.VMEM((R, N), BF),
            pltpu.VMEM((F - 1, C, R, NR), BF),
            pltpu.VMEM((F - 1, C, R, NR), BF),
            pltpu.VMEM((C, R, NR), BF),
            pltpu.VMEM((Q, W), BF),
            pltpu.VMEM((Q, W), BF),
            sem(2),
            sem(2),
            pltpu.SemaphoreType.DMA,
            sem(C),
            sem(C),
            sem(C, F),
            sem(C, F),
        ]
        + chain_sems(C)
        + scatter_scratch(C, Q, W),
        compiler_params=params(3),
        name="k_middle",
    )(sn.reshape(N, W), ogo.reshape(N, W), full, mid, go, vecs)

    branch = gb.reshape(N, W)
    H = 2
    gt, out, gsum, mlp_grads, vsum = pl.pallas_call(
        functools.partial(backward_kernel, dims, (S, B, halves, HV)),
        out_shape=(
            sds((T, Q, W), BF),
            sds((T, Q, W), BF),
            sds((C, R, NO), BF),
            sds((C, R, NR), BF),
            sds((8, R), F32),
        ),
        in_specs=[ANY, ANY] + [VMEM] * 9 + [ANY, ANY, VMEM, VMEM, ANY, VMEM],
        out_specs=[ANY] * 4 + [VMEM],
        scratch_shapes=[
            pltpu.VMEM((2, B, W), BF),
            pltpu.VMEM((2, N, R), BF),
            pltpu.VMEM((F * C, N, R), BF),
            pltpu.VMEM((R, N), BF),
            pltpu.VMEM((R, N), BF),
            pltpu.VMEM((N, HV), F32),
            pltpu.VMEM((N, NI), BF),
            pltpu.VMEM((S, KEY, HV), F32),
            pltpu.VMEM((halves, 8, N), F32),
            pltpu.VMEM((C, T, Q, W), BF),
            pltpu.VMEM((F - 1, C, R, NO), BF),
            pltpu.VMEM((F - 1, C, R, NO), BF),
            pltpu.VMEM((C, R, NO), BF),
            pltpu.VMEM((Q, W), BF),
            pltpu.VMEM((Q, W), BF),
            sem(2),
            sem(2),
            sem(halves),
            sem(halves),
            sem(C),
            sem(C),
            sem(C, F),
            sem(C, F),
            sem(C, F, H),
            sem(C, F, H),
            sem(C, H),
            sem(C, H),
            sem(H),
        ]
        + [pltpu.SemaphoreType.DMA] * 3
        + share_sems() * 2
        + vector_scratch(F, C, R)
        + [pltpu.VMEM((Q, W), BF), pltpu.SemaphoreType.DMA]
        + local_scratch(C, Q, W)
        + scatter_scratch(C, Q, W) * 2,
        compiler_params=params(4),
        name="k_backward",
    )(
        branch,
        normed,
        owin,
        proj,
        states,
        normal,
        inv,
        gated,
        old,
        vecs,
        gm,
        tok,
        mlp_sum,
        dgain2,
        dbias2,
        down,
        mid,
    )

    steps = 1

    def quarter(n):
        return pl.BlockSpec((R // steps, n), lambda h, c: (h, c))

    def piece(n):
        return pl.BlockSpec((1, R // steps, n), lambda h, c: (c, h, 0))

    rows = pl.BlockSpec((L // (steps * C), W), lambda h, c: (h * C + c, 0))
    per_head = pl.BlockSpec((R // steps, KEY), lambda h, c: (h, c // halves))
    gq, gk, gv, gg, gw, gfg, gfu, gfd, output, grad_tokens, *gvecs = pl.pallas_call(
        functools.partial(assemble_kernel, halves, KEY, HV),
        out_shape=[sds((R, heads * KEY), F32)] * 2
        + [sds((R, C * HV), F32)] * 3
        + [sds((R, C * U), F32)] * 3
        + [sds((L, W), BF)] * 2
        + [sds((R,), F32)] * 4,
        grid=(steps, C),
        in_specs=[piece(NO), piece(NR), rows, rows, pl.BlockSpec((8, R), lambda h, c: (0, 0))],
        out_specs=[per_head, per_head]
        + [quarter(HV)] * 3
        + [quarter(U)] * 3
        + [rows, rows]
        + [pl.BlockSpec((R,), lambda h, c: (0,))] * 4,
        name="k_assemble",
    )(gsum, mlp_grads, out.reshape(L, W), gt.reshape(L, W), vsum)
    return (
        output.reshape(tokens.shape),
        grad_tokens.reshape(tokens.shape),
        gq,
        gk,
        gv,
        gg,
        gw,
        gvecs[0],
        gvecs[1],
        gfg,
        gfu,
        gfd,
        gvecs[2],
        gvecs[3],
    )


def solution(mesh):
    dims = (mesh.shape["fsdp"], mesh.shape["ctx"], mesh.shape["tp"])
    rows, vec = P(("fsdp", "ctx"), "tp"), P(("fsdp", "ctx"))
    acts = P("fsdp", "ctx", None)
    return jax.shard_map(
        functools.partial(shards, dims),
        mesh=mesh,
        in_specs=(acts, P("fsdp", "ctx", "tp"), rows, rows, rows, rows, rows, vec, vec, rows, rows, rows, vec, vec, acts),
        out_specs=(acts, acts, rows, rows, rows, rows, rows, vec, vec, rows, rows, rows, vec, vec),
        check_vma=False,
    )
```
